8 devices in a mesh: dp: 2 (over z, y), sp: 4 (over x, core).
Axes of the slice: x: 2, y: 2, z: 1, core: 2. Of those that a mesh axis runs over, the one named last changes fastest.
Arguments:
- u_in: bfloat16 [4, 1024, 4096], P('dp', 'sp'), parts along dimension 0
- w_in: bfloat16 [4096, 12288], replicated
- b_in: float32 [12288], replicated
- conv_taps: float32 [3, 12288], replicated
- w_out: bfloat16 [4096, 4096], replicated
- skip_one: float32 [4096], replicated
- skip_two: float32 [4096], replicated
- filt_one: float32 [1024, 4096], P('sp')
- filt_two: float32 [1024, 4096], P('sp')
Outputs:
- output: bfloat16 [4, 1024, 4096], P('dp', 'sp'), parts along dimension 0
There are 2 independent parts. The reference program is written for one: setup_inputs(seed, part) draws one part's arguments, and reference() takes and returns one part's arrays. A program takes and returns all parts, laid end to end along the dimension named above; an argument that names none is the same for every part.
All inputs are finite; a program needn't handle non-finite values.
Results may differ from the reference program's by a relative error of at most 0.014832.
Values sent between devices are 32-bit elements.
A program may use at most 1 GiB of HBM per device.

```python
import jax
import jax.numpy as jnp
from jax import lax

BATCH_SIZE = 2
SEQ_LEN = 1024
MODEL_DIM = 4096
CHAN_BLOCK = 128


def draw_filter(filt_key):
    noise_key, rate_key = jax.random.split(filt_key)
    decay_rates = jax.random.uniform(rate_key, (MODEL_DIM,), jnp.float32, 0.0, 2.0)
    rel_pos = jnp.arange(SEQ_LEN, dtype=jnp.float32)[:, None] / SEQ_LEN
    noise_vals = jax.random.normal(noise_key, (SEQ_LEN, MODEL_DIM), jnp.float32)
    return noise_vals * jnp.exp(-decay_rates[None, :] * rel_pos) * (1.5 * SEQ_LEN ** -0.5)


def setup_inputs(seed: int = 0, part: int = 0) -> dict:
    key_list = jax.random.split(jax.random.key(seed), 9)
    model_width = MODEL_DIM
    fan_scale = model_width ** -0.5
    u_in = jax.random.normal(jax.random.fold_in(key_list[0], part), (BATCH_SIZE, SEQ_LEN, model_width), jnp.float32)
    w_in = jax.random.normal(key_list[1], (model_width, 3 * model_width), jnp.float32) * fan_scale
    b_in = 0.5 * jax.random.normal(key_list[2], (3 * model_width,), jnp.float32)
    conv_taps = 0.6 * jax.random.normal(key_list[3], (3, 3 * model_width), jnp.float32)
    w_out = jax.random.normal(key_list[4], (model_width, model_width), jnp.float32) * fan_scale
    skip_one = jax.random.normal(key_list[5], (model_width,), jnp.float32)
    skip_two = jax.random.normal(key_list[6], (model_width,), jnp.float32)
    return {'u_in': u_in.astype(jnp.bfloat16), 'w_in': w_in.astype(jnp.bfloat16), 'b_in': b_in, 'conv_taps': conv_taps, 'w_out': w_out.astype(jnp.bfloat16), 'skip_one': skip_one, 'skip_two': skip_two, 'filt_one': draw_filter(key_list[7]), 'filt_two': draw_filter(key_list[8])}


def causal_conv(signal, filt):
    seq_len = signal.shape[0]
    spectrum = jnp.fft.rfft(signal, n=2 * seq_len, axis=0) * jnp.fft.rfft(filt, n=2 * seq_len, axis=0)
    return jnp.fft.irfft(spectrum, n=2 * seq_len, axis=0)[:seq_len]


def reference(u_in, w_in, b_in, conv_taps, w_out, skip_one, skip_two, filt_one, filt_two):
    n_blocks = MODEL_DIM // CHAN_BLOCK

    def by_blocks(array_2d):
        return jnp.moveaxis(array_2d.reshape(array_2d.shape[0], n_blocks, CHAN_BLOCK), 1, 0)

    filt_blocks = (by_blocks(filt_one), by_blocks(filt_two), skip_one.reshape(n_blocks, CHAN_BLOCK), skip_two.reshape(n_blocks, CHAN_BLOCK))

    def one_block(block_args):
        gate_one, gate_two, values, h_one, h_two, d_one, d_two = block_args
        z_one = gate_one * (causal_conv(values, h_one) + d_one * values)
        return gate_two * (causal_conv(z_one, h_two) + d_two * z_one)

    def one_row(seq_row):
        projected = (jnp.dot(seq_row, w_in, preferred_element_type=jnp.float32) + b_in).astype(jnp.bfloat16).astype(jnp.float32)
        prev_one = jnp.pad(projected[:-1], ((1, 0), (0, 0)))
        prev_two = jnp.pad(projected[:-2], ((2, 0), (0, 0)))
        mixed = (conv_taps[0] * projected + conv_taps[1] * prev_one + conv_taps[2] * prev_two).astype(jnp.bfloat16).astype(jnp.float32)
        gate_one = by_blocks(mixed[:, :MODEL_DIM])
        gate_two = by_blocks(mixed[:, MODEL_DIM:2 * MODEL_DIM])
        values = by_blocks(mixed[:, 2 * MODEL_DIM:])
        gated = lax.map(one_block, (gate_one, gate_two, values) + filt_blocks)
        gated = jnp.moveaxis(gated, 0, 1).reshape(SEQ_LEN, MODEL_DIM)
        out_sum = seq_row.astype(jnp.float32) + jnp.dot(gated.astype(jnp.bfloat16), w_out, preferred_element_type=jnp.float32)
        return out_sum.astype(jnp.bfloat16)

    return lax.map(one_row, u_in)
```

```python
import functools

import jax
import jax.numpy as jnp
import numpy as np
from jax import lax
from jax.experimental import pallas as pl
from jax.experimental.pallas import tpu as pltpu
from jax.sharding import PartitionSpec as P

F32, BF16 = jnp.float32, jnp.bfloat16
BLK = 128
TN = 512
TC = 256
N_CHUNK = 4


def split_table(table):
    parts, rest = [], table.astype(np.float64)
    for _ in range(3):
        part = rest.astype(np.float32).astype(jnp.bfloat16)
        parts.append(part)
        rest = rest - part.astype(np.float64)
    return parts


def transform_tables():
    freq = np.concatenate([np.arange(0, BLK, 2), np.arange(1, BLK, 2)]) + 0.5
    angle = 2.0 * np.pi * freq[:, None] * np.arange(BLK)[None, :] / (2 * BLK)
    fwd = np.concatenate([np.cos(angle), -np.sin(angle)], 0)
    inv = np.concatenate([np.cos(angle).T, -np.sin(angle).T], 1) / BLK
    f1, f2, f3 = split_table(fwd)
    e1, e2, e3 = split_table(inv)
    fwd3 = np.concatenate([f1, f2, f3], 1)
    fwd6 = np.concatenate([f1, f1, f2, f2, f1, f3], 1)
    inv6 = np.concatenate([e1, e1, e2, e2, e1, e3], 1)
    return fwd3, fwd6, inv6


def dot(a, b):
    return jnp.dot(a, b, preferred_element_type=F32)


def split3(x):
    hi = x.astype(BF16)
    rest = x - hi.astype(F32)
    mid = rest.astype(BF16)
    low = (rest - mid.astype(F32)).astype(BF16)
    return hi, mid, low


def stack6(hi, mid, low):
    return jnp.concatenate([hi, mid, hi, mid, low, hi], axis=0)


def in_own_body(sc_ref, own_ref, part_ref, tail_ref, w_ref, b_ref, p_ref, pt_ref, lhs):
    c = sc_ref[0]
    n_seq, half = own_ref.shape[0], own_ref.shape[1]
    rows = 2 * n_seq * half

    @pl.when(pl.program_id(0) == 0)
    def _():
        for s in range(n_seq):
            base = s * 2 * half
            lhs[pl.ds(pl.multiple_of(base + c * half, half), half), :] = own_ref[s]
            lhs[pl.ds(pl.multiple_of(base + (1 - c) * half, half), half), :] = part_ref[s].astype(BF16)
        lhs[rows:, :] = tail_ref[...].astype(BF16)

    acc = dot(lhs[...], w_ref[...])
    p = (acc + b_ref[...]).astype(BF16)
    p_ref[...] = p[:rows].reshape(p_ref.shape)
    pt_ref[...] = p[rows:]


def in_prev_body(sc_ref, near_ref, far_ref, w_ref, b_ref, p_ref, lhs):
    c = sc_ref[0]
    half = near_ref.shape[0]

    @pl.when(pl.program_id(0) == 0)
    def _():
        lhs[pl.ds(pl.multiple_of(c * half, half), half), :] = near_ref[...].astype(BF16)
        lhs[pl.ds(pl.multiple_of((1 - c) * half, half), half), :] = far_ref[...].astype(BF16)

    p_ref[...] = (dot(lhs[...], w_ref[...]) + b_ref[...]).astype(BF16)


def out_body(sc_ref, keep_ref, part_ref, wk_ref, wp_ref, u_ref, o_ref, lhs_k, lhs_p):
    @pl.when(pl.program_id(0) == 0)
    def _():
        rows = keep_ref.shape[0] * keep_ref.shape[1]
        lhs_k[...] = keep_ref[...].reshape(rows, -1)
        lhs_p[...] = part_ref[...].reshape(rows, -1).astype(BF16)

    acc = dot(lhs_k[...], wk_ref[...]) + dot(lhs_p[...], wp_ref[...])
    o_ref[...] = (u_ref[...].astype(F32) + acc.reshape(o_ref.shape)).astype(BF16)


def conv_body(sc_ref, fwd3_ref, fwd6_ref, inv6_ref, px1_ref, px2_ref, pv_ref, pp0x_ref, pp0v_ref, pp1x_ref, pp1v_ref, pt_ref,
              t1_ref, t2_ref, tv_ref, sk1_ref, sk2_ref, own1_ref, own2_ref, pf_ref, xs_ref, xc_ref, ys_ref, yc_ref,
              keep_ref, send_ref, pbuf, vq, x1q, x2q, hraw, vhat, zhat, ghat, sparts, zval, ybuf):
    c, is_b, d = sc_ref[0], sc_ref[1], sc_ref[2]
    n_seq, n_own = px2_ref.shape[0], px2_ref.shape[1]
    n_prev = pp0v_ref.shape[0]
    n_all = n_prev + n_own
    nb, nb_prev = n_all // BLK, n_prev // BLK
    half = n_prev // 2
    on_b = is_b == 1

    def taps(t_ref, rows):
        return (t_ref[0:1] * pbuf[8:8 + rows] + t_ref[1:2] * pbuf[7:7 + rows] + t_ref[2:3] * pbuf[6:6 + rows]).astype(BF16)

    for s in range(n_seq):
        for own, prev, t_ref, dst in ((px1_ref, (pp0x_ref, pp1x_ref)[s], t1_ref, x1q), (pv_ref, (pp0v_ref, pp1v_ref)[s], tv_ref, vq)):
            pbuf[0:8] = jnp.zeros((8, TC), F32)
            pbuf[8:8 + n_prev] = jnp.where(on_b, prev[...].astype(F32), 0.0)
            pbuf[8 + n_prev:8 + n_all] = own[s].astype(F32)
            dst[s] = taps(t_ref, n_all)
        pbuf[0:8] = jnp.where(on_b, pt_ref[s * 8:(s + 1) * 8].astype(F32), 0.0)
        pbuf[8:8 + n_own] = px2_ref[s].astype(F32)
        x2q[s] = taps(t2_ref, n_own)

    here = pl.ds(pl.multiple_of(c * half, half), half)
    there = pl.ds(pl.multiple_of((1 - c) * half, half), half)
    here_far = pl.ds(pl.multiple_of(n_prev + c * half, half), half)
    there_far = pl.ds(pl.multiple_of(n_prev + (1 - c) * half, half), half)
    for f in range(2):
        own, part = (own1_ref, own2_ref)[f][...], pf_ref[f]
        direct = d == f
        hraw[f, here] = jnp.where(on_b, jnp.where(direct, xs_ref[...], ys_ref[...]), own)
        hraw[f, there] = jnp.where(on_b, jnp.where(direct, xc_ref[...], yc_ref[...]), part)
        hraw[f, here_far] = own
        hraw[f, there_far] = part

    for s in range(n_seq):
        for j in range(nb):
            blk = vq[s, j * BLK:(j + 1) * BLK]
            vhat[s, j] = dot(fwd3_ref[...], jnp.concatenate([blk, blk, blk], axis=0))
    hb = BLK // 2
    for f in range(2):
        for j in range(nb - 1, -1, -1):
            ghat[f, j] = dot(fwd6_ref[...], stack6(*split3(hraw[f, j * BLK:(j + 1) * BLK])))
        for j in range(nb - 1, 0, -1):
            for lo, sign in ((0, 1.0), (hb, -1.0)):
                re, im = slice(lo, lo + hb), slice(BLK + lo, BLK + lo + hb)
                ghat[f, j, re] = ghat[f, j, re] - sign * ghat[f, j - 1, im]
                ghat[f, j, im] = ghat[f, j, im] + sign * ghat[f, j - 1, re]

    def pointwise(xhat, f, s, k, slot):
        def unit(r, carry):
            re, im = pl.ds(pl.multiple_of(r * 16, 16), 16), pl.ds(pl.multiple_of(BLK + r * 16, 16), 16)
            acc_re = acc_im = None
            for j in range(k + 1):
                xr, xi, gr, gi = xhat[s, j, re], xhat[s, j, im], ghat[f, k - j, re], ghat[f, k - j, im]
                t_re, t_im = xr * gr - xi * gi, xr * gi + xi * gr
                acc_re = t_re if acc_re is None else acc_re + t_re
                acc_im = t_im if acc_im is None else acc_im + t_im
            for part, (a, b) in enumerate(zip(split3(acc_re), split3(acc_im))):
                sparts[slot, part, re], sparts[slot, part, im] = a, b
            return carry

        lax.fori_loop(0, BLK // 16, unit, 0)

    def inverse(slot):
        return dot(inv6_ref[...], stack6(sparts[slot, 0], sparts[slot, 1], sparts[slot, 2]))

    for k in range(nb):
        rows = slice(k * BLK, (k + 1) * BLK)
        for s in range(n_seq):
            pointwise(vhat, 0, s, k, s)
        for s in range(n_seq):
            conv = inverse(s)
            z = x1q[s, rows].astype(F32) * (conv + sk1_ref[...] * vq[s, rows].astype(F32))
            zval[s, rows] = z
            zhat[s, k] = dot(fwd6_ref[...], stack6(*split3(z)))

    for k in range(nb_prev, nb):
        rows, orow = slice(k * BLK, (k + 1) * BLK), slice((k - nb_prev) * BLK, (k - nb_prev + 1) * BLK)
        for s in range(n_seq):
            pointwise(zhat, 1, s, k, s)
        for s in range(n_seq):
            y = x2q[s, orow].astype(F32) * (inverse(s) + sk2_ref[...] * zval[s, rows])
            ybuf[s, orow] = y.astype(BF16)
    for s in range(n_seq):
        keep_ref[s] = ybuf[s, here]
        send_ref[s] = ybuf[s, there].astype(F32)


def vmem_params(mib=60):
    return pltpu.CompilerParams(vmem_limit_bytes=mib << 20, dimension_semantics=("arbitrary",))


def solution(mesh):
    n_sp = mesh.shape["sp"]
    half_sp = n_sp // 2
    partner = [(i, i ^ 1) for i in range(n_sp)]
    over_same = [(i, i + half_sp) for i in range(half_sp)]
    over_cross = [(i, (i ^ 1) + half_sp) for i in range(half_sp)]
    swap_dp = [(0, 1), (1, 0)]
    fwd3, fwd6, inv6 = transform_tables()

    def local_step(u_in, w_in, b_in, conv_taps, w_out, skip_one, skip_two, filt_one, filt_two):
        sp, dp = lax.axis_index("sp"), lax.axis_index("dp")
        c = sp % 2
        scalars = jnp.stack([c, (sp >= half_sp).astype(jnp.int32), dp]).astype(jnp.int32)
        n_seq, n_pos, width = u_in.shape
        half_w = width // 2
        n_own = 2 * n_pos
        n_all = 2 * n_own

        def hop(x, perm):
            return lax.ppermute(x, "sp", perm)

        u32 = [u_in[s].astype(F32) for s in range(n_seq)]
        over = [hop(u, over_same) for u in u32]
        tail = jnp.concatenate([u[-8:] for u in u32], axis=0)
        u_tail = hop(tail, [(1, 2)]) + hop(tail, [(1, 3)])
        u_part = jnp.stack([hop(u, partner) for u in u32])
        over_part = [hop(u, partner) for u in over]

        mine = c * half_w
        other = (1 - c) * half_w

        def chan_half(f, start):
            return lax.dynamic_slice(f, (0, start), (n_pos, half_w))

        f_part = hop(jnp.stack([chan_half(filt_one, other), chan_half(filt_two, other)]), partner)
        f_link = jnp.where(dp == 0, filt_one, filt_two)
        f_mine, f_other = chan_half(f_link, mine), chan_half(f_link, other)
        nch = half_w // N_CHUNK
        near = []
        for j in range(N_CHUNK):
            cols = slice(j * nch, (j + 1) * nch)
            xs, xc = hop(f_mine[:, cols], over_same), hop(f_other[:, cols], over_cross)
            ys, yc = lax.ppermute(xs, "dp", swap_dp), lax.ppermute(xc, "dp", swap_dp)
            near.append((xs, xc, ys, yc))

        bias = b_in.reshape(1, -1)
        nt = half_w // TN
        wt = width // TN
        n_out3 = 3 * half_w

        p_own, p_tail = pl.pallas_call(
            in_own_body,
            grid_spec=pltpu.PrefetchScalarGridSpec(
                num_scalar_prefetch=1,
                grid=(3 * nt,),
                in_specs=[
                    pl.BlockSpec((n_seq, n_pos, width), lambda j, sc: (0, 0, 0)),
                    pl.BlockSpec((n_seq, n_pos, width), lambda j, sc: (0, 0, 0)),
                    pl.BlockSpec((16, width), lambda j, sc: (0, 0)),
                    pl.BlockSpec((width, TN), lambda j, sc: (0, (j // nt) * wt + sc[0] * nt + j % nt)),
                    pl.BlockSpec((1, TN), lambda j, sc: (0, (j // nt) * wt + sc[0] * nt + j % nt)),
                ],
                out_specs=[
                    pl.BlockSpec((n_seq, n_own, TN), lambda j, sc: (0, 0, j)),
                    pl.BlockSpec((16, TN), lambda j, sc: (0, j)),
                ],
                scratch_shapes=[pltpu.VMEM((n_seq * n_own + 16, width), BF16)],
            ),
            out_shape=[jax.ShapeDtypeStruct((n_seq, n_own, n_out3), BF16), jax.ShapeDtypeStruct((16, n_out3), BF16)],
            compiler_params=vmem_params(),
            cost_estimate=pl.CostEstimate(flops=2 * n_seq * n_own * width * n_out3, bytes_accessed=2 * width * n_out3, transcendentals=0),
            name="in_own",
        )(scalars, u_in, u_part, u_tail, w_in, bias)

        def in_prev(direct, forwarded):
            def col(j, sc):
                return 2 * (j // nt) * wt + sc[0] * nt + j % nt

            return pl.pallas_call(
                in_prev_body,
                grid_spec=pltpu.PrefetchScalarGridSpec(
                    num_scalar_prefetch=1,
                    grid=(2 * nt,),
                    in_specs=[
                        pl.BlockSpec((n_pos, width), lambda j, sc: (0, 0)),
                        pl.BlockSpec((n_pos, width), lambda j, sc: (0, 0)),
                        pl.BlockSpec((width, TN), lambda j, sc: (0, col(j, sc))),
                        pl.BlockSpec((1, TN), lambda j, sc: (0, col(j, sc))),
                    ],
                    out_specs=pl.BlockSpec((n_own, TN), lambda j, sc: (0, j)),
                    scratch_shapes=[pltpu.VMEM((n_own, width), BF16)],
                ),
                out_shape=jax.ShapeDtypeStruct((n_own, width), BF16),
                compiler_params=vmem_params(),
                cost_estimate=pl.CostEstimate(flops=2 * n_own * width * width, bytes_accessed=2 * width * width, transcendentals=0),
                name="in_prev",
            )(scalars, direct, forwarded, w_in, bias)

        p_prev = [in_prev(over[s], over_part[s]) for s in range(n_seq)]

        tiles = nch // TC
        ht = half_w // TC
        full_t = width // TC

        def conv(j, xs, xc, ys, yc):
            base = j * tiles

            def fixed(shape):
                return pl.BlockSpec(shape, lambda t, sc: (0,) * len(shape))

            def own_col(g):
                return pl.BlockSpec((n_seq, n_own, TC), lambda t, sc: (0, 0, g * ht + base + t))

            def prev_col(g):
                return pl.BlockSpec((n_own, TC), lambda t, sc: (0, g * ht + base + t))

            def tap_col(g):
                return pl.BlockSpec((3, TC), lambda t, sc: (0, g * full_t + sc[0] * ht + base + t))

            chan = pl.BlockSpec((1, TC), lambda t, sc: (0, sc[0] * ht + base + t))
            own_f = pl.BlockSpec((n_pos, TC), lambda t, sc: (0, sc[0] * ht + base + t))
            local = pl.BlockSpec((n_pos, TC), lambda t, sc: (0, t))
            nb = n_all // BLK
            return pl.pallas_call(
                conv_body,
                grid_spec=pltpu.PrefetchScalarGridSpec(
                    num_scalar_prefetch=1,
                    grid=(tiles,),
                    in_specs=[
                        fixed(fwd3.shape), fixed(fwd6.shape), fixed(inv6.shape),
                        own_col(0), own_col(1), own_col(2), prev_col(0), prev_col(1), prev_col(0), prev_col(1),
                        pl.BlockSpec((16, TC), lambda t, sc: (0, ht + base + t)),
                        tap_col(0), tap_col(1), tap_col(2), chan, chan, own_f, own_f,
                        pl.BlockSpec((2, n_pos, TC), lambda t, sc: (0, 0, base + t)),
                        local, local, local, local,
                    ],
                    out_specs=[pl.BlockSpec((n_seq, n_pos, TC), lambda t, sc: (0, 0, t))] * 2,
                    scratch_shapes=[
                        pltpu.VMEM((n_all + 8, TC), F32),
                        pltpu.VMEM((n_seq, n_all, TC), BF16),
                        pltpu.VMEM((n_seq, n_all, TC), BF16),
                        pltpu.VMEM((n_seq, n_own, TC), BF16),
                        pltpu.VMEM((2, n_all, TC), F32),
                        pltpu.VMEM((n_seq, nb, 2 * BLK, TC), F32),
                        pltpu.VMEM((n_seq, nb, 2 * BLK, TC), F32),
                        pltpu.VMEM((2, nb, 2 * BLK, TC), F32),
                        pltpu.VMEM((n_seq, 3, 2 * BLK, TC), BF16),
                        pltpu.VMEM((n_seq, n_all, TC), F32),
                        pltpu.VMEM((n_seq, n_own, TC), BF16),
                    ],
                ),
                out_shape=[jax.ShapeDtypeStruct((n_seq, n_pos, nch), BF16), jax.ShapeDtypeStruct((n_seq, n_pos, nch), F32)],
                compiler_params=vmem_params(),
                cost_estimate=pl.CostEstimate(flops=40_000_000_000 // N_CHUNK, bytes_accessed=50_000_000 // N_CHUNK, transcendentals=0),
                name="long_conv",
            )(scalars, fwd3, fwd6, inv6, p_own, p_own, p_own, p_prev[0], p_prev[0], p_prev[1], p_prev[1], p_tail,
              conv_taps, conv_taps, conv_taps, skip_one.reshape(1, -1), skip_two.reshape(1, -1),
              filt_one, filt_two, f_part, xs, xc, ys, yc)

        keeps, parts = [], []
        for j in range(N_CHUNK):
            keep, send = conv(j, *near[j])
            keeps.append(keep)
            parts.append(hop(send, partner))
        keep = jnp.concatenate(keeps, axis=-1)
        part = jnp.concatenate(parts, axis=-1)

        return pl.pallas_call(
            out_body,
            grid_spec=pltpu.PrefetchScalarGridSpec(
                num_scalar_prefetch=1,
                grid=(wt,),
                in_specs=[
                    pl.BlockSpec((n_seq, n_pos, half_w), lambda j, sc: (0, 0, 0)),
                    pl.BlockSpec((n_seq, n_pos, half_w), lambda j, sc: (0, 0, 0)),
                    pl.BlockSpec((half_w, TN), lambda j, sc: (sc[0], j)),
                    pl.BlockSpec((half_w, TN), lambda j, sc: (1 - sc[0], j)),
                    pl.BlockSpec((n_seq, n_pos, TN), lambda j, sc: (0, 0, j)),
                ],
                out_specs=pl.BlockSpec((n_seq, n_pos, TN), lambda j, sc: (0, 0, j)),
                scratch_shapes=[pltpu.VMEM((n_seq * n_pos, half_w), BF16)] * 2,
            ),
            out_shape=jax.ShapeDtypeStruct((n_seq, n_pos, width), BF16),
            compiler_params=vmem_params(),
            cost_estimate=pl.CostEstimate(flops=2 * n_seq * n_pos * width * width, bytes_accessed=2 * width * width, transcendentals=0),
            name="out_proj",
        )(scalars, keep, part, w_out, w_out, u_in)

    seq_spec = P("dp", "sp", None)
    filt_spec = P("sp", None)
    return jax.shard_map(local_step, mesh=mesh, in_specs=(seq_spec, P(), P(), P(), P(), P(), P(), filt_spec, filt_spec), out_specs=seq_spec, check_vma=False)
```

```python
import functools

import jax
import jax.numpy as jnp
import numpy as np
from jax import lax
from jax.experimental import pallas as pl
from jax.experimental.pallas import tpu as pltpu
from jax.sharding import PartitionSpec as P

F32, BF16 = jnp.float32, jnp.bfloat16
BLK = 128
TN = 512
TC = 256
N_CHUNK = 4


def split_table(table):
    parts, rest = [], table.astype(np.float64)
    for _ in range(3):
        part = rest.astype(np.float32).astype(jnp.bfloat16)
        parts.append(part)
        rest = rest - part.astype(np.float64)
    return parts


def transform_tables():
    freq = np.concatenate([np.arange(0, BLK, 2), np.arange(1, BLK, 2)]) + 0.5
    angle = 2.0 * np.pi * freq[:, None] * np.arange(BLK)[None, :] / (2 * BLK)
    fwd = np.concatenate([np.cos(angle), -np.sin(angle)], 0)
    inv = np.concatenate([np.cos(angle).T, -np.sin(angle).T], 1) / BLK
    f1, f2, f3 = split_table(fwd)
    e1, e2, e3 = split_table(inv)
    fwd3 = np.concatenate([f1, f2, f3], 1)
    fwd6 = np.concatenate([f1, f1, f2, f2, f1, f3], 1)
    inv6 = np.concatenate([e1, e1, e2, e2, e1, e3], 1)
    return fwd3, fwd6, inv6


def dot(a, b):
    return jnp.dot(a, b, preferred_element_type=F32)


def split3(x):
    hi = x.astype(BF16)
    rest = x - hi.astype(F32)
    mid = rest.astype(BF16)
    low = (rest - mid.astype(F32)).astype(BF16)
    return hi, mid, low


def stack6(hi, mid, low):
    return jnp.concatenate([hi, mid, hi, mid, low, hi], axis=0)


def short_conv(pbuf, t_ref, rows):
    return (t_ref[0:1] * pbuf[8:8 + rows] + t_ref[1:2] * pbuf[7:7 + rows] + t_ref[2:3] * pbuf[6:6 + rows]).astype(BF16)


def value_spectrum(fwd3_ref, q, dst):
    for j in range(q.shape[0] // BLK):
        blk = q[j * BLK:(j + 1) * BLK]
        dst[j] = dot(fwd3_ref[...], jnp.concatenate([blk, blk, blk], axis=0))


def in_own_body(nt, sc_ref, fwd3_ref, own_ref, pa_ref, pb_ref, pc_ref, pd_ref, tail_ref, w_ref, b_ref, t_ref, q_ref, q2_ref, vhat_ref, lhs, pbuf):
    c, on_b = sc_ref[0], sc_ref[1] == 1
    j = pl.program_id(0)
    n_seq, half = own_ref.shape[0], own_ref.shape[1]
    n_own = 2 * half
    rows = n_seq * n_own

    @pl.when(j == 0)
    def _():
        for s in range(n_seq):
            base = s * n_own
            lhs[pl.ds(pl.multiple_of(base + c * half, half), half), :] = own_ref[s]
            for h in range(2):
                piece = (pa_ref, pb_ref, pc_ref, pd_ref)[2 * s + h]
                start = base + (1 - c) * half + h * (half // 2)
                lhs[pl.ds(pl.multiple_of(start, half // 2), half // 2), :] = piece[...].astype(BF16)
        lhs[rows:, :] = tail_ref[...].astype(BF16)

    p = (dot(lhs[...], w_ref[...]) + b_ref[...]).astype(BF16).astype(F32)
    for s in range(n_seq):
        pbuf[s, 0:8] = jnp.where(on_b, p[rows + 8 * s:rows + 8 * s + 8], 0.0)
        pbuf[s, 8:] = p[s * n_own:(s + 1) * n_own]

    @pl.when(j < 2 * nt)
    def _():
        for s in range(n_seq):
            q_ref[s] = short_conv(pbuf.at[s], t_ref, n_own).reshape(q_ref.shape[1:])

    @pl.when(j >= 2 * nt)
    def _():
        for s in range(n_seq):
            q2_ref[s] = short_conv(pbuf.at[s], t_ref, n_own)

    @pl.when((j >= nt) & (j < 2 * nt))
    def _():
        for s in range(n_seq):
            value_spectrum(fwd3_ref, q_ref[s].reshape(n_own, -1), vhat_ref.at[s])


def gather_rows(sc_ref, near_ref, far_ref, lhs):
    c, rows = sc_ref[0], near_ref.shape[0]

    @pl.when(pl.program_id(0) == 0)
    def _():
        lhs[pl.ds(pl.multiple_of(c * rows, rows), rows), :] = near_ref[...].astype(BF16)
        lhs[pl.ds(pl.multiple_of((1 - c) * rows, rows), rows), :] = far_ref[...].astype(BF16)


def prev_a_body(sc_ref, near_ref, far_ref, w_ref, b_ref, p_ref, lhs):
    gather_rows(sc_ref, near_ref, far_ref, lhs)
    p_ref[...] = (dot(lhs[...], w_ref[...]) + b_ref[...]).astype(BF16)


def prev_b_body(nt, sc_ref, fwd3_ref, near_ref, far_ref, w_ref, b_ref, t_ref, pa_ref, q_in, vhat_in, q_ref, vhat_ref, lhs, pbuf):
    on_b = sc_ref[1] == 1
    rows = near_ref.shape[0]
    gather_rows(sc_ref, near_ref, far_ref, lhs)
    p = (dot(lhs[...], w_ref[...]) + b_ref[...]).astype(BF16).astype(F32)
    pbuf[0:8] = jnp.zeros((8, p.shape[1]), F32)
    for core in range(2):
        for h, piece in enumerate((pa_ref[...].astype(F32), p)):
            base = 8 + (2 * core + h) * rows
            pbuf[base:base + rows] = jnp.where(on_b, piece[core * rows:(core + 1) * rows], 0.0)
    q_ref[0] = short_conv(pbuf, t_ref, 4 * rows).reshape(q_ref.shape[1:])

    @pl.when(pl.program_id(0) >= nt)
    def _():
        value_spectrum(fwd3_ref, q_ref[0].reshape(4 * rows, -1), vhat_ref.at[0])


def split_blocks(src, parts, first):
    for j in range(src.shape[0] // BLK):
        for i, a in enumerate(split3(src[j * BLK:(j + 1) * BLK])):
            parts[first + j, i] = a


def block_spectrum(fwd6_ref, parts, j):
    return dot(fwd6_ref[...], stack6(parts[j, 0], parts[j, 1], parts[j, 2]))


def shifted_add(cur, old, lo, sign):
    re, im = slice(lo, lo + BLK // 2), slice(BLK + lo, BLK + lo + BLK // 2)
    return re, im, cur[re] - sign * old[im], cur[im] + sign * old[re]


SIDES = ((0, 1.0), (BLK // 2, -1.0))


def far_body(sc_ref, fwd6_ref, own1_ref, own2_ref, pf1_ref, pf2_ref, g_ref, parts):
    c = sc_ref[0]
    hk = own1_ref.shape[0] // BLK
    for f in range(2):
        split_blocks((own1_ref, own2_ref)[f], parts.at[f], c * hk)
        split_blocks((pf1_ref, pf2_ref)[f], parts.at[f], (1 - c) * hk)
        for j in range(2 * hk):
            g_ref[f, j] = block_spectrum(fwd6_ref, parts.at[f], j)
        for j in range(2 * hk - 1, 0, -1):
            for lo, sign in SIDES:
                re, im, new_re, new_im = shifted_add(g_ref.at[f, j], g_ref.at[f, j - 1], lo, sign)
                g_ref[f, j, re], g_ref[f, j, im] = new_re, new_im


def out_body(n_chunk, sc_ref, *refs):
    keeps, parts = refs[:n_chunk], refs[n_chunk:2 * n_chunk]
    wk_ref, wp_ref, u_ref, o_ref, lhs_k, lhs_p = refs[2 * n_chunk:]

    @pl.when(pl.program_id(0) == 0)
    def _():
        n_seq, n_pos, nch = keeps[0].shape
        for i in range(n_chunk):
            cols = slice(i * nch, (i + 1) * nch)
            lhs_k[:, cols] = keeps[i][...].reshape(n_seq * n_pos, nch)
            lhs_p[:, cols] = parts[i][...].reshape(n_seq * n_pos, nch).astype(BF16)

    acc = dot(lhs_k[...], wk_ref[...]) + dot(lhs_p[...], wp_ref[...])
    o_ref[...] = (u_ref[...].astype(F32) + acc.reshape(o_ref.shape)).astype(BF16)


def conv_body(sc_ref, fwd6_ref, inv6_ref, x1_ref, v_ref, x2_ref, vhat, far_ref, sk1_ref, sk2_ref,
              own1_ref, own2_ref, pf1_ref, pf2_ref, xs_ref, xc_ref, ys_ref, yc_ref,
              keep_ref, send_ref, hparts, g1, g2, sp0, sp1, zp0, zp1, zv0, zv1, zh0, zh1, ybuf):
    c, on_b, d = sc_ref[0], sc_ref[1] == 1, sc_ref[2]
    n_seq, nb = vhat.shape[0], vhat.shape[1]
    nbo = nb // 2
    hk = own1_ref.shape[0] // BLK
    g, sparts, zparts, zval, zhat = (g1, g2), (sp0, sp1), (zp0, zp1), (zv0, zv1), (zh0, zh1)

    @pl.when(on_b)
    def _():
        for ref, f, side in ((xs_ref, d, c), (xc_ref, d, 1 - c), (ys_ref, 1 - d, c), (yc_ref, 1 - d, 1 - c)):
            split_blocks(ref, hparts.at[f], side * hk)

    @pl.when(jnp.logical_not(on_b))
    def _():
        for ref, f, side in ((own1_ref, 0, c), (pf1_ref, 0, 1 - c), (own2_ref, 1, c), (pf2_ref, 1, 1 - c)):
            split_blocks(ref, hparts.at[f], side * hk)

    def near_spectrum(f, j):
        g[f][j] = block_spectrum(fwd6_ref, hparts.at[f], j)

    def window(f):
        for j in range(nbo, 0, -1):
            cur = far_ref.at[f, 0] if j == nbo else g[f].at[j]
            for lo, sign in SIDES:
                re, im, new_re, new_im = shifted_add(cur, g[f].at[j - 1], lo, sign)
                g[f][j, re], g[f][j, im] = new_re, new_im

    def pointwise(xhat, f, dst, r, first):
        re, im = pl.ds(pl.multiple_of(r * 16, 16), 16), pl.ds(pl.multiple_of(BLK + r * 16, 16), 16)
        for k in range(first, nb):
            acc_re = acc_im = None
            for j in range(k + 1):
                i = k - j
                gr, gi = (g[f][i, re], g[f][i, im]) if i <= nbo else (far_ref[f, i - nbo, re], far_ref[f, i - nbo, im])
                xr, xi = xhat[j, re], xhat[j, im]
                t_re, t_im = xr * gr - xi * gi, xr * gi + xi * gr
                acc_re = t_re if acc_re is None else acc_re + t_re
                acc_im = t_im if acc_im is None else acc_im + t_im
            for part, (a, b) in enumerate(zip(split3(acc_re), split3(acc_im))):
                dst[k, part, re], dst[k, part, im] = a, b

    def inverse(s, k):
        return dot(inv6_ref[...], stack6(sparts[s][k, 0], sparts[s][k, 1], sparts[s][k, 2]))

    def gate_one(s, k):
        z = x1_ref[s, k].astype(F32) * (inverse(s, k) + sk1_ref[...] * v_ref[s, k].astype(F32))
        zval[s][k] = z
        for part, a in enumerate(split3(z)):
            zparts[s][k, part] = a

    def spectrum(s, k):
        zhat[s][k] = block_spectrum(fwd6_ref, zparts[s], k)

    def gate_two(s, k):
        y = x2_ref[s, k].astype(F32) * (inverse(s, nbo + k) + sk2_ref[...] * zval[s][nbo + k])
        ybuf[s, k] = y.astype(BF16)

    def loop(body, trips=nb // 2):
        def run(i, carry):
            body(i)
            return carry

        lax.fori_loop(0, trips, run, 0)

    for j in range(nbo):
        near_spectrum(0, j)
    window(0)

    @loop
    def _(i):
        pointwise(vhat.at[0], 0, sparts[0], 2 * i, 0)
        near_spectrum(1, i)
        pointwise(vhat.at[0], 0, sparts[0], 2 * i + 1, 0)

    window(1)

    @loop
    def _(i):
        for r in range(2):
            pointwise(vhat.at[1], 0, sparts[1], 2 * i + r, 0)
            gate_one(0, 2 * i + r)

    @functools.partial(loop, trips=nb // 4)
    def _(i):
        for r in range(4):
            gate_one(1, 4 * i + r)
            spectrum(0, 4 * i + r)

    @loop
    def _(i):
        for r in range(2):
            pointwise(zhat[0], 1, sparts[0], 2 * i + r, nbo)
            spectrum(1, 2 * i + r)

    @functools.partial(loop, trips=nbo // 2)
    def _(i):
        for r in range(4):
            pointwise(zhat[1], 1, sparts[1], 4 * i + r, nbo)
            if r % 2:
                gate_two(0, 2 * i + r // 2)

    for k in range(nbo):
        gate_two(1, k)

    for s in range(n_seq):
        for b in range(hk):
            keep_ref[s, b * BLK:(b + 1) * BLK] = ybuf[s, c * hk + b]
            send_ref[s, b * BLK:(b + 1) * BLK] = ybuf[s, (1 - c) * hk + b].astype(F32)


def params(mib=60):
    return pltpu.CompilerParams(vmem_limit_bytes=mib << 20, dimension_semantics=("arbitrary",))


def cost(flops, nbytes):
    return pl.CostEstimate(flops=int(flops), bytes_accessed=int(nbytes), transcendentals=0)


def solution(mesh):
    n_sp = mesh.shape["sp"]
    half_sp = n_sp // 2
    partner = [(i, i ^ 1) for i in range(n_sp)]
    over_same = [(i, i + half_sp) for i in range(half_sp)]
    over_cross = [(i, (i ^ 1) + half_sp) for i in range(half_sp)]
    swap_dp = [(0, 1), (1, 0)]
    fwd3, fwd6, inv6 = transform_tables()

    def hop(x, perm, axis="sp"):
        return lax.ppermute(x, axis, perm)

    def compute(u_in, w_in, b_in, conv_taps, w_out, skip_one, skip_two, filt_one, filt_two):
        sp, dp = lax.axis_index("sp"), lax.axis_index("dp")
        c = sp % 2
        scalars = jnp.stack([c, (sp >= half_sp).astype(jnp.int32), dp]).astype(jnp.int32)
        n_seq, n_pos, width = u_in.shape
        half_w = width // 2
        n_own = 2 * n_pos
        nb = 2 * n_own // BLK
        nbo = nb // 2

        hp = n_pos // 2
        pieces, gate = [], u_in[0, 0, :128].astype(F32)
        for s in range(n_seq):
            for h in range(2):
                raw, gate = lax.optimization_barrier((u_in[s, h * hp:(h + 1) * hp], gate))
                pieces.append(raw.astype(F32))
                gate = pieces[-1]
        over = [hop(x, over_same) for x in pieces]
        over_part = [hop(x, partner) for x in over]
        u_part = [hop(x, partner) for x in pieces]
        tail = jnp.concatenate([pieces[2 * s + 1][-8:] for s in range(n_seq)], axis=0)
        u_tail = hop(tail, [(half_sp - 1, half_sp)]) + hop(tail, [(half_sp - 1, half_sp + 1)])

        mine, other = c * half_w, (1 - c) * half_w

        def chan_half(f, start):
            return lax.dynamic_slice(f, (0, start), (n_pos, half_w))

        f_part = [hop(chan_half(f, other), partner) for f in (filt_one, filt_two)]
        f_link = jnp.where(dp == 0, filt_one, filt_two)
        f_mine, f_other = chan_half(f_link, mine), chan_half(f_link, other)
        nch = half_w // N_CHUNK
        near = []
        for j in range(N_CHUNK):
            cols = slice(j * nch, (j + 1) * nch)
            xs, xc = hop(f_mine[:, cols], over_same), hop(f_other[:, cols], over_cross)
            ys, yc = hop(xs, swap_dp, "dp"), hop(xc, swap_dp, "dp")
            near.append((xs, xc, ys, yc))

        bias = b_in.reshape(1, -1)
        nt = half_w // TN
        wt = width // TN
        any_spec = pl.BlockSpec(memory_space=pl.ANY)

        def fixed(shape):
            return pl.BlockSpec(shape, lambda *a: (0,) * len(shape))

        def own_col(j, sc):
            group = jnp.where(j < nt, 0, jnp.where(j < 2 * nt, 2, 1))
            return (0, group * wt + sc[0] * nt + j % nt)

        q_shape = jax.ShapeDtypeStruct((n_seq, nb, BLK, width), BF16)
        vhat_shape = jax.ShapeDtypeStruct((n_seq, nb, 2 * BLK, half_w), F32)
        q, q2, vhat = pl.pallas_call(
            functools.partial(in_own_body, nt),
            grid_spec=pltpu.PrefetchScalarGridSpec(
                num_scalar_prefetch=1,
                grid=(3 * nt,),
                in_specs=[
                    fixed(fwd3.shape),
                    fixed((n_seq, n_pos, width)),
                    *[fixed((hp, width))] * 4,
                    fixed((16, width)),
                    pl.BlockSpec((width, TN), own_col),
                    pl.BlockSpec((1, TN), own_col),
                    pl.BlockSpec((3, TN), own_col),
                ],
                out_specs=[
                    pl.BlockSpec((n_seq, nbo, BLK, TN), lambda j, sc: (0, 1, 0, jnp.minimum(j, 2 * nt - 1))),
                    pl.BlockSpec((n_seq, n_own, TN), lambda j, sc: (0, 0, jnp.maximum(j - 2 * nt, 0))),
                    pl.BlockSpec((n_seq, nbo, 2 * BLK, TN), lambda j, sc: (0, 1, 0, jnp.clip(j - nt, 0, nt - 1))),
                ],
                scratch_shapes=[pltpu.VMEM((n_seq * n_own + 16, width), BF16), pltpu.VMEM((n_seq, n_own + 8, TN), F32)],
            ),
            out_shape=[q_shape, jax.ShapeDtypeStruct((n_seq, n_own, half_w), BF16), vhat_shape],
            compiler_params=params(),
            cost_estimate=cost(2 * n_seq * n_own * width * 3 * half_w, 2 * width * 3 * half_w),
            name="in_own",
        )(scalars, fwd3, u_in, *u_part, u_tail, w_in, bias, conv_taps)

        def prev_col(j, sc):
            return (0, jnp.where(j < nt, 0, 2) * wt + sc[0] * nt + j % nt)

        def prev_a(i):
            return pl.pallas_call(
                prev_a_body,
                grid_spec=pltpu.PrefetchScalarGridSpec(
                    num_scalar_prefetch=1,
                    grid=(2 * nt,),
                    in_specs=[
                        fixed((hp, width)),
                        fixed((hp, width)),
                        pl.BlockSpec((width, TN), prev_col),
                        pl.BlockSpec((1, TN), prev_col),
                    ],
                    out_specs=pl.BlockSpec((n_pos, TN), lambda j, sc: (0, j)),
                    scratch_shapes=[pltpu.VMEM((n_pos, width), BF16)],
                ),
                out_shape=jax.ShapeDtypeStruct((n_pos, width), BF16),
                compiler_params=params(),
                cost_estimate=cost(2 * n_pos * width * width, 2 * width * width),
                name="prev_a",
            )(scalars, over[i], over_part[i], w_in, bias)

        def prev_b(s, pa, q, vhat):
            i = 2 * s + 1
            return pl.pallas_call(
                functools.partial(prev_b_body, nt),
                grid_spec=pltpu.PrefetchScalarGridSpec(
                    num_scalar_prefetch=1,
                    grid=(2 * nt,),
                    in_specs=[
                        fixed(fwd3.shape),
                        fixed((hp, width)),
                        fixed((hp, width)),
                        pl.BlockSpec((width, TN), prev_col),
                        pl.BlockSpec((1, TN), prev_col),
                        pl.BlockSpec((3, TN), prev_col),
                        pl.BlockSpec((n_pos, TN), lambda j, sc: (0, j)),
                        any_spec,
                        any_spec,
                    ],
                    out_specs=[
                        pl.BlockSpec((1, nbo, BLK, TN), lambda j, sc: (s, 0, 0, j)),
                        pl.BlockSpec((1, nbo, 2 * BLK, TN), lambda j, sc: (s, 0, 0, jnp.maximum(j - nt, 0))),
                    ],
                    scratch_shapes=[pltpu.VMEM((n_pos, width), BF16), pltpu.VMEM((n_own + 8, TN), F32)],
                ),
                out_shape=[q_shape, vhat_shape],
                input_output_aliases={8: 0, 9: 1},
                compiler_params=params(),
                cost_estimate=cost(2 * n_pos * width * width, 2 * width * width),
                name="prev_b",
            )(scalars, fwd3, over[i], over_part[i], w_in, bias, conv_taps, pa, q, vhat)

        for s in range(n_seq):
            pa = prev_a(2 * s)
            q, vhat = prev_b(s, pa, q, vhat)

        tf = TN
        far = pl.pallas_call(
            far_body,
            grid_spec=pltpu.PrefetchScalarGridSpec(
                num_scalar_prefetch=1,
                grid=(half_w // tf,),
                in_specs=[
                    fixed(fwd6.shape),
                    pl.BlockSpec((n_pos, tf), lambda j, sc: (0, sc[0] * (half_w // tf) + j)),
                    pl.BlockSpec((n_pos, tf), lambda j, sc: (0, sc[0] * (half_w // tf) + j)),
                    pl.BlockSpec((n_pos, tf), lambda j, sc: (0, j)),
                    pl.BlockSpec((n_pos, tf), lambda j, sc: (0, j)),
                ],
                out_specs=pl.BlockSpec((2, nbo, 2 * BLK, tf), lambda j, sc: (0, 0, 0, j)),
                scratch_shapes=[pltpu.VMEM((2, nbo, 3, BLK, tf), BF16)],
            ),
            out_shape=jax.ShapeDtypeStruct((2, nbo, 2 * BLK, half_w), F32),
            compiler_params=params(),
            cost_estimate=cost(6e9, 3e7),
            name="far_spectrum",
        )(scalars, fwd6, filt_one, filt_two, *f_part)

        tiles = nch // TC
        ht = half_w // TC
        q2 = q2.reshape(n_seq, nbo, BLK, half_w)

        def conv(j, xs, xc, ys, yc):
            base = j * tiles

            def col4(shape, first):
                return pl.BlockSpec(shape + (TC,), lambda t, sc: (0, 0, 0, first + base + t))

            chan = pl.BlockSpec((1, TC), lambda t, sc: (0, sc[0] * ht + base + t))
            own_f = pl.BlockSpec((n_pos, TC), lambda t, sc: (0, sc[0] * ht + base + t))
            part_f = pl.BlockSpec((n_pos, TC), lambda t, sc: (0, base + t))
            local = pl.BlockSpec((n_pos, TC), lambda t, sc: (0, t))
            return pl.pallas_call(
                conv_body,
                grid_spec=pltpu.PrefetchScalarGridSpec(
                    num_scalar_prefetch=1,
                    grid=(tiles,),
                    in_specs=[
                        fixed(fwd6.shape), fixed(inv6.shape),
                        col4((n_seq, nb, BLK), 0), col4((n_seq, nb, BLK), ht), col4((n_seq, nbo, BLK), 0),
                        col4((n_seq, nb, 2 * BLK), 0), col4((2, nbo, 2 * BLK), 0),
                        chan, chan, own_f, own_f,
                        part_f, part_f, local, local, local, local,
                    ],
                    out_specs=[pl.BlockSpec((n_seq, n_pos, TC), lambda t, sc: (0, 0, t))] * 2,
                    scratch_shapes=[
                        pltpu.VMEM((2, nbo, 3, BLK, TC), BF16),
                        *[pltpu.VMEM((nbo + 1, 2 * BLK, TC), F32)] * 2,
                        *[pltpu.VMEM((nb, 3, 2 * BLK, TC), BF16)] * n_seq,
                        *[pltpu.VMEM((nb, 3, BLK, TC), BF16)] * n_seq,
                        *[pltpu.VMEM((nb, BLK, TC), F32)] * n_seq,
                        *[pltpu.VMEM((nb, 2 * BLK, TC), F32)] * n_seq,
                        pltpu.VMEM((n_seq, nbo, BLK, TC), BF16),
                    ],
                ),
                out_shape=[jax.ShapeDtypeStruct((n_seq, n_pos, nch), BF16), jax.ShapeDtypeStruct((n_seq, n_pos, nch), F32)],
                compiler_params=params(),
                cost_estimate=cost(24e9 / N_CHUNK, 8e7 / N_CHUNK),
                name="long_conv",
            )(scalars, fwd6, inv6, q, q, q2, vhat, far, skip_one.reshape(1, -1), skip_two.reshape(1, -1),
              filt_one, filt_two, *f_part, xs, xc, ys, yc)

        keeps, parts = [], []
        for j in range(N_CHUNK):
            keep, send = conv(j, *near[j])
            keeps.append(keep)
            parts.append(hop(send, partner))
        return pl.pallas_call(
            functools.partial(out_body, N_CHUNK),
            grid_spec=pltpu.PrefetchScalarGridSpec(
                num_scalar_prefetch=1,
                grid=(wt,),
                in_specs=[
                    *[fixed((n_seq, n_pos, nch))] * (2 * N_CHUNK),
                    pl.BlockSpec((half_w, TN), lambda j, sc: (sc[0], j)),
                    pl.BlockSpec((half_w, TN), lambda j, sc: (1 - sc[0], j)),
                    pl.BlockSpec((n_seq, n_pos, TN), lambda j, sc: (0, 0, j)),
                ],
                out_specs=pl.BlockSpec((n_seq, n_pos, TN), lambda j, sc: (0, 0, j)),
                scratch_shapes=[pltpu.VMEM((n_seq * n_pos, half_w), BF16)] * 2,
            ),
            out_shape=jax.ShapeDtypeStruct((n_seq, n_pos, width), BF16),
            compiler_params=params(),
            cost_estimate=cost(2 * n_seq * n_pos * width * width, 2 * width * width),
            name="out_proj",
        )(scalars, *keeps, *parts, w_out, w_out, u_in)

    seq_spec = P("dp", "sp", None)
    filt_spec = P("sp", None)
    return jax.shard_map(compute, mesh=mesh, in_specs=(seq_spec, P(), P(), P(), P(), P(), P(), filt_spec, filt_spec), out_specs=seq_spec, check_vma=False)
```

```python
import functools

import jax
import jax.numpy as jnp
import numpy as np
from jax import lax
from jax.experimental import pallas as pl
from jax.experimental.pallas import tpu as pltpu
from jax.sharding import PartitionSpec as P

F32, BF16 = jnp.float32, jnp.bfloat16
BLK = 128
TN = 512
TC = 256
N_PRE = 2
MESH = pl.DeviceIdType.MESH


def split_table(table):
    parts, rest = [], table.astype(np.float64)
    for _ in range(3):
        part = rest.astype(np.float32).astype(jnp.bfloat16)
        parts.append(part)
        rest = rest - part.astype(np.float64)
    return parts


def transform_tables():
    freq = np.concatenate([np.arange(0, BLK, 2), np.arange(1, BLK, 2)]) + 0.5
    angle = 2.0 * np.pi * freq[:, None] * np.arange(BLK)[None, :] / (2 * BLK)
    fwd = np.concatenate([np.cos(angle), -np.sin(angle)], 0)
    inv = np.concatenate([np.cos(angle).T, -np.sin(angle).T], 1) / BLK
    f1, f2, f3 = split_table(fwd)
    e1, e2, e3 = split_table(inv)
    fwd3 = np.concatenate([f1, f2, f3], 1)
    fwd6 = np.concatenate([f1, f1, f2, f2, f1, f3], 1)
    inv6 = np.concatenate([e1, e1, e2, e2, e1, e3], 1)
    return fwd3, fwd6, inv6


def dot(a, b):
    return jnp.dot(a, b, preferred_element_type=F32)


def split3(x):
    hi = x.astype(BF16)
    rest = x - hi.astype(F32)
    mid = rest.astype(BF16)
    low = (rest - mid.astype(F32)).astype(BF16)
    return hi, mid, low


def stack6(hi, mid, low):
    return jnp.concatenate([hi, mid, hi, mid, low, hi], axis=0)


def short_conv(pbuf, t_ref, rows):
    return (t_ref[0:1] * pbuf[8:8 + rows] + t_ref[1:2] * pbuf[7:7 + rows] + t_ref[2:3] * pbuf[6:6 + rows]).astype(BF16)


def value_spectrum(fwd3_ref, q, dst):
    for j in range(q.shape[0] // BLK):
        blk = q[j * BLK:(j + 1) * BLK]
        dst[j] = dot(fwd3_ref[...], jnp.concatenate([blk, blk, blk], axis=0))


def in_own_body(nt, sc_ref, fwd3_ref, own_ref, pa_ref, pb_ref, pc_ref, pd_ref, tail_ref, w_ref, b_ref, t_ref, q_ref, q2_ref, vhat_ref, lhs, pbuf):
    c, on_b = sc_ref[0], sc_ref[1] == 1
    j = pl.program_id(0)
    n_seq, half = own_ref.shape[0], own_ref.shape[1]
    n_own = 2 * half
    rows = n_seq * n_own

    @pl.when(j == 0)
    def _():
        for s in range(n_seq):
            base = s * n_own
            lhs[pl.ds(pl.multiple_of(base + c * half, half), half), :] = own_ref[s]
            for h in range(2):
                piece = (pa_ref, pb_ref, pc_ref, pd_ref)[2 * s + h]
                start = base + (1 - c) * half + h * (half // 2)
                lhs[pl.ds(pl.multiple_of(start, half // 2), half // 2), :] = piece[...].astype(BF16)
        lhs[rows:, :] = tail_ref[...].astype(BF16)

    p = (dot(lhs[...], w_ref[...]) + b_ref[...]).astype(BF16).astype(F32)
    for s in range(n_seq):
        pbuf[s, 0:8] = jnp.where(on_b, p[rows + 8 * s:rows + 8 * s + 8], 0.0)
        pbuf[s, 8:] = p[s * n_own:(s + 1) * n_own]

    @pl.when(j < 2 * nt)
    def _():
        for s in range(n_seq):
            q_ref[s] = short_conv(pbuf.at[s], t_ref, n_own).reshape(q_ref.shape[1:])

    @pl.when(j >= 2 * nt)
    def _():
        for s in range(n_seq):
            q2_ref[s] = short_conv(pbuf.at[s], t_ref, n_own)

    @pl.when((j >= nt) & (j < 2 * nt))
    def _():
        for s in range(n_seq):
            value_spectrum(fwd3_ref, q_ref[s].reshape(n_own, -1), vhat_ref.at[s])


def gather_rows(sc_ref, near_ref, far_ref, lhs):
    c, rows = sc_ref[0], near_ref.shape[0]

    @pl.when(pl.program_id(0) == 0)
    def _():
        lhs[pl.ds(pl.multiple_of(c * rows, rows), rows), :] = near_ref[...].astype(BF16)
        lhs[pl.ds(pl.multiple_of((1 - c) * rows, rows), rows), :] = far_ref[...].astype(BF16)


def prev_a_body(sc_ref, near_ref, far_ref, w_ref, b_ref, p_ref, lhs):
    gather_rows(sc_ref, near_ref, far_ref, lhs)
    p_ref[...] = (dot(lhs[...], w_ref[...]) + b_ref[...]).astype(BF16)


def prev_b_body(nt, sc_ref, fwd3_ref, near_ref, far_ref, w_ref, b_ref, t_ref, pa_ref, q_in, vhat_in, q_ref, vhat_ref, lhs, pbuf):
    on_b = sc_ref[1] == 1
    rows = near_ref.shape[0]
    gather_rows(sc_ref, near_ref, far_ref, lhs)
    p = (dot(lhs[...], w_ref[...]) + b_ref[...]).astype(BF16).astype(F32)
    pbuf[0:8] = jnp.zeros((8, p.shape[1]), F32)
    for core in range(2):
        for h, piece in enumerate((pa_ref[...].astype(F32), p)):
            base = 8 + (2 * core + h) * rows
            pbuf[base:base + rows] = jnp.where(on_b, piece[core * rows:(core + 1) * rows], 0.0)
    q_ref[0] = short_conv(pbuf, t_ref, 4 * rows).reshape(q_ref.shape[1:])

    @pl.when(pl.program_id(0) >= nt)
    def _():
        value_spectrum(fwd3_ref, q_ref[0].reshape(4 * rows, -1), vhat_ref.at[0])


def split_blocks(src, parts, first):
    for j in range(src.shape[0] // BLK):
        for i, a in enumerate(split3(src[j * BLK:(j + 1) * BLK])):
            parts[first + j, i] = a


def block_spectrum(fwd6_ref, parts, j):
    return dot(fwd6_ref[...], stack6(parts[j, 0], parts[j, 1], parts[j, 2]))


def shifted_add(cur, old, lo, sign):
    re, im = slice(lo, lo + BLK // 2), slice(BLK + lo, BLK + lo + BLK // 2)
    return re, im, cur[re] - sign * old[im], cur[im] + sign * old[re]


SIDES = ((0, 1.0), (BLK // 2, -1.0))


def far_body(sc_ref, fwd6_ref, own1_ref, own2_ref, pf1_ref, pf2_ref, g_ref, parts):
    c = sc_ref[0]
    hk = own1_ref.shape[0] // BLK
    for f in range(2):
        split_blocks((own1_ref, own2_ref)[f], parts.at[f], c * hk)
        split_blocks((pf1_ref, pf2_ref)[f], parts.at[f], (1 - c) * hk)
        for j in range(2 * hk):
            g_ref[f, j] = block_spectrum(fwd6_ref, parts.at[f], j)
        for j in range(2 * hk - 1, 0, -1):
            for lo, sign in SIDES:
                re, im, new_re, new_im = shifted_add(g_ref.at[f, j], g_ref.at[f, j - 1], lo, sign)
                g_ref[f, j, re], g_ref[f, j, im] = new_re, new_im


def out_body(sc_ref, keep_ref, part_ref, wk_ref, wp_ref, u_ref, o_ref, lhs_k, lhs_p):
    @pl.when(pl.program_id(0) == 0)
    def _():
        rows = keep_ref.shape[0] * keep_ref.shape[1]
        lhs_k[...] = keep_ref[...].reshape(rows, -1)
        lhs_p[...] = part_ref[...].reshape(rows, -1).astype(BF16)

    acc = dot(lhs_k[...], wk_ref[...]) + dot(lhs_p[...], wp_ref[...])
    o_ref[...] = (u_ref[...].astype(F32) + acc.reshape(o_ref.shape)).astype(BF16)


def conv_body(n_tile, fwd6_ref, inv6_ref, x1_ref, v_ref, x2_ref, vhat, far_ref, sk1_ref, sk2_ref,
              f1_any, f2_any, pf1_any, pf2_any, xs_any, xc_any, ys_any, yc_any,
              keep_ref, part_any, hparts, g1, g2, sp0, sp1, zp0, zp1, zv0, zv1, zh0, zh1, ybuf, land, sendbuf,
              l_sem, x_send, x_recv, y_send, y_recv, p_send, p_recv):
    t = pl.program_id(0)
    sp, dp = lax.axis_index("sp"), lax.axis_index("dp")
    c, d = lax.rem(sp, 2), dp
    on_b = sp >= 2
    n_seq, nb = vhat.shape[0], vhat.shape[1]
    nbo = nb // 2
    half_w = n_tile * TC
    hk = f1_any.shape[0] // BLK
    g, sparts, zparts, zval, zhat = (g1, g2), (sp0, sp1), (zp0, zp1), (zv0, zv1), (zh0, zh1)

    def cols(start):
        return pl.ds(pl.multiple_of(start, TC), TC)

    def fill(f, u, side, src, start):
        return pltpu.make_async_copy(src.at[:, cols(start)], land.at[f, u, side], l_sem.at[f, u, side])

    def over(src, u, k):
        return pltpu.make_async_remote_copy(
            src.at[:, cols(k * half_w + u * TC)], land.at[d, u, c], x_send.at[u, k], x_recv.at[u, c],
            device_id=(dp, 2 + k), device_id_type=MESH)

    def landed(u, side):
        return pltpu.make_async_remote_copy(
            land.at[d, u, side], land.at[d, u, side], x_send.at[u, side], x_recv.at[u, side],
            device_id=(dp, sp), device_id_type=MESH)

    def across(u, side, f):
        return pltpu.make_async_remote_copy(
            land.at[f, u, side], land.at[f, u, side], y_send.at[u, side], y_recv.at[u, side],
            device_id=(1 - dp, sp), device_id_type=MESH)

    def swap(u):
        return pltpu.make_async_remote_copy(
            sendbuf.at[lax.rem(u, 2)], part_any.at[:, :, cols(u * TC)], p_send.at[u], p_recv.at[u],
            device_id=(dp, sp + 1 - 2 * c), device_id_type=MESH)

    @pl.when(t == 0)
    def _():
        barrier = pltpu.get_barrier_semaphore()
        other = sp + 1 - 2 * c
        across_x, across_both = lax.rem(sp + 2, 4), lax.rem(other + 2, 4)
        for peer in ((dp, other), (dp, across_x), (dp, across_both), (1 - dp, sp)):
            pl.semaphore_signal(barrier, inc=1, device_id=peer, device_id_type=MESH)
        pl.semaphore_wait(barrier, 4)

        @pl.when(jnp.logical_not(on_b))
        def _():
            for which, src in ((0, f1_any), (1, f2_any)):
                @pl.when(d == which)
                def _():
                    for u in range(N_PRE, n_tile):
                        for k in range(2):
                            over(src, u, k).start()
            for u in range(n_tile):
                for f, (own, part) in enumerate(((f1_any, pf1_any), (f2_any, pf2_any))):
                    fill(f, u, c, own, c * half_w + u * TC).start()
                    fill(f, u, 1 - c, part, u * TC).start()

        @pl.when(on_b)
        def _():
            for u in range(N_PRE):
                for f, (same, cross) in ((d, (xs_any, xc_any)), (1 - d, (ys_any, yc_any))):
                    fill(f, u, c, same, u * TC).start()
                    fill(f, u, 1 - c, cross, u * TC).start()

    @pl.when(jnp.logical_or(jnp.logical_not(on_b), t < N_PRE))
    def _():
        for f in range(2):
            for side in range(2):
                fill(f, t, side, xs_any, 0).wait()

    @pl.when(jnp.logical_and(on_b, t >= N_PRE))
    def _():
        for side in range(2):
            across(t, side, 1 - d).wait_recv()

    for f in range(2):
        for side in range(2):
            split_blocks(land.at[f, t, side], hparts.at[f], side * hk)

    def near_spectrum(f, j):
        g[f][j] = block_spectrum(fwd6_ref, hparts.at[f], j)

    def window(f):
        for j in range(nbo, 0, -1):
            cur = far_ref.at[f, 0] if j == nbo else g[f].at[j]
            for lo, sign in SIDES:
                re, im, new_re, new_im = shifted_add(cur, g[f].at[j - 1], lo, sign)
                g[f][j, re], g[f][j, im] = new_re, new_im

    def pointwise(xhat, f, dst, r, first):
        re, im = pl.ds(pl.multiple_of(r * 16, 16), 16), pl.ds(pl.multiple_of(BLK + r * 16, 16), 16)
        for k in range(first, nb):
            acc_re = acc_im = None
            for j in range(k + 1):
                i = k - j
                gr, gi = (g[f][i, re], g[f][i, im]) if i <= nbo else (far_ref[f, i - nbo, re], far_ref[f, i - nbo, im])
                xr, xi = xhat[j, re], xhat[j, im]
                t_re, t_im = xr * gr - xi * gi, xr * gi + xi * gr
                acc_re = t_re if acc_re is None else acc_re + t_re
                acc_im = t_im if acc_im is None else acc_im + t_im
            for part, (a, b) in enumerate(zip(split3(acc_re), split3(acc_im))):
                dst[k, part, re], dst[k, part, im] = a, b

    def inverse(s, k):
        return dot(inv6_ref[...], stack6(sparts[s][k, 0], sparts[s][k, 1], sparts[s][k, 2]))

    def gate_one(s, k):
        z = x1_ref[s, k].astype(F32) * (inverse(s, k) + sk1_ref[...] * v_ref[s, k].astype(F32))
        zval[s][k] = z
        for part, a in enumerate(split3(z)):
            zparts[s][k, part] = a

    def spectrum(s, k):
        zhat[s][k] = block_spectrum(fwd6_ref, zparts[s], k)

    def gate_two(s, k):
        y = x2_ref[s, k].astype(F32) * (inverse(s, nbo + k) + sk2_ref[...] * zval[s][nbo + k])
        ybuf[s, k] = y.astype(BF16)

    def loop(body, trips=nb // 2):
        def run(i, carry):
            body(i)
            return carry

        lax.fori_loop(0, trips, run, 0)

    for j in range(nbo):
        near_spectrum(0, j)
    window(0)

    @loop
    def _(i):
        pointwise(vhat.at[0], 0, sparts[0], 2 * i, 0)
        near_spectrum(1, i)
        pointwise(vhat.at[0], 0, sparts[0], 2 * i + 1, 0)

    window(1)

    @loop
    def _(i):
        for r in range(2):
            pointwise(vhat.at[1], 0, sparts[1], 2 * i + r, 0)
            gate_one(0, 2 * i + r)

    @functools.partial(loop, trips=nb // 4)
    def _(i):
        for r in range(4):
            gate_one(1, 4 * i + r)
            spectrum(0, 4 * i + r)

    @loop
    def _(i):
        for r in range(2):
            pointwise(zhat[0], 1, sparts[0], 2 * i + r, nbo)
            spectrum(1, 2 * i + r)

    @functools.partial(loop, trips=nbo // 2)
    def _(i):
        for r in range(4):
            pointwise(zhat[1], 1, sparts[1], 4 * i + r, nbo)
            if r % 2:
                gate_two(0, 2 * i + r // 2)

    for k in range(nbo):
        gate_two(1, k)

    slot = lax.rem(t, 2)

    @pl.when(t >= 2)
    def _():
        swap(t - 2).wait_send()

    for s in range(n_seq):
        for b in range(hk):
            keep_ref[s, b * BLK:(b + 1) * BLK] = ybuf[s, c * hk + b]
            sendbuf[slot, s, b * BLK:(b + 1) * BLK] = ybuf[s, (1 - c) * hk + b].astype(F32)

    nxt = t + 2

    @pl.when(jnp.logical_and(on_b, nxt < n_tile))
    def _():
        for side in range(2):
            landed(nxt, side).wait_recv()
            across(nxt, side, d).start()

    swap(t).start()

    @pl.when(t == n_tile - 1)
    def _():
        for u in (n_tile - 2, n_tile - 1):
            swap(u).wait_send()
        for u in range(n_tile):
            swap(u).wait_recv()

        @pl.when(on_b)
        def _():
            for u in range(N_PRE, n_tile):
                for side in range(2):
                    across(u, side, d).wait_send()

        @pl.when(jnp.logical_not(on_b))
        def _():
            for u in range(N_PRE, n_tile):
                for k in range(2):
                    over(f1_any, u, k).wait_send()


def params(mib=60):
    return pltpu.CompilerParams(vmem_limit_bytes=mib << 20, dimension_semantics=("arbitrary",))


def cost(flops, nbytes):
    return pl.CostEstimate(flops=int(flops), bytes_accessed=int(nbytes), transcendentals=0)


def solution(mesh):
    n_sp = mesh.shape["sp"]
    half_sp = n_sp // 2
    partner = [(i, i ^ 1) for i in range(n_sp)]
    over_same = [(i, i + half_sp) for i in range(half_sp)]
    over_cross = [(i, (i ^ 1) + half_sp) for i in range(half_sp)]
    swap_dp = [(0, 1), (1, 0)]
    fwd3, fwd6, inv6 = transform_tables()

    def hop(x, perm, axis="sp"):
        return lax.ppermute(x, axis, perm)

    def compute(u_in, w_in, b_in, conv_taps, w_out, skip_one, skip_two, filt_one, filt_two):
        sp, dp = lax.axis_index("sp"), lax.axis_index("dp")
        c = sp % 2
        scalars = jnp.stack([c, (sp >= half_sp).astype(jnp.int32), dp]).astype(jnp.int32)
        n_seq, n_pos, width = u_in.shape
        half_w = width // 2
        n_own = 2 * n_pos
        nb = 2 * n_own // BLK
        nbo = nb // 2

        hp = n_pos // 2
        pieces, gate = [], u_in[0, 0, :128].astype(F32)
        for s in range(n_seq):
            for h in range(2):
                raw, gate = lax.optimization_barrier((u_in[s, h * hp:(h + 1) * hp], gate))
                pieces.append(raw.astype(F32))
                gate = pieces[-1]
        over = [hop(x, over_same) for x in pieces]
        over_part = [hop(x, partner) for x in over]
        u_part = [hop(x, partner) for x in pieces]
        tail = u_in[:, -8:].reshape(-1, width).astype(F32)
        u_tail = hop(tail, [(half_sp - 1, half_sp)]) + hop(tail, [(half_sp - 1, half_sp + 1)])

        mine, other = c * half_w, (1 - c) * half_w

        def chan_half(f, start):
            return lax.dynamic_slice(f, (0, start), (n_pos, half_w))

        f_part = [hop(chan_half(f, other), partner) for f in (filt_one, filt_two)]
        npre = N_PRE * TC

        def pre(start):
            f_link = [lax.dynamic_slice(f, (0, start), (n_pos, npre)) for f in (filt_one, filt_two)]
            return jnp.where(dp == 0, *f_link)

        xs, xc = hop(pre(mine), over_same), hop(pre(other), over_cross)
        ys, yc = hop(xs, swap_dp, "dp"), hop(xc, swap_dp, "dp")

        bias = b_in.reshape(1, -1)
        nt = half_w // TN
        wt = width // TN
        any_spec = pl.BlockSpec(memory_space=pl.ANY)

        def fixed(shape):
            return pl.BlockSpec(shape, lambda *a: (0,) * len(shape))

        def own_col(j, sc):
            group = jnp.where(j < nt, 0, jnp.where(j < 2 * nt, 2, 1))
            return (0, group * wt + sc[0] * nt + j % nt)

        q_shape = jax.ShapeDtypeStruct((n_seq, nb, BLK, width), BF16)
        vhat_shape = jax.ShapeDtypeStruct((n_seq, nb, 2 * BLK, half_w), F32)
        q, q2, vhat = pl.pallas_call(
            functools.partial(in_own_body, nt),
            grid_spec=pltpu.PrefetchScalarGridSpec(
                num_scalar_prefetch=1,
                grid=(3 * nt,),
                in_specs=[
                    fixed(fwd3.shape),
                    fixed((n_seq, n_pos, width)),
                    *[fixed((hp, width))] * 4,
                    fixed((16, width)),
                    pl.BlockSpec((width, TN), own_col),
                    pl.BlockSpec((1, TN), own_col),
                    pl.BlockSpec((3, TN), own_col),
                ],
                out_specs=[
                    pl.BlockSpec((n_seq, nbo, BLK, TN), lambda j, sc: (0, 1, 0, jnp.minimum(j, 2 * nt - 1))),
                    pl.BlockSpec((n_seq, n_own, TN), lambda j, sc: (0, 0, jnp.maximum(j - 2 * nt, 0))),
                    pl.BlockSpec((n_seq, nbo, 2 * BLK, TN), lambda j, sc: (0, 1, 0, jnp.clip(j - nt, 0, nt - 1))),
                ],
                scratch_shapes=[pltpu.VMEM((n_seq * n_own + 16, width), BF16), pltpu.VMEM((n_seq, n_own + 8, TN), F32)],
            ),
            out_shape=[q_shape, jax.ShapeDtypeStruct((n_seq, n_own, half_w), BF16), vhat_shape],
            compiler_params=params(),
            cost_estimate=cost(2 * n_seq * n_own * width * 3 * half_w, 2 * width * 3 * half_w),
            name="in_own",
        )(scalars, fwd3, u_in, *u_part, u_tail, w_in, bias, conv_taps)

        def prev_col(j, sc):
            return (0, jnp.where(j < nt, 0, 2) * wt + sc[0] * nt + j % nt)

        def prev_a(i):
            return pl.pallas_call(
                prev_a_body,
                grid_spec=pltpu.PrefetchScalarGridSpec(
                    num_scalar_prefetch=1,
                    grid=(2 * nt,),
                    in_specs=[
                        fixed((hp, width)),
                        fixed((hp, width)),
                        pl.BlockSpec((width, TN), prev_col),
                        pl.BlockSpec((1, TN), prev_col),
                    ],
                    out_specs=pl.BlockSpec((n_pos, TN), lambda j, sc: (0, j)),
                    scratch_shapes=[pltpu.VMEM((n_pos, width), BF16)],
                ),
                out_shape=jax.ShapeDtypeStruct((n_pos, width), BF16),
                compiler_params=params(),
                cost_estimate=cost(2 * n_pos * width * width, 2 * width * width),
                name="prev_a",
            )(scalars, over[i], over_part[i], w_in, bias)

        def prev_b(s, pa, q, vhat):
            i = 2 * s + 1
            return pl.pallas_call(
                functools.partial(prev_b_body, nt),
                grid_spec=pltpu.PrefetchScalarGridSpec(
                    num_scalar_prefetch=1,
                    grid=(2 * nt,),
                    in_specs=[
                        fixed(fwd3.shape),
                        fixed((hp, width)),
                        fixed((hp, width)),
                        pl.BlockSpec((width, TN), prev_col),
                        pl.BlockSpec((1, TN), prev_col),
                        pl.BlockSpec((3, TN), prev_col),
                        pl.BlockSpec((n_pos, TN), lambda j, sc: (0, j)),
                        any_spec,
                        any_spec,
                    ],
                    out_specs=[
                        pl.BlockSpec((1, nbo, BLK, TN), lambda j, sc: (s, 0, 0, j)),
                        pl.BlockSpec((1, nbo, 2 * BLK, TN), lambda j, sc: (s, 0, 0, jnp.maximum(j - nt, 0))),
                    ],
                    scratch_shapes=[pltpu.VMEM((n_pos, width), BF16), pltpu.VMEM((n_own + 8, TN), F32)],
                ),
                out_shape=[q_shape, vhat_shape],
                input_output_aliases={8: 0, 9: 1},
                compiler_params=params(),
                cost_estimate=cost(2 * n_pos * width * width, 2 * width * width),
                name="prev_b",
            )(scalars, fwd3, over[i], over_part[i], w_in, bias, conv_taps, pa, q, vhat)

        for s in range(n_seq):
            pa = prev_a(2 * s)
            q, vhat = prev_b(s, pa, q, vhat)

        tf = TN
        far = pl.pallas_call(
            far_body,
            grid_spec=pltpu.PrefetchScalarGridSpec(
                num_scalar_prefetch=1,
                grid=(half_w // tf,),
                in_specs=[
                    fixed(fwd6.shape),
                    pl.BlockSpec((n_pos, tf), lambda j, sc: (0, sc[0] * (half_w // tf) + j)),
                    pl.BlockSpec((n_pos, tf), lambda j, sc: (0, sc[0] * (half_w // tf) + j)),
                    pl.BlockSpec((n_pos, tf), lambda j, sc: (0, j)),
                    pl.BlockSpec((n_pos, tf), lambda j, sc: (0, j)),
                ],
                out_specs=pl.BlockSpec((2, nbo, 2 * BLK, tf), lambda j, sc: (0, 0, 0, j)),
                scratch_shapes=[pltpu.VMEM((2, nbo, 3, BLK, tf), BF16)],
            ),
            out_shape=jax.ShapeDtypeStruct((2, nbo, 2 * BLK, half_w), F32),
            compiler_params=params(),
            cost_estimate=cost(6e9, 3e7),
            name="far_spectrum",
        )(scalars, fwd6, filt_one, filt_two, *f_part)

        n_tile = half_w // TC
        q2 = q2.reshape(n_seq, nbo, BLK, half_w)

        def col4(shape, first):
            return pl.BlockSpec(shape + (TC,), lambda t: (0, 0, 0, first + t))

        def my_half(x):
            return lax.dynamic_slice(x, (mine,), (half_w,)).reshape(1, -1)

        chan = pl.BlockSpec((1, TC), lambda t: (0, t))
        keep, part = pl.pallas_call(
            functools.partial(conv_body, n_tile),
            grid_spec=pltpu.PrefetchScalarGridSpec(
                num_scalar_prefetch=0,
                grid=(n_tile,),
                in_specs=[
                    fixed(fwd6.shape), fixed(inv6.shape),
                    col4((n_seq, nb, BLK), 0), col4((n_seq, nb, BLK), n_tile), col4((n_seq, nbo, BLK), 0),
                    col4((n_seq, nb, 2 * BLK), 0), col4((2, nbo, 2 * BLK), 0), chan, chan,
                    *[any_spec] * 8,
                ],
                out_specs=[pl.BlockSpec((n_seq, n_pos, TC), lambda t: (0, 0, t)), any_spec],
                scratch_shapes=[
                    pltpu.VMEM((2, nbo, 3, BLK, TC), BF16),
                    *[pltpu.VMEM((nbo + 1, 2 * BLK, TC), F32)] * 2,
                    *[pltpu.VMEM((nb, 3, 2 * BLK, TC), BF16)] * n_seq,
                    *[pltpu.VMEM((nb, 3, BLK, TC), BF16)] * n_seq,
                    *[pltpu.VMEM((nb, BLK, TC), F32)] * n_seq,
                    *[pltpu.VMEM((nb, 2 * BLK, TC), F32)] * n_seq,
                    pltpu.VMEM((n_seq, nbo, BLK, TC), BF16),
                    pltpu.VMEM((2, n_tile, 2, n_pos, TC), F32),
                    pltpu.VMEM((2, n_seq, n_pos, TC), F32),
                    pltpu.SemaphoreType.DMA((2, n_tile, 2)),
                    *[pltpu.SemaphoreType.DMA((n_tile, 2))] * 4,
                    *[pltpu.SemaphoreType.DMA((n_tile,))] * 2,
                ],
            ),
            out_shape=[jax.ShapeDtypeStruct((n_seq, n_pos, half_w), BF16), jax.ShapeDtypeStruct((n_seq, n_pos, half_w), F32)],
            compiler_params=pltpu.CompilerParams(
                vmem_limit_bytes=60 << 20, dimension_semantics=("arbitrary",), collective_id=0, has_side_effects=True),
            cost_estimate=cost(24e9, 8e7),
            name="long_conv",
        )(fwd6, inv6, q, q, q2, vhat, far, my_half(skip_one), my_half(skip_two), filt_one, filt_two, *f_part, xs, xc, ys, yc)

        return pl.pallas_call(
            out_body,
            grid_spec=pltpu.PrefetchScalarGridSpec(
                num_scalar_prefetch=1,
                grid=(wt,),
                in_specs=[
                    fixed((n_seq, n_pos, half_w)),
                    fixed((n_seq, n_pos, half_w)),
                    pl.BlockSpec((half_w, TN), lambda j, sc: (sc[0], j)),
                    pl.BlockSpec((half_w, TN), lambda j, sc: (1 - sc[0], j)),
                    pl.BlockSpec((n_seq, n_pos, TN), lambda j, sc: (0, 0, j)),
                ],
                out_specs=pl.BlockSpec((n_seq, n_pos, TN), lambda j, sc: (0, 0, j)),
                scratch_shapes=[pltpu.VMEM((n_seq * n_pos, half_w), BF16)] * 2,
            ),
            out_shape=jax.ShapeDtypeStruct((n_seq, n_pos, width), BF16),
            compiler_params=params(),
            cost_estimate=cost(2 * n_seq * n_pos * width * width, 2 * width * width),
            name="out_proj",
        )(scalars, keep, part, w_out, w_out, u_in)

    seq_spec = P("dp", "sp", None)
    filt_spec = P("sp", None)
    return jax.shard_map(compute, mesh=mesh, in_specs=(seq_spec, P(), P(), P(), P(), P(), P(), filt_spec, filt_spec), out_specs=seq_spec, check_vma=False)
```

```python
import functools

import jax
import jax.numpy as jnp
import numpy as np
from jax import lax
from jax.experimental import pallas as pl
from jax.experimental.pallas import tpu as pltpu
from jax.sharding import PartitionSpec as P

F32, BF16 = jnp.float32, jnp.bfloat16
BLK = 128
TN = 512
TC = 256
MESH = pl.DeviceIdType.MESH


def split_table(table):
    parts, rest = [], table.astype(np.float64)
    for _ in range(3):
        part = rest.astype(np.float32).astype(jnp.bfloat16)
        parts.append(part)
        rest = rest - part.astype(np.float64)
    return parts


def transform_tables():
    freq = np.concatenate([np.arange(0, BLK, 2), np.arange(1, BLK, 2)]) + 0.5
    angle = 2.0 * np.pi * freq[:, None] * np.arange(BLK)[None, :] / (2 * BLK)
    fwd = np.concatenate([np.cos(angle), -np.sin(angle)], 0)
    inv = np.concatenate([np.cos(angle).T, -np.sin(angle).T], 1) / BLK
    f1, f2, f3 = split_table(fwd)
    e1, e2, e3 = split_table(inv)
    fwd3 = np.concatenate([f1, f2, f3], 1)
    fwd6 = np.concatenate([f1, f1, f2, f2, f1, f3], 1)
    inv6 = np.concatenate([e1, e1, e2, e2, e1, e3], 1)
    return fwd3, fwd6, inv6


def dot(a, b):
    return jnp.dot(a, b, preferred_element_type=F32)


def split3(x):
    hi = x.astype(BF16)
    rest = x - hi.astype(F32)
    mid = rest.astype(BF16)
    low = (rest - mid.astype(F32)).astype(BF16)
    return hi, mid, low


def stack6(hi, mid, low):
    return jnp.concatenate([hi, mid, hi, mid, low, hi], axis=0)


def split_blocks(src, parts, first):
    for j in range(src.shape[0] // BLK):
        for i, a in enumerate(split3(src[j * BLK:(j + 1) * BLK])):
            parts[first + j, i] = a


def block_spectrum(fwd6_ref, parts, j):
    return dot(fwd6_ref[...], stack6(parts[j, 0], parts[j, 1], parts[j, 2]))


def shifted_add(cur, old, lo, sign):
    re, im = slice(lo, lo + BLK // 2), slice(BLK + lo, BLK + lo + BLK // 2)
    return re, im, cur[re] - sign * old[im], cur[im] + sign * old[re]


SIDES = ((0, 1.0), (BLK // 2, -1.0))


def short_conv(pbuf, t, first, rows):
    return (t[0:1] * pbuf[8 + first:8 + first + rows] + t[1:2] * pbuf[7 + first:7 + first + rows] + t[2:3] * pbuf[6 + first:6 + first + rows]).astype(BF16)


def block_values(fwd3_ref, blk):
    return dot(fwd3_ref[...], jnp.concatenate([blk, blk, blk], axis=0))


def main_body(fwd3_ref, fwd6_ref, inv6_ref, bias_ref, taps_ref, sk1_ref, sk2_ref, u_bf, u32, w_in, f1, f2,
              keep, part, qx, qv, vhat, far, u_sw, u_x, u_fw, tail, pf,
              land, ts, tr, os, orr, ws, wr, ss, sr, fs, fr, l_sem, x_send, x_recv, y_send, y_recv, p_send, p_recv):
    sp, dp = lax.axis_index("sp"), lax.axis_index("dp")
    c = lax.rem(sp, 2)
    on_b = sp >= 2
    on_a = jnp.logical_not(on_b)
    other = sp + 1 - 2 * c
    n_seq, n_pos, width = u_bf.shape
    half_w = width // 2
    nt, n_tile = half_w // TN, half_w // TC
    n_own, hp = 2 * n_pos, n_pos // 2
    nbo = n_own // BLK
    n_piece = 2 * n_seq

    def remote(src, dst, send, recv, peer):
        return pltpu.make_async_remote_copy(src, dst, send, recv, device_id=peer, device_id_type=MESH)

    def at(start, size):
        return pl.ds(pl.multiple_of(start, size), size)

    def piece(ref, s, h):
        return ref.at[s, h * hp:(h + 1) * hp]

    def tail_copy(k):
        return remote(u32.at[:, n_pos - 8:], tail, ts.at[k], tr.at[0], (dp, 2 + k))

    def over(s, h):
        return remote(piece(u32, s, h), piece(u_x, s, h), os.at[s, h], orr.at[s, h], (dp, lax.rem(sp + 2, 4)))

    def onward(s, h):
        return remote(piece(u_x, s, h), piece(u_fw, s, h), ws.at[s, h], wr.at[s, h], (dp, other))

    def swap_u(s):
        return remote(u32.at[s], u_sw.at[s], ss.at[s], sr.at[s], (dp, other))

    def swap_f(f):
        return remote((f1, f2)[f].at[:, at((1 - c) * half_w, half_w)], pf.at[f], fs.at[f], fr.at[f], (dp, other))

    def filt(src, u, k):
        return remote(src.at[:, at(k * half_w + u * TC, TC)], land.at[dp, u, c], x_send.at[u, k], x_recv.at[u, c], (dp, 2 + k))

    def landed(u, side):
        return remote(land.at[dp, u, side], land.at[dp, u, side], x_send.at[u, side], x_recv.at[u, side], (dp, sp))

    def across(u, side, f):
        return remote(land.at[f, u, side], land.at[f, u, side], y_send.at[u, side], y_recv.at[u, side], (1 - dp, sp))

    def fill(f, u, side, src, start):
        return pltpu.make_async_copy(src.at[:, at(start, TC)], land.at[f, u, side], l_sem.at[f, u, side])

    barrier = pltpu.get_barrier_semaphore()
    for peer in ((dp, other), (dp, lax.rem(sp + 2, 4)), (dp, lax.rem(other + 2, 4)), (1 - dp, sp)):
        pl.semaphore_signal(barrier, inc=1, device_id=peer, device_id_type=MESH)
    pl.semaphore_wait(barrier, 4)

    @pl.when(sp == 1)
    def _():
        for k in range(2):
            tail_copy(k).start()

    @pl.when(on_a)
    def _():
        for i in range(n_piece):
            over(*divmod(i, 2)).start()
        for which, src in ((0, f1), (1, f2)):
            @pl.when(dp == which)
            def _():
                for u in range(n_tile):
                    for k in range(2):
                        filt(src, u, k).start()

    for i in range(n_seq):
        swap_u(i).start()
    for f in range(2):
        swap_f(f).start()

    def front(wbuf, wsem, lhs, lhs_p, stage, st_sem, lhs_sem, tailbuf, q_st, q_sem, vh_st, vh_sem, pbuf, pstash):
        def column(g, j):
            return (g + j // nt) * width + c * half_w + lax.rem(j, nt) * TN

        def weights(g, j, slot):
            rows = width // 4
            return [pltpu.make_async_copy(w_in.at[i * rows:(i + 1) * rows, at(column(g, j), TN)],
                                          wbuf.at[slot, i * rows:(i + 1) * rows], wsem.at[slot, i]) for i in range(4)]

        def stream(g, body, following, n=nt):
            def step(j, carry):
                slot = lax.rem(j, 2)

                @pl.when(j + 1 < n)
                def _():
                    for copy in weights(g, j + 1, 1 - slot):
                        copy.start()

                @pl.when(j + 1 == n)
                def _():
                    following(1 - slot)

                for copy in weights(g, j, slot):
                    copy.wait()
                body(j, slot, bias_ref[:, at(column(g, j), TN)], taps_ref[:, at(column(g, j), TN)])
                return carry

            lax.fori_loop(0, n, step, 0)

        def begin(g):
            def start(slot):
                for copy in weights(g, 0, slot):
                    copy.start()
            return start

        def project(rows_ref, slot, bias):
            return (dot(rows_ref, wbuf[slot]) + bias).astype(BF16).astype(F32)

        def load_rows(n, src, dst_row):
            def copy(i):
                return pltpu.make_async_copy(src(i), stage.at[i % 2], st_sem.at[i % 2])

            copy(0).start()
            for i in range(n):
                if i + 1 < n:
                    copy(i + 1).start()
                copy(i).wait()
                ref, row = dst_row(i)
                ref[pl.ds(pl.multiple_of(row, 16), hp), :] = stage[i % 2].astype(BF16)

        tail_rows = n_seq * 8
        begin(0)(0)
        own_rows = [pltpu.make_async_copy(u_bf.at[s], lhs.at[pl.ds(pl.multiple_of(tail_rows + s * n_own + c * n_pos, 16), n_pos)], lhs_sem.at[s])
                    for s in range(n_seq)]
        for copy in own_rows:
            copy.start()
        for s in range(n_seq):
            swap_u(s).wait_recv()
        load_rows(n_piece, lambda i: piece(u_sw, *divmod(i, 2)), lambda i: (lhs, tail_rows + (i // 2) * n_own + (1 - c) * n_pos + (i % 2) * hp))
        for copy in own_rows:
            copy.wait()

        @pl.when(on_b)
        def _():
            tail_copy(0).wait_recv()
            copy = pltpu.make_async_copy(tail, tailbuf, lhs_sem.at[0])
            copy.start()
            copy.wait()

        @pl.when(on_a)
        def _():
            tailbuf[...] = jnp.zeros_like(tailbuf)

        lhs[:tail_rows, :] = tailbuf[...].reshape(tail_rows, width).astype(BF16)
        chunk = n_pos

        def own_phase(g, n, dst, spectrum, following):
            def flush(j, slot):
                cols = at(lax.rem(j, nt) * TN, TN)
                blocks = pl.ds(nbo * (1 + j // nt), nbo)
                copies = [pltpu.make_async_copy(q_st.at[slot], dst.at[:, blocks, :, cols], q_sem.at[slot])]
                if spectrum:
                    copies.append(pltpu.make_async_copy(vh_st.at[slot], vhat.at[:, nbo:, :, cols], vh_sem.at[slot]))
                return copies

            def body(j, slot, bias, taps):
                @pl.when(j >= 2)
                def _():
                    for copy in flush(j - 2, slot):
                        copy.wait()

                for i in range(n_seq * n_own // chunk):
                    s, r = divmod(i * chunk, n_own)
                    p = project(lhs[(tail_rows + i * chunk if i else 0):tail_rows + (i + 1) * chunk, :], slot, bias)
                    if i == 0:
                        for k in range(n_seq):
                            pbuf[k, 0:8] = jnp.where(on_b, p[8 * k:8 * k + 8], 0.0)
                        p = p[tail_rows:]
                    pbuf[s, 8 + r:8 + r + chunk] = p
                    q = short_conv(pbuf.at[s], taps, r, chunk)
                    for b in range(chunk // BLK):
                        blk = q[b * BLK:(b + 1) * BLK]
                        q_st[slot, s, r // BLK + b] = blk
                        if spectrum:
                            vh_st[slot, s, r // BLK + b] = block_values(fwd3_ref, blk)
                for copy in flush(j, slot):
                    copy.start()

            stream(g, body, following, n)
            for j in (n - 2, n - 1):
                for copy in flush(j, j % 2):
                    copy.wait()

        own_phase(0, 2 * nt, qx, False, begin(2))
        own_phase(2, nt, qv, True, begin(0))

        def far_phase(fin, fin_sem, fout, fout_sem, parts):
            hk = n_pos // BLK

            def fetch(j, slot):
                mine = at(c * half_w + j * TC, TC)
                srcs = (f1.at[:, mine], f2.at[:, mine], pf.at[0, :, at(j * TC, TC)], pf.at[1, :, at(j * TC, TC)])
                return [pltpu.make_async_copy(src, fin.at[slot, i], fin_sem.at[slot, i]) for i, src in enumerate(srcs)]

            def flush(j, slot):
                return pltpu.make_async_copy(fout.at[slot], far.at[:, :, :, at(j * TC, TC)], fout_sem.at[slot])

            for copy in fetch(0, 0):
                copy.start()

            def step(j, carry):
                slot = lax.rem(j, 2)

                @pl.when(j + 1 < n_tile)
                def _():
                    for copy in fetch(j + 1, 1 - slot):
                        copy.start()

                for copy in fetch(j, slot):
                    copy.wait()

                @pl.when(j >= 2)
                def _():
                    flush(j - 2, slot).wait()

                for f in range(2):
                    split_blocks(fin.at[slot, f], parts.at[f], c * hk)
                    split_blocks(fin.at[slot, 2 + f], parts.at[f], (1 - c) * hk)
                g_ref = fout.at[slot]
                for f in range(2):
                    for b in range(2 * hk):
                        g_ref[f, b] = block_spectrum(fwd6_ref, parts.at[f], b)
                    for b in range(2 * hk - 1, 0, -1):
                        for lo, sign in SIDES:
                            re, im, new_re, new_im = shifted_add(g_ref.at[f, b], g_ref.at[f, b - 1], lo, sign)
                            g_ref[f, b, re], g_ref[f, b, im] = new_re, new_im
                flush(j, slot).start()
                return carry

            lax.fori_loop(0, n_tile, step, 0)
            for j in (n_tile - 2, n_tile - 1):
                flush(j, j % 2).wait()

        for f in range(2):
            swap_f(f).wait_recv()
        pl.run_scoped(
            far_phase, pltpu.VMEM((2, 4, n_pos, TC), F32), pltpu.SemaphoreType.DMA((2, 4)),
            pltpu.VMEM((2, 2, nbo, 2 * BLK, TC), F32), pltpu.SemaphoreType.DMA((2,)), pltpu.VMEM((2, nbo, 3, BLK, TC), BF16))

        def prev_rows(s, h):
            @pl.when(on_b)
            def _():
                over(s, h).wait_recv()
                onward(s, h).start()
                load_rows(1, lambda _: piece(u_x, s, h), lambda _: (lhs_p, c * hp))
                onward(s, h).wait_recv()
                load_rows(1, lambda _: piece(u_fw, s, h), lambda _: (lhs_p, (1 - c) * hp))

            @pl.when(on_a)
            def _():
                lhs_p[...] = jnp.zeros_like(lhs_p)

        def prev_first(g, base, following):
            def body(j, slot, bias, taps):
                pstash[:, at(base + j * TN, TN)] = project(lhs_p[...], slot, bias).astype(BF16)

            stream(g, body, following)

        def prev_second(s, g, base, dst, spectrum, following):
            def flush(j, slot):
                cols = at(j * TN, TN)
                copies = [pltpu.make_async_copy(q_st.at[slot, 0], dst.at[s, :nbo, :, cols], q_sem.at[slot])]
                if spectrum:
                    copies.append(pltpu.make_async_copy(vh_st.at[slot, 0], vhat.at[s, :nbo, :, cols], vh_sem.at[slot]))
                return copies

            def body(j, slot, bias, taps):
                @pl.when(j >= 2)
                def _():
                    for copy in flush(j - 2, slot):
                        copy.wait()

                p = project(lhs_p[...], slot, bias)
                old = pstash[:, at(base + j * TN, TN)].astype(F32)
                pbuf[0, 0:8] = jnp.zeros((8, TN), F32)
                for core in range(2):
                    for h, rows in enumerate((old, p)):
                        first = 8 + (2 * core + h) * hp
                        pbuf[0, first:first + hp] = jnp.where(on_b, rows[core * hp:(core + 1) * hp], 0.0)
                for b in range(nbo):
                    blk = short_conv(pbuf.at[0], taps, b * BLK, BLK)
                    q_st[slot, 0, b] = blk
                    if spectrum:
                        vh_st[slot, 0, b] = block_values(fwd3_ref, blk)
                for copy in flush(j, slot):
                    copy.start()

            stream(g, body, following)
            for j in (nt - 2, nt - 1):
                for copy in flush(j, j % 2):
                    copy.wait()

        def prev_seq(s, carry):
            prev_rows(s, 0)
            prev_first(0, 0, begin(2))
            prev_first(2, half_w, begin(0))
            prev_rows(s, 1)
            prev_second(s, 0, 0, qx, False, begin(2))

            def again(slot):
                @pl.when(s + 1 < n_seq)
                def _():
                    begin(0)(slot)

            prev_second(s, 2, half_w, qv, True, again)
            return carry

        lax.fori_loop(0, n_seq, prev_seq, 0)

    pl.run_scoped(
        front,
        pltpu.VMEM((2, width, TN), BF16), pltpu.SemaphoreType.DMA((2, 4)),
        pltpu.VMEM((n_seq * n_own + 8 * n_seq, width), BF16), pltpu.VMEM((2 * hp, width), BF16),
        pltpu.VMEM((2, hp, width), F32), pltpu.SemaphoreType.DMA((2,)), pltpu.SemaphoreType.DMA((n_seq,)), pltpu.VMEM((n_seq, 8, width), F32),
        pltpu.VMEM((2, n_seq, nbo, BLK, TN), BF16), pltpu.SemaphoreType.DMA((2,)),
        pltpu.VMEM((2, n_seq, nbo, 2 * BLK, TN), F32), pltpu.SemaphoreType.DMA((2,)),
        pltpu.VMEM((n_seq, n_own + 8, TN), F32), pltpu.VMEM((2 * hp, 2 * half_w), BF16))

    @pl.when(on_a)
    def _():
        for u in range(n_tile):
            for f, own in enumerate((f1, f2)):
                fill(f, u, c, own, c * half_w + u * TC).start()
                fill(f, u, 1 - c, pf.at[f], u * TC).start()

    def forward(u):
        @pl.when(on_b)
        def _():
            for side in range(2):
                landed(u, side).wait_recv()
                across(u, side, dp).start()

    def conv(x1b, vb, x2b, vhb, farb, in_sem, kst, k_sem, sendbuf, *scratch):
        def fetch(t, slot):
            cols = at(t * TC, TC)
            srcs = (qx.at[:, :2 * nbo], qv, qx.at[:, 2 * nbo:], far)
            pairs = [(r.at[:, :, :, cols], b.at[slot]) for r, b in zip(srcs, (x1b, vb, x2b, farb))]
            pairs += [(vhat.at[s, :, :, cols], vhb.at[slot, s]) for s in range(n_seq)]
            return [pltpu.make_async_copy(src, dst, in_sem.at[slot, i]) for i, (src, dst) in enumerate(pairs)]

        def flush(t, slot):
            return pltpu.make_async_copy(kst.at[slot], keep.at[:, :, at(t * TC, TC)], k_sem.at[slot])

        def swap_y(u):
            return remote(sendbuf.at[lax.rem(u, 2)], part.at[:, :, at(u * TC, TC)], p_send.at[u], p_recv.at[u], (dp, other))

        for copy in fetch(0, 0):
            copy.start()
        forward(0)
        forward(1)

        def step(t, carry):
            slot = lax.rem(t, 2)

            @pl.when(t + 1 < n_tile)
            def _():
                for copy in fetch(t + 1, 1 - slot):
                    copy.start()

            @pl.when(on_a)
            def _():
                for f in range(2):
                    for side in range(2):
                        fill(f, t, side, f1, 0).wait()

            @pl.when(on_b)
            def _():
                for side in range(2):
                    across(t, side, 1 - dp).wait_recv()

            for copy in fetch(t, slot):
                copy.wait()

            @pl.when(t >= 2)
            def _():
                flush(t - 2, slot).wait()
                swap_y(t - 2).wait_send()

            cols = at(c * half_w + t * TC, TC)
            conv_tile(c, fwd6_ref, inv6_ref, x1b.at[slot], vb.at[slot], x2b.at[slot], vhb.at[slot], farb.at[slot],
                      sk1_ref[:, cols], sk2_ref[:, cols], land, t, kst.at[slot], sendbuf.at[slot], *scratch)
            flush(t, slot).start()

            @pl.when(t + 2 < n_tile)
            def _():
                forward(t + 2)

            swap_y(t).start()
            return carry

        lax.fori_loop(0, n_tile, step, 0)
        for u in (n_tile - 2, n_tile - 1):
            flush(u, u % 2).wait()
            swap_y(u).wait_send()
        for u in range(n_tile):
            swap_y(u).wait_recv()

    nb = 2 * nbo
    pl.run_scoped(
        conv,
        pltpu.VMEM((2, n_seq, nb, BLK, TC), BF16), pltpu.VMEM((2, n_seq, nb, BLK, TC), BF16), pltpu.VMEM((2, n_seq, nbo, BLK, TC), BF16),
        pltpu.VMEM((2, n_seq, nb, 2 * BLK, TC), F32), pltpu.VMEM((2, 2, nbo, 2 * BLK, TC), F32), pltpu.SemaphoreType.DMA((2, 4 + n_seq)),
        pltpu.VMEM((2, n_seq, n_pos, TC), BF16), pltpu.SemaphoreType.DMA((2,)), pltpu.VMEM((2, n_seq, n_pos, TC), F32),
        pltpu.VMEM((2, nbo, 3, BLK, TC), BF16),
        *[pltpu.VMEM((nbo + 1, 2 * BLK, TC), F32)] * 2,
        *[pltpu.VMEM((nb, 3, 2 * BLK, TC), BF16)] * n_seq,
        *[pltpu.VMEM((nb, 3, BLK, TC), BF16)] * n_seq,
        *[pltpu.VMEM((nb, BLK, TC), F32)] * n_seq,
        *[pltpu.VMEM((nb, 2 * BLK, TC), F32)] * n_seq,
        pltpu.VMEM((n_seq, nbo, BLK, TC), BF16))

    for s in range(n_seq):
        swap_u(s).wait_send()
    for f in range(2):
        swap_f(f).wait_send()

    @pl.when(sp == 1)
    def _():
        for k in range(2):
            tail_copy(k).wait_send()

    @pl.when(on_a)
    def _():
        for i in range(n_piece):
            over(*divmod(i, 2)).wait_send()
        for u in range(n_tile):
            for k in range(2):
                filt(f1, u, k).wait_send()

    @pl.when(on_b)
    def _():
        for i in range(n_piece):
            onward(*divmod(i, 2)).wait_send()
        for u in range(n_tile):
            for side in range(2):
                across(u, side, dp).wait_send()


def conv_tile(c, fwd6_ref, inv6_ref, x1_ref, v_ref, x2_ref, vhat, far_ref, sk1, sk2, land, t, keep_ref, send_ref,
              hparts, g1, g2, sp0, sp1, zp0, zp1, zv0, zv1, zh0, zh1, ybuf):
    n_seq, nb = vhat.shape[0], vhat.shape[1]
    nbo = nb // 2
    hk = nbo // 2
    g, sparts, zparts, zval, zhat = (g1, g2), (sp0, sp1), (zp0, zp1), (zv0, zv1), (zh0, zh1)

    for f in range(2):
        for side in range(2):
            split_blocks(land.at[f, t, side], hparts.at[f], side * hk)

    def near_spectrum(f, j):
        g[f][j] = block_spectrum(fwd6_ref, hparts.at[f], j)

    def window(f):
        for j in range(nbo, 0, -1):
            cur = far_ref.at[f, 0] if j == nbo else g[f].at[j]
            for lo, sign in SIDES:
                re, im, new_re, new_im = shifted_add(cur, g[f].at[j - 1], lo, sign)
                g[f][j, re], g[f][j, im] = new_re, new_im

    def pointwise(xhat, f, dst, r, first):
        re, im = pl.ds(pl.multiple_of(r * 16, 16), 16), pl.ds(pl.multiple_of(BLK + r * 16, 16), 16)
        for k in range(first, nb):
            acc_re = acc_im = None
            for j in range(k + 1):
                i = k - j
                gr, gi = (g[f][i, re], g[f][i, im]) if i <= nbo else (far_ref[f, i - nbo, re], far_ref[f, i - nbo, im])
                xr, xi = xhat[j, re], xhat[j, im]
                t_re, t_im = xr * gr - xi * gi, xr * gi + xi * gr
                acc_re = t_re if acc_re is None else acc_re + t_re
                acc_im = t_im if acc_im is None else acc_im + t_im
            for part, (a, b) in enumerate(zip(split3(acc_re), split3(acc_im))):
                dst[k, part, re], dst[k, part, im] = a, b

    def inverse(s, k):
        return dot(inv6_ref[...], stack6(sparts[s][k, 0], sparts[s][k, 1], sparts[s][k, 2]))

    def gate_one(s, k):
        z = x1_ref[s, k].astype(F32) * (inverse(s, k) + sk1 * v_ref[s, k].astype(F32))
        zval[s][k] = z
        for part, a in enumerate(split3(z)):
            zparts[s][k, part] = a

    def spectrum(s, k):
        zhat[s][k] = block_spectrum(fwd6_ref, zparts[s], k)

    def gate_two(s, k):
        y = x2_ref[s, k].astype(F32) * (inverse(s, nbo + k) + sk2 * zval[s][nbo + k])
        ybuf[s, k] = y.astype(BF16)

    def loop(body, trips=nb // 2):
        def run(i, carry):
            body(i)
            return carry
        lax.fori_loop(0, trips, run, 0)

    for j in range(nbo):
        near_spectrum(0, j)
    window(0)

    @loop
    def _(i):
        pointwise(vhat.at[0], 0, sparts[0], 2 * i, 0)
        near_spectrum(1, i)
        pointwise(vhat.at[0], 0, sparts[0], 2 * i + 1, 0)

    window(1)

    @loop
    def _(i):
        for r in range(2):
            pointwise(vhat.at[1], 0, sparts[1], 2 * i + r, 0)
            gate_one(0, 2 * i + r)

    @functools.partial(loop, trips=nb // 4)
    def _(i):
        for r in range(4):
            gate_one(1, 4 * i + r)
            spectrum(0, 4 * i + r)

    @loop
    def _(i):
        for r in range(2):
            pointwise(zhat[0], 1, sparts[0], 2 * i + r, nbo)
            spectrum(1, 2 * i + r)

    @functools.partial(loop, trips=nbo // 2)
    def _(i):
        for r in range(4):
            pointwise(zhat[1], 1, sparts[1], 4 * i + r, nbo)
            if r % 2:
                gate_two(0, 2 * i + r // 2)

    for k in range(nbo):
        gate_two(1, k)

    for s in range(n_seq):
        for b in range(hk):
            keep_ref[s, b * BLK:(b + 1) * BLK] = ybuf[s, c * hk + b]
            send_ref[s, b * BLK:(b + 1) * BLK] = ybuf[s, (1 - c) * hk + b].astype(F32)


def out_body(sc_ref, keep_ref, part_ref, wk_ref, wp_ref, u_ref, o_ref, lhs_k, lhs_p):
    @pl.when(pl.program_id(0) == 0)
    def _():
        rows = keep_ref.shape[0] * keep_ref.shape[1]
        lhs_k[...] = keep_ref[...].reshape(rows, -1)
        lhs_p[...] = part_ref[...].reshape(rows, -1).astype(BF16)

    acc = dot(lhs_k[...], wk_ref[...]) + dot(lhs_p[...], wp_ref[...])
    o_ref[...] = (u_ref[...].astype(F32) + acc.reshape(o_ref.shape)).astype(BF16)


def params(mib=60):
    return pltpu.CompilerParams(vmem_limit_bytes=mib << 20, dimension_semantics=("arbitrary",))


def solution(mesh):
    fwd3, fwd6, inv6 = transform_tables()

    def local_step(u_in, w_in, b_in, conv_taps, w_out, skip_one, skip_two, filt_one, filt_two):
        c = lax.axis_index("sp") % 2
        n_seq, n_pos, width = u_in.shape
        half_w = width // 2
        n_own = 2 * n_pos
        nb = 2 * n_own // BLK
        nbo = nb // 2
        n_tile, wt = half_w // TC, width // TN
        small, large = pl.BlockSpec(memory_space=pltpu.VMEM), pl.BlockSpec(memory_space=pl.ANY)
        dma = pltpu.SemaphoreType.DMA

        def shape(dims, dtype=F32):
            return jax.ShapeDtypeStruct(dims, dtype)

        keep, part, *_ = pl.pallas_call(
            main_body,
            in_specs=[small] * 7 + [large] * 5,
            out_specs=[large] * 11,
            out_shape=[
                shape((n_seq, n_pos, half_w), BF16), shape((n_seq, n_pos, half_w)),
                shape((n_seq, nb + nbo, BLK, half_w), BF16), shape((n_seq, nb, BLK, half_w), BF16),
                shape((n_seq, nb, 2 * BLK, half_w)), shape((2, nbo, 2 * BLK, half_w)),
                shape((n_seq, n_pos, width)), shape((n_seq, n_pos, width)), shape((n_seq, n_pos, width)),
                shape((n_seq, 8, width)), shape((2, n_pos, half_w)),
            ],
            scratch_shapes=[
                pltpu.VMEM((2, n_tile, 2, n_pos, TC), F32),
                dma((2,)), dma((1,)), *[dma((n_seq, 2))] * 4, *[dma((n_seq,))] * 2, *[dma((2,))] * 2,
                dma((2, n_tile, 2)), *[dma((n_tile, 2))] * 4, *[dma((n_tile,))] * 2,
            ],
            compiler_params=pltpu.CompilerParams(vmem_limit_bytes=62 << 20, collective_id=0, has_side_effects=True),
            name="hyena_main",
        )(fwd3, fwd6, inv6, b_in.reshape(1, -1), conv_taps, skip_one.reshape(1, -1), skip_two.reshape(1, -1),
          u_in, u_in.astype(F32), w_in, filt_one, filt_two)

        def fixed(dims):
            return pl.BlockSpec(dims, lambda *a: (0,) * len(dims))

        return pl.pallas_call(
            out_body,
            grid_spec=pltpu.PrefetchScalarGridSpec(
                num_scalar_prefetch=1,
                grid=(wt,),
                in_specs=[
                    fixed((n_seq, n_pos, half_w)),
                    fixed((n_seq, n_pos, half_w)),
                    pl.BlockSpec((half_w, TN), lambda j, sc: (sc[0], j)),
                    pl.BlockSpec((half_w, TN), lambda j, sc: (1 - sc[0], j)),
                    pl.BlockSpec((n_seq, n_pos, TN), lambda j, sc: (0, 0, j)),
                ],
                out_specs=pl.BlockSpec((n_seq, n_pos, TN), lambda j, sc: (0, 0, j)),
                scratch_shapes=[pltpu.VMEM((n_seq * n_pos, half_w), BF16)] * 2,
            ),
            out_shape=jax.ShapeDtypeStruct((n_seq, n_pos, width), BF16),
            compiler_params=params(),
            name="out_proj",
        )(c.astype(jnp.int32).reshape(1), keep, part, w_out, w_out, u_in)

    seq_spec = P("dp", "sp", None)
    filt_spec = P("sp", None)
    return jax.shard_map(local_step, mesh=mesh, in_specs=(seq_spec, P(), P(), P(), P(), P(), P(), filt_spec, filt_spec), out_specs=seq_spec, check_vma=False)
```

```python
import functools

import jax
import jax.numpy as jnp
import numpy as np
from jax import lax
from jax.experimental import pallas as pl
from jax.experimental.pallas import tpu as pltpu
from jax.sharding import PartitionSpec as P

F32, BF16 = jnp.float32, jnp.bfloat16
BLK = 128
TN = 512
TC = 256
MESH = pl.DeviceIdType.MESH


def split_table(table):
    parts, rest = [], table.astype(np.float64)
    for _ in range(3):
        part = rest.astype(np.float32).astype(jnp.bfloat16)
        parts.append(part)
        rest = rest - part.astype(np.float64)
    return parts


def transform_tables():
    freq = np.concatenate([np.arange(0, BLK, 2), np.arange(1, BLK, 2)]) + 0.5
    angle = 2.0 * np.pi * freq[:, None] * np.arange(BLK)[None, :] / (2 * BLK)
    fwd = np.concatenate([np.cos(angle), -np.sin(angle)], 0)
    inv = np.concatenate([np.cos(angle).T, -np.sin(angle).T], 1) / BLK
    f1, f2, f3 = split_table(fwd)
    e1, e2, e3 = split_table(inv)
    fwd3 = np.concatenate([f1, f2, f3], 1)
    fwd6 = np.concatenate([f1, f1, f2, f2, f1, f3], 1)
    inv6 = np.concatenate([e1, e1, e2, e2, e1, e3], 1)
    return fwd3, fwd6, inv6


def dot(a, b):
    return jnp.dot(a, b, preferred_element_type=F32)


def split3(x):
    hi = x.astype(BF16)
    rest = x - hi.astype(F32)
    mid = rest.astype(BF16)
    low = (rest - mid.astype(F32)).astype(BF16)
    return hi, mid, low


def stack6(hi, mid, low):
    return jnp.concatenate([hi, mid, hi, mid, low, hi], axis=0)


def split_blocks(src, parts, first):
    for j in range(src.shape[0] // BLK):
        for i, a in enumerate(split3(src[j * BLK:(j + 1) * BLK])):
            parts[first + j, i] = a


def block_spectrum(fwd6_ref, parts, j):
    return dot(fwd6_ref[...], stack6(parts[j, 0], parts[j, 1], parts[j, 2]))


def shifted_add(cur, old, lo, sign):
    re, im = slice(lo, lo + BLK // 2), slice(BLK + lo, BLK + lo + BLK // 2)
    return re, im, cur[re] - sign * old[im], cur[im] + sign * old[re]


SIDES = ((0, 1.0), (BLK // 2, -1.0))


def short_conv(pbuf, t, first, rows):
    return (t[0:1] * pbuf[8 + first:8 + first + rows] + t[1:2] * pbuf[7 + first:7 + first + rows] + t[2:3] * pbuf[6 + first:6 + first + rows]).astype(BF16)


def block_values(fwd3_ref, blk):
    return dot(fwd3_ref[...], jnp.concatenate([blk, blk, blk], axis=0))


def main_body(fwd3_ref, fwd6_ref, inv6_ref, bias_ref, taps_ref, sk1_ref, sk2_ref, u_bf, u32, w_in, f1, f2,
              keep, part, qx, qv, vhat, far, u_sw, u_x, u_fw, tail, pf,
              land, ts, tr, os, orr, ws, wr, ss, sr, fs, fr, l_sem, x_send, x_recv, y_send, y_recv, p_send, p_recv):
    sp, dp = lax.axis_index("sp"), lax.axis_index("dp")
    c = lax.rem(sp, 2)
    on_b = sp >= 2
    on_a = jnp.logical_not(on_b)
    other = sp + 1 - 2 * c
    n_seq, n_pos, width = u_bf.shape
    half_w = width // 2
    nt, n_tile = half_w // TN, half_w // TC
    n_own, hp = 2 * n_pos, n_pos // 2
    nbo = n_own // BLK
    n_piece = 2 * n_seq

    def remote(src, dst, send, recv, peer):
        return pltpu.make_async_remote_copy(src, dst, send, recv, device_id=peer, device_id_type=MESH)

    def at(start, size):
        return pl.ds(pl.multiple_of(start, size), size)

    def piece(ref, s, h):
        return ref.at[s, h * hp:(h + 1) * hp]

    def tail_copy(k):
        return remote(u32.at[:, n_pos - 8:], tail, ts.at[k], tr.at[0], (dp, 2 + k))

    def over(s, h):
        return remote(piece(u32, s, h), piece(u_x, s, h), os.at[s, h], orr.at[s, h], (dp, lax.rem(sp + 2, 4)))

    def onward(s, h):
        return remote(piece(u_x, s, h), piece(u_fw, s, h), ws.at[s, h], wr.at[s, h], (dp, other))

    def swap_u(s):
        return remote(u32.at[s], u_sw.at[s], ss.at[s], sr.at[s], (dp, other))

    def swap_f(f):
        return remote((f1, f2)[f].at[:, at((1 - c) * half_w, half_w)], pf.at[f], fs.at[f], fr.at[f], (dp, other))

    def filt(src, u, k):
        return remote(src.at[:, at(k * half_w + u * TC, TC)], land.at[dp, u, c], x_send.at[u, k], x_recv.at[u, c], (dp, 2 + k))

    def landed(u, side):
        return remote(land.at[dp, u, side], land.at[dp, u, side], x_send.at[u, side], x_recv.at[u, side], (dp, sp))

    def across(u, side, f):
        return remote(land.at[f, u, side], land.at[f, u, side], y_send.at[u, side], y_recv.at[u, side], (1 - dp, sp))

    def fill(f, u, side, src, start):
        return pltpu.make_async_copy(src.at[:, at(start, TC)], land.at[f, u, side], l_sem.at[f, u, side])

    barrier = pltpu.get_barrier_semaphore()
    for peer in ((dp, other), (dp, lax.rem(sp + 2, 4)), (dp, lax.rem(other + 2, 4)), (1 - dp, sp)):
        pl.semaphore_signal(barrier, inc=1, device_id=peer, device_id_type=MESH)
    pl.semaphore_wait(barrier, 4)

    @pl.when(sp == 1)
    def _():
        for k in range(2):
            tail_copy(k).start()

    @pl.when(on_a)
    def _():
        for i in range(n_piece):
            over(*divmod(i, 2)).start()
        for which, src in ((0, f1), (1, f2)):
            @pl.when(dp == which)
            def _():
                for u in range(n_tile):
                    for k in range(2):
                        filt(src, u, k).start()

    for i in range(n_seq):
        swap_u(i).start()
    for f in range(2):
        swap_f(f).start()

    def forward(u):
        @pl.when(on_b)
        def _():
            for side in range(2):
                landed(u, side).wait_recv()
                across(u, side, dp).start()

    def front(wbuf, wsem, lhs, lhs_p, stage, st_sem, lhs_sem, tailbuf, q_st, q_sem, vh_st, vh_sem, pbuf, pstash):
        def column(g, j):
            return (g + j // nt) * width + c * half_w + lax.rem(j, nt) * TN

        def weights(g, j, slot):
            rows = width // 4
            return [pltpu.make_async_copy(w_in.at[i * rows:(i + 1) * rows, at(column(g, j), TN)],
                                          wbuf.at[slot, i * rows:(i + 1) * rows], wsem.at[slot, i]) for i in range(4)]

        def stream(g, body, following, n=nt):
            def step(j, carry):
                slot = lax.rem(j, 2)

                @pl.when(j + 1 < n)
                def _():
                    for copy in weights(g, j + 1, 1 - slot):
                        copy.start()

                @pl.when(j + 1 == n)
                def _():
                    following(1 - slot)

                for copy in weights(g, j, slot):
                    copy.wait()
                body(j, slot, bias_ref[:, at(column(g, j), TN)], taps_ref[:, at(column(g, j), TN)])
                return carry

            lax.fori_loop(0, n, step, 0)

        def begin(g):
            def start(slot):
                for copy in weights(g, 0, slot):
                    copy.start()
            return start

        def project(rows_ref, slot, bias):
            return (dot(rows_ref, wbuf[slot]) + bias).astype(BF16).astype(F32)

        def load_rows(n, src, dst_row):
            def copy(i):
                return pltpu.make_async_copy(src(i), stage.at[i % 2], st_sem.at[i % 2])

            copy(0).start()
            for i in range(n):
                if i + 1 < n:
                    copy(i + 1).start()
                copy(i).wait()
                ref, row = dst_row(i)
                ref[pl.ds(pl.multiple_of(row, 16), hp), :] = stage[i % 2].astype(BF16)

        tail_rows = n_seq * 8
        begin(0)(0)
        own_rows = [pltpu.make_async_copy(u_bf.at[s], lhs.at[pl.ds(pl.multiple_of(tail_rows + s * n_own + c * n_pos, 16), n_pos)], lhs_sem.at[s])
                    for s in range(n_seq)]
        for copy in own_rows:
            copy.start()
        for s in range(n_seq):
            swap_u(s).wait_recv()
        load_rows(n_piece, lambda i: piece(u_sw, *divmod(i, 2)), lambda i: (lhs, tail_rows + (i // 2) * n_own + (1 - c) * n_pos + (i % 2) * hp))
        for copy in own_rows:
            copy.wait()

        @pl.when(on_b)
        def _():
            tail_copy(0).wait_recv()
            copy = pltpu.make_async_copy(tail, tailbuf, lhs_sem.at[0])
            copy.start()
            copy.wait()

        @pl.when(on_a)
        def _():
            tailbuf[...] = jnp.zeros_like(tailbuf)

        lhs[:tail_rows, :] = tailbuf[...].reshape(tail_rows, width).astype(BF16)
        chunk = n_pos

        def own_phase(g, n, dst, spectrum, following):
            def flush(j, slot):
                cols = at(lax.rem(j, nt) * TN, TN)
                blocks = pl.ds(nbo * (1 + j // nt), nbo)
                copies = [pltpu.make_async_copy(q_st.at[slot], dst.at[:, blocks, :, cols], q_sem.at[slot])]
                if spectrum:
                    copies.append(pltpu.make_async_copy(vh_st.at[slot], vhat.at[:, nbo:, :, cols], vh_sem.at[slot]))
                return copies

            def body(j, slot, bias, taps):
                @pl.when(j >= 2)
                def _():
                    for copy in flush(j - 2, slot):
                        copy.wait()

                for i in range(n_seq * n_own // chunk):
                    s, r = divmod(i * chunk, n_own)
                    p = project(lhs[(tail_rows + i * chunk if i else 0):tail_rows + (i + 1) * chunk, :], slot, bias)
                    if i == 0:
                        for k in range(n_seq):
                            pbuf[k, 0:8] = jnp.where(on_b, p[8 * k:8 * k + 8], 0.0)
                        p = p[tail_rows:]
                    pbuf[s, 8 + r:8 + r + chunk] = p
                    q = short_conv(pbuf.at[s], taps, r, chunk)
                    for b in range(chunk // BLK):
                        blk = q[b * BLK:(b + 1) * BLK]
                        q_st[slot, s, r // BLK + b] = blk
                        if spectrum:
                            vh_st[slot, s, r // BLK + b] = block_values(fwd3_ref, blk)
                for copy in flush(j, slot):
                    copy.start()

            stream(g, body, following, n)
            for j in (n - 2, n - 1):
                for copy in flush(j, j % 2):
                    copy.wait()

        own_phase(0, 2 * nt, qx, False, begin(2))
        own_phase(2, nt, qv, True, begin(0))

        def far_phase(fin, fin_sem, fout, fout_sem, parts):
            hk = n_pos // BLK

            def fetch(j, slot):
                mine = at(c * half_w + j * TC, TC)
                srcs = (f1.at[:, mine], f2.at[:, mine], pf.at[0, :, at(j * TC, TC)], pf.at[1, :, at(j * TC, TC)])
                return [pltpu.make_async_copy(src, fin.at[slot, i], fin_sem.at[slot, i]) for i, src in enumerate(srcs)]

            def flush(j, slot):
                return pltpu.make_async_copy(fout.at[slot], far.at[:, :, :, at(j * TC, TC)], fout_sem.at[slot])

            for copy in fetch(0, 0):
                copy.start()

            def step(j, carry):
                slot = lax.rem(j, 2)

                @pl.when(j + 1 < n_tile)
                def _():
                    for copy in fetch(j + 1, 1 - slot):
                        copy.start()

                for copy in fetch(j, slot):
                    copy.wait()

                @pl.when(j >= 2)
                def _():
                    flush(j - 2, slot).wait()

                for f in range(2):
                    split_blocks(fin.at[slot, f], parts.at[f], c * hk)
                    split_blocks(fin.at[slot, 2 + f], parts.at[f], (1 - c) * hk)
                g_ref = fout.at[slot]
                for f in range(2):
                    for b in range(2 * hk):
                        g_ref[f, b] = block_spectrum(fwd6_ref, parts.at[f], b)
                    for b in range(2 * hk - 1, 0, -1):
                        for lo, sign in SIDES:
                            re, im, new_re, new_im = shifted_add(g_ref.at[f, b], g_ref.at[f, b - 1], lo, sign)
                            g_ref[f, b, re], g_ref[f, b, im] = new_re, new_im
                flush(j, slot).start()
                return carry

            lax.fori_loop(0, n_tile, step, 0)
            for j in (n_tile - 2, n_tile - 1):
                flush(j, j % 2).wait()

        for f in range(2):
            swap_f(f).wait_recv()
        pl.run_scoped(
            far_phase, pltpu.VMEM((2, 4, n_pos, TC), F32), pltpu.SemaphoreType.DMA((2, 4)),
            pltpu.VMEM((2, 2, nbo, 2 * BLK, TC), F32), pltpu.SemaphoreType.DMA((2,)), pltpu.VMEM((2, nbo, 3, BLK, TC), BF16))

        def prev_rows(s, h):
            @pl.when(on_b)
            def _():
                over(s, h).wait_recv()
                onward(s, h).start()
                load_rows(1, lambda _: piece(u_x, s, h), lambda _: (lhs_p, c * hp))
                onward(s, h).wait_recv()
                load_rows(1, lambda _: piece(u_fw, s, h), lambda _: (lhs_p, (1 - c) * hp))

            @pl.when(on_a)
            def _():
                lhs_p[...] = jnp.zeros_like(lhs_p)

        def prev_first(g, base, following):
            def body(j, slot, bias, taps):
                pstash[:, at(base + j * TN, TN)] = project(lhs_p[...], slot, bias).astype(BF16)

            stream(g, body, following)

        def prev_second(s, g, base, dst, spectrum, following):
            def flush(j, slot):
                cols = at(j * TN, TN)
                copies = [pltpu.make_async_copy(q_st.at[slot, 0], dst.at[s, :nbo, :, cols], q_sem.at[slot])]
                if spectrum:
                    copies.append(pltpu.make_async_copy(vh_st.at[slot, 0], vhat.at[s, :nbo, :, cols], vh_sem.at[slot]))
                return copies

            def body(j, slot, bias, taps):
                @pl.when(j >= 2)
                def _():
                    for copy in flush(j - 2, slot):
                        copy.wait()

                p = project(lhs_p[...], slot, bias)
                old = pstash[:, at(base + j * TN, TN)].astype(F32)
                pbuf[0, 0:8] = jnp.zeros((8, TN), F32)
                for core in range(2):
                    for h, rows in enumerate((old, p)):
                        first = 8 + (2 * core + h) * hp
                        pbuf[0, first:first + hp] = jnp.where(on_b, rows[core * hp:(core + 1) * hp], 0.0)
                for b in range(nbo):
                    blk = short_conv(pbuf.at[0], taps, b * BLK, BLK)
                    q_st[slot, 0, b] = blk
                    if spectrum:
                        vh_st[slot, 0, b] = block_values(fwd3_ref, blk)
                for copy in flush(j, slot):
                    copy.start()

            stream(g, body, following)
            for j in (nt - 2, nt - 1):
                for copy in flush(j, j % 2):
                    copy.wait()

        def prev_seq(s, carry):
            prev_rows(s, 0)
            prev_first(0, 0, begin(2))
            prev_first(2, half_w, begin(0))
            prev_rows(s, 1)
            prev_second(s, 0, 0, qx, False, begin(2))

            @pl.when(s + 1 == n_seq)
            def _():
                forward(0)

            def again(slot):
                @pl.when(s + 1 < n_seq)
                def _():
                    begin(0)(slot)

            prev_second(s, 2, half_w, qv, True, again)
            return carry

        lax.fori_loop(0, n_seq, prev_seq, 0)

    pl.run_scoped(
        front,
        pltpu.VMEM((2, width, TN), BF16), pltpu.SemaphoreType.DMA((2, 4)),
        pltpu.VMEM((n_seq * n_own + 8 * n_seq, width), BF16), pltpu.VMEM((2 * hp, width), BF16),
        pltpu.VMEM((2, hp, width), F32), pltpu.SemaphoreType.DMA((2,)), pltpu.SemaphoreType.DMA((n_seq,)), pltpu.VMEM((n_seq, 8, width), F32),
        pltpu.VMEM((2, n_seq, nbo, BLK, TN), BF16), pltpu.SemaphoreType.DMA((2,)),
        pltpu.VMEM((2, n_seq, nbo, 2 * BLK, TN), F32), pltpu.SemaphoreType.DMA((2,)),
        pltpu.VMEM((n_seq, n_own + 8, TN), F32), pltpu.VMEM((2 * hp, 2 * half_w), BF16))

    @pl.when(on_a)
    def _():
        for u in range(n_tile):
            for f, own in enumerate((f1, f2)):
                fill(f, u, c, own, c * half_w + u * TC).start()
                fill(f, u, 1 - c, pf.at[f], u * TC).start()

    def conv(x1b, vb, x2b, vhb, farb, in_sem, vh_sem, kst, k_sem, sendbuf, *scratch):
        def fetch(t):
            cols, slot = at(t * TC, TC), lax.rem(t, 3)
            srcs = (qx.at[:, :2 * nbo], qv, qx.at[:, 2 * nbo:], far)
            copies = [pltpu.make_async_copy(r.at[:, :, :, cols], b.at[slot], in_sem.at[slot, i])
                      for i, (r, b) in enumerate(zip(srcs, (x1b, vb, x2b, farb)))]
            two = lax.rem(t, 2)
            return copies + [pltpu.make_async_copy(vhat.at[s, :, :, cols], vhb.at[two, s], vh_sem.at[two, s]) for s in range(n_seq)]

        def flush(t):
            slot = lax.rem(t, 2)
            return pltpu.make_async_copy(kst.at[slot], keep.at[:, :, at(t * TC, TC)], k_sem.at[slot])

        def swap_y(u):
            return remote(sendbuf.at[lax.rem(u, 2)], part.at[:, :, at(u * TC, TC)], p_send.at[u], p_recv.at[u], (dp, other))

        tile = ConvTile(fwd6_ref, inv6_ref, *scratch)

        def inputs(t, back):
            slot, cols = lax.rem(t + 3 - back, 3), at(c * half_w + lax.rem(t + n_tile - back, n_tile) * TC, TC)
            return x1b.at[slot], vb.at[slot], x2b.at[slot], farb.at[slot], sk1_ref[:, cols], sk2_ref[:, cols]

        def emit(t):
            slot = lax.rem(t, 2)

            @pl.when(t >= 2)
            def _():
                flush(t - 2).wait()
                swap_y(t - 2).wait_send()

            tile.result(c, kst.at[slot], sendbuf.at[slot])
            flush(t).start()
            swap_y(t).start()

        for copy in fetch(0):
            copy.start()
        forward(1)

        def step(t, carry):
            @pl.when(t + 1 < n_tile)
            def _():
                for copy in fetch(t + 1):
                    copy.start()

            @pl.when(on_a)
            def _():
                for f in range(2):
                    for side in range(2):
                        fill(f, t, side, f1, 0).wait()

            @pl.when(on_b)
            def _():
                for side in range(2):
                    across(t, side, 1 - dp).wait_recv()

            for copy in fetch(t):
                copy.wait()

            tile.step(land, t, vhb.at[lax.rem(t, 2)], inputs(t, 0), inputs(t, 1))

            @pl.when(t + 2 < n_tile)
            def _():
                forward(t + 2)

            @pl.when(t >= 1)
            def _():
                emit(t - 1)
            return carry

        lax.fori_loop(0, n_tile, step, 0)
        tile.drain(inputs(n_tile, 1))
        emit(n_tile - 1)
        for u in (n_tile - 2, n_tile - 1):
            flush(u).wait()
            swap_y(u).wait_send()
        for u in range(n_tile):
            swap_y(u).wait_recv()

    nb = 2 * nbo
    pl.run_scoped(
        conv,
        pltpu.VMEM((3, n_seq, nb, BLK, TC), BF16), pltpu.VMEM((3, n_seq, nb, BLK, TC), BF16), pltpu.VMEM((3, n_seq, nbo, BLK, TC), BF16),
        pltpu.VMEM((2, n_seq, nb, 2 * BLK, TC), F32), pltpu.VMEM((3, 2, nbo, 2 * BLK, TC), F32),
        pltpu.SemaphoreType.DMA((3, 4)), pltpu.SemaphoreType.DMA((2, n_seq)),
        pltpu.VMEM((2, n_seq, n_pos, TC), BF16), pltpu.SemaphoreType.DMA((2,)), pltpu.VMEM((2, n_seq, n_pos, TC), F32),
        pltpu.VMEM((2, nbo, 3, BLK, TC), BF16),
        pltpu.VMEM((nbo + 1, 2 * BLK, TC), F32), pltpu.VMEM((nbo + 1, 2 * BLK, TC), F32), pltpu.VMEM((nbo, 2 * BLK, TC), F32),
        *[pltpu.VMEM((nb, 3, 2 * BLK, TC), BF16)] * n_seq,
        pltpu.VMEM((nb, 3, BLK, TC), BF16),
        *[pltpu.VMEM((nb, BLK, TC), F32)] * n_seq,
        pltpu.VMEM((nb, 2 * BLK, TC), F32),
        *[pltpu.VMEM((nbo, 3, 2 * BLK, TC), BF16)] * n_seq,
        pltpu.VMEM((n_seq, nbo, BLK, TC), BF16))

    for s in range(n_seq):
        swap_u(s).wait_send()
    for f in range(2):
        swap_f(f).wait_send()

    @pl.when(sp == 1)
    def _():
        for k in range(2):
            tail_copy(k).wait_send()

    @pl.when(on_a)
    def _():
        for i in range(n_piece):
            over(*divmod(i, 2)).wait_send()
        for u in range(n_tile):
            for k in range(2):
                filt(f1, u, k).wait_send()

    @pl.when(on_b)
    def _():
        for i in range(n_piece):
            onward(*divmod(i, 2)).wait_send()
        for u in range(n_tile):
            for side in range(2):
                across(u, side, dp).wait_send()


def loop(trips):
    def run(body):
        def step(i, carry):
            body(i)
            return carry
        lax.fori_loop(0, trips, step, 0)
    return run


class ConvTile:
    def __init__(self, fwd6, inv6, hparts, g1, g2, raw2, sp0, sp1, zparts, zv0, zv1, zhat, sq0, sq1, ybuf):
        self.fwd6, self.inv6, self.hparts, self.g, self.raw2 = fwd6, inv6, hparts, (g1, g2), raw2
        self.first, self.second, self.zparts, self.zval, self.zhat, self.ybuf = (sp0, sp1), (sq0, sq1), zparts, (zv0, zv1), zhat, ybuf
        self.nb, self.nbo = sp0.shape[0], sq0.shape[0]

    def near(self, land, t, f):
        for side in range(2):
            split_blocks(land.at[f, t, side], self.hparts.at[f], side * self.nbo // 2)

    def window(self, f, raw, far):
        g, nbo = self.g[f], self.nbo
        for j in range(nbo, 0, -1):
            cur = far.at[f, 0] if j == nbo else raw.at[j]
            for lo, sign in SIDES:
                re, im, new_re, new_im = shifted_add(cur, raw.at[j - 1], lo, sign)
                g[j, re], g[j, im] = new_re, new_im
        if raw is not g:
            g[0] = raw[0]

    def pointwise(self, xhat, f, far, dst, r, first):
        g, nbo = self.g[f], self.nbo
        re, im = pl.ds(pl.multiple_of(r * 16, 16), 16), pl.ds(pl.multiple_of(BLK + r * 16, 16), 16)
        for k in range(first, self.nb):
            acc_re = acc_im = None
            for j in range(k + 1):
                i = k - j
                gr, gi = (g[i, re], g[i, im]) if i <= nbo else (far[f, i - nbo, re], far[f, i - nbo, im])
                xr, xi = xhat[j, re], xhat[j, im]
                t_re, t_im = xr * gr - xi * gi, xr * gi + xi * gr
                acc_re = t_re if acc_re is None else acc_re + t_re
                acc_im = t_im if acc_im is None else acc_im + t_im
            for part, (a, b) in enumerate(zip(split3(acc_re), split3(acc_im))):
                dst[k - first, part, re], dst[k - first, part, im] = a, b

    def inverse(self, parts, k):
        return dot(self.inv6[...], stack6(parts[k, 0], parts[k, 1], parts[k, 2]))

    def gate_one(self, s, k, data):
        x1, v, _, _, skip, _ = data
        z = x1[s, k].astype(F32) * (self.inverse(self.first[s], k) + skip * v[s, k].astype(F32))
        self.zval[s][k] = z
        for part, a in enumerate(split3(z)):
            self.zparts[k, part] = a

    def spectrum(self, k):
        self.zhat[k] = block_spectrum(self.fwd6, self.zparts, k)

    def gate_two(self, s, k, data):
        y = data[2][s, k].astype(F32) * (self.inverse(self.second[s], k) + data[5] * self.zval[s][self.nbo + k])
        self.ybuf[s, k] = y.astype(BF16)

    def middle(self, s, data, i, point=None):
        for q in range(4):
            if point is not None:
                point(4 * i + q)
            for k in range(2):
                if q < 2:
                    self.gate_one(s, 4 * i + 2 * q + k, data)
                else:
                    self.spectrum(4 * i + 2 * (q - 2) + k)

    def step(self, land, t, vhat, data, old):
        nb, nbo = self.nb, self.nbo
        far = data[3]
        self.near(land, t, 0)
        for j in range(nbo):
            self.g[0][j] = block_spectrum(self.fwd6, self.hparts.at[0], j)
        self.near(land, t, 1)
        self.window(0, self.g[0], far)

        @loop(nb // 4)
        def _(i):
            self.middle(1, old, i, lambda r: self.pointwise(vhat.at[0], 0, far, self.first[0], r, 0))

        @loop(nbo // 2)
        def _(i):
            for q in range(4):
                self.pointwise(self.zhat, 1, old[3], self.second[1], 4 * i + q, nbo)
                if q < 2:
                    self.gate_two(0, 2 * i + q, old)
                else:
                    j = 2 * i + q - 2
                    self.raw2[j] = block_spectrum(self.fwd6, self.hparts.at[1], j)

        self.window(1, self.raw2, far)

        @loop(nb // 4)
        def _(i):
            self.middle(0, data, i, lambda r: self.pointwise(vhat.at[1], 0, far, self.first[1], r, 0))

        @loop(nbo // 2)
        def _(i):
            for q in range(4):
                self.pointwise(self.zhat, 1, far, self.second[0], 4 * i + q, nbo)
                if q % 2 == 0:
                    self.gate_two(1, 2 * i + q // 2, old)

    def drain(self, data):
        nb, nbo = self.nb, self.nbo

        @loop(nb // 4)
        def _(i):
            self.middle(1, data, i)

        @loop(nbo // 2)
        def _(i):
            for q in range(4):
                self.pointwise(self.zhat, 1, data[3], self.second[1], 4 * i + q, nbo)
                if q % 2 == 0:
                    self.gate_two(0, 2 * i + q // 2, data)

        for k in range(nbo):
            self.gate_two(1, k, data)

    def result(self, c, keep, send):
        hk = self.nbo // 2
        for s in range(self.ybuf.shape[0]):
            for b in range(hk):
                keep[s, b * BLK:(b + 1) * BLK] = self.ybuf[s, c * hk + b]
                send[s, b * BLK:(b + 1) * BLK] = self.ybuf[s, (1 - c) * hk + b].astype(F32)


def out_body(sc_ref, keep_ref, part_ref, wk_ref, wp_ref, u_ref, o_ref, lhs_k, lhs_p):
    @pl.when(pl.program_id(0) == 0)
    def _():
        rows = keep_ref.shape[0] * keep_ref.shape[1]
        lhs_k[...] = keep_ref[...].reshape(rows, -1)
        lhs_p[...] = part_ref[...].reshape(rows, -1).astype(BF16)

    acc = dot(lhs_k[...], wk_ref[...]) + dot(lhs_p[...], wp_ref[...])
    o_ref[...] = (u_ref[...].astype(F32) + acc.reshape(o_ref.shape)).astype(BF16)


def params(mib=60):
    return pltpu.CompilerParams(vmem_limit_bytes=mib << 20, dimension_semantics=("arbitrary",))


def solution(mesh):
    fwd3, fwd6, inv6 = transform_tables()

    def local_step(u_in, w_in, b_in, conv_taps, w_out, skip_one, skip_two, filt_one, filt_two):
        c = lax.axis_index("sp") % 2
        n_seq, n_pos, width = u_in.shape
        half_w = width // 2
        n_own = 2 * n_pos
        nb = 2 * n_own // BLK
        nbo = nb // 2
        n_tile, wt = half_w // TC, width // TN
        small, large = pl.BlockSpec(memory_space=pltpu.VMEM), pl.BlockSpec(memory_space=pl.ANY)
        dma = pltpu.SemaphoreType.DMA

        def shape(dims, dtype=F32):
            return jax.ShapeDtypeStruct(dims, dtype)

        keep, part, *_ = pl.pallas_call(
            main_body,
            in_specs=[small] * 7 + [large] * 5,
            out_specs=[large] * 11,
            out_shape=[
                shape((n_seq, n_pos, half_w), BF16), shape((n_seq, n_pos, half_w)),
                shape((n_seq, nb + nbo, BLK, half_w), BF16), shape((n_seq, nb, BLK, half_w), BF16),
                shape((n_seq, nb, 2 * BLK, half_w)), shape((2, nbo, 2 * BLK, half_w)),
                shape((n_seq, n_pos, width)), shape((n_seq, n_pos, width)), shape((n_seq, n_pos, width)),
                shape((n_seq, 8, width)), shape((2, n_pos, half_w)),
            ],
            scratch_shapes=[
                pltpu.VMEM((2, n_tile, 2, n_pos, TC), F32),
                dma((2,)), dma((1,)), *[dma((n_seq, 2))] * 4, *[dma((n_seq,))] * 2, *[dma((2,))] * 2,
                dma((2, n_tile, 2)), *[dma((n_tile, 2))] * 4, *[dma((n_tile,))] * 2,
            ],
            compiler_params=pltpu.CompilerParams(vmem_limit_bytes=62 << 20, collective_id=0, has_side_effects=True),
            name="hyena_main",
        )(fwd3, fwd6, inv6, b_in.reshape(1, -1), conv_taps, skip_one.reshape(1, -1), skip_two.reshape(1, -1),
          u_in, u_in.astype(F32), w_in, filt_one, filt_two)

        def fixed(dims):
            return pl.BlockSpec(dims, lambda *a: (0,) * len(dims))

        return pl.pallas_call(
            out_body,
            grid_spec=pltpu.PrefetchScalarGridSpec(
                num_scalar_prefetch=1,
                grid=(wt,),
                in_specs=[
                    fixed((n_seq, n_pos, half_w)),
                    fixed((n_seq, n_pos, half_w)),
                    pl.BlockSpec((half_w, TN), lambda j, sc: (sc[0], j)),
                    pl.BlockSpec((half_w, TN), lambda j, sc: (1 - sc[0], j)),
                    pl.BlockSpec((n_seq, n_pos, TN), lambda j, sc: (0, 0, j)),
                ],
                out_specs=pl.BlockSpec((n_seq, n_pos, TN), lambda j, sc: (0, 0, j)),
                scratch_shapes=[pltpu.VMEM((n_seq * n_pos, half_w), BF16)] * 2,
            ),
            out_shape=jax.ShapeDtypeStruct((n_seq, n_pos, width), BF16),
            compiler_params=params(),
            name="out_proj",
        )(c.astype(jnp.int32).reshape(1), keep, part, w_out, w_out, u_in)

    seq_spec = P("dp", "sp", None)
    filt_spec = P("sp", None)
    return jax.shard_map(local_step, mesh=mesh, in_specs=(seq_spec, P(), P(), P(), P(), P(), P(), filt_spec, filt_spec), out_specs=seq_spec, check_vma=False)
```

```python
import functools

import jax
import jax.numpy as jnp
import numpy as np
from jax import lax
from jax.experimental import pallas as pl
from jax.experimental.pallas import tpu as pltpu
from jax.sharding import PartitionSpec as P

F32, BF16 = jnp.float32, jnp.bfloat16
BLK = 128
TN = 512
TC = 256
MESH = pl.DeviceIdType.MESH


def split_table(table):
    parts, rest = [], table.astype(np.float64)
    for _ in range(3):
        part = rest.astype(np.float32).astype(jnp.bfloat16)
        parts.append(part)
        rest = rest - part.astype(np.float64)
    return parts


def transform_tables():
    freq = np.concatenate([np.arange(0, BLK, 2), np.arange(1, BLK, 2)]) + 0.5
    angle = 2.0 * np.pi * freq[:, None] * np.arange(BLK)[None, :] / (2 * BLK)
    fwd = np.concatenate([np.cos(angle), -np.sin(angle)], 0)
    inv = np.concatenate([np.cos(angle).T, -np.sin(angle).T], 1) / BLK
    f1, f2, f3 = split_table(fwd)
    e1, e2, e3 = split_table(inv)
    fwd3 = np.concatenate([f1, f2, f3], 1)
    fwd6 = np.concatenate([f1, f1, f2, f2, f1, f3], 1)
    inv6 = np.concatenate([e1, e1, e2, e2, e1, e3], 1)
    return fwd3, fwd6, inv6


def dot(a, b):
    return jnp.dot(a, b, preferred_element_type=F32)


def split3(x):
    hi = x.astype(BF16)
    rest = x - hi.astype(F32)
    mid = rest.astype(BF16)
    low = (rest - mid.astype(F32)).astype(BF16)
    return hi, mid, low


def stack6(hi, mid, low):
    return jnp.concatenate([hi, mid, hi, mid, low, hi], axis=0)


def split_blocks(src, parts, first):
    for j in range(src.shape[0] // BLK):
        for i, a in enumerate(split3(src[j * BLK:(j + 1) * BLK])):
            parts[first + j, i] = a


def block_spectrum(fwd6_ref, parts, j):
    return dot(fwd6_ref[...], stack6(parts[j, 0], parts[j, 1], parts[j, 2]))


def shifted_add(cur, old, lo, sign):
    re, im = slice(lo, lo + BLK // 2), slice(BLK + lo, BLK + lo + BLK // 2)
    return re, im, cur[re] - sign * old[im], cur[im] + sign * old[re]


SIDES = ((0, 1.0), (BLK // 2, -1.0))


def short_conv(pbuf, t, first, rows):
    return (t[0:1] * pbuf[8 + first:8 + first + rows] + t[1:2] * pbuf[7 + first:7 + first + rows] + t[2:3] * pbuf[6 + first:6 + first + rows]).astype(BF16)


def block_values(fwd3_ref, blk):
    return dot(fwd3_ref[...], jnp.concatenate([blk, blk, blk], axis=0))


def main_body(fwd3_ref, fwd6_ref, inv6_ref, bias_ref, taps_ref, sk1_ref, sk2_ref, u_bf, u32, w_in, f1, f2,
              keep, part, qx, qv, vhat, far, u_sw, u_x, u_fw, tail, pf,
              land, ts, tr, os, orr, ws, wr, ss, sr, fs, fr, l_sem, x_send, x_recv, y_send, y_recv, p_send, p_recv):
    sp, dp = lax.axis_index("sp"), lax.axis_index("dp")
    c = lax.rem(sp, 2)
    on_b = sp >= 2
    on_a = jnp.logical_not(on_b)
    other = sp + 1 - 2 * c
    n_seq, n_pos, width = u_bf.shape
    half_w = width // 2
    nt, n_tile = half_w // TN, half_w // TC
    n_own, hp = 2 * n_pos, n_pos // 2
    nbo = n_own // BLK
    n_piece = 2 * n_seq

    def remote(src, dst, send, recv, peer):
        return pltpu.make_async_remote_copy(src, dst, send, recv, device_id=peer, device_id_type=MESH)

    def at(start, size):
        return pl.ds(pl.multiple_of(start, size), size)

    def piece(ref, s, h):
        return ref.at[s, h * hp:(h + 1) * hp]

    def tail_copy(k):
        return remote(u32.at[:, n_pos - 8:], tail, ts.at[k], tr.at[0], (dp, 2 + k))

    def over(s, h):
        return remote(piece(u32, s, h), piece(u_x, s, h), os.at[s, h], orr.at[s, h], (dp, lax.rem(sp + 2, 4)))

    def onward(s, h):
        return remote(piece(u_x, s, h), piece(u_fw, s, h), ws.at[s, h], wr.at[s, h], (dp, other))

    def swap_u(s):
        return remote(u32.at[s], u_sw.at[s], ss.at[s], sr.at[s], (dp, other))

    def swap_f(f):
        return remote((f1, f2)[f].at[:, at((1 - c) * half_w, half_w)], pf.at[f], fs.at[f], fr.at[f], (dp, other))

    def filt(src, u, k):
        return remote(src.at[:, at(k * half_w + u * TC, TC)], land.at[dp, u, c], x_send.at[u, k], x_recv.at[u, c], (dp, 2 + k))

    def landed(u, side):
        return remote(land.at[dp, u, side], land.at[dp, u, side], x_send.at[u, side], x_recv.at[u, side], (dp, sp))

    def across(u, side, f):
        return remote(land.at[f, u, side], land.at[f, u, side], y_send.at[u, side], y_recv.at[u, side], (1 - dp, sp))

    def fill(f, u, side, src, start):
        return pltpu.make_async_copy(src.at[:, at(start, TC)], land.at[f, u, side], l_sem.at[f, u, side])

    def column(g, j):
        return (g + j // nt) * width + c * half_w + lax.rem(j, nt) * TN

    def load_rows(stage, st_sem, n, src, dst_row):
        def copy(i):
            return pltpu.make_async_copy(src(i), stage.at[i % 2], st_sem.at[i % 2])

        copy(0).start()
        for i in range(n):
            if i + 1 < n:
                copy(i + 1).start()
            copy(i).wait()
            ref, row = dst_row(i)
            ref[pl.ds(pl.multiple_of(row, 16), hp), :] = stage[i % 2].astype(BF16)

    barrier = pltpu.get_barrier_semaphore()
    for peer in ((dp, other), (dp, lax.rem(sp + 2, 4)), (dp, lax.rem(other + 2, 4)), (1 - dp, sp)):
        pl.semaphore_signal(barrier, inc=1, device_id=peer, device_id_type=MESH)
    pl.semaphore_wait(barrier, 4)

    @pl.when(sp == 1)
    def _():
        for k in range(2):
            tail_copy(k).start()

    @pl.when(on_a)
    def _():
        for i in range(n_piece):
            over(*divmod(i, 2)).start()
        for which, src in ((0, f1), (1, f2)):
            @pl.when(dp == which)
            def _():
                for u in range(n_tile):
                    for k in range(2):
                        filt(src, u, k).start()

    for i in range(n_seq):
        swap_u(i).start()
    for f in range(2):
        swap_f(f).start()

    def forward(u):
        @pl.when(on_b)
        def _():
            for side in range(2):
                landed(u, side).wait_recv()
                across(u, side, dp).start()

    def front(wbuf, wsem, lhs, stage, st_sem, lhs_sem, tailbuf, q_st, q_sem, vh_st, vh_sem, pbuf):
        def weights(g, j, slot):
            rows = width // 4
            return [pltpu.make_async_copy(w_in.at[i * rows:(i + 1) * rows, at(column(g, j), TN)],
                                          wbuf.at[slot, i * rows:(i + 1) * rows], wsem.at[slot, i]) for i in range(4)]

        def stream(g, body, following, n=nt):
            def step(j, carry):
                slot = lax.rem(j, 2)

                @pl.when(j + 1 < n)
                def _():
                    for copy in weights(g, j + 1, 1 - slot):
                        copy.start()

                if following is not None:
                    @pl.when(j + 1 == n)
                    def _():
                        following(1 - slot)

                for copy in weights(g, j, slot):
                    copy.wait()
                body(j, slot, bias_ref[:, at(column(g, j), TN)], taps_ref[:, at(column(g, j), TN)])
                return carry

            lax.fori_loop(0, n, step, 0)

        def begin(g):
            def start(slot):
                for copy in weights(g, 0, slot):
                    copy.start()
            return start

        def project(rows_ref, slot, bias):
            return (dot(rows_ref, wbuf[slot]) + bias).astype(BF16).astype(F32)

        tail_rows = n_seq * 8
        begin(0)(0)
        own_rows = [pltpu.make_async_copy(u_bf.at[s], lhs.at[pl.ds(pl.multiple_of(tail_rows + s * n_own + c * n_pos, 16), n_pos)], lhs_sem.at[s])
                    for s in range(n_seq)]
        for copy in own_rows:
            copy.start()
        for s in range(n_seq):
            swap_u(s).wait_recv()
        load_rows(stage, st_sem, n_piece, lambda i: piece(u_sw, *divmod(i, 2)), lambda i: (lhs, tail_rows + (i // 2) * n_own + (1 - c) * n_pos + (i % 2) * hp))
        for copy in own_rows:
            copy.wait()

        @pl.when(on_b)
        def _():
            tail_copy(0).wait_recv()
            copy = pltpu.make_async_copy(tail, tailbuf, lhs_sem.at[0])
            copy.start()
            copy.wait()

        @pl.when(on_a)
        def _():
            tailbuf[...] = jnp.zeros_like(tailbuf)

        lhs[:tail_rows, :] = tailbuf[...].reshape(tail_rows, width).astype(BF16)
        chunk = n_pos

        def own_phase(g, n, dst, spectrum, following):
            def flush(j, slot):
                cols = at(lax.rem(j, nt) * TN, TN)
                blocks = pl.ds(nbo * (1 + j // nt), nbo)
                copies = [pltpu.make_async_copy(q_st.at[slot], dst.at[:, blocks, :, cols], q_sem.at[slot])]
                if spectrum:
                    copies.append(pltpu.make_async_copy(vh_st.at[slot], vhat.at[:, nbo:, :, cols], vh_sem.at[slot]))
                return copies

            def body(j, slot, bias, taps):
                @pl.when(j >= 2)
                def _():
                    for copy in flush(j - 2, slot):
                        copy.wait()

                for i in range(n_seq * n_own // chunk):
                    s, r = divmod(i * chunk, n_own)
                    p = project(lhs[(tail_rows + i * chunk if i else 0):tail_rows + (i + 1) * chunk, :], slot, bias)
                    if i == 0:
                        for k in range(n_seq):
                            pbuf[k, 0:8] = jnp.where(on_b, p[8 * k:8 * k + 8], 0.0)
                        p = p[tail_rows:]
                    pbuf[s, 8 + r:8 + r + chunk] = p
                    q = short_conv(pbuf.at[s], taps, r, chunk)
                    for b in range(chunk // BLK):
                        blk = q[b * BLK:(b + 1) * BLK]
                        q_st[slot, s, r // BLK + b] = blk
                        if spectrum:
                            vh_st[slot, s, r // BLK + b] = block_values(fwd3_ref, blk)
                for copy in flush(j, slot):
                    copy.start()

            stream(g, body, following, n)
            for j in (n - 2, n - 1):
                for copy in flush(j, j % 2):
                    copy.wait()

        own_phase(0, 2 * nt, qx, False, begin(2))
        own_phase(2, nt, qv, True, None)

        def far_phase(fin, fin_sem, fout, fout_sem, parts):
            hk = n_pos // BLK

            def fetch(j, slot):
                mine = at(c * half_w + j * TC, TC)
                srcs = (f1.at[:, mine], f2.at[:, mine], pf.at[0, :, at(j * TC, TC)], pf.at[1, :, at(j * TC, TC)])
                return [pltpu.make_async_copy(src, fin.at[slot, i], fin_sem.at[slot, i]) for i, src in enumerate(srcs)]

            def flush(j, slot):
                return pltpu.make_async_copy(fout.at[slot], far.at[:, :, :, at(j * TC, TC)], fout_sem.at[slot])

            for copy in fetch(0, 0):
                copy.start()

            def step(j, carry):
                slot = lax.rem(j, 2)

                @pl.when(j + 1 < n_tile)
                def _():
                    for copy in fetch(j + 1, 1 - slot):
                        copy.start()

                for copy in fetch(j, slot):
                    copy.wait()

                @pl.when(j >= 2)
                def _():
                    flush(j - 2, slot).wait()

                for f in range(2):
                    split_blocks(fin.at[slot, f], parts.at[f], c * hk)
                    split_blocks(fin.at[slot, 2 + f], parts.at[f], (1 - c) * hk)
                g_ref = fout.at[slot]
                for f in range(2):
                    for b in range(2 * hk):
                        g_ref[f, b] = block_spectrum(fwd6_ref, parts.at[f], b)
                    for b in range(2 * hk - 1, 0, -1):
                        for lo, sign in SIDES:
                            re, im, new_re, new_im = shifted_add(g_ref.at[f, b], g_ref.at[f, b - 1], lo, sign)
                            g_ref[f, b, re], g_ref[f, b, im] = new_re, new_im
                flush(j, slot).start()
                return carry

            lax.fori_loop(0, n_tile, step, 0)
            for j in (n_tile - 2, n_tile - 1):
                flush(j, j % 2).wait()

        for f in range(2):
            swap_f(f).wait_recv()
        pl.run_scoped(
            far_phase, pltpu.VMEM((2, 4, n_pos, TC), F32), pltpu.SemaphoreType.DMA((2, 4)),
            pltpu.VMEM((2, 2, nbo, 2 * BLK, TC), F32), pltpu.SemaphoreType.DMA((2,)), pltpu.VMEM((2, nbo, 3, BLK, TC), BF16))

    pl.run_scoped(
        front,
        pltpu.VMEM((2, width, TN), BF16), pltpu.SemaphoreType.DMA((2, 4)),
        pltpu.VMEM((n_seq * n_own + 8 * n_seq, width), BF16),
        pltpu.VMEM((2, hp, width), F32), pltpu.SemaphoreType.DMA((2,)), pltpu.SemaphoreType.DMA((n_seq,)), pltpu.VMEM((n_seq, 8, width), F32),
        pltpu.VMEM((2, n_seq, nbo, BLK, TN), BF16), pltpu.SemaphoreType.DMA((2,)),
        pltpu.VMEM((2, n_seq, nbo, 2 * BLK, TN), F32), pltpu.SemaphoreType.DMA((2,)),
        pltpu.VMEM((n_seq, n_own + 8, TN), F32))

    def prev(wres, w_sem, lhs_p, stage, st_sem, q_st, q_sem, vh_st, vh_sem, pbuf, pstash):
        groups = ((0, 0, qx, False), (nt, 2, qv, True))

        def weights(base, g, j):
            rows = width // 4
            return [pltpu.make_async_copy(w_in.at[i * rows:(i + 1) * rows, at(column(g, j), TN)],
                                          wres.at[base + j, i * rows:(i + 1) * rows], w_sem.at[base + j, i]) for i in range(4)]

        for base, g, _, _ in groups:
            for j in range(nt):
                for copy in weights(base, g, j):
                    copy.start()

        def rows(s, h):
            @pl.when(on_b)
            def _():
                over(s, h).wait_recv()
                onward(s, h).start()
                load_rows(stage, st_sem, 1, lambda _: piece(u_x, s, h), lambda _: (lhs_p, c * hp))
                onward(s, h).wait_recv()
                load_rows(stage, st_sem, 1, lambda _: piece(u_fw, s, h), lambda _: (lhs_p, (1 - c) * hp))

            @pl.when(on_a)
            def _():
                lhs_p[...] = jnp.zeros_like(lhs_p)

        def project(base, g, j):
            return (dot(lhs_p[...], wres[base + j]) + bias_ref[:, at(column(g, j), TN)]).astype(BF16)

        def first(s, base, g):
            def body(j, carry):
                @pl.when(s == 0)
                def _():
                    for copy in weights(base, g, j):
                        copy.wait()

                pstash[:, at((base + j) * TN, TN)] = project(base, g, j)
                return carry

            lax.fori_loop(0, nt, body, 0)

        def second(s, base, g, dst, spectrum):
            def flush(j):
                slot, cols = lax.rem(j, 2), at(j * TN, TN)
                copies = [pltpu.make_async_copy(q_st.at[slot], dst.at[s, :nbo, :, cols], q_sem.at[slot])]
                if spectrum:
                    copies.append(pltpu.make_async_copy(vh_st.at[slot], vhat.at[s, :nbo, :, cols], vh_sem.at[slot]))
                return copies

            def body(j, carry):
                slot = lax.rem(j, 2)

                @pl.when(j >= 2)
                def _():
                    for copy in flush(j - 2):
                        copy.wait()

                taps = taps_ref[:, at(column(g, j), TN)]
                old = pstash[:, at((base + j) * TN, TN)].astype(F32)
                pbuf[0:8] = jnp.zeros((8, TN), F32)
                p = project(base, g, j).astype(F32)
                for core in range(2):
                    for h, part_rows in enumerate((old, p)):
                        start = 8 + (2 * core + h) * hp
                        pbuf[start:start + hp] = jnp.where(on_b, part_rows[core * hp:(core + 1) * hp], 0.0)
                for b in range(nbo):
                    blk = short_conv(pbuf, taps, b * BLK, BLK)
                    q_st[slot, b] = blk
                    if spectrum:
                        vh_st[slot, b] = block_values(fwd3_ref, blk)
                for copy in flush(j):
                    copy.start()
                return carry

            lax.fori_loop(0, nt, body, 0)
            for j in (nt - 2, nt - 1):
                for copy in flush(j):
                    copy.wait()

        def one_seq(s, carry):
            rows(s, 0)
            for base, g, _, _ in groups:
                first(s, base, g)
            rows(s, 1)
            second(s, *groups[0])

            @pl.when(s + 1 == n_seq)
            def _():
                forward(0)

            second(s, *groups[1])
            return carry

        lax.fori_loop(0, n_seq, one_seq, 0)

    pl.run_scoped(
        prev,
        pltpu.VMEM((2 * nt, width, TN), BF16), pltpu.SemaphoreType.DMA((2 * nt, 4)),
        pltpu.VMEM((2 * hp, width), BF16), pltpu.VMEM((2, hp, width), F32), pltpu.SemaphoreType.DMA((2,)),
        pltpu.VMEM((2, nbo, BLK, TN), BF16), pltpu.SemaphoreType.DMA((2,)),
        pltpu.VMEM((2, nbo, 2 * BLK, TN), F32), pltpu.SemaphoreType.DMA((2,)),
        pltpu.VMEM((n_own + 8, TN), F32), pltpu.VMEM((2 * hp, 2 * half_w), BF16))

    @pl.when(on_a)
    def _():
        for u in range(n_tile):
            for f, own in enumerate((f1, f2)):
                fill(f, u, c, own, c * half_w + u * TC).start()
                fill(f, u, 1 - c, pf.at[f], u * TC).start()

    def conv(x1b, vb, x2b, vhb, farb, in_sem, vh_sem, kst, k_sem, sendbuf, *scratch):
        def fetch(t):
            cols, slot = at(t * TC, TC), lax.rem(t, 3)
            srcs = (qx.at[:, :2 * nbo], qv, qx.at[:, 2 * nbo:], far)
            copies = [pltpu.make_async_copy(r.at[:, :, :, cols], b.at[slot], in_sem.at[slot, i])
                      for i, (r, b) in enumerate(zip(srcs, (x1b, vb, x2b, farb)))]
            two = lax.rem(t, 2)
            return copies + [pltpu.make_async_copy(vhat.at[s, :, :, cols], vhb.at[two, s], vh_sem.at[two, s]) for s in range(n_seq)]

        def flush(t):
            slot = lax.rem(t, 2)
            return pltpu.make_async_copy(kst.at[slot], keep.at[:, :, at(t * TC, TC)], k_sem.at[slot])

        def swap_y(u):
            return remote(sendbuf.at[lax.rem(u, 2)], part.at[:, :, at(u * TC, TC)], p_send.at[u], p_recv.at[u], (dp, other))

        tile = ConvTile(fwd6_ref, inv6_ref, *scratch)

        def inputs(t, back):
            slot, cols = lax.rem(t + 3 - back, 3), at(c * half_w + lax.rem(t + n_tile - back, n_tile) * TC, TC)
            return x1b.at[slot], vb.at[slot], x2b.at[slot], farb.at[slot], sk1_ref[:, cols], sk2_ref[:, cols]

        def emit(t):
            slot = lax.rem(t, 2)

            @pl.when(t >= 2)
            def _():
                flush(t - 2).wait()
                swap_y(t - 2).wait_send()

            tile.result(c, kst.at[slot], sendbuf.at[slot])
            flush(t).start()
            swap_y(t).start()

        for copy in fetch(0):
            copy.start()
        forward(1)

        def step(t, carry):
            @pl.when(t + 1 < n_tile)
            def _():
                for copy in fetch(t + 1):
                    copy.start()

            @pl.when(on_a)
            def _():
                for f in range(2):
                    for side in range(2):
                        fill(f, t, side, f1, 0).wait()

            @pl.when(on_b)
            def _():
                for side in range(2):
                    across(t, side, 1 - dp).wait_recv()

            for copy in fetch(t):
                copy.wait()

            tile.step(land, t, vhb.at[lax.rem(t, 2)], inputs(t, 0), inputs(t, 1))

            @pl.when(t + 2 < n_tile)
            def _():
                forward(t + 2)

            @pl.when(t >= 1)
            def _():
                emit(t - 1)
            return carry

        lax.fori_loop(0, n_tile, step, 0)
        tile.drain(inputs(n_tile, 1))
        emit(n_tile - 1)
        for u in (n_tile - 2, n_tile - 1):
            flush(u).wait()
            swap_y(u).wait_send()
        for u in range(n_tile):
            swap_y(u).wait_recv()

    nb = 2 * nbo
    pl.run_scoped(
        conv,
        pltpu.VMEM((3, n_seq, nb, BLK, TC), BF16), pltpu.VMEM((3, n_seq, nb, BLK, TC), BF16), pltpu.VMEM((3, n_seq, nbo, BLK, TC), BF16),
        pltpu.VMEM((2, n_seq, nb, 2 * BLK, TC), F32), pltpu.VMEM((3, 2, nbo, 2 * BLK, TC), F32),
        pltpu.SemaphoreType.DMA((3, 4)), pltpu.SemaphoreType.DMA((2, n_seq)),
        pltpu.VMEM((2, n_seq, n_pos, TC), BF16), pltpu.SemaphoreType.DMA((2,)), pltpu.VMEM((2, n_seq, n_pos, TC), F32),
        pltpu.VMEM((2, nbo, 3, BLK, TC), BF16),
        pltpu.VMEM((nbo + 1, 2 * BLK, TC), F32), pltpu.VMEM((nbo + 1, 2 * BLK, TC), F32), pltpu.VMEM((nbo, 2 * BLK, TC), F32),
        *[pltpu.VMEM((nb, 3, 2 * BLK, TC), BF16)] * n_seq,
        pltpu.VMEM((nb, 3, BLK, TC), BF16),
        *[pltpu.VMEM((nb, BLK, TC), F32)] * n_seq,
        pltpu.VMEM((nb, 2 * BLK, TC), F32),
        *[pltpu.VMEM((nbo, 3, 2 * BLK, TC), BF16)] * n_seq,
        pltpu.VMEM((n_seq, nbo, BLK, TC), BF16))

    for s in range(n_seq):
        swap_u(s).wait_send()
    for f in range(2):
        swap_f(f).wait_send()

    @pl.when(sp == 1)
    def _():
        for k in range(2):
            tail_copy(k).wait_send()

    @pl.when(on_a)
    def _():
        for i in range(n_piece):
            over(*divmod(i, 2)).wait_send()
        for u in range(n_tile):
            for k in range(2):
                filt(f1, u, k).wait_send()

    @pl.when(on_b)
    def _():
        for i in range(n_piece):
            onward(*divmod(i, 2)).wait_send()
        for u in range(n_tile):
            for side in range(2):
                across(u, side, dp).wait_send()


def loop(trips):
    def run(body):
        def step(i, carry):
            body(i)
            return carry
        lax.fori_loop(0, trips, step, 0)
    return run


class ConvTile:
    def __init__(self, fwd6, inv6, hparts, g1, g2, raw2, sp0, sp1, zparts, zv0, zv1, zhat, sq0, sq1, ybuf):
        self.fwd6, self.inv6, self.hparts, self.g, self.raw2 = fwd6, inv6, hparts, (g1, g2), raw2
        self.first, self.second, self.zparts, self.zval, self.zhat, self.ybuf = (sp0, sp1), (sq0, sq1), zparts, (zv0, zv1), zhat, ybuf
        self.nb, self.nbo = sp0.shape[0], sq0.shape[0]

    def near(self, land, t, f):
        for side in range(2):
            split_blocks(land.at[f, t, side], self.hparts.at[f], side * self.nbo // 2)

    def window(self, f, raw, far):
        g, nbo = self.g[f], self.nbo
        for j in range(nbo, 0, -1):
            cur = far.at[f, 0] if j == nbo else raw.at[j]
            for lo, sign in SIDES:
                re, im, new_re, new_im = shifted_add(cur, raw.at[j - 1], lo, sign)
                g[j, re], g[j, im] = new_re, new_im
        if raw is not g:
            g[0] = raw[0]

    def pointwise(self, xhat, f, far, dst, r, first):
        g, nbo = self.g[f], self.nbo
        re, im = pl.ds(pl.multiple_of(r * 16, 16), 16), pl.ds(pl.multiple_of(BLK + r * 16, 16), 16)
        for k in range(first, self.nb):
            acc_re = acc_im = None
            for j in range(k + 1):
                i = k - j
                gr, gi = (g[i, re], g[i, im]) if i <= nbo else (far[f, i - nbo, re], far[f, i - nbo, im])
                xr, xi = xhat[j, re], xhat[j, im]
                t_re, t_im = xr * gr - xi * gi, xr * gi + xi * gr
                acc_re = t_re if acc_re is None else acc_re + t_re
                acc_im = t_im if acc_im is None else acc_im + t_im
            for part, (a, b) in enumerate(zip(split3(acc_re), split3(acc_im))):
                dst[k - first, part, re], dst[k - first, part, im] = a, b

    def inverse(self, parts, k):
        return dot(self.inv6[...], stack6(parts[k, 0], parts[k, 1], parts[k, 2]))

    def gate_one(self, s, k, data):
        x1, v, _, _, skip, _ = data
        z = x1[s, k].astype(F32) * (self.inverse(self.first[s], k) + skip * v[s, k].astype(F32))
        self.zval[s][k] = z
        for part, a in enumerate(split3(z)):
            self.zparts[k, part] = a

    def spectrum(self, k):
        self.zhat[k] = block_spectrum(self.fwd6, self.zparts, k)

    def gate_two(self, s, k, data):
        y = data[2][s, k].astype(F32) * (self.inverse(self.second[s], k) + data[5] * self.zval[s][self.nbo + k])
        self.ybuf[s, k] = y.astype(BF16)

    def middle(self, s, data, i, point=None):
        for q in range(4):
            if point is not None:
                point(4 * i + q)
            for k in range(2):
                if q < 2:
                    self.gate_one(s, 4 * i + 2 * q + k, data)
                else:
                    self.spectrum(4 * i + 2 * (q - 2) + k)

    def step(self, land, t, vhat, data, old):
        nb, nbo = self.nb, self.nbo
        far = data[3]
        self.near(land, t, 0)
        for j in range(nbo):
            self.g[0][j] = block_spectrum(self.fwd6, self.hparts.at[0], j)
        self.near(land, t, 1)
        self.window(0, self.g[0], far)

        @loop(nb // 4)
        def _(i):
            self.middle(1, old, i, lambda r: self.pointwise(vhat.at[0], 0, far, self.first[0], r, 0))

        @loop(nbo // 2)
        def _(i):
            for q in range(4):
                self.pointwise(self.zhat, 1, old[3], self.second[1], 4 * i + q, nbo)
                if q < 2:
                    self.gate_two(0, 2 * i + q, old)
                else:
                    j = 2 * i + q - 2
                    self.raw2[j] = block_spectrum(self.fwd6, self.hparts.at[1], j)

        self.window(1, self.raw2, far)

        @loop(nb // 4)
        def _(i):
            self.middle(0, data, i, lambda r: self.pointwise(vhat.at[1], 0, far, self.first[1], r, 0))

        @loop(nbo // 2)
        def _(i):
            for q in range(4):
                self.pointwise(self.zhat, 1, far, self.second[0], 4 * i + q, nbo)
                if q % 2 == 0:
                    self.gate_two(1, 2 * i + q // 2, old)

    def drain(self, data):
        nb, nbo = self.nb, self.nbo

        @loop(nb // 4)
        def _(i):
            self.middle(1, data, i)

        @loop(nbo // 2)
        def _(i):
            for q in range(4):
                self.pointwise(self.zhat, 1, data[3], self.second[1], 4 * i + q, nbo)
                if q % 2 == 0:
                    self.gate_two(0, 2 * i + q // 2, data)

        for k in range(nbo):
            self.gate_two(1, k, data)

    def result(self, c, keep, send):
        hk = self.nbo // 2
        for s in range(self.ybuf.shape[0]):
            for b in range(hk):
                keep[s, b * BLK:(b + 1) * BLK] = self.ybuf[s, c * hk + b]
                send[s, b * BLK:(b + 1) * BLK] = self.ybuf[s, (1 - c) * hk + b].astype(F32)


def out_body(keep, part, w_out, u_in, out, wbuf, w_sem, lhs, keep_v, stage, in_sem, u_v, o_st, o_sem):
    c = lax.rem(lax.axis_index("sp"), 2)
    n_seq, n_pos, half_w = keep.shape
    width = 2 * half_w
    n_col, rows = width // TN, width // 4

    def weights(j, slot):
        return [pltpu.make_async_copy(w_out.at[i * rows:(i + 1) * rows, pl.ds(pl.multiple_of(j * TN, TN), TN)],
                                      wbuf.at[slot, i * rows:(i + 1) * rows], w_sem.at[slot, i]) for i in range(4)]

    def flush(j):
        slot = lax.rem(j, 2)
        return pltpu.make_async_copy(o_st.at[slot], out.at[:, :, pl.ds(pl.multiple_of(j * TN, TN), TN)], o_sem.at[slot])

    loads = [pltpu.make_async_copy(part.at[s], stage.at[s], in_sem.at[s]) for s in range(n_seq)]
    loads += [pltpu.make_async_copy(keep.at[s], keep_v.at[s], in_sem.at[n_seq + s]) for s in range(n_seq)]
    for copy in loads:
        copy.start()
    for copy in weights(0, 0):
        copy.start()
    resid = pltpu.make_async_copy(u_in, u_v, in_sem.at[2 * n_seq])
    resid.start()
    mine, theirs = (pl.ds(pl.multiple_of(k * half_w, half_w), half_w) for k in (c, 1 - c))
    for s in range(n_seq):
        loads[s].wait()
        lhs[s, :, theirs] = stage[s].astype(BF16)
    for s in range(n_seq):
        loads[n_seq + s].wait()
        lhs[s, :, mine] = keep_v[s]
    resid.wait()

    def step(j, carry):
        slot = lax.rem(j, 2)

        @pl.when(j + 1 < n_col)
        def _():
            for copy in weights(j + 1, 1 - slot):
                copy.start()

        for copy in weights(j, slot):
            copy.wait()

        @pl.when(j >= 2)
        def _():
            flush(j - 2).wait()

        cols = pl.ds(pl.multiple_of(j * TN, TN), TN)
        for s in range(n_seq):
            o_st[slot, s] = (u_v[s, :, cols].astype(F32) + dot(lhs[s], wbuf[slot])).astype(BF16)
        flush(j).start()
        return carry

    lax.fori_loop(0, n_col, step, 0)
    for j in (n_col - 2, n_col - 1):
        flush(j).wait()


def solution(mesh):
    fwd3, fwd6, inv6 = transform_tables()

    def local_step(u_in, w_in, b_in, conv_taps, w_out, skip_one, skip_two, filt_one, filt_two):
        n_seq, n_pos, width = u_in.shape
        half_w = width // 2
        n_own = 2 * n_pos
        nb = 2 * n_own // BLK
        nbo = nb // 2
        n_tile = half_w // TC
        small, large = pl.BlockSpec(memory_space=pltpu.VMEM), pl.BlockSpec(memory_space=pl.ANY)
        dma = pltpu.SemaphoreType.DMA

        def shape(dims, dtype=F32):
            return jax.ShapeDtypeStruct(dims, dtype)

        keep, part, *_ = pl.pallas_call(
            main_body,
            in_specs=[small] * 7 + [large] * 5,
            out_specs=[large] * 11,
            out_shape=[
                shape((n_seq, n_pos, half_w), BF16), shape((n_seq, n_pos, half_w)),
                shape((n_seq, nb + nbo, BLK, half_w), BF16), shape((n_seq, nb, BLK, half_w), BF16),
                shape((n_seq, nb, 2 * BLK, half_w)), shape((2, nbo, 2 * BLK, half_w)),
                shape((n_seq, n_pos, width)), shape((n_seq, n_pos, width)), shape((n_seq, n_pos, width)),
                shape((n_seq, 8, width)), shape((2, n_pos, half_w)),
            ],
            scratch_shapes=[
                pltpu.VMEM((2, n_tile, 2, n_pos, TC), F32),
                dma((2,)), dma((1,)), *[dma((n_seq, 2))] * 4, *[dma((n_seq,))] * 2, *[dma((2,))] * 2,
                dma((2, n_tile, 2)), *[dma((n_tile, 2))] * 4, *[dma((n_tile,))] * 2,
            ],
            compiler_params=pltpu.CompilerParams(vmem_limit_bytes=62 << 20, collective_id=0, has_side_effects=True),
            name="hyena_main",
        )(fwd3, fwd6, inv6, b_in.reshape(1, -1), conv_taps, skip_one.reshape(1, -1), skip_two.reshape(1, -1),
          u_in, u_in.astype(F32), w_in, filt_one, filt_two)

        return pl.pallas_call(
            out_body,
            in_specs=[large] * 4,
            out_specs=large,
            out_shape=shape((n_seq, n_pos, width), BF16),
            scratch_shapes=[
                pltpu.VMEM((2, width, TN), BF16), dma((2, 4)),
                pltpu.VMEM((n_seq, n_pos, width), BF16), pltpu.VMEM((n_seq, n_pos, half_w), BF16), pltpu.VMEM((n_seq, n_pos, half_w), F32),
                dma((2 * n_seq + 1,)), pltpu.VMEM((n_seq, n_pos, width), BF16), pltpu.VMEM((2, n_seq, n_pos, TN), BF16), dma((2,)),
            ],
            compiler_params=pltpu.CompilerParams(vmem_limit_bytes=60 << 20),
            name="out_proj",
        )(keep, part, w_out, u_in)

    seq_spec = P("dp", "sp", None)
    filt_spec = P("sp", None)
    return jax.shard_map(local_step, mesh=mesh, in_specs=(seq_spec, P(), P(), P(), P(), P(), P(), filt_spec, filt_spec), out_specs=seq_spec, check_vma=False)
```

```python
import functools

import jax
import jax.numpy as jnp
import numpy as np
from jax import lax
from jax.experimental import pallas as pl
from jax.experimental.pallas import tpu as pltpu
from jax.sharding import PartitionSpec as P

F32, BF16 = jnp.float32, jnp.bfloat16
BLK = 128
TN = 512
TC = 256
Q = 4
MESH = pl.DeviceIdType.MESH


def split_table(table):
    parts, rest = [], table.astype(np.float64)
    for _ in range(3):
        part = rest.astype(np.float32).astype(jnp.bfloat16)
        parts.append(part)
        rest = rest - part.astype(np.float64)
    return parts


def transform_tables():
    freq = np.concatenate([np.arange(0, BLK, 2), np.arange(1, BLK, 2)]) + 0.5
    angle = 2.0 * np.pi * freq[:, None] * np.arange(BLK)[None, :] / (2 * BLK)
    fwd = np.concatenate([np.cos(angle), -np.sin(angle)], 0)
    inv = np.concatenate([np.cos(angle).T, -np.sin(angle).T], 1) / BLK
    f1, f2, f3 = split_table(fwd)
    e1, e2, e3 = split_table(inv)
    fwd3 = np.concatenate([f1, f2, f3], 1)
    fwd6 = np.concatenate([f1, f1, f2, f2, f1, f3], 1)
    inv6 = np.concatenate([e1, e1, e2, e2, e1, e3], 1)
    return fwd3, fwd6, inv6


def dot(a, b):
    return jnp.dot(a, b, preferred_element_type=F32)


def split3(x):
    hi = x.astype(BF16)
    rest = x - hi.astype(F32)
    mid = rest.astype(BF16)
    low = (rest - mid.astype(F32)).astype(BF16)
    return hi, mid, low


def stack6(hi, mid, low):
    return jnp.concatenate([hi, mid, hi, mid, low, hi], axis=0)


def split_blocks(src, parts, first):
    for j in range(src.shape[0] // BLK):
        for i, a in enumerate(split3(src[j * BLK:(j + 1) * BLK])):
            parts[first + j, i] = a


def block_spectrum(fwd6_ref, parts, j):
    return dot(fwd6_ref[...], stack6(parts[j, 0], parts[j, 1], parts[j, 2]))


def shifted_add(cur, old, lo, sign):
    re, im = slice(lo, lo + BLK // 2), slice(BLK + lo, BLK + lo + BLK // 2)
    return re, im, cur[re] - sign * old[im], cur[im] + sign * old[re]


SIDES = ((0, 1.0), (BLK // 2, -1.0))


def short_conv(pbuf, t, first, rows):
    return (t[0:1] * pbuf[8 + first:8 + first + rows] + t[1:2] * pbuf[7 + first:7 + first + rows] + t[2:3] * pbuf[6 + first:6 + first + rows]).astype(BF16)


def block_values(fwd3_ref, blk):
    return dot(fwd3_ref[...], jnp.concatenate([blk, blk, blk], axis=0))


def main_body(fwd3_ref, fwd6_ref, inv6_ref, bias_ref, taps_ref, sk1_ref, sk2_ref, u_bf, u32, w_in, f1, f2,
              keep, part, qx, qv, vhat, far, u_sw, u_x, u_fw, tail, pf,
              land, ts, tr, os, orr, ws, wr, ss, sr, fs, fr, l_sem, x_send, x_recv, y_send, y_recv, p_send, p_recv):
    sp, dp = lax.axis_index("sp"), lax.axis_index("dp")
    c = lax.rem(sp, 2)
    on_b = sp >= 2
    on_a = jnp.logical_not(on_b)
    other = sp + 1 - 2 * c
    n_seq, n_pos, width = u_bf.shape
    half_w = width // 2
    nt, n_tile, per = half_w // TN, half_w // TC, TN // TC
    n_own, hp = 2 * n_pos, n_pos // 2
    nbo = n_own // BLK
    cuts = (0, n_pos // 2, 3 * n_pos // 4, n_pos)
    n_cut = len(cuts) - 1

    def remote(src, dst, send, recv, peer):
        return pltpu.make_async_remote_copy(src, dst, send, recv, device_id=peer, device_id_type=MESH)

    def at(start, size):
        return pl.ds(pl.multiple_of(start, size), size)

    def piece(ref, s, h):
        return ref.at[s, cuts[h]:cuts[h + 1]]

    def tail_copy(k):
        return remote(u32.at[:, n_pos - 8:], tail, ts.at[k], tr.at[0], (dp, 2 + k))

    def over(s, h):
        return remote(piece(u32, s, h), piece(u_x, s, h), os.at[s, h], orr.at[s, h], (dp, lax.rem(sp + 2, 4)))

    def onward(s, h):
        return remote(piece(u_x, s, h), piece(u_fw, s, h), ws.at[s, h], wr.at[s, h], (dp, other))

    def swap_u(s):
        return remote(u32.at[s], u_sw.at[s], ss.at[s], sr.at[s], (dp, other))

    def swap_f(f):
        return remote((f1, f2)[f].at[:, at((1 - c) * half_w, half_w)], pf.at[f], fs.at[f], fr.at[f], (dp, other))

    qr = n_pos // Q

    def filt(src, u, k, q):
        return remote(src.at[q * qr:(q + 1) * qr, at(k * half_w + u * TC, TC)], land.at[dp, u, c, q * qr:(q + 1) * qr],
                      x_send.at[u, q, k], x_recv.at[u, q, c], (dp, 2 + k))

    def landed(u, side, q):
        ref = land.at[dp, u, side, q * qr:(q + 1) * qr]
        return remote(ref, ref, x_send.at[u, q, side], x_recv.at[u, q, side], (dp, sp))

    def across(u, side, f, q):
        ref = land.at[f, u, side, q * qr:(q + 1) * qr]
        return remote(ref, ref, y_send.at[u, q, side], y_recv.at[u, q, side], (1 - dp, sp))

    def fill(f, u, side, src, start):
        return pltpu.make_async_copy(src.at[:, at(start, TC)], land.at[f, u, side], l_sem.at[f, u, side])

    def column(g, j):
        return (g + j // nt) * width + c * half_w + lax.rem(j, nt) * TN

    def load_rows(stage, st_sem, items):
        def copy(i):
            src, rows, _, _ = items[i]
            return pltpu.make_async_copy(src, stage.at[i % 2, :rows], st_sem.at[i % 2])

        copy(0).start()
        for i, (_, rows, dst, row) in enumerate(items):
            if i + 1 < len(items):
                copy(i + 1).start()
            copy(i).wait()
            dst[pl.ds(pl.multiple_of(row, 16), rows), :] = stage[i % 2, :rows].astype(BF16)

    barrier = pltpu.get_barrier_semaphore()
    for peer in ((dp, other), (dp, lax.rem(sp + 2, 4)), (dp, lax.rem(other + 2, 4)), (1 - dp, sp)):
        pl.semaphore_signal(barrier, inc=1, device_id=peer, device_id_type=MESH)
    pl.semaphore_wait(barrier, 4)

    @pl.when(sp == 1)
    def _():
        for k in range(2):
            tail_copy(k).start()

    @pl.when(on_a)
    def _():
        for i in range(n_seq * n_cut):
            over(*divmod(i, n_cut)).start()
        for which, src in ((0, f1), (1, f2)):
            @pl.when(dp == which)
            def _():
                for u in range(n_tile):
                    for q in range(Q):
                        for k in range(2):
                            filt(src, u, k, q).start()

    for i in range(n_seq):
        swap_u(i).start()
    for f in range(2):
        swap_f(f).start()

    def forward(u, quarters):
        @pl.when(on_b)
        def _():
            for q in quarters:
                for side in range(2):
                    landed(u, side, q).wait_recv()
                    across(u, side, dp, q).start()

    def front(wbuf, wsem, lhs, stage, st_sem, lhs_sem, tailbuf, q_st, q_sem, vh_st, vh_sem, pbuf):
        def weights(g, j, slot):
            rows = width // 4
            return [pltpu.make_async_copy(w_in.at[i * rows:(i + 1) * rows, at(column(g, j), TN)],
                                          wbuf.at[slot, i * rows:(i + 1) * rows], wsem.at[slot, i]) for i in range(4)]

        def stream(g, body, following, n=nt):
            def step(j, carry):
                slot = lax.rem(j, 2)

                @pl.when(j + 1 < n)
                def _():
                    for copy in weights(g, j + 1, 1 - slot):
                        copy.start()

                if following is not None:
                    @pl.when(j + 1 == n)
                    def _():
                        following(1 - slot)

                for copy in weights(g, j, slot):
                    copy.wait()
                body(j, slot, bias_ref[:, at(column(g, j), TN)], taps_ref[:, at(column(g, j), TN)])
                return carry

            lax.fori_loop(0, n, step, 0)

        def begin(g):
            def start(slot):
                for copy in weights(g, 0, slot):
                    copy.start()
            return start

        def project(rows_ref, slot, bias):
            return (dot(rows_ref, wbuf[slot]) + bias).astype(BF16).astype(F32)

        tail_rows = n_seq * 8
        begin(0)(0)
        own_rows = [pltpu.make_async_copy(u_bf.at[s], lhs.at[pl.ds(pl.multiple_of(tail_rows + s * n_own + c * n_pos, 16), n_pos)], lhs_sem.at[s])
                    for s in range(n_seq)]
        for copy in own_rows:
            copy.start()
        for s in range(n_seq):
            swap_u(s).wait_recv()
        load_rows(stage, st_sem, [(u_sw.at[s, h * hp:(h + 1) * hp], hp, lhs, tail_rows + s * n_own + (1 - c) * n_pos + h * hp)
                                  for s in range(n_seq) for h in range(2)])
        for copy in own_rows:
            copy.wait()

        @pl.when(on_b)
        def _():
            tail_copy(0).wait_recv()
            copy = pltpu.make_async_copy(tail, tailbuf, lhs_sem.at[0])
            copy.start()
            copy.wait()

        @pl.when(on_a)
        def _():
            tailbuf[...] = jnp.zeros_like(tailbuf)

        lhs[:tail_rows, :] = tailbuf[...].reshape(tail_rows, width).astype(BF16)
        chunk = n_pos

        def own_phase(g, n, dst, spectrum, following):
            def flush(j, slot):
                blocks = pl.ds(nbo * (1 + j // nt), nbo)
                copies = []
                for h in range(per):
                    u = lax.rem(j, nt) * per + h
                    copies.append(pltpu.make_async_copy(q_st.at[slot, h], dst.at[u, :, blocks], q_sem.at[slot, h]))
                    if spectrum:
                        copies.append(pltpu.make_async_copy(vh_st.at[slot, h], vhat.at[u, :, nbo:], vh_sem.at[slot, h]))
                return copies

            def body(j, slot, bias, taps):
                @pl.when(j >= 2)
                def _():
                    for copy in flush(j - 2, slot):
                        copy.wait()

                for i in range(n_seq * n_own // chunk):
                    s, r = divmod(i * chunk, n_own)
                    p = project(lhs[(tail_rows + i * chunk if i else 0):tail_rows + (i + 1) * chunk, :], slot, bias)
                    if i == 0:
                        for k in range(n_seq):
                            pbuf[k, 0:8] = jnp.where(on_b, p[8 * k:8 * k + 8], 0.0)
                        p = p[tail_rows:]
                    pbuf[s, 8 + r:8 + r + chunk] = p
                    q = short_conv(pbuf.at[s], taps, r, chunk)
                    for b in range(chunk // BLK):
                        blk = q[b * BLK:(b + 1) * BLK]
                        for h in range(per):
                            q_st[slot, h, s, r // BLK + b] = blk[:, h * TC:(h + 1) * TC]
                        if spectrum:
                            spec = block_values(fwd3_ref, blk)
                            for h in range(per):
                                vh_st[slot, h, s, r // BLK + b] = spec[:, h * TC:(h + 1) * TC]
                for copy in flush(j, slot):
                    copy.start()

            stream(g, body, following, n)
            for j in (n - 2, n - 1):
                for copy in flush(j, j % 2):
                    copy.wait()

        own_phase(0, 2 * nt, qx, False, begin(2))
        own_phase(2, nt, qv, True, None)

        def far_phase(fin, fin_sem, fout, fout_sem, parts):
            hk = n_pos // BLK

            def fetch(j, slot):
                mine = at(c * half_w + j * TC, TC)
                srcs = (f1.at[:, mine], f2.at[:, mine], pf.at[0, :, at(j * TC, TC)], pf.at[1, :, at(j * TC, TC)])
                return [pltpu.make_async_copy(src, fin.at[slot, i], fin_sem.at[slot, i]) for i, src in enumerate(srcs)]

            def flush(j, slot):
                return pltpu.make_async_copy(fout.at[slot], far.at[j], fout_sem.at[slot])

            for copy in fetch(0, 0):
                copy.start()

            def step(j, carry):
                slot = lax.rem(j, 2)

                @pl.when(j + 1 < n_tile)
                def _():
                    for copy in fetch(j + 1, 1 - slot):
                        copy.start()

                for copy in fetch(j, slot):
                    copy.wait()

                @pl.when(j >= 2)
                def _():
                    flush(j - 2, slot).wait()

                for f in range(2):
                    split_blocks(fin.at[slot, f], parts.at[f], c * hk)
                    split_blocks(fin.at[slot, 2 + f], parts.at[f], (1 - c) * hk)
                g_ref = fout.at[slot]
                for f in range(2):
                    for b in range(2 * hk):
                        g_ref[f, b] = block_spectrum(fwd6_ref, parts.at[f], b)
                    for b in range(2 * hk - 1, 0, -1):
                        for lo, sign in SIDES:
                            re, im, new_re, new_im = shifted_add(g_ref.at[f, b], g_ref.at[f, b - 1], lo, sign)
                            g_ref[f, b, re], g_ref[f, b, im] = new_re, new_im
                flush(j, slot).start()
                return carry

            lax.fori_loop(0, n_tile, step, 0)
            for j in (n_tile - 2, n_tile - 1):
                flush(j, j % 2).wait()

        for f in range(2):
            swap_f(f).wait_recv()
        pl.run_scoped(
            far_phase, pltpu.VMEM((2, 4, n_pos, TC), F32), pltpu.SemaphoreType.DMA((2, 4)),
            pltpu.VMEM((2, 2, nbo, 2 * BLK, TC), F32), pltpu.SemaphoreType.DMA((2,)), pltpu.VMEM((2, nbo, 3, BLK, TC), BF16))

    pl.run_scoped(
        front,
        pltpu.VMEM((2, width, TN), BF16), pltpu.SemaphoreType.DMA((2, 4)),
        pltpu.VMEM((n_seq * n_own + 8 * n_seq, width), BF16),
        pltpu.VMEM((2, hp, width), F32), pltpu.SemaphoreType.DMA((2,)), pltpu.SemaphoreType.DMA((n_seq,)), pltpu.VMEM((n_seq, 8, width), F32),
        pltpu.VMEM((2, per, n_seq, nbo, BLK, TC), BF16), pltpu.SemaphoreType.DMA((2, per)),
        pltpu.VMEM((2, per, n_seq, nbo, 2 * BLK, TC), F32), pltpu.SemaphoreType.DMA((2, per)),
        pltpu.VMEM((n_seq, n_own + 8, TN), F32))

    def prev(wres, w_sem, lhs_p, stage, st_sem, q_st, q_sem, vh_st, vh_sem, pbuf, pstash):
        def weights(j):
            rows = width // 4
            return [pltpu.make_async_copy(w_in.at[i * rows:(i + 1) * rows, at(which(j), TN)],
                                          wres.at[j, i * rows:(i + 1) * rows], w_sem.at[j, i]) for i in range(4)]

        def which(j):
            return 2 * (j // nt) * width + c * half_w + lax.rem(j, nt) * TN

        def begin(j, carry):
            for copy in weights(j):
                copy.start()
            return carry

        lax.fori_loop(0, 2 * nt, begin, 0)

        def rows(s, h):
            n = cuts[h + 1] - cuts[h]

            @pl.when(on_b)
            def _():
                over(s, h).wait_recv()
                onward(s, h).start()
                load_rows(stage, st_sem, [(piece(u_x, s, h), n, lhs_p, c * n)])
                onward(s, h).wait_recv()
                load_rows(stage, st_sem, [(piece(u_fw, s, h), n, lhs_p, (1 - c) * n)])

            @pl.when(on_a)
            def _():
                lhs_p[...] = jnp.zeros_like(lhs_p)

        def project(h, j):
            n = 2 * (cuts[h + 1] - cuts[h])
            return (dot(lhs_p[:n, :], wres[j]) + bias_ref[:, at(which(j), TN)]).astype(BF16)

        def first(s, h):
            n = cuts[h + 1] - cuts[h]

            def body(j, carry):
                if h == 0:
                    @pl.when(s == 0)
                    def _():
                        for copy in weights(j):
                            copy.wait()

                p = project(h, j)
                for core in range(2):
                    pstash[core, cuts[h]:cuts[h + 1], at(j * TN, TN)] = p[core * n:(core + 1) * n]
                return carry

            lax.fori_loop(0, 2 * nt, body, 0)

        def last(s, base, dst, spectrum):
            h = n_cut - 1
            n = cuts[h + 1] - cuts[h]

            def flush(j):
                slot, copies = lax.rem(j, 2), []
                for half in range(per):
                    copies.append(pltpu.make_async_copy(q_st.at[slot, half], dst.at[j * per + half, s, :nbo], q_sem.at[slot, half]))
                    if spectrum:
                        copies.append(pltpu.make_async_copy(vh_st.at[slot, half], vhat.at[j * per + half, s, :nbo], vh_sem.at[slot, half]))
                return copies

            def body(j, carry):
                slot = lax.rem(j, 2)

                @pl.when(j >= 2)
                def _():
                    for copy in flush(j - 2):
                        copy.wait()

                taps = taps_ref[:, at(which(base + j), TN)]
                pbuf[0:8] = jnp.zeros((8, TN), F32)
                for core in range(2):
                    old = pstash[core, :cuts[h], at((base + j) * TN, TN)].astype(F32)
                    pbuf[8 + core * n_pos:8 + core * n_pos + cuts[h]] = jnp.where(on_b, old, 0.0)
                p = project(h, base + j).astype(F32)
                for core in range(2):
                    start = 8 + core * n_pos + cuts[h]
                    pbuf[start:start + n] = jnp.where(on_b, p[core * n:(core + 1) * n], 0.0)
                for b in range(nbo):
                    blk = short_conv(pbuf, taps, b * BLK, BLK)
                    for half in range(per):
                        q_st[slot, half, b] = blk[:, half * TC:(half + 1) * TC]
                    if spectrum:
                        spec = block_values(fwd3_ref, blk)
                        for half in range(per):
                            vh_st[slot, half, b] = spec[:, half * TC:(half + 1) * TC]
                for copy in flush(j):
                    copy.start()
                return carry

            lax.fori_loop(0, nt, body, 0)
            for j in (nt - 2, nt - 1):
                for copy in flush(j):
                    copy.wait()

        def one_seq(s, carry):
            for h in range(n_cut - 1):
                rows(s, h)
                first(s, h)
            rows(s, n_cut - 1)
            last(s, 0, qx, False)

            @pl.when(s + 1 == n_seq)
            def _():
                forward(0, range(Q))

            last(s, nt, qv, True)
            return carry

        lax.fori_loop(0, n_seq, one_seq, 0)

    pl.run_scoped(
        prev,
        pltpu.VMEM((2 * nt, width, TN), BF16), pltpu.SemaphoreType.DMA((2 * nt, 4)),
        pltpu.VMEM((2 * hp, width), BF16), pltpu.VMEM((2, hp, width), F32), pltpu.SemaphoreType.DMA((2,)),
        pltpu.VMEM((2, per, nbo, BLK, TC), BF16), pltpu.SemaphoreType.DMA((2, per)),
        pltpu.VMEM((2, per, nbo, 2 * BLK, TC), F32), pltpu.SemaphoreType.DMA((2, per)),
        pltpu.VMEM((n_own + 8, TN), F32), pltpu.VMEM((2, cuts[-2], 2 * half_w), BF16))

    @pl.when(on_a)
    def _():
        for u in range(n_tile):
            for f, own in enumerate((f1, f2)):
                fill(f, u, c, own, c * half_w + u * TC).start()
                fill(f, u, 1 - c, pf.at[f], u * TC).start()

    def conv(x1b, vb, x2b, vhb, farb, in_sem, vh_sem, kst, k_sem, sendbuf, *scratch):
        def fetch(t):
            slot, two = lax.rem(t, 3), lax.rem(t, 2)
            srcs = (qx.at[t, :, :2 * nbo], qv.at[t], qx.at[t, :, 2 * nbo:], far.at[t])
            copies = [pltpu.make_async_copy(r, b.at[slot], in_sem.at[slot, i])
                      for i, (r, b) in enumerate(zip(srcs, (x1b, vb, x2b, farb)))]
            return copies + [pltpu.make_async_copy(vhat.at[t, s], vhb.at[two, s], vh_sem.at[two, s]) for s in range(n_seq)]

        def flush(t):
            slot = lax.rem(t, 2)
            return pltpu.make_async_copy(kst.at[slot], keep.at[t], k_sem.at[slot])

        def swap_y(u):
            return remote(sendbuf.at[lax.rem(u, 2)], part.at[u], p_send.at[u], p_recv.at[u], (dp, other))

        tile = ConvTile(fwd6_ref, inv6_ref, *scratch)

        def inputs(t, back):
            slot, cols = lax.rem(t + 3 - back, 3), at(c * half_w + lax.rem(t + n_tile - back, n_tile) * TC, TC)
            return x1b.at[slot], vb.at[slot], x2b.at[slot], farb.at[slot], sk1_ref[:, cols], sk2_ref[:, cols]

        def emit(t):
            slot = lax.rem(t, 2)

            @pl.when(t >= 2)
            def _():
                flush(t - 2).wait()
                swap_y(t - 2).wait_send()

            tile.result(c, kst.at[slot], sendbuf.at[slot])
            flush(t).start()
            swap_y(t).start()

        for copy in fetch(0):
            copy.start()
        forward(1, range(Q // 2))

        def step(t, carry):
            @pl.when(t + 1 < n_tile)
            def _():
                for copy in fetch(t + 1):
                    copy.start()

            @pl.when(on_a)
            def _():
                for f in range(2):
                    for side in range(2):
                        fill(f, t, side, f1, 0).wait()

            @pl.when(on_b)
            def _():
                for q in range(Q):
                    for side in range(2):
                        across(t, side, 1 - dp, q).wait_recv()

            for copy in fetch(t):
                copy.wait()

            def relay(phase):
                ahead = 1 + 2 * phase // Q

                @pl.when(t + ahead < n_tile)
                def _():
                    forward(t + ahead, ((phase + Q // 2) % Q,))

            tile.step(land, t, vhb.at[lax.rem(t, 2)], inputs(t, 0), inputs(t, 1), relay)

            @pl.when(t >= 1)
            def _():
                emit(t - 1)
            return carry

        lax.fori_loop(0, n_tile, step, 0)
        tile.drain(inputs(n_tile, 1))
        emit(n_tile - 1)
        for u in (n_tile - 2, n_tile - 1):
            flush(u).wait()
            swap_y(u).wait_send()
        for u in range(n_tile):
            swap_y(u).wait_recv()

    nb = 2 * nbo
    pl.run_scoped(
        conv,
        pltpu.VMEM((3, n_seq, nb, BLK, TC), BF16), pltpu.VMEM((3, n_seq, nb, BLK, TC), BF16), pltpu.VMEM((3, n_seq, nbo, BLK, TC), BF16),
        pltpu.VMEM((2, n_seq, nb, 2 * BLK, TC), F32), pltpu.VMEM((3, 2, nbo, 2 * BLK, TC), F32),
        pltpu.SemaphoreType.DMA((3, 4)), pltpu.SemaphoreType.DMA((2, n_seq)),
        pltpu.VMEM((2, n_seq, n_pos, TC), BF16), pltpu.SemaphoreType.DMA((2,)), pltpu.VMEM((2, n_seq, n_pos, TC), F32),
        pltpu.VMEM((2, nbo, 3, BLK, TC), BF16),
        pltpu.VMEM((nbo + 1, 2 * BLK, TC), F32), pltpu.VMEM((nbo + 1, 2 * BLK, TC), F32), pltpu.VMEM((nbo, 2 * BLK, TC), F32),
        *[pltpu.VMEM((nb, 3, 2 * BLK, TC), BF16)] * n_seq,
        pltpu.VMEM((nb, 3, BLK, TC), BF16),
        *[pltpu.VMEM((nb, BLK, TC), F32)] * n_seq,
        pltpu.VMEM((nb, 2 * BLK, TC), F32),
        *[pltpu.VMEM((nbo, 3, 2 * BLK, TC), BF16)] * n_seq,
        pltpu.VMEM((n_seq, nbo, BLK, TC), BF16))

    for s in range(n_seq):
        swap_u(s).wait_send()
    for f in range(2):
        swap_f(f).wait_send()

    @pl.when(sp == 1)
    def _():
        for k in range(2):
            tail_copy(k).wait_send()

    @pl.when(on_a)
    def _():
        for i in range(n_seq * n_cut):
            over(*divmod(i, n_cut)).wait_send()
        for u in range(n_tile):
            for q in range(Q):
                for k in range(2):
                    filt(f1, u, k, q).wait_send()

    @pl.when(on_b)
    def _():
        for i in range(n_seq * n_cut):
            onward(*divmod(i, n_cut)).wait_send()
        for u in range(n_tile):
            for q in range(Q):
                for side in range(2):
                    across(u, side, dp, q).wait_send()


def loop(trips):
    def run(body):
        def step(i, carry):
            body(i)
            return carry
        lax.fori_loop(0, trips, step, 0)
    return run


class ConvTile:
    def __init__(self, fwd6, inv6, hparts, g1, g2, raw2, sp0, sp1, zparts, zv0, zv1, zhat, sq0, sq1, ybuf):
        self.fwd6, self.inv6, self.hparts, self.g, self.raw2 = fwd6, inv6, hparts, (g1, g2), raw2
        self.first, self.second, self.zparts, self.zval, self.zhat, self.ybuf = (sp0, sp1), (sq0, sq1), zparts, (zv0, zv1), zhat, ybuf
        self.nb, self.nbo = sp0.shape[0], sq0.shape[0]

    def near(self, land, t, f):
        for side in range(2):
            split_blocks(land.at[f, t, side], self.hparts.at[f], side * self.nbo // 2)

    def window(self, f, raw, far):
        g, nbo = self.g[f], self.nbo
        for j in range(nbo, 0, -1):
            cur = far.at[f, 0] if j == nbo else raw.at[j]
            for lo, sign in SIDES:
                re, im, new_re, new_im = shifted_add(cur, raw.at[j - 1], lo, sign)
                g[j, re], g[j, im] = new_re, new_im
        if raw is not g:
            g[0] = raw[0]

    def pointwise(self, xhat, f, far, dst, r, first):
        g, nbo = self.g[f], self.nbo
        re, im = pl.ds(pl.multiple_of(r * 16, 16), 16), pl.ds(pl.multiple_of(BLK + r * 16, 16), 16)
        for k in range(first, self.nb):
            acc_re = acc_im = None
            for j in range(k + 1):
                i = k - j
                gr, gi = (g[i, re], g[i, im]) if i <= nbo else (far[f, i - nbo, re], far[f, i - nbo, im])
                xr, xi = xhat[j, re], xhat[j, im]
                t_re, t_im = xr * gr - xi * gi, xr * gi + xi * gr
                acc_re = t_re if acc_re is None else acc_re + t_re
                acc_im = t_im if acc_im is None else acc_im + t_im
            for part, (a, b) in enumerate(zip(split3(acc_re), split3(acc_im))):
                dst[k - first, part, re], dst[k - first, part, im] = a, b

    def inverse(self, parts, k):
        return dot(self.inv6[...], stack6(parts[k, 0], parts[k, 1], parts[k, 2]))

    def gate_one(self, s, k, data):
        x1, v, _, _, skip, _ = data
        z = x1[s, k].astype(F32) * (self.inverse(self.first[s], k) + skip * v[s, k].astype(F32))
        self.zval[s][k] = z
        for part, a in enumerate(split3(z)):
            self.zparts[k, part] = a

    def spectrum(self, k):
        self.zhat[k] = block_spectrum(self.fwd6, self.zparts, k)

    def gate_two(self, s, k, data):
        y = data[2][s, k].astype(F32) * (self.inverse(self.second[s], k) + data[5] * self.zval[s][self.nbo + k])
        self.ybuf[s, k] = y.astype(BF16)

    def middle(self, s, data, i, point=None):
        for q in range(4):
            if point is not None:
                point(4 * i + q)
            for k in range(2):
                if q < 2:
                    self.gate_one(s, 4 * i + 2 * q + k, data)
                else:
                    self.spectrum(4 * i + 2 * (q - 2) + k)

    def step(self, land, t, vhat, data, old, relay):
        nb, nbo = self.nb, self.nbo
        far = data[3]
        self.near(land, t, 0)
        for j in range(nbo):
            self.g[0][j] = block_spectrum(self.fwd6, self.hparts.at[0], j)
        self.near(land, t, 1)
        self.window(0, self.g[0], far)

        @loop(nb // 4)
        def _(i):
            self.middle(1, old, i, lambda r: self.pointwise(vhat.at[0], 0, far, self.first[0], r, 0))

        relay(0)

        @loop(nbo // 2)
        def _(i):
            for q in range(4):
                self.pointwise(self.zhat, 1, old[3], self.second[1], 4 * i + q, nbo)
                if q < 2:
                    self.gate_two(0, 2 * i + q, old)
                else:
                    j = 2 * i + q - 2
                    self.raw2[j] = block_spectrum(self.fwd6, self.hparts.at[1], j)

        relay(1)
        self.window(1, self.raw2, far)

        @loop(nb // 4)
        def _(i):
            self.middle(0, data, i, lambda r: self.pointwise(vhat.at[1], 0, far, self.first[1], r, 0))

        relay(2)

        @loop(nbo // 2)
        def _(i):
            for q in range(4):
                self.pointwise(self.zhat, 1, far, self.second[0], 4 * i + q, nbo)
                if q % 2 == 0:
                    self.gate_two(1, 2 * i + q // 2, old)

        relay(3)

    def drain(self, data):
        nb, nbo = self.nb, self.nbo

        @loop(nb // 4)
        def _(i):
            self.middle(1, data, i)

        @loop(nbo // 2)
        def _(i):
            for q in range(4):
                self.pointwise(self.zhat, 1, data[3], self.second[1], 4 * i + q, nbo)
                if q % 2 == 0:
                    self.gate_two(0, 2 * i + q // 2, data)

        for k in range(nbo):
            self.gate_two(1, k, data)

    def result(self, c, keep, send):
        hk = self.nbo // 2
        for s in range(self.ybuf.shape[0]):
            for b in range(hk):
                keep[s, b * BLK:(b + 1) * BLK] = self.ybuf[s, c * hk + b]
                send[s, b * BLK:(b + 1) * BLK] = self.ybuf[s, (1 - c) * hk + b].astype(F32)


def out_body(keep, part, w_out, u_in, out, wbuf, w_sem, lhs, keep_v, stage, in_sem, u_v, o_st, o_sem):
    c = lax.rem(lax.axis_index("sp"), 2)
    n_tile, n_seq, n_pos, _ = keep.shape
    half_w = n_tile * TC
    width = 2 * half_w
    n_col, rows = width // TN, width // 4

    def weights(j, slot):
        return [pltpu.make_async_copy(w_out.at[i * rows:(i + 1) * rows, pl.ds(pl.multiple_of(j * TN, TN), TN)],
                                      wbuf.at[slot, i * rows:(i + 1) * rows], w_sem.at[slot, i]) for i in range(4)]

    def flush(j):
        slot = lax.rem(j, 2)
        return pltpu.make_async_copy(o_st.at[slot], out.at[:, :, pl.ds(pl.multiple_of(j * TN, TN), TN)], o_sem.at[slot])

    loads = [pltpu.make_async_copy(part.at[u], stage.at[u], in_sem.at[u]) for u in range(n_tile)]
    loads += [pltpu.make_async_copy(keep.at[u], keep_v.at[u], in_sem.at[n_tile + u]) for u in range(n_tile)]
    for copy in loads:
        copy.start()
    for copy in weights(0, 0):
        copy.start()
    resid = pltpu.make_async_copy(u_in, u_v, in_sem.at[2 * n_tile])
    resid.start()
    for u in range(n_tile):
        loads[u].wait()
        loads[n_tile + u].wait()
        for s in range(n_seq):
            lhs[s, :, pl.ds(pl.multiple_of((1 - c) * half_w + u * TC, TC), TC)] = stage[u, s].astype(BF16)
            lhs[s, :, pl.ds(pl.multiple_of(c * half_w + u * TC, TC), TC)] = keep_v[u, s]
    resid.wait()

    def step(j, carry):
        slot = lax.rem(j, 2)

        @pl.when(j + 1 < n_col)
        def _():
            for copy in weights(j + 1, 1 - slot):
                copy.start()

        for copy in weights(j, slot):
            copy.wait()

        @pl.when(j >= 2)
        def _():
            flush(j - 2).wait()

        cols = pl.ds(pl.multiple_of(j * TN, TN), TN)
        for s in range(n_seq):
            o_st[slot, s] = (u_v[s, :, cols].astype(F32) + dot(lhs[s], wbuf[slot])).astype(BF16)
        flush(j).start()
        return carry

    lax.fori_loop(0, n_col, step, 0)
    for j in (n_col - 2, n_col - 1):
        flush(j).wait()


def solution(mesh):
    fwd3, fwd6, inv6 = transform_tables()

    def local_step(u_in, w_in, b_in, conv_taps, w_out, skip_one, skip_two, filt_one, filt_two):
        n_seq, n_pos, width = u_in.shape
        half_w = width // 2
        n_own = 2 * n_pos
        nb = 2 * n_own // BLK
        nbo = nb // 2
        n_tile = half_w // TC
        small, large = pl.BlockSpec(memory_space=pltpu.VMEM), pl.BlockSpec(memory_space=pl.ANY)
        dma = pltpu.SemaphoreType.DMA

        def shape(dims, dtype=F32):
            return jax.ShapeDtypeStruct(dims, dtype)

        keep, part, *_ = pl.pallas_call(
            main_body,
            in_specs=[small] * 7 + [large] * 5,
            out_specs=[large] * 11,
            out_shape=[
                shape((n_tile, n_seq, n_pos, TC), BF16), shape((n_tile, n_seq, n_pos, TC)),
                shape((n_tile, n_seq, nb + nbo, BLK, TC), BF16), shape((n_tile, n_seq, nb, BLK, TC), BF16),
                shape((n_tile, n_seq, nb, 2 * BLK, TC)), shape((n_tile, 2, nbo, 2 * BLK, TC)),
                shape((n_seq, n_pos, width)), shape((n_seq, n_pos, width)), shape((n_seq, n_pos, width)),
                shape((n_seq, 8, width)), shape((2, n_pos, half_w)),
            ],
            scratch_shapes=[
                pltpu.VMEM((2, n_tile, 2, n_pos, TC), F32),
                dma((2,)), dma((1,)), *[dma((n_seq, 3))] * 4, *[dma((n_seq,))] * 2, *[dma((2,))] * 2,
                dma((2, n_tile, 2)), *[dma((n_tile, Q, 2))] * 4, *[dma((n_tile,))] * 2,
            ],
            compiler_params=pltpu.CompilerParams(vmem_limit_bytes=62 << 20, collective_id=0, has_side_effects=True),
            name="hyena_main",
        )(fwd3, fwd6, inv6, b_in.reshape(1, -1), conv_taps, skip_one.reshape(1, -1), skip_two.reshape(1, -1),
          u_in, u_in.astype(F32), w_in, filt_one, filt_two)

        return pl.pallas_call(
            out_body,
            in_specs=[large] * 4,
            out_specs=large,
            out_shape=shape((n_seq, n_pos, width), BF16),
            scratch_shapes=[
                pltpu.VMEM((2, width, TN), BF16), dma((2, 4)),
                pltpu.VMEM((n_seq, n_pos, width), BF16), pltpu.VMEM((n_tile, n_seq, n_pos, TC), BF16), pltpu.VMEM((n_tile, n_seq, n_pos, TC), F32),
                dma((2 * n_tile + 1,)), pltpu.VMEM((n_seq, n_pos, width), BF16), pltpu.VMEM((2, n_seq, n_pos, TN), BF16), dma((2,)),
            ],
            compiler_params=pltpu.CompilerParams(vmem_limit_bytes=60 << 20),
            name="out_proj",
        )(keep, part, w_out, u_in)

    seq_spec = P("dp", "sp", None)
    filt_spec = P("sp", None)
    return jax.shard_map(local_step, mesh=mesh, in_specs=(seq_spec, P(), P(), P(), P(), P(), P(), filt_spec, filt_spec), out_specs=seq_spec, check_vma=False)
```

```python
import functools

import jax
import jax.numpy as jnp
import numpy as np
from jax import lax
from jax.experimental import pallas as pl
from jax.experimental.pallas import tpu as pltpu
from jax.sharding import PartitionSpec as P

F32, BF16 = jnp.float32, jnp.bfloat16
BLK = 128
TN = 512
TC = 256
Q = 4
RC = 32
MESH = pl.DeviceIdType.MESH


def split_table(table):
    parts, rest = [], table.astype(np.float64)
    for _ in range(3):
        part = rest.astype(np.float32).astype(jnp.bfloat16)
        parts.append(part)
        rest = rest - part.astype(np.float64)
    return parts


def transform_tables():
    freq = np.concatenate([np.arange(0, BLK, 2), np.arange(1, BLK, 2)]) + 0.5
    angle = 2.0 * np.pi * freq[:, None] * np.arange(BLK)[None, :] / (2 * BLK)
    fwd = np.concatenate([np.cos(angle), -np.sin(angle)], 0)
    inv = np.concatenate([np.cos(angle).T, -np.sin(angle).T], 1) / BLK
    f1, f2, f3 = split_table(fwd)
    e1, e2, e3 = split_table(inv)
    fwd3 = np.concatenate([f1, f2, f3], 1)
    fwd6 = np.concatenate([f1, f1, f2, f2, f1, f3], 1)
    inv6 = np.concatenate([e1, e1, e2, e2, e1, e3], 1)
    return fwd3, fwd6, inv6


def dot(a, b):
    return jnp.dot(a, b, preferred_element_type=F32)


def split3(x):
    hi = x.astype(BF16)
    rest = x - hi.astype(F32)
    mid = rest.astype(BF16)
    low = (rest - mid.astype(F32)).astype(BF16)
    return hi, mid, low


def stack6(hi, mid, low):
    return jnp.concatenate([hi, mid, hi, mid, low, hi], axis=0)


def split_blocks(src, parts, first):
    for j in range(src.shape[0] // BLK):
        for i, a in enumerate(split3(src[j * BLK:(j + 1) * BLK])):
            parts[first + j, i] = a


def block_spectrum(fwd6_ref, parts, j):
    return dot(fwd6_ref[...], stack6(parts[j, 0], parts[j, 1], parts[j, 2]))


def shifted_add(cur, old, lo, sign):
    re, im = slice(lo, lo + BLK // 2), slice(BLK + lo, BLK + lo + BLK // 2)
    return re, im, cur[re] - sign * old[im], cur[im] + sign * old[re]


SIDES = ((0, 1.0), (BLK // 2, -1.0))


def short_conv(pbuf, t, first, rows):
    return (t[0:1] * pbuf[8 + first:8 + first + rows] + t[1:2] * pbuf[7 + first:7 + first + rows] + t[2:3] * pbuf[6 + first:6 + first + rows]).astype(BF16)


def block_values(fwd3_ref, blk):
    return dot(fwd3_ref[...], jnp.concatenate([blk, blk, blk], axis=0))


def main_body(fwd3_ref, fwd6_ref, inv6_ref, bias_ref, taps_ref, sk1_ref, sk2_ref, u_bf, u32, w_in, f1, f2,
              keep, part, qx, qv, vhat, far, u_sw, u_x, u_fw, tail, pf,
              land, ts, tr, os, orr, ws, wr, ss, sr, fs, fr, l_sem, x_send, x_recv, y_send, y_recv, p_send, p_recv):
    sp, dp = lax.axis_index("sp"), lax.axis_index("dp")
    c = lax.rem(sp, 2)
    on_b = sp >= 2
    on_a = jnp.logical_not(on_b)
    other = sp + 1 - 2 * c
    n_seq, n_pos, width = u_bf.shape
    half_w = width // 2
    nt, n_tile, per = half_w // TN, half_w // TC, TN // TC
    n_own, hp = 2 * n_pos, n_pos // 2
    nbo = n_own // BLK
    cuts = (0, n_pos // 2, 3 * n_pos // 4, n_pos)
    n_cut, n_over = len(cuts) - 1, n_pos // RC

    def remote(src, dst, send, recv, peer):
        return pltpu.make_async_remote_copy(src, dst, send, recv, device_id=peer, device_id_type=MESH)

    def at(start, size):
        return pl.ds(pl.multiple_of(start, size), size)

    def piece(ref, s, h):
        return ref.at[s, cuts[h]:cuts[h + 1]]

    def tail_copy(k):
        return remote(u32.at[:, n_pos - 8:], tail, ts.at[k], tr.at[0], (dp, 2 + k))

    def over(s, i):
        rows = pl.ds(i * RC, RC)
        return remote(u32.at[s, rows], u_x.at[s, rows], os.at[s, i], orr.at[s, i], (dp, lax.rem(sp + 2, 4)))

    def onward(s, h):
        return remote(piece(u_x, s, h), piece(u_fw, s, h), ws.at[s, h], wr.at[s, h], (dp, other))

    def swap_u(s):
        return remote(u32.at[s], u_sw.at[s], ss.at[s], sr.at[s], (dp, other))

    def swap_f(f):
        return remote((f1, f2)[f].at[:, at((1 - c) * half_w, half_w)], pf.at[f], fs.at[f], fr.at[f], (dp, other))

    qr = n_pos // Q

    def filt(src, u, k, q):
        return remote(src.at[q * qr:(q + 1) * qr, at(k * half_w + u * TC, TC)], land.at[dp, u, c, q * qr:(q + 1) * qr],
                      x_send.at[u, q, k], x_recv.at[u, q, c], (dp, 2 + k))

    def landed(u, side, q):
        ref = land.at[dp, u, side, q * qr:(q + 1) * qr]
        return remote(ref, ref, x_send.at[u, q, side], x_recv.at[u, q, side], (dp, sp))

    def across(u, side, f, q):
        ref = land.at[f, u, side, q * qr:(q + 1) * qr]
        return remote(ref, ref, y_send.at[u, q, side], y_recv.at[u, q, side], (1 - dp, sp))

    def fill(f, u, side, src, start):
        return pltpu.make_async_copy(src.at[:, at(start, TC)], land.at[f, u, side], l_sem.at[f, u, side])

    def column(g, j):
        return (g + j // nt) * width + c * half_w + lax.rem(j, nt) * TN

    def load_rows(stage, st_sem, items):
        def copy(i):
            src, rows, _, _ = items[i]
            return pltpu.make_async_copy(src, stage.at[i % 2, :rows], st_sem.at[i % 2])

        copy(0).start()
        for i, (_, rows, dst, row) in enumerate(items):
            if i + 1 < len(items):
                copy(i + 1).start()
            copy(i).wait()
            dst[pl.ds(pl.multiple_of(row, 16), rows), :] = stage[i % 2, :rows].astype(BF16)

    barrier = pltpu.get_barrier_semaphore()
    for peer in ((dp, other), (dp, lax.rem(sp + 2, 4)), (dp, lax.rem(other + 2, 4)), (1 - dp, sp)):
        pl.semaphore_signal(barrier, inc=1, device_id=peer, device_id_type=MESH)
    pl.semaphore_wait(barrier, 4)

    @pl.when(sp == 1)
    def _():
        for k in range(2):
            tail_copy(k).start()

    @pl.when(on_a)
    def _():
        for i in range(n_seq * n_over):
            over(*divmod(i, n_over)).start()
        for which, src in ((0, f1), (1, f2)):
            @pl.when(dp == which)
            def _():
                for u in range(n_tile):
                    for q in range(Q):
                        for k in range(2):
                            filt(src, u, k, q).start()

    for i in range(n_seq):
        swap_u(i).start()
    for f in range(2):
        swap_f(f).start()

    def forward(u, quarters):
        @pl.when(on_b)
        def _():
            for q in quarters:
                for side in range(2):
                    landed(u, side, q).wait_recv()
                    across(u, side, dp, q).start()

    def front(wbuf, wsem, lhs, stage, st_sem, lhs_sem, tailbuf, q_st, q_sem, vh_st, vh_sem, pbuf):
        def weights(g, j, slot):
            rows = width // 4
            return [pltpu.make_async_copy(w_in.at[i * rows:(i + 1) * rows, at(column(g, j), TN)],
                                          wbuf.at[slot, i * rows:(i + 1) * rows], wsem.at[slot, i]) for i in range(4)]

        def stream(g, body, following, n=nt):
            def step(j, carry):
                slot = lax.rem(j, 2)

                @pl.when(j + 1 < n)
                def _():
                    for copy in weights(g, j + 1, 1 - slot):
                        copy.start()

                if following is not None:
                    @pl.when(j + 1 == n)
                    def _():
                        following(1 - slot)

                for copy in weights(g, j, slot):
                    copy.wait()
                body(j, slot, bias_ref[:, at(column(g, j), TN)], taps_ref[:, at(column(g, j), TN)])
                return carry

            lax.fori_loop(0, n, step, 0)

        def begin(g):
            def start(slot):
                for copy in weights(g, 0, slot):
                    copy.start()
            return start

        def project(rows_ref, slot, bias):
            return (dot(rows_ref, wbuf[slot]) + bias).astype(BF16).astype(F32)

        tail_rows = n_seq * 8
        begin(0)(0)
        own_rows = [pltpu.make_async_copy(u_bf.at[s], lhs.at[pl.ds(pl.multiple_of(tail_rows + s * n_own + c * n_pos, 16), n_pos)], lhs_sem.at[s])
                    for s in range(n_seq)]
        for copy in own_rows:
            copy.start()
        for s in range(n_seq):
            swap_u(s).wait_recv()
        load_rows(stage, st_sem, [(u_sw.at[s, h * hp:(h + 1) * hp], hp, lhs, tail_rows + s * n_own + (1 - c) * n_pos + h * hp)
                                  for s in range(n_seq) for h in range(2)])
        for copy in own_rows:
            copy.wait()

        @pl.when(on_b)
        def _():
            tail_copy(0).wait_recv()
            copy = pltpu.make_async_copy(tail, tailbuf, lhs_sem.at[0])
            copy.start()
            copy.wait()

        @pl.when(on_a)
        def _():
            tailbuf[...] = jnp.zeros_like(tailbuf)

        lhs[:tail_rows, :] = tailbuf[...].reshape(tail_rows, width).astype(BF16)
        chunk = n_pos

        def own_phase(g, n, dst, spectrum, following):
            def flush(j, slot):
                blocks = pl.ds(nbo * (1 + j // nt), nbo)
                copies = []
                for h in range(per):
                    u = lax.rem(j, nt) * per + h
                    copies.append(pltpu.make_async_copy(q_st.at[slot, h], dst.at[u, :, blocks], q_sem.at[slot, h]))
                    if spectrum:
                        copies.append(pltpu.make_async_copy(vh_st.at[slot, h], vhat.at[u, :, nbo:], vh_sem.at[slot, h]))
                return copies

            def body(j, slot, bias, taps):
                @pl.when(j >= 2)
                def _():
                    for copy in flush(j - 2, slot):
                        copy.wait()

                for i in range(n_seq * n_own // chunk):
                    s, r = divmod(i * chunk, n_own)
                    p = project(lhs[(tail_rows + i * chunk if i else 0):tail_rows + (i + 1) * chunk, :], slot, bias)
                    if i == 0:
                        for k in range(n_seq):
                            pbuf[k, 0:8] = jnp.where(on_b, p[8 * k:8 * k + 8], 0.0)
                        p = p[tail_rows:]
                    pbuf[s, 8 + r:8 + r + chunk] = p
                    q = short_conv(pbuf.at[s], taps, r, chunk)
                    for b in range(chunk // BLK):
                        blk = q[b * BLK:(b + 1) * BLK]
                        for h in range(per):
                            q_st[slot, h, s, r // BLK + b] = blk[:, h * TC:(h + 1) * TC]
                        if spectrum:
                            spec = block_values(fwd3_ref, blk)
                            for h in range(per):
                                vh_st[slot, h, s, r // BLK + b] = spec[:, h * TC:(h + 1) * TC]
                for copy in flush(j, slot):
                    copy.start()

            stream(g, body, following, n)
            for j in (n - 2, n - 1):
                for copy in flush(j, j % 2):
                    copy.wait()

        own_phase(0, 2 * nt, qx, False, begin(2))
        own_phase(2, nt, qv, True, None)

        def far_phase(fin, fin_sem, fout, fout_sem, parts):
            hk = n_pos // BLK

            def fetch(j, slot):
                mine = at(c * half_w + j * TC, TC)
                srcs = (f1.at[:, mine], f2.at[:, mine], pf.at[0, :, at(j * TC, TC)], pf.at[1, :, at(j * TC, TC)])
                return [pltpu.make_async_copy(src, fin.at[slot, i], fin_sem.at[slot, i]) for i, src in enumerate(srcs)]

            def flush(j, slot):
                return pltpu.make_async_copy(fout.at[slot], far.at[j], fout_sem.at[slot])

            for copy in fetch(0, 0):
                copy.start()

            def step(j, carry):
                slot = lax.rem(j, 2)

                @pl.when(j + 1 < n_tile)
                def _():
                    for copy in fetch(j + 1, 1 - slot):
                        copy.start()

                for copy in fetch(j, slot):
                    copy.wait()

                @pl.when(j >= 2)
                def _():
                    flush(j - 2, slot).wait()

                for f in range(2):
                    split_blocks(fin.at[slot, f], parts.at[f], c * hk)
                    split_blocks(fin.at[slot, 2 + f], parts.at[f], (1 - c) * hk)
                g_ref = fout.at[slot]
                for f in range(2):
                    for b in range(2 * hk):
                        g_ref[f, b] = block_spectrum(fwd6_ref, parts.at[f], b)
                    for b in range(2 * hk - 1, 0, -1):
                        for lo, sign in SIDES:
                            re, im, new_re, new_im = shifted_add(g_ref.at[f, b], g_ref.at[f, b - 1], lo, sign)
                            g_ref[f, b, re], g_ref[f, b, im] = new_re, new_im
                flush(j, slot).start()
                return carry

            lax.fori_loop(0, n_tile, step, 0)
            for j in (n_tile - 2, n_tile - 1):
                flush(j, j % 2).wait()

        for f in range(2):
            swap_f(f).wait_recv()
        pl.run_scoped(
            far_phase, pltpu.VMEM((2, 4, n_pos, TC), F32), pltpu.SemaphoreType.DMA((2, 4)),
            pltpu.VMEM((2, 2, nbo, 2 * BLK, TC), F32), pltpu.SemaphoreType.DMA((2,)), pltpu.VMEM((2, nbo, 3, BLK, TC), BF16))

    pl.run_scoped(
        front,
        pltpu.VMEM((2, width, TN), BF16), pltpu.SemaphoreType.DMA((2, 4)),
        pltpu.VMEM((n_seq * n_own + 8 * n_seq, width), BF16),
        pltpu.VMEM((2, hp, width), F32), pltpu.SemaphoreType.DMA((2,)), pltpu.SemaphoreType.DMA((n_seq,)), pltpu.VMEM((n_seq, 8, width), F32),
        pltpu.VMEM((2, per, n_seq, nbo, BLK, TC), BF16), pltpu.SemaphoreType.DMA((2, per)),
        pltpu.VMEM((2, per, n_seq, nbo, 2 * BLK, TC), F32), pltpu.SemaphoreType.DMA((2, per)),
        pltpu.VMEM((n_seq, n_own + 8, TN), F32))

    def prev(wres, w_sem, lhs_p, stage, st_sem, q_st, q_sem, vh_st, vh_sem, pbuf, pstash):
        def weights(j):
            rows = width // 4
            return [pltpu.make_async_copy(w_in.at[i * rows:(i + 1) * rows, at(which(j), TN)],
                                          wres.at[j, i * rows:(i + 1) * rows], w_sem.at[j, i]) for i in range(4)]

        def which(j):
            return 2 * (j // nt) * width + c * half_w + lax.rem(j, nt) * TN

        def begin(j, carry):
            for copy in weights(j):
                copy.start()
            return carry

        lax.fori_loop(0, 2 * nt, begin, 0)

        def rows(s, h):
            n = cuts[h + 1] - cuts[h]

            @pl.when(on_b)
            def _():
                for i in range(cuts[h] // RC, cuts[h + 1] // RC):
                    over(s, i).wait_recv()
                onward(s, h).start()
                load_rows(stage, st_sem, [(piece(u_x, s, h), n, lhs_p, c * n)])
                onward(s, h).wait_recv()
                load_rows(stage, st_sem, [(piece(u_fw, s, h), n, lhs_p, (1 - c) * n)])

            @pl.when(on_a)
            def _():
                lhs_p[...] = jnp.zeros_like(lhs_p)

        def project(h, j):
            n = 2 * (cuts[h + 1] - cuts[h])
            return (dot(lhs_p[:n, :], wres[j]) + bias_ref[:, at(which(j), TN)]).astype(BF16)

        def first(s, h):
            n = cuts[h + 1] - cuts[h]

            def body(j, carry):
                if h == 0:
                    @pl.when(s == 0)
                    def _():
                        for copy in weights(j):
                            copy.wait()

                p = project(h, j)
                for core in range(2):
                    pstash[core, cuts[h]:cuts[h + 1], at(j * TN, TN)] = p[core * n:(core + 1) * n]
                return carry

            lax.fori_loop(0, 2 * nt, body, 0)

        def last(s, base, dst, spectrum):
            h = n_cut - 1
            n = cuts[h + 1] - cuts[h]

            def flush(j):
                slot, copies = lax.rem(j, 2), []
                for half in range(per):
                    copies.append(pltpu.make_async_copy(q_st.at[slot, half], dst.at[j * per + half, s, :nbo], q_sem.at[slot, half]))
                    if spectrum:
                        copies.append(pltpu.make_async_copy(vh_st.at[slot, half], vhat.at[j * per + half, s, :nbo], vh_sem.at[slot, half]))
                return copies

            def body(j, carry):
                slot = lax.rem(j, 2)

                @pl.when(j >= 2)
                def _():
                    for copy in flush(j - 2):
                        copy.wait()

                taps = taps_ref[:, at(which(base + j), TN)]
                pbuf[0:8] = jnp.zeros((8, TN), F32)
                for core in range(2):
                    old = pstash[core, :cuts[h], at((base + j) * TN, TN)].astype(F32)
                    pbuf[8 + core * n_pos:8 + core * n_pos + cuts[h]] = jnp.where(on_b, old, 0.0)
                p = project(h, base + j).astype(F32)
                for core in range(2):
                    start = 8 + core * n_pos + cuts[h]
                    pbuf[start:start + n] = jnp.where(on_b, p[core * n:(core + 1) * n], 0.0)
                for b in range(nbo):
                    blk = short_conv(pbuf, taps, b * BLK, BLK)
                    for half in range(per):
                        q_st[slot, half, b] = blk[:, half * TC:(half + 1) * TC]
                    if spectrum:
                        spec = block_values(fwd3_ref, blk)
                        for half in range(per):
                            vh_st[slot, half, b] = spec[:, half * TC:(half + 1) * TC]
                for copy in flush(j):
                    copy.start()

                if spectrum:
                    @pl.when(jnp.logical_and(s == n_seq - 1, j == 1))
                    def _():
                        forward(0, (Q - 1,))
                return carry

            lax.fori_loop(0, nt, body, 0)
            for j in (nt - 2, nt - 1):
                for copy in flush(j):
                    copy.wait()

        def one_seq(s, carry):
            for h in range(n_cut - 1):
                rows(s, h)
                first(s, h)
            rows(s, n_cut - 1)

            @pl.when(s + 1 == n_seq)
            def _():
                forward(0, (0,))

            last(s, 0, qx, False)

            @pl.when(s + 1 == n_seq)
            def _():
                forward(0, range(1, Q - 1))

            last(s, nt, qv, True)
            return carry

        lax.fori_loop(0, n_seq, one_seq, 0)

    pl.run_scoped(
        prev,
        pltpu.VMEM((2 * nt, width, TN), BF16), pltpu.SemaphoreType.DMA((2 * nt, 4)),
        pltpu.VMEM((2 * hp, width), BF16), pltpu.VMEM((2, hp, width), F32), pltpu.SemaphoreType.DMA((2,)),
        pltpu.VMEM((2, per, nbo, BLK, TC), BF16), pltpu.SemaphoreType.DMA((2, per)),
        pltpu.VMEM((2, per, nbo, 2 * BLK, TC), F32), pltpu.SemaphoreType.DMA((2, per)),
        pltpu.VMEM((n_own + 8, TN), F32), pltpu.VMEM((2, cuts[-2], 2 * half_w), BF16))

    @pl.when(on_a)
    def _():
        for u in range(n_tile):
            for f, own in enumerate((f1, f2)):
                fill(f, u, c, own, c * half_w + u * TC).start()
                fill(f, u, 1 - c, pf.at[f], u * TC).start()

    def conv(x1b, vb, x2b, vhb, farb, in_sem, vh_sem, kst, k_sem, sendbuf, *scratch):
        def fetch(t):
            slot, two = lax.rem(t, 3), lax.rem(t, 2)
            srcs = (qx.at[t, :, :2 * nbo], qv.at[t], qx.at[t, :, 2 * nbo:], far.at[t])
            copies = [pltpu.make_async_copy(r, b.at[slot], in_sem.at[slot, i])
                      for i, (r, b) in enumerate(zip(srcs, (x1b, vb, x2b, farb)))]
            return copies + [pltpu.make_async_copy(vhat.at[t, s], vhb.at[two, s], vh_sem.at[two, s]) for s in range(n_seq)]

        def flush(t):
            slot = lax.rem(t, 2)
            return pltpu.make_async_copy(kst.at[slot], keep.at[t], k_sem.at[slot])

        def swap_y(u):
            return remote(sendbuf.at[lax.rem(u, 2)], part.at[u], p_send.at[u], p_recv.at[u], (dp, other))

        tile = ConvTile(fwd6_ref, inv6_ref, *scratch)

        def inputs(t, back):
            slot, cols = lax.rem(t + 3 - back, 3), at(c * half_w + lax.rem(t + n_tile - back, n_tile) * TC, TC)
            return x1b.at[slot], vb.at[slot], x2b.at[slot], farb.at[slot], sk1_ref[:, cols], sk2_ref[:, cols]

        def emit(t):
            slot = lax.rem(t, 2)

            @pl.when(t >= 2)
            def _():
                flush(t - 2).wait()
                swap_y(t - 2).wait_send()

            tile.result(c, kst.at[slot], sendbuf.at[slot])
            flush(t).start()
            swap_y(t).start()

        for copy in fetch(0):
            copy.start()
        forward(1, range(Q // 2))

        def step(t, carry):
            @pl.when(t + 1 < n_tile)
            def _():
                for copy in fetch(t + 1):
                    copy.start()

            @pl.when(on_a)
            def _():
                for f in range(2):
                    for side in range(2):
                        fill(f, t, side, f1, 0).wait()

            @pl.when(on_b)
            def _():
                for q in range(Q):
                    for side in range(2):
                        across(t, side, 1 - dp, q).wait_recv()

            for copy in fetch(t):
                copy.wait()

            def relay(phase):
                ahead = 1 + 2 * phase // Q

                @pl.when(t + ahead < n_tile)
                def _():
                    forward(t + ahead, ((phase + Q // 2) % Q,))

            tile.step(land, t, vhb.at[lax.rem(t, 2)], inputs(t, 0), inputs(t, 1), relay)

            @pl.when(t >= 1)
            def _():
                emit(t - 1)
            return carry

        lax.fori_loop(0, n_tile, step, 0)
        tile.drain(inputs(n_tile, 1))
        emit(n_tile - 1)
        for u in (n_tile - 2, n_tile - 1):
            flush(u).wait()
            swap_y(u).wait_send()
        for u in range(n_tile):
            swap_y(u).wait_recv()

    nb = 2 * nbo
    pl.run_scoped(
        conv,
        pltpu.VMEM((3, n_seq, nb, BLK, TC), BF16), pltpu.VMEM((3, n_seq, nb, BLK, TC), BF16), pltpu.VMEM((3, n_seq, nbo, BLK, TC), BF16),
        pltpu.VMEM((2, n_seq, nb, 2 * BLK, TC), F32), pltpu.VMEM((3, 2, nbo, 2 * BLK, TC), F32),
        pltpu.SemaphoreType.DMA((3, 4)), pltpu.SemaphoreType.DMA((2, n_seq)),
        pltpu.VMEM((2, n_seq, n_pos, TC), BF16), pltpu.SemaphoreType.DMA((2,)), pltpu.VMEM((2, n_seq, n_pos, TC), F32),
        pltpu.VMEM((2, nbo, 3, BLK, TC), BF16),
        pltpu.VMEM((nbo + 1, 2 * BLK, TC), F32), pltpu.VMEM((nbo + 1, 2 * BLK, TC), F32), pltpu.VMEM((nbo, 2 * BLK, TC), F32),
        *[pltpu.VMEM((nb, 3, 2 * BLK, TC), BF16)] * n_seq,
        pltpu.VMEM((nb, 3, BLK, TC), BF16),
        *[pltpu.VMEM((nb, BLK, TC), F32)] * n_seq,
        pltpu.VMEM((nb, 2 * BLK, TC), F32),
        *[pltpu.VMEM((nbo, 3, 2 * BLK, TC), BF16)] * n_seq,
        pltpu.VMEM((n_seq, nbo, BLK, TC), BF16))

    for s in range(n_seq):
        swap_u(s).wait_send()
    for f in range(2):
        swap_f(f).wait_send()

    @pl.when(sp == 1)
    def _():
        for k in range(2):
            tail_copy(k).wait_send()

    @pl.when(on_a)
    def _():
        for i in range(n_seq * n_over):
            over(*divmod(i, n_over)).wait_send()
        for u in range(n_tile):
            for q in range(Q):
                for k in range(2):
                    filt(f1, u, k, q).wait_send()

    @pl.when(on_b)
    def _():
        for i in range(n_seq * n_cut):
            onward(*divmod(i, n_cut)).wait_send()
        for u in range(n_tile):
            for q in range(Q):
                for side in range(2):
                    across(u, side, dp, q).wait_send()


def loop(trips):
    def run(body):
        def step(i, carry):
            body(i)
            return carry
        lax.fori_loop(0, trips, step, 0)
    return run


class ConvTile:
    def __init__(self, fwd6, inv6, hparts, g1, g2, raw2, sp0, sp1, zparts, zv0, zv1, zhat, sq0, sq1, ybuf):
        self.fwd6, self.inv6, self.hparts, self.g, self.raw2 = fwd6, inv6, hparts, (g1, g2), raw2
        self.first, self.second, self.zparts, self.zval, self.zhat, self.ybuf = (sp0, sp1), (sq0, sq1), zparts, (zv0, zv1), zhat, ybuf
        self.nb, self.nbo = sp0.shape[0], sq0.shape[0]

    def near(self, land, t, f):
        for side in range(2):
            split_blocks(land.at[f, t, side], self.hparts.at[f], side * self.nbo // 2)

    def window(self, f, raw, far):
        g, nbo = self.g[f], self.nbo
        for j in range(nbo, 0, -1):
            cur = far.at[f, 0] if j == nbo else raw.at[j]
            for lo, sign in SIDES:
                re, im, new_re, new_im = shifted_add(cur, raw.at[j - 1], lo, sign)
                g[j, re], g[j, im] = new_re, new_im
        if raw is not g:
            g[0] = raw[0]

    def pointwise(self, xhat, f, far, dst, r, first):
        g, nbo = self.g[f], self.nbo
        re, im = pl.ds(pl.multiple_of(r * 16, 16), 16), pl.ds(pl.multiple_of(BLK + r * 16, 16), 16)
        for k in range(first, self.nb):
            acc_re = acc_im = None
            for j in range(k + 1):
                i = k - j
                gr, gi = (g[i, re], g[i, im]) if i <= nbo else (far[f, i - nbo, re], far[f, i - nbo, im])
                xr, xi = xhat[j, re], xhat[j, im]
                t_re, t_im = xr * gr - xi * gi, xr * gi + xi * gr
                acc_re = t_re if acc_re is None else acc_re + t_re
                acc_im = t_im if acc_im is None else acc_im + t_im
            for part, (a, b) in enumerate(zip(split3(acc_re), split3(acc_im))):
                dst[k - first, part, re], dst[k - first, part, im] = a, b

    def inverse(self, parts, k):
        return dot(self.inv6[...], stack6(parts[k, 0], parts[k, 1], parts[k, 2]))

    def gate_one(self, s, k, data):
        x1, v, _, _, skip, _ = data
        z = x1[s, k].astype(F32) * (self.inverse(self.first[s], k) + skip * v[s, k].astype(F32))
        self.zval[s][k] = z
        for part, a in enumerate(split3(z)):
            self.zparts[k, part] = a

    def spectrum(self, k):
        self.zhat[k] = block_spectrum(self.fwd6, self.zparts, k)

    def gate_two(self, s, k, data):
        y = data[2][s, k].astype(F32) * (self.inverse(self.second[s], k) + data[5] * self.zval[s][self.nbo + k])
        self.ybuf[s, k] = y.astype(BF16)

    def middle(self, s, data, i, point=None):
        for q in range(4):
            if point is not None:
                point(4 * i + q)
            for k in range(2):
                if q < 2:
                    self.gate_one(s, 4 * i + 2 * q + k, data)
                else:
                    self.spectrum(4 * i + 2 * (q - 2) + k)

    def step(self, land, t, vhat, data, old, relay):
        nb, nbo = self.nb, self.nbo
        far = data[3]
        self.near(land, t, 0)
        for j in range(nbo):
            self.g[0][j] = block_spectrum(self.fwd6, self.hparts.at[0], j)
        self.near(land, t, 1)
        self.window(0, self.g[0], far)

        @loop(nb // 4)
        def _(i):
            self.middle(1, old, i, lambda r: self.pointwise(vhat.at[0], 0, far, self.first[0], r, 0))

        relay(0)

        @loop(nbo // 2)
        def _(i):
            for q in range(4):
                self.pointwise(self.zhat, 1, old[3], self.second[1], 4 * i + q, nbo)
                if q < 2:
                    self.gate_two(0, 2 * i + q, old)
                else:
                    j = 2 * i + q - 2
                    self.raw2[j] = block_spectrum(self.fwd6, self.hparts.at[1], j)

        relay(1)
        self.window(1, self.raw2, far)

        @loop(nb // 4)
        def _(i):
            self.middle(0, data, i, lambda r: self.pointwise(vhat.at[1], 0, far, self.first[1], r, 0))

        relay(2)

        @loop(nbo // 2)
        def _(i):
            for q in range(4):
                self.pointwise(self.zhat, 1, far, self.second[0], 4 * i + q, nbo)
                if q % 2 == 0:
                    self.gate_two(1, 2 * i + q // 2, old)

        relay(3)

    def drain(self, data):
        nb, nbo = self.nb, self.nbo

        @loop(nb // 4)
        def _(i):
            self.middle(1, data, i)

        @loop(nbo // 2)
        def _(i):
            for q in range(4):
                self.pointwise(self.zhat, 1, data[3], self.second[1], 4 * i + q, nbo)
                if q % 2 == 0:
                    self.gate_two(0, 2 * i + q // 2, data)

        for k in range(nbo):
            self.gate_two(1, k, data)

    def result(self, c, keep, send):
        hk = self.nbo // 2
        for s in range(self.ybuf.shape[0]):
            for b in range(hk):
                keep[s, b * BLK:(b + 1) * BLK] = self.ybuf[s, c * hk + b]
                send[s, b * BLK:(b + 1) * BLK] = self.ybuf[s, (1 - c) * hk + b].astype(F32)


def out_body(keep, part, w_out, u_in, out, wbuf, w_sem, lhs, keep_v, stage, in_sem, u_v, o_st, o_sem):
    c = lax.rem(lax.axis_index("sp"), 2)
    n_tile, n_seq, n_pos, _ = keep.shape
    half_w = n_tile * TC
    width = 2 * half_w
    n_col, rows = width // TN, width // 4

    def weights(j, slot):
        return [pltpu.make_async_copy(w_out.at[i * rows:(i + 1) * rows, pl.ds(pl.multiple_of(j * TN, TN), TN)],
                                      wbuf.at[slot, i * rows:(i + 1) * rows], w_sem.at[slot, i]) for i in range(4)]

    def flush(j):
        slot = lax.rem(j, 2)
        return pltpu.make_async_copy(o_st.at[slot], out.at[:, :, pl.ds(pl.multiple_of(j * TN, TN), TN)], o_sem.at[slot])

    loads = [pltpu.make_async_copy(part.at[u], stage.at[u], in_sem.at[u]) for u in range(n_tile)]
    loads += [pltpu.make_async_copy(keep.at[u], keep_v.at[u], in_sem.at[n_tile + u]) for u in range(n_tile)]
    for copy in loads:
        copy.start()
    for copy in weights(0, 0):
        copy.start()
    resid = pltpu.make_async_copy(u_in, u_v, in_sem.at[2 * n_tile])
    resid.start()
    for u in range(n_tile):
        loads[u].wait()
        loads[n_tile + u].wait()
        for s in range(n_seq):
            lhs[s, :, pl.ds(pl.multiple_of((1 - c) * half_w + u * TC, TC), TC)] = stage[u, s].astype(BF16)
            lhs[s, :, pl.ds(pl.multiple_of(c * half_w + u * TC, TC), TC)] = keep_v[u, s]
    resid.wait()

    def step(j, carry):
        slot = lax.rem(j, 2)

        @pl.when(j + 1 < n_col)
        def _():
            for copy in weights(j + 1, 1 - slot):
                copy.start()

        for copy in weights(j, slot):
            copy.wait()

        @pl.when(j >= 2)
        def _():
            flush(j - 2).wait()

        cols = pl.ds(pl.multiple_of(j * TN, TN), TN)
        for s in range(n_seq):
            o_st[slot, s] = (u_v[s, :, cols].astype(F32) + dot(lhs[s], wbuf[slot])).astype(BF16)
        flush(j).start()
        return carry

    lax.fori_loop(0, n_col, step, 0)
    for j in (n_col - 2, n_col - 1):
        flush(j).wait()


def solution(mesh):
    fwd3, fwd6, inv6 = transform_tables()

    def local_step(u_in, w_in, b_in, conv_taps, w_out, skip_one, skip_two, filt_one, filt_two):
        n_seq, n_pos, width = u_in.shape
        half_w = width // 2
        n_own = 2 * n_pos
        nb = 2 * n_own // BLK
        nbo = nb // 2
        n_tile = half_w // TC
        small, large = pl.BlockSpec(memory_space=pltpu.VMEM), pl.BlockSpec(memory_space=pl.ANY)
        dma = pltpu.SemaphoreType.DMA

        def shape(dims, dtype=F32):
            return jax.ShapeDtypeStruct(dims, dtype)

        keep, part, *_ = pl.pallas_call(
            main_body,
            in_specs=[small] * 7 + [large] * 5,
            out_specs=[large] * 11,
            out_shape=[
                shape((n_tile, n_seq, n_pos, TC), BF16), shape((n_tile, n_seq, n_pos, TC)),
                shape((n_tile, n_seq, nb + nbo, BLK, TC), BF16), shape((n_tile, n_seq, nb, BLK, TC), BF16),
                shape((n_tile, n_seq, nb, 2 * BLK, TC)), shape((n_tile, 2, nbo, 2 * BLK, TC)),
                shape((n_seq, n_pos, width)), shape((n_seq, n_pos, width)), shape((n_seq, n_pos, width)),
                shape((n_seq, 8, width)), shape((2, n_pos, half_w)),
            ],
            scratch_shapes=[
                pltpu.VMEM((2, n_tile, 2, n_pos, TC), F32),
                dma((2,)), dma((1,)), *[dma((n_seq, n_pos // RC))] * 2, *[dma((n_seq, 3))] * 2, *[dma((n_seq,))] * 2, *[dma((2,))] * 2,
                dma((2, n_tile, 2)), *[dma((n_tile, Q, 2))] * 4, *[dma((n_tile,))] * 2,
            ],
            compiler_params=pltpu.CompilerParams(vmem_limit_bytes=62 << 20, collective_id=0, has_side_effects=True),
            name="hyena_main",
        )(fwd3, fwd6, inv6, b_in.reshape(1, -1), conv_taps, skip_one.reshape(1, -1), skip_two.reshape(1, -1),
          u_in, u_in.astype(F32), w_in, filt_one, filt_two)

        return pl.pallas_call(
            out_body,
            in_specs=[large] * 4,
            out_specs=large,
            out_shape=shape((n_seq, n_pos, width), BF16),
            scratch_shapes=[
                pltpu.VMEM((2, width, TN), BF16), dma((2, 4)),
                pltpu.VMEM((n_seq, n_pos, width), BF16), pltpu.VMEM((n_tile, n_seq, n_pos, TC), BF16), pltpu.VMEM((n_tile, n_seq, n_pos, TC), F32),
                dma((2 * n_tile + 1,)), pltpu.VMEM((n_seq, n_pos, width), BF16), pltpu.VMEM((2, n_seq, n_pos, TN), BF16), dma((2,)),
            ],
            compiler_params=pltpu.CompilerParams(vmem_limit_bytes=60 << 20),
            name="out_proj",
        )(keep, part, w_out, u_in)

    seq_spec = P("dp", "sp", None)
    filt_spec = P("sp", None)
    return jax.shard_map(local_step, mesh=mesh, in_specs=(seq_spec, P(), P(), P(), P(), P(), P(), filt_spec, filt_spec), out_specs=seq_spec, check_vma=False)
```

```python
import functools

import jax
import jax.numpy as jnp
import numpy as np
from jax import lax
from jax.experimental import pallas as pl
from jax.experimental.pallas import tpu as pltpu
from jax.sharding import PartitionSpec as P

F32, BF16 = jnp.float32, jnp.bfloat16
BLK = 128
TN = 512
TC = 256
Q = 2
PAIR = (0, 1)
MESH = pl.DeviceIdType.MESH


def split_table(table):
    parts, rest = [], table.astype(np.float64)
    for _ in range(3):
        part = rest.astype(np.float32).astype(jnp.bfloat16)
        parts.append(part)
        rest = rest - part.astype(np.float64)
    return parts


def transform_tables():
    freq = np.concatenate([np.arange(0, BLK, 2), np.arange(1, BLK, 2)]) + 0.5
    angle = 2.0 * np.pi * freq[:, None] * np.arange(BLK)[None, :] / (2 * BLK)
    fwd = np.concatenate([np.cos(angle), -np.sin(angle)], 0)
    inv = np.concatenate([np.cos(angle).T, -np.sin(angle).T], 1) / BLK
    f1, f2, f3 = split_table(fwd)
    e1, e2, e3 = split_table(inv)
    fwd3 = np.concatenate([f1, f2, f3], 1)
    fwd6 = np.concatenate([f1, f1, f2, f2, f1, f3], 1)
    inv6 = np.concatenate([e1, e1, e2, e2, e1, e3], 1)
    return fwd3, fwd6, inv6


def dot(a, b):
    return jnp.dot(a, b, preferred_element_type=F32)


def split3(x):
    hi = x.astype(BF16)
    rest = x - hi.astype(F32)
    mid = rest.astype(BF16)
    low = (rest - mid.astype(F32)).astype(BF16)
    return hi, mid, low


def stack6(hi, mid, low):
    return jnp.concatenate([hi, mid, hi, mid, low, hi], axis=0)


def split_blocks(src, parts, first):
    for j in range(src.shape[0] // BLK):
        for i, a in enumerate(split3(src[j * BLK:(j + 1) * BLK])):
            parts[first + j, i] = a


def block_spectrum(fwd6_ref, parts, j):
    return dot(fwd6_ref[...], stack6(parts[j, 0], parts[j, 1], parts[j, 2]))


def shifted_add(cur, old, lo, sign):
    re, im = slice(lo, lo + BLK // 2), slice(BLK + lo, BLK + lo + BLK // 2)
    return re, im, cur[re] - sign * old[im], cur[im] + sign * old[re]


SIDES = ((0, 1.0), (BLK // 2, -1.0))


def short_conv(pbuf, t, first, rows):
    return (t[0:1] * pbuf[8 + first:8 + first + rows] + t[1:2] * pbuf[7 + first:7 + first + rows] + t[2:3] * pbuf[6 + first:6 + first + rows]).astype(BF16)


def block_values(fwd3_ref, blk):
    return dot(fwd3_ref[...], jnp.concatenate([blk, blk, blk], axis=0))


def main_body(fwd3_ref, fwd6_ref, inv6_ref, bias_ref, taps_ref, sk1_ref, sk2_ref, u_bf, w_in, f1, f2,
              keep, part, qx, qv, vhat, far, u32, tsrc, u_sw, u_x, u_fw, tail, pf,
              land, ts, tr, os, orr, ws, wr, ss, sr, fs, fr, l_sem, x_send, x_recv, y_send, y_recv, p_send, p_recv):
    sp, dp = lax.axis_index("sp"), lax.axis_index("dp")
    c = lax.rem(sp, 2)
    on_b = sp >= 2
    on_a = jnp.logical_not(on_b)
    other = sp + 1 - 2 * c
    n_seq, n_pos, width = u_bf.shape
    half_w = width // 2
    nt, n_tile, per = half_w // TN, half_w // TC, TN // TC
    n_own, hp = 2 * n_pos, n_pos // 2
    nbo = n_own // BLK
    cuts = (0, hp, hp + hp // 2, n_pos)
    n_cut = len(cuts) - 1

    def remote(src, dst, send, recv, peer):
        return pltpu.make_async_remote_copy(src, dst, send, recv, device_id=peer, device_id_type=MESH)

    def at(start, size):
        return pl.ds(pl.multiple_of(start, size), size)

    def piece(ref, s, h):
        return ref.at[s, cuts[h]:cuts[h + 1]]

    def tail_copy(k):
        return remote(tsrc, tail, ts.at[k], tr.at[0], (dp, 2 + k))

    def over(s, h):
        return remote(piece(u32, s, h), piece(u_x, s, h), os.at[s, h], orr.at[s, h], (dp, lax.rem(sp + 2, 4)))

    def onward(s, h):
        return remote(piece(u_x, s, h), piece(u_fw, s, h), ws.at[s, h], wr.at[s, h], (dp, other))

    def swap_u(s):
        return remote(u32.at[s], u_sw.at[s], ss.at[s], sr.at[s], (dp, other))

    def swap_f(f):
        return remote((f1, f2)[f].at[:, at((1 - c) * half_w, half_w)], pf.at[f], fs.at[f], fr.at[f], (dp, other))

    qr = n_pos // Q

    def filt(src, u, k, q):
        return remote(src.at[q * qr:(q + 1) * qr, at(k * half_w + u * TC, TC)], land.at[dp, u, c, q * qr:(q + 1) * qr],
                      x_send.at[u, q, k], x_recv.at[u, q, c], (dp, 2 + k))

    def landed(u, side, q):
        ref = land.at[dp, u, side, at(q * qr, qr)]
        return remote(ref, ref, x_send.at[u, q, side], x_recv.at[u, q, side], (dp, sp))

    def across(u, side, f, q):
        ref = land.at[f, u, side, at(q * qr, qr)]
        return remote(ref, ref, y_send.at[u, q, side], y_recv.at[u, q, side], (1 - dp, sp))

    def fill(f, u, side, src, start):
        return pltpu.make_async_copy(src.at[:, at(start, TC)], land.at[f, u, side], l_sem.at[f, u, side])

    def column(g, j):
        return (g + j // nt) * width + c * half_w + lax.rem(j, nt) * TN

    def load_rows(stage, st_sem, items):
        def copy(i):
            src, rows, _, _ = items[i]
            return pltpu.make_async_copy(src, stage.at[i % 2, :rows], st_sem.at[i % 2])

        copy(0).start()
        for i, (_, rows, dst, row) in enumerate(items):
            if i + 1 < len(items):
                copy(i + 1).start()
            copy(i).wait()
            dst[pl.ds(pl.multiple_of(row, 16), rows), :] = stage[i % 2, :rows].astype(BF16)

    barrier = pltpu.get_barrier_semaphore()
    for peer in ((dp, other), (dp, lax.rem(sp + 2, 4)), (dp, lax.rem(other + 2, 4)), (1 - dp, sp)):
        pl.semaphore_signal(barrier, inc=1, device_id=peer, device_id_type=MESH)
    pl.semaphore_wait(barrier, 4)

    def widen(raw, wide, tail_raw, tail_wide, in_sem, out_sem):
        def half(ref, s, h):
            return ref.at[s, h * hp:h * hp + hp]

        def load(s, h):
            return pltpu.make_async_copy(half(u_bf, s, h), raw.at[h], in_sem.at[h])

        last_rows = pltpu.make_async_copy(u_bf.at[:, n_pos - 8:], tail_raw, in_sem.at[2])
        last_out = pltpu.make_async_copy(tail_wide, tsrc, out_sem.at[2])
        order = [(s, h) for s in range(n_seq) for h in PAIR]
        last_rows.start()
        load(*order[0]).start()
        last_rows.wait()
        tail_wide[...] = tail_raw[...].astype(F32)
        last_out.start()
        pending = {}
        for (s, h), following in zip(order, order[1:] + [None]):
            if following:
                load(*following).start()
            load(s, h).wait()
            if h in pending:
                pending.pop(h).wait()
            wide[h] = raw[h].astype(F32)
            store = pltpu.make_async_copy(wide.at[h], half(u32, s, h), out_sem.at[h])
            store.start()
            if s + h:
                pending[h] = store
                continue
            last_out.wait()

            @pl.when(sp == 1)
            def _():
                for k in PAIR:
                    tail_copy(k).start()

            store.wait()

            @pl.when(on_a)
            def _():
                over(s, h).start()

        for store in pending.values():
            store.wait()

    pl.run_scoped(
        widen, pltpu.VMEM((2, hp, width), BF16), pltpu.VMEM((2, hp, width), F32), pltpu.VMEM((n_seq, 8, width), BF16),
        pltpu.VMEM((n_seq, 8, width), F32), pltpu.SemaphoreType.DMA((3,)), pltpu.SemaphoreType.DMA((3,)))

    @pl.when(on_a)
    def _():
        for i in range(1, n_seq * n_cut):
            over(*divmod(i, n_cut)).start()
        for which, src in ((0, f1), (1, f2)):
            @pl.when(dp == which)
            def _():
                for u in range(n_tile):
                    for q in range(Q):
                        for k in PAIR:
                            filt(src, u, k, q).start()

    for i in range(n_seq):
        swap_u(i).start()
    for f in PAIR:
        swap_f(f).start()

    def forward(u, q):
        @pl.when(on_b)
        def _():
            for side in PAIR:
                landed(u, side, q).wait_recv()
                across(u, side, dp, q).start()

    def front(wbuf, wsem, lhs, stage, st_sem, lhs_sem, tailbuf, q_st, q_sem, vh_st, vh_sem, pbuf):
        def weights(g, j, slot):
            rows = width // 4
            return [pltpu.make_async_copy(w_in.at[i * rows:(i + 1) * rows, at(column(g, j), TN)],
                                          wbuf.at[slot, i * rows:(i + 1) * rows], wsem.at[slot, i]) for i in range(4)]

        def stream(g, body, following, n=nt):
            def step(j, carry):
                slot = lax.rem(j, 2)

                @pl.when(j + 1 < n)
                def _():
                    for copy in weights(g, j + 1, 1 - slot):
                        copy.start()

                if following is not None:
                    @pl.when(j + 1 == n)
                    def _():
                        following(1 - slot)

                for copy in weights(g, j, slot):
                    copy.wait()
                body(j, slot, bias_ref[:, at(column(g, j), TN)], taps_ref[:, at(column(g, j), TN)])
                return carry

            lax.fori_loop(0, n, step, 0)

        def begin(g):
            def start(slot):
                for copy in weights(g, 0, slot):
                    copy.start()
            return start

        def project(rows_ref, slot, bias):
            return (dot(rows_ref, wbuf[slot]) + bias).astype(BF16).astype(F32)

        tail_rows = n_seq * 8
        begin(0)(0)
        own_rows = [pltpu.make_async_copy(u_bf.at[s], lhs.at[pl.ds(pl.multiple_of(tail_rows + s * n_own + c * n_pos, 16), n_pos)], lhs_sem.at[s])
                    for s in range(n_seq)]
        for copy in own_rows:
            copy.start()
        for s in range(n_seq):
            swap_u(s).wait_recv()
        load_rows(stage, st_sem, [(u_sw.at[s, h * hp:(h + 1) * hp], hp, lhs, tail_rows + s * n_own + (1 - c) * n_pos + h * hp)
                                  for s in range(n_seq) for h in PAIR])
        for copy in own_rows:
            copy.wait()

        @pl.when(on_b)
        def _():
            tail_copy(0).wait_recv()
            copy = pltpu.make_async_copy(tail, tailbuf, lhs_sem.at[0])
            copy.start()
            copy.wait()

        @pl.when(on_a)
        def _():
            tailbuf[...] = jnp.zeros_like(tailbuf)

        lhs[:tail_rows, :] = tailbuf[...].reshape(tail_rows, width).astype(BF16)
        chunk = n_pos

        def own_phase(g, n, dst, spectrum, following):
            def flush(j, slot):
                blocks = pl.ds(nbo * (1 + j // nt), nbo)
                copies = []
                for h in range(per):
                    u = lax.rem(j, nt) * per + h
                    copies.append(pltpu.make_async_copy(q_st.at[slot, h], dst.at[u, :, blocks], q_sem.at[slot, h]))
                    if spectrum:
                        copies.append(pltpu.make_async_copy(vh_st.at[slot, h], vhat.at[u, :, nbo:], vh_sem.at[slot, h]))
                return copies

            def body(j, slot, bias, taps):
                @pl.when(j >= 2)
                def _():
                    for copy in flush(j - 2, slot):
                        copy.wait()

                for i in range(n_seq * n_own // chunk):
                    s, r = divmod(i * chunk, n_own)
                    p = project(lhs[(tail_rows + i * chunk if i else 0):tail_rows + (i + 1) * chunk, :], slot, bias)
                    if i == 0:
                        for k in range(n_seq):
                            pbuf[k, 0:8] = jnp.where(on_b, p[8 * k:8 * k + 8], 0.0)
                        p = p[tail_rows:]
                    pbuf[s, 8 + r:8 + r + chunk] = p
                    q = short_conv(pbuf.at[s], taps, r, chunk)
                    for b in range(chunk // BLK):
                        blk = q[b * BLK:(b + 1) * BLK]
                        for h in range(per):
                            q_st[slot, h, s, r // BLK + b] = blk[:, h * TC:(h + 1) * TC]
                        if spectrum:
                            spec = block_values(fwd3_ref, blk)
                            for h in range(per):
                                vh_st[slot, h, s, r // BLK + b] = spec[:, h * TC:(h + 1) * TC]
                for copy in flush(j, slot):
                    copy.start()

            stream(g, body, following, n)
            for j in (n - 2, n - 1):
                for copy in flush(j, j % 2):
                    copy.wait()

        own_phase(0, 2 * nt, qx, False, begin(2))
        own_phase(2, nt, qv, True, None)

        def far_phase(fin, fin_sem, fout, fout_sem, parts):
            hk = n_pos // BLK

            def fetch(j, slot):
                mine = at(c * half_w + j * TC, TC)
                srcs = (f1.at[:, mine], f2.at[:, mine], pf.at[0, :, at(j * TC, TC)], pf.at[1, :, at(j * TC, TC)])
                return [pltpu.make_async_copy(src, fin.at[slot, i], fin_sem.at[slot, i]) for i, src in enumerate(srcs)]

            def flush(j, slot):
                return pltpu.make_async_copy(fout.at[slot], far.at[j], fout_sem.at[slot])

            for copy in fetch(0, 0):
                copy.start()

            def step(j, carry):
                slot = lax.rem(j, 2)

                @pl.when(j + 1 < n_tile)
                def _():
                    for copy in fetch(j + 1, 1 - slot):
                        copy.start()

                for copy in fetch(j, slot):
                    copy.wait()

                @pl.when(j >= 2)
                def _():
                    flush(j - 2, slot).wait()

                for f in PAIR:
                    split_blocks(fin.at[slot, f], parts.at[f], c * hk)
                    split_blocks(fin.at[slot, 2 + f], parts.at[f], (1 - c) * hk)
                g_ref = fout.at[slot]
                for f in PAIR:
                    for b in range(2 * hk):
                        g_ref[f, b] = block_spectrum(fwd6_ref, parts.at[f], b)
                    for b in range(2 * hk - 1, 0, -1):
                        for lo, sign in SIDES:
                            re, im, new_re, new_im = shifted_add(g_ref.at[f, b], g_ref.at[f, b - 1], lo, sign)
                            g_ref[f, b, re], g_ref[f, b, im] = new_re, new_im
                flush(j, slot).start()
                return carry

            lax.fori_loop(0, n_tile, step, 0)
            for j in (n_tile - 2, n_tile - 1):
                flush(j, j % 2).wait()

        for f in PAIR:
            swap_f(f).wait_recv()
        pl.run_scoped(
            far_phase, pltpu.VMEM((2, 4, n_pos, TC), F32), pltpu.SemaphoreType.DMA((2, 4)),
            pltpu.VMEM((2, 2, nbo, 2 * BLK, TC), F32), pltpu.SemaphoreType.DMA((2,)), pltpu.VMEM((2, nbo, 3, BLK, TC), BF16))

    pl.run_scoped(
        front,
        pltpu.VMEM((2, width, TN), BF16), pltpu.SemaphoreType.DMA((2, 4)),
        pltpu.VMEM((n_seq * n_own + 8 * n_seq, width), BF16),
        pltpu.VMEM((2, hp, width), F32), pltpu.SemaphoreType.DMA((2,)), pltpu.SemaphoreType.DMA((n_seq,)), pltpu.VMEM((n_seq, 8, width), F32),
        pltpu.VMEM((2, per, n_seq, nbo, BLK, TC), BF16), pltpu.SemaphoreType.DMA((2, per)),
        pltpu.VMEM((2, per, n_seq, nbo, 2 * BLK, TC), F32), pltpu.SemaphoreType.DMA((2, per)),
        pltpu.VMEM((n_seq, n_own + 8, TN), F32))

    def prev(wres, w_sem, lhs_p, stage, st_sem, q_st, q_sem, vh_st, vh_sem, pbuf, pstash):
        def weights(j):
            rows = width // 4
            return [pltpu.make_async_copy(w_in.at[i * rows:(i + 1) * rows, at(which(j), TN)],
                                          wres.at[j, i * rows:(i + 1) * rows], w_sem.at[j, i]) for i in range(4)]

        def which(j):
            return 2 * (j // nt) * width + c * half_w + lax.rem(j, nt) * TN

        def begin(j, carry):
            for copy in weights(j):
                copy.start()
            return carry

        lax.fori_loop(0, 2 * nt, begin, 0)

        def rows(s, h):
            n = cuts[h + 1] - cuts[h]

            @pl.when(on_b)
            def _():
                over(s, h).wait_recv()
                onward(s, h).start()
                load_rows(stage, st_sem, [(piece(u_x, s, h), n, lhs_p, c * n)])
                onward(s, h).wait_recv()
                load_rows(stage, st_sem, [(piece(u_fw, s, h), n, lhs_p, (1 - c) * n)])

            @pl.when(on_a)
            def _():
                lhs_p[...] = jnp.zeros_like(lhs_p)

        def project(h, j):
            n = 2 * (cuts[h + 1] - cuts[h])
            return (dot(lhs_p[:n, :], wres[j]) + bias_ref[:, at(which(j), TN)]).astype(BF16)

        def first(s, h):
            n = cuts[h + 1] - cuts[h]

            def body(j, carry):
                if h == 0:
                    @pl.when(s == 0)
                    def _():
                        for copy in weights(j):
                            copy.wait()

                p = project(h, j)
                for core in PAIR:
                    pstash[core, cuts[h]:cuts[h + 1], at(j * TN, TN)] = p[core * n:(core + 1) * n]
                return carry

            lax.fori_loop(0, 2 * nt, body, 0)

        def last(s, u, dst):
            base, spectrum = u * nt, u > 0
            h = n_cut - 1
            n = cuts[h + 1] - cuts[h]

            def flush(j):
                slot, copies = lax.rem(j, 2), []
                for half in range(per):
                    copies.append(pltpu.make_async_copy(q_st.at[slot, half], dst.at[j * per + half, s, :nbo], q_sem.at[slot, half]))
                    if spectrum:
                        copies.append(pltpu.make_async_copy(vh_st.at[slot, half], vhat.at[j * per + half, s, :nbo], vh_sem.at[slot, half]))
                return copies

            def body(j, carry):
                slot = lax.rem(j, 2)

                @pl.when(j >= 2)
                def _():
                    for copy in flush(j - 2):
                        copy.wait()

                taps = taps_ref[:, at(which(base + j), TN)]
                pbuf[0:8] = jnp.zeros((8, TN), F32)
                for core in PAIR:
                    old = pstash[core, :cuts[h], at((base + j) * TN, TN)].astype(F32)
                    pbuf[8 + core * n_pos:8 + core * n_pos + cuts[h]] = jnp.where(on_b, old, 0.0)
                p = project(h, base + j).astype(F32)
                for core in PAIR:
                    start = 8 + core * n_pos + cuts[h]
                    pbuf[start:start + n] = jnp.where(on_b, p[core * n:(core + 1) * n], 0.0)
                for b in range(nbo):
                    blk = short_conv(pbuf, taps, b * BLK, BLK)
                    for half in range(per):
                        q_st[slot, half, b] = blk[:, half * TC:(half + 1) * TC]
                    if spectrum:
                        spec = block_values(fwd3_ref, blk)
                        for half in range(per):
                            vh_st[slot, half, b] = spec[:, half * TC:(half + 1) * TC]
                for copy in flush(j):
                    copy.start()

                @pl.when(jnp.logical_and(s == n_seq - 1, jnp.logical_and(lax.rem(j, Q) == 1, j < nt - Q * u)))
                def _():
                    forward(u, j // Q)
                return carry

            lax.fori_loop(0, nt, body, 0)
            for j in (nt - 2, nt - 1):
                for copy in flush(j):
                    copy.wait()

        def one_seq(s, carry):
            for h in range(n_cut - 1):
                rows(s, h)
                first(s, h)
            rows(s, n_cut - 1)
            last(s, 0, qx)
            last(s, 1, qv)
            return carry

        lax.fori_loop(0, n_seq, one_seq, 0)

    pl.run_scoped(
        prev,
        pltpu.VMEM((2 * nt, width, TN), BF16), pltpu.SemaphoreType.DMA((2 * nt, 4)),
        pltpu.VMEM((2 * hp, width), BF16), pltpu.VMEM((2, hp, width), F32), pltpu.SemaphoreType.DMA((2,)),
        pltpu.VMEM((2, per, nbo, BLK, TC), BF16), pltpu.SemaphoreType.DMA((2, per)),
        pltpu.VMEM((2, per, nbo, 2 * BLK, TC), F32), pltpu.SemaphoreType.DMA((2, per)),
        pltpu.VMEM((n_own + 8, TN), F32), pltpu.VMEM((2, cuts[-2], 2 * half_w), BF16))

    @pl.when(on_a)
    def _():
        for u in range(n_tile):
            for f, own in enumerate((f1, f2)):
                fill(f, u, c, own, c * half_w + u * TC).start()
                fill(f, u, 1 - c, pf.at[f], u * TC).start()

    def conv(x1b, vb, x2b, vhb, farb, in_sem, vh_sem, kst, k_sem, sendbuf, *scratch):
        def fetch(t):
            slot, two = lax.rem(t, 3), lax.rem(t, 2)
            srcs = (qx.at[t, :, :2 * nbo], qv.at[t], qx.at[t, :, 2 * nbo:], far.at[t])
            copies = [pltpu.make_async_copy(r, b.at[slot], in_sem.at[slot, i])
                      for i, (r, b) in enumerate(zip(srcs, (x1b, vb, x2b, farb)))]
            return copies + [pltpu.make_async_copy(vhat.at[t, s], vhb.at[two, s], vh_sem.at[two, s]) for s in range(n_seq)]

        def flush(t):
            slot = lax.rem(t, 2)
            return pltpu.make_async_copy(kst.at[slot], keep.at[t], k_sem.at[slot])

        def swap_y(u):
            return remote(sendbuf.at[lax.rem(u, 2)], part.at[u], p_send.at[u], p_recv.at[u], (dp, other))

        tile = ConvTile(fwd6_ref, inv6_ref, *scratch)

        def inputs(t, back):
            slot, cols = lax.rem(t + 3 - back, 3), at(c * half_w + lax.rem(t + n_tile - back, n_tile) * TC, TC)
            return x1b.at[slot], vb.at[slot], x2b.at[slot], farb.at[slot], sk1_ref[:, cols], sk2_ref[:, cols]

        def emit(t):
            slot = lax.rem(t, 2)

            @pl.when(t >= 2)
            def _():
                flush(t - 2).wait()
                swap_y(t - 2).wait_send()

            tile.result(c, kst.at[slot], sendbuf.at[slot])
            flush(t).start()
            swap_y(t).start()

        for copy in fetch(0):
            copy.start()
        forward(1, Q - 1)

        def step(t, carry):
            @pl.when(t + 1 < n_tile)
            def _():
                for copy in fetch(t + 1):
                    copy.start()

            @pl.when(on_a)
            def _():
                for f in PAIR:
                    for side in PAIR:
                        fill(f, t, side, f1, 0).wait()

            @pl.when(on_b)
            def _():
                for q in range(Q):
                    for side in PAIR:
                        across(t, side, 1 - dp, q).wait_recv()

            for copy in fetch(t):
                copy.wait()

            def relay(q):
                @pl.when(t + 2 < n_tile)
                def _():
                    forward(t + 2, q)

            tile.step(land, t, vhb.at[lax.rem(t, 2)], inputs(t, 0), inputs(t, 1), relay)

            @pl.when(t >= 1)
            def _():
                emit(t - 1)
            return carry

        lax.fori_loop(0, n_tile, step, 0)
        tile.drain(inputs(n_tile, 1))
        emit(n_tile - 1)
        for u in (n_tile - 2, n_tile - 1):
            flush(u).wait()
            swap_y(u).wait_send()
        for u in range(n_tile):
            swap_y(u).wait_recv()

    nb = 2 * nbo
    pl.run_scoped(
        conv,
        pltpu.VMEM((3, n_seq, nb, BLK, TC), BF16), pltpu.VMEM((3, n_seq, nb, BLK, TC), BF16), pltpu.VMEM((3, n_seq, nbo, BLK, TC), BF16),
        pltpu.VMEM((2, n_seq, nb, 2 * BLK, TC), F32), pltpu.VMEM((3, 2, nbo, 2 * BLK, TC), F32),
        pltpu.SemaphoreType.DMA((3, 4)), pltpu.SemaphoreType.DMA((2, n_seq)),
        pltpu.VMEM((2, n_seq, n_pos, TC), BF16), pltpu.SemaphoreType.DMA((2,)), pltpu.VMEM((2, n_seq, n_pos, TC), F32),
        pltpu.VMEM((2, nbo, 3, BLK, TC), BF16),
        pltpu.VMEM((nbo + 1, 2 * BLK, TC), F32), pltpu.VMEM((nbo + 1, 2 * BLK, TC), F32), pltpu.VMEM((nbo, 2 * BLK, TC), F32),
        *[pltpu.VMEM((nb, 3, 2 * BLK, TC), BF16)] * n_seq,
        pltpu.VMEM((nb, 3, BLK, TC), BF16),
        *[pltpu.VMEM((nb, BLK, TC), F32)] * n_seq,
        pltpu.VMEM((nb, 2 * BLK, TC), F32),
        *[pltpu.VMEM((nbo, 3, 2 * BLK, TC), BF16)] * n_seq,
        pltpu.VMEM((n_seq, nbo, BLK, TC), BF16))

    for s in range(n_seq):
        swap_u(s).wait_send()
    for f in PAIR:
        swap_f(f).wait_send()

    @pl.when(sp == 1)
    def _():
        for k in PAIR:
            tail_copy(k).wait_send()

    @pl.when(on_a)
    def _():
        for i in range(n_seq * n_cut):
            over(*divmod(i, n_cut)).wait_send()
        for u in range(n_tile):
            for q in range(Q):
                for k in PAIR:
                    filt(f1, u, k, q).wait_send()

    @pl.when(on_b)
    def _():
        for i in range(n_seq * n_cut):
            onward(*divmod(i, n_cut)).wait_send()
        for u in range(n_tile):
            for q in range(Q):
                for side in PAIR:
                    across(u, side, dp, q).wait_send()


def loop(trips):
    def run(body):
        def step(i, carry):
            body(i)
            return carry
        lax.fori_loop(0, trips, step, 0)
    return run


class ConvTile:
    def __init__(self, fwd6, inv6, hparts, g1, g2, raw2, sp0, sp1, zparts, zv0, zv1, zhat, sq0, sq1, ybuf):
        self.fwd6, self.inv6, self.hparts, self.g, self.raw2 = fwd6, inv6, hparts, (g1, g2), raw2
        self.first, self.second, self.zparts, self.zval, self.zhat, self.ybuf = (sp0, sp1), (sq0, sq1), zparts, (zv0, zv1), zhat, ybuf
        self.nb, self.nbo = sp0.shape[0], sq0.shape[0]

    def near(self, land, t, f):
        for side in PAIR:
            split_blocks(land.at[f, t, side], self.hparts.at[f], side * self.nbo // 2)

    def window(self, f, raw, far):
        g, nbo = self.g[f], self.nbo
        for j in range(nbo, 0, -1):
            cur = far.at[f, 0] if j == nbo else raw.at[j]
            for lo, sign in SIDES:
                re, im, new_re, new_im = shifted_add(cur, raw.at[j - 1], lo, sign)
                g[j, re], g[j, im] = new_re, new_im
        if raw is not g:
            g[0] = raw[0]

    def pointwise(self, xhat, f, far, dst, r, first):
        g, nbo = self.g[f], self.nbo
        re, im = pl.ds(pl.multiple_of(r * 16, 16), 16), pl.ds(pl.multiple_of(BLK + r * 16, 16), 16)
        for k in range(first, self.nb):
            acc_re = acc_im = None
            for j in range(k + 1):
                i = k - j
                gr, gi = (g[i, re], g[i, im]) if i <= nbo else (far[f, i - nbo, re], far[f, i - nbo, im])
                xr, xi = xhat[j, re], xhat[j, im]
                t_re, t_im = xr * gr - xi * gi, xr * gi + xi * gr
                acc_re = t_re if acc_re is None else acc_re + t_re
                acc_im = t_im if acc_im is None else acc_im + t_im
            for part, (a, b) in enumerate(zip(split3(acc_re), split3(acc_im))):
                dst[k - first, part, re], dst[k - first, part, im] = a, b

    def inverse(self, parts, k):
        return dot(self.inv6[...], stack6(parts[k, 0], parts[k, 1], parts[k, 2]))

    def gate_one(self, s, k, data):
        x1, v, _, _, skip, _ = data
        z = x1[s, k].astype(F32) * (self.inverse(self.first[s], k) + skip * v[s, k].astype(F32))
        self.zval[s][k] = z
        for part, a in enumerate(split3(z)):
            self.zparts[k, part] = a

    def spectrum(self, k):
        self.zhat[k] = block_spectrum(self.fwd6, self.zparts, k)

    def gate_two(self, s, k, data):
        y = data[2][s, k].astype(F32) * (self.inverse(self.second[s], k) + data[5] * self.zval[s][self.nbo + k])
        self.ybuf[s, k] = y.astype(BF16)

    def middle(self, s, data, i, point=None):
        for q in range(4):
            if point is not None:
                point(4 * i + q)
            for k in PAIR:
                if q < 2:
                    self.gate_one(s, 4 * i + 2 * q + k, data)
                else:
                    self.spectrum(4 * i + 2 * (q - 2) + k)

    def step(self, land, t, vhat, data, old, relay):
        nb, nbo = self.nb, self.nbo
        far = data[3]
        self.near(land, t, 0)
        for j in range(nbo):
            self.g[0][j] = block_spectrum(self.fwd6, self.hparts.at[0], j)
        self.near(land, t, 1)
        self.window(0, self.g[0], far)

        @loop(nb // 4)
        def _(i):
            self.middle(1, old, i, lambda r: self.pointwise(vhat.at[0], 0, far, self.first[0], r, 0))


        @loop(nbo // 2)
        def _(i):
            for q in range(4):
                self.pointwise(self.zhat, 1, old[3], self.second[1], 4 * i + q, nbo)
                if q < 2:
                    self.gate_two(0, 2 * i + q, old)
                else:
                    j = 2 * i + q - 2
                    self.raw2[j] = block_spectrum(self.fwd6, self.hparts.at[1], j)

        relay(0)
        self.window(1, self.raw2, far)

        @loop(nb // 4)
        def _(i):
            self.middle(0, data, i, lambda r: self.pointwise(vhat.at[1], 0, far, self.first[1], r, 0))

        @loop(nbo // 2)
        def _(i):
            for q in range(4):
                self.pointwise(self.zhat, 1, far, self.second[0], 4 * i + q, nbo)
                if q % 2 == 0:
                    self.gate_two(1, 2 * i + q // 2, old)

        relay(1)

    def drain(self, data):
        nb, nbo = self.nb, self.nbo

        @loop(nb // 4)
        def _(i):
            self.middle(1, data, i)

        @loop(nbo // 2)
        def _(i):
            for q in range(4):
                self.pointwise(self.zhat, 1, data[3], self.second[1], 4 * i + q, nbo)
                if q % 2 == 0:
                    self.gate_two(0, 2 * i + q // 2, data)

        for k in range(nbo):
            self.gate_two(1, k, data)

    def result(self, c, keep, send):
        hk = self.nbo // 2
        for s in range(self.ybuf.shape[0]):
            for b in range(hk):
                keep[s, b * BLK:(b + 1) * BLK] = self.ybuf[s, c * hk + b]
                send[s, b * BLK:(b + 1) * BLK] = self.ybuf[s, (1 - c) * hk + b].astype(F32)


def out_body(keep, part, w_out, u_in, out, wbuf, w_sem, lhs, keep_v, stage, in_sem, u_v, o_st, o_sem):
    c = lax.rem(lax.axis_index("sp"), 2)
    n_tile, n_seq, n_pos, _ = keep.shape
    half_w = n_tile * TC
    width = 2 * half_w
    n_col, rows = width // TN, width // 4

    def weights(j, slot):
        cols = pl.ds(pl.multiple_of(j * TN, TN), TN)
        return [pltpu.make_async_copy(w_out.at[i * rows:(i + 1) * rows, cols],
                                      wbuf.at[slot, i * rows:(i + 1) * rows], w_sem.at[slot, i]) for i in range(4)] + [
                    pltpu.make_async_copy(u_in.at[:, :, cols], u_v.at[slot], w_sem.at[slot, 4])]

    def flush(j):
        slot = lax.rem(j, 2)
        return pltpu.make_async_copy(o_st.at[slot], out.at[:, :, pl.ds(pl.multiple_of(j * TN, TN), TN)], o_sem.at[slot])

    loads = [pltpu.make_async_copy(part.at[u], stage.at[u], in_sem.at[u]) for u in range(n_tile)]
    loads += [pltpu.make_async_copy(keep.at[u], keep_v.at[u], in_sem.at[n_tile + u]) for u in range(n_tile)]
    for copy in loads:
        copy.start()
    for copy in weights(0, 0):
        copy.start()
    for u in range(n_tile):
        loads[u].wait()
        loads[n_tile + u].wait()
        for s in range(n_seq):
            lhs[s, :, pl.ds(pl.multiple_of((1 - c) * half_w + u * TC, TC), TC)] = stage[u, s].astype(BF16)
            lhs[s, :, pl.ds(pl.multiple_of(c * half_w + u * TC, TC), TC)] = keep_v[u, s]

    def step(j, carry):
        slot = lax.rem(j, 2)

        @pl.when(j + 1 < n_col)
        def _():
            for copy in weights(j + 1, 1 - slot):
                copy.start()

        for copy in weights(j, slot):
            copy.wait()

        @pl.when(j >= 2)
        def _():
            flush(j - 2).wait()

        for s in range(n_seq):
            o_st[slot, s] = (u_v[slot, s].astype(F32) + dot(lhs[s], wbuf[slot])).astype(BF16)
        flush(j).start()
        return carry

    lax.fori_loop(0, n_col, step, 0)
    for j in (n_col - 2, n_col - 1):
        flush(j).wait()


def solution(mesh):
    fwd3, fwd6, inv6 = transform_tables()

    def local_step(u_in, w_in, b_in, conv_taps, w_out, skip_one, skip_two, filt_one, filt_two):
        n_seq, n_pos, width = u_in.shape
        half_w = width // 2
        n_own = 2 * n_pos
        nb = 2 * n_own // BLK
        nbo = nb // 2
        n_tile = half_w // TC
        small, large = pl.BlockSpec(memory_space=pltpu.VMEM), pl.BlockSpec(memory_space=pl.ANY)
        dma = pltpu.SemaphoreType.DMA

        def shape(dims, dtype=F32):
            return jax.ShapeDtypeStruct(dims, dtype)

        keep, part, *_ = pl.pallas_call(
            main_body,
            in_specs=[small] * 7 + [large] * 4,
            out_specs=[large] * 13,
            out_shape=[
                shape((n_tile, n_seq, n_pos, TC), BF16), shape((n_tile, n_seq, n_pos, TC)),
                shape((n_tile, n_seq, nb + nbo, BLK, TC), BF16), shape((n_tile, n_seq, nb, BLK, TC), BF16),
                shape((n_tile, n_seq, nb, 2 * BLK, TC)), shape((n_tile, 2, nbo, 2 * BLK, TC)),
                shape((n_seq, n_pos, width)), shape((n_seq, 8, width)), *[shape((n_seq, n_pos, width))] * 3,
                shape((n_seq, 8, width)), shape((2, n_pos, half_w)),
            ],
            scratch_shapes=[
                pltpu.VMEM((2, n_tile, 2, n_pos, TC), F32),
                dma((2,)), dma((1,)), *[dma((n_seq, 3))] * 4, *[dma((n_seq,))] * 2, *[dma((2,))] * 2,
                dma((2, n_tile, 2)), *[dma((n_tile, Q, 2))] * 4, *[dma((n_tile,))] * 2,
            ],
            compiler_params=pltpu.CompilerParams(vmem_limit_bytes=62 << 20, collective_id=0, has_side_effects=True),
            name="hyena_main",
        )(fwd3, fwd6, inv6, b_in.reshape(1, -1), conv_taps, skip_one.reshape(1, -1), skip_two.reshape(1, -1),
          u_in, w_in, filt_one, filt_two)

        return pl.pallas_call(
            out_body,
            in_specs=[large] * 4,
            out_specs=large,
            out_shape=shape((n_seq, n_pos, width), BF16),
            scratch_shapes=[
                pltpu.VMEM((2, width, TN), BF16), dma((2, 5)),
                pltpu.VMEM((n_seq, n_pos, width), BF16), pltpu.VMEM((n_tile, n_seq, n_pos, TC), BF16), pltpu.VMEM((n_tile, n_seq, n_pos, TC), F32),
                dma((2 * n_tile,)), pltpu.VMEM((2, n_seq, n_pos, TN), BF16), pltpu.VMEM((2, n_seq, n_pos, TN), BF16), dma((2,)),
            ],
            compiler_params=pltpu.CompilerParams(vmem_limit_bytes=60 << 20),
            name="out_proj",
        )(keep, part, w_out, u_in)

    seq_spec = P("dp", "sp", None)
    filt_spec = P("sp", None)
    return jax.shard_map(local_step, mesh=mesh, in_specs=(seq_spec, P(), P(), P(), P(), P(), P(), filt_spec, filt_spec), out_specs=seq_spec, check_vma=False)
```

```python
import functools

import jax
import jax.numpy as jnp
import numpy as np
from jax import lax
from jax.experimental import pallas as pl
from jax.experimental.pallas import tpu as pltpu
from jax.sharding import PartitionSpec as P

F32, BF16 = jnp.float32, jnp.bfloat16
BLK = 128
TN = 512
TC = 256
Q = 2
PAIR = (0, 1)
MESH = pl.DeviceIdType.MESH


def split_table(table):
    parts, rest = [], table.astype(np.float64)
    for _ in range(3):
        part = rest.astype(np.float32).astype(jnp.bfloat16)
        parts.append(part)
        rest = rest - part.astype(np.float64)
    return parts


def transform_tables():
    freq = np.concatenate([np.arange(0, BLK, 2), np.arange(1, BLK, 2)]) + 0.5
    angle = 2.0 * np.pi * freq[:, None] * np.arange(BLK)[None, :] / (2 * BLK)
    fwd = np.concatenate([np.cos(angle), -np.sin(angle)], 0)
    inv = np.concatenate([np.cos(angle).T, -np.sin(angle).T], 1) / BLK
    f1, f2, f3 = split_table(fwd)
    e1, e2, e3 = split_table(inv)
    fwd3 = np.concatenate([f1, f2, f3], 1)
    fwd6 = np.concatenate([f1, f1, f2, f2, f1, f3], 1)
    inv6 = np.concatenate([e1, e1, e2, e2, e1, e3], 1)
    return fwd3, fwd6, inv6


def dot(a, b):
    return jnp.dot(a, b, preferred_element_type=F32)


def split3(x):
    hi = x.astype(BF16)
    rest = x - hi.astype(F32)
    mid = rest.astype(BF16)
    low = (rest - mid.astype(F32)).astype(BF16)
    return hi, mid, low


def stack6(hi, mid, low):
    return jnp.concatenate([hi, mid, hi, mid, low, hi], axis=0)


def split_blocks(src, parts, first):
    for j in range(src.shape[0] // BLK):
        for i, a in enumerate(split3(src[j * BLK:(j + 1) * BLK])):
            parts[first + j, i] = a


def block_spectrum(fwd6_ref, parts, j):
    return dot(fwd6_ref[...], stack6(parts[j, 0], parts[j, 1], parts[j, 2]))


def shifted_add(cur, old, lo, sign):
    re, im = slice(lo, lo + BLK // 2), slice(BLK + lo, BLK + lo + BLK // 2)
    return re, im, cur[re] - sign * old[im], cur[im] + sign * old[re]


SIDES = ((0, 1.0), (BLK // 2, -1.0))


def short_conv(pbuf, t, first, rows):
    return (t[0:1] * pbuf[8 + first:8 + first + rows] + t[1:2] * pbuf[7 + first:7 + first + rows] + t[2:3] * pbuf[6 + first:6 + first + rows]).astype(BF16)


def block_values(fwd3_ref, blk):
    return dot(fwd3_ref[...], jnp.concatenate([blk, blk, blk], axis=0))


def main_body(fwd3_ref, fwd6_ref, inv6_ref, bias_ref, taps_ref, sk1_ref, sk2_ref, u_bf, w_in, f1, f2,
              keep, part, qx, qv, vhat, far, u32, tsrc, u_sw, u_x, tail, pf,
              land, ts, tr, os, orr, ws, wr, ss, sr, fs, fr, l_sem, x_send, x_recv, y_send, y_recv, p_send, p_recv):
    sp, dp = lax.axis_index("sp"), lax.axis_index("dp")
    c = lax.rem(sp, 2)
    on_b = sp >= 2
    on_a = jnp.logical_not(on_b)
    other = sp + 1 - 2 * c
    n_seq, n_pos, width = u_bf.shape
    half_w = width // 2
    nt, n_tile, per = half_w // TN, half_w // TC, TN // TC
    n_own, hp = 2 * n_pos, n_pos // 2
    nbo = n_own // BLK
    cuts = (0, hp, hp + hp // 2, n_pos)
    n_cut = len(cuts) - 1

    def remote(src, dst, send, recv, peer):
        return pltpu.make_async_remote_copy(src, dst, send, recv, device_id=peer, device_id_type=MESH)

    def at(start, size):
        return pl.ds(pl.multiple_of(start, size), size)

    def share(s, h, k):
        rows = (cuts[h + 1] - cuts[h]) // 2
        return s, pl.ds(pl.multiple_of(cuts[h] + k * rows, rows), rows)

    def tail_copy():
        return remote(tsrc, tail, ts.at[0], tr.at[0], (dp, 3))

    def tail_across():
        return remote(tail, tail, ts.at[0], tr.at[0], (dp, other))

    def over(s, h, k):
        s, rows = share(s, h, k)
        return remote(u32.at[s, rows], u_x.at[c, s, rows], os.at[s, h, k], orr.at[s, h, c], (dp, 2 + k))

    def arrived(s, h, src):
        at_s, rows = share(s, h, 0)
        ref = u_x.at[src, at_s, rows]
        return remote(ref, ref, os.at[s, h, src], orr.at[s, h, src], (dp, sp))

    def onward(s, h, src):
        at_s, rows = share(s, h, c)
        ref = u_x.at[src, at_s, rows]
        return remote(ref, ref, ws.at[s, h, src], wr.at[s, h, src], (dp, other))

    def swap_u(s):
        return remote(u32.at[s], u_sw.at[s], ss.at[s], sr.at[s], (dp, other))

    def swap_f(f):
        return remote((f1, f2)[f].at[:, at((1 - c) * half_w, half_w)], pf.at[f], fs.at[f], fr.at[f], (dp, other))

    qr = n_pos // Q

    def filt(src, u, k, q):
        return remote(src.at[q * qr:(q + 1) * qr, at(k * half_w + u * TC, TC)], land.at[dp, u, c, q * qr:(q + 1) * qr],
                      x_send.at[u, q, k], x_recv.at[u, q, c], (dp, 2 + k))

    def landed(u, side, q):
        ref = land.at[dp, u, side, at(q * qr, qr)]
        return remote(ref, ref, x_send.at[u, q, side], x_recv.at[u, q, side], (dp, sp))

    def across(u, side, f, q):
        ref = land.at[f, u, side, at(q * qr, qr)]
        return remote(ref, ref, y_send.at[u, q, side], y_recv.at[u, q, side], (1 - dp, sp))

    def fill(f, u, side, src, start):
        return pltpu.make_async_copy(src.at[:, at(start, TC)], land.at[f, u, side], l_sem.at[f, u, side])

    def column(g, j):
        return (g + j // nt) * width + c * half_w + lax.rem(j, nt) * TN

    def load_rows(stage, st_sem, items):
        def copy(i):
            src, rows, _, _ = items[i]
            return pltpu.make_async_copy(src, stage.at[i % 2, :rows], st_sem.at[i % 2])

        copy(0).start()
        for i, (_, rows, dst, row) in enumerate(items):
            if i + 1 < len(items):
                copy(i + 1).start()
            copy(i).wait()
            dst[pl.ds(pl.multiple_of(row, 16), rows), :] = stage[i % 2, :rows].astype(BF16)

    barrier = pltpu.get_barrier_semaphore()
    for peer in ((dp, other), (dp, lax.rem(sp + 2, 4)), (dp, lax.rem(other + 2, 4)), (1 - dp, sp)):
        pl.semaphore_signal(barrier, inc=1, device_id=peer, device_id_type=MESH)
    pl.semaphore_wait(barrier, 4)

    def widen(raw, wide, tail_raw, tail_wide, in_sem, out_sem):
        def half(ref, s, h):
            return ref.at[s, h * hp:h * hp + hp]

        def load(s, h):
            return pltpu.make_async_copy(half(u_bf, s, h), raw.at[h], in_sem.at[h])

        last_rows = pltpu.make_async_copy(u_bf.at[:, n_pos - 8:], tail_raw, in_sem.at[2])
        last_out = pltpu.make_async_copy(tail_wide, tsrc, out_sem.at[2])
        order = [(s, h) for s in range(n_seq) for h in PAIR]
        last_rows.start()
        load(*order[0]).start()
        last_rows.wait()
        tail_wide[...] = tail_raw[...].astype(F32)
        last_out.start()
        pending = {}
        for (s, h), following in zip(order, order[1:] + [None]):
            if following:
                load(*following).start()
            load(s, h).wait()
            if h in pending:
                pending.pop(h).wait()
            wide[h] = raw[h].astype(F32)
            store = pltpu.make_async_copy(wide.at[h], half(u32, s, h), out_sem.at[h])
            store.start()
            if s + h:
                pending[h] = store
                continue
            last_out.wait()

            @pl.when(sp == 1)
            def _():
                tail_copy().start()

            store.wait()

            @pl.when(on_a)
            def _():
                for k in PAIR:
                    over(s, h, k).start()

        for store in pending.values():
            store.wait()

    pl.run_scoped(
        widen, pltpu.VMEM((2, hp, width), BF16), pltpu.VMEM((2, hp, width), F32), pltpu.VMEM((n_seq, 8, width), BF16),
        pltpu.VMEM((n_seq, 8, width), F32), pltpu.SemaphoreType.DMA((3,)), pltpu.SemaphoreType.DMA((3,)))

    @pl.when(on_a)
    def _():
        for i in range(1, n_seq * n_cut):
            for k in PAIR:
                over(*divmod(i, n_cut), k).start()
        for which, src in ((0, f1), (1, f2)):
            @pl.when(dp == which)
            def _():
                for u in range(n_tile):
                    for q in range(Q):
                        for k in PAIR:
                            filt(src, u, k, q).start()

    for i in range(n_seq):
        swap_u(i).start()
    for f in PAIR:
        swap_f(f).start()

    def forward(u, q):
        @pl.when(on_b)
        def _():
            for side in PAIR:
                landed(u, side, q).wait_recv()
                across(u, side, dp, q).start()

    def front(wbuf, wsem, lhs, stage, st_sem, lhs_sem, tailbuf, q_st, q_sem, vh_st, vh_sem, pbuf):
        def weights(g, j, slot):
            rows = width // 4
            return [pltpu.make_async_copy(w_in.at[i * rows:(i + 1) * rows, at(column(g, j), TN)],
                                          wbuf.at[slot, i * rows:(i + 1) * rows], wsem.at[slot, i]) for i in range(4)]

        def stream(g, body, following, n=nt):
            def step(j, carry):
                slot = lax.rem(j, 2)

                @pl.when(j + 1 < n)
                def _():
                    for copy in weights(g, j + 1, 1 - slot):
                        copy.start()

                if following is not None:
                    @pl.when(j + 1 == n)
                    def _():
                        following(1 - slot)

                for copy in weights(g, j, slot):
                    copy.wait()
                body(j, slot, bias_ref[:, at(column(g, j), TN)], taps_ref[:, at(column(g, j), TN)])
                return carry

            lax.fori_loop(0, n, step, 0)

        def begin(g):
            def start(slot):
                for copy in weights(g, 0, slot):
                    copy.start()
            return start

        def project(rows_ref, slot, bias):
            return (dot(rows_ref, wbuf[slot]) + bias).astype(BF16).astype(F32)

        tail_rows = n_seq * 8
        begin(0)(0)
        own_rows = [pltpu.make_async_copy(u_bf.at[s], lhs.at[pl.ds(pl.multiple_of(tail_rows + s * n_own + c * n_pos, 16), n_pos)], lhs_sem.at[s])
                    for s in range(n_seq)]
        for copy in own_rows:
            copy.start()
        for s in range(n_seq):
            swap_u(s).wait_recv()
        load_rows(stage, st_sem, [(u_sw.at[s, h * hp:(h + 1) * hp], hp, lhs, tail_rows + s * n_own + (1 - c) * n_pos + h * hp)
                                  for s in range(n_seq) for h in PAIR])
        for copy in own_rows:
            copy.wait()

        @pl.when(on_b)
        def _():
            tail_copy().wait_recv()

            @pl.when(sp == 3)
            def _():
                tail_across().start()

            copy = pltpu.make_async_copy(tail, tailbuf, lhs_sem.at[0])
            copy.start()
            copy.wait()

        @pl.when(on_a)
        def _():
            tailbuf[...] = jnp.zeros_like(tailbuf)

        lhs[:tail_rows, :] = tailbuf[...].reshape(tail_rows, width).astype(BF16)
        chunk = n_pos

        def own_phase(g, n, dst, spectrum, following):
            def flush(j, slot):
                blocks = pl.ds(nbo * (1 + j // nt), nbo)
                copies = []
                for h in range(per):
                    u = lax.rem(j, nt) * per + h
                    copies.append(pltpu.make_async_copy(q_st.at[slot, h], dst.at[u, :, blocks], q_sem.at[slot, h]))
                    if spectrum:
                        copies.append(pltpu.make_async_copy(vh_st.at[slot, h], vhat.at[u, :, nbo:], vh_sem.at[slot, h]))
                return copies

            def body(j, slot, bias, taps):
                @pl.when(j >= 2)
                def _():
                    for copy in flush(j - 2, slot):
                        copy.wait()

                for i in range(n_seq * n_own // chunk):
                    s, r = divmod(i * chunk, n_own)
                    p = project(lhs[(tail_rows + i * chunk if i else 0):tail_rows + (i + 1) * chunk, :], slot, bias)
                    if i == 0:
                        for k in range(n_seq):
                            pbuf[k, 0:8] = jnp.where(on_b, p[8 * k:8 * k + 8], 0.0)
                        p = p[tail_rows:]
                    pbuf[s, 8 + r:8 + r + chunk] = p
                    q = short_conv(pbuf.at[s], taps, r, chunk)
                    for b in range(chunk // BLK):
                        blk = q[b * BLK:(b + 1) * BLK]
                        for h in range(per):
                            q_st[slot, h, s, r // BLK + b] = blk[:, h * TC:(h + 1) * TC]
                        if spectrum:
                            spec = block_values(fwd3_ref, blk)
                            for h in range(per):
                                vh_st[slot, h, s, r // BLK + b] = spec[:, h * TC:(h + 1) * TC]
                for copy in flush(j, slot):
                    copy.start()

            stream(g, body, following, n)
            for j in (n - 2, n - 1):
                for copy in flush(j, j % 2):
                    copy.wait()

        own_phase(0, 2 * nt, qx, False, begin(2))
        own_phase(2, nt, qv, True, None)

        def far_phase(fin, fin_sem, fout, fout_sem, parts):
            hk = n_pos // BLK

            def fetch(j, slot):
                mine = at(c * half_w + j * TC, TC)
                srcs = (f1.at[:, mine], f2.at[:, mine], pf.at[0, :, at(j * TC, TC)], pf.at[1, :, at(j * TC, TC)])
                return [pltpu.make_async_copy(src, fin.at[slot, i], fin_sem.at[slot, i]) for i, src in enumerate(srcs)]

            def flush(j, slot):
                return pltpu.make_async_copy(fout.at[slot], far.at[j], fout_sem.at[slot])

            for copy in fetch(0, 0):
                copy.start()

            def step(j, carry):
                slot = lax.rem(j, 2)

                @pl.when(j + 1 < n_tile)
                def _():
                    for copy in fetch(j + 1, 1 - slot):
                        copy.start()

                for copy in fetch(j, slot):
                    copy.wait()

                @pl.when(j >= 2)
                def _():
                    flush(j - 2, slot).wait()

                for f in PAIR:
                    split_blocks(fin.at[slot, f], parts.at[f], c * hk)
                    split_blocks(fin.at[slot, 2 + f], parts.at[f], (1 - c) * hk)
                g_ref = fout.at[slot]
                for f in PAIR:
                    for b in range(2 * hk):
                        g_ref[f, b] = block_spectrum(fwd6_ref, parts.at[f], b)
                    for b in range(2 * hk - 1, 0, -1):
                        for lo, sign in SIDES:
                            re, im, new_re, new_im = shifted_add(g_ref.at[f, b], g_ref.at[f, b - 1], lo, sign)
                            g_ref[f, b, re], g_ref[f, b, im] = new_re, new_im
                flush(j, slot).start()
                return carry

            lax.fori_loop(0, n_tile, step, 0)
            for j in (n_tile - 2, n_tile - 1):
                flush(j, j % 2).wait()

        for f in PAIR:
            swap_f(f).wait_recv()
        pl.run_scoped(
            far_phase, pltpu.VMEM((2, 4, n_pos, TC), F32), pltpu.SemaphoreType.DMA((2, 4)),
            pltpu.VMEM((2, 2, nbo, 2 * BLK, TC), F32), pltpu.SemaphoreType.DMA((2,)), pltpu.VMEM((2, nbo, 3, BLK, TC), BF16))

    pl.run_scoped(
        front,
        pltpu.VMEM((2, width, TN), BF16), pltpu.SemaphoreType.DMA((2, 4)),
        pltpu.VMEM((n_seq * n_own + 8 * n_seq, width), BF16),
        pltpu.VMEM((2, hp, width), F32), pltpu.SemaphoreType.DMA((2,)), pltpu.SemaphoreType.DMA((n_seq,)), pltpu.VMEM((n_seq, 8, width), F32),
        pltpu.VMEM((2, per, n_seq, nbo, BLK, TC), BF16), pltpu.SemaphoreType.DMA((2, per)),
        pltpu.VMEM((2, per, n_seq, nbo, 2 * BLK, TC), F32), pltpu.SemaphoreType.DMA((2, per)),
        pltpu.VMEM((n_seq, n_own + 8, TN), F32))

    def prev(wres, w_sem, lhs_p, stage, st_sem, q_st, q_sem, vh_st, vh_sem, pbuf, pstash):
        def weights(j):
            rows = width // 4
            return [pltpu.make_async_copy(w_in.at[i * rows:(i + 1) * rows, at(which(j), TN)],
                                          wres.at[j, i * rows:(i + 1) * rows], w_sem.at[j, i]) for i in range(4)]

        def which(j):
            return 2 * (j // nt) * width + c * half_w + lax.rem(j, nt) * TN

        def begin(j, carry):
            for copy in weights(j):
                copy.start()
            return carry

        lax.fori_loop(0, 2 * nt, begin, 0)

        def rows(s, h):
            n = cuts[h + 1] - cuts[h]

            @pl.when(on_b)
            def _():
                for src in PAIR:
                    arrived(s, h, src).wait_recv()
                    onward(s, h, src).start()
                for src in PAIR:
                    onward(s, h, src).wait_recv()
                load_rows(stage, st_sem, [(u_x.at[src, s, cuts[h]:cuts[h + 1]], n, lhs_p, src * n) for src in PAIR])

            @pl.when(on_a)
            def _():
                lhs_p[...] = jnp.zeros_like(lhs_p)

        def project(h, j):
            n = 2 * (cuts[h + 1] - cuts[h])
            return (dot(lhs_p[:n, :], wres[j]) + bias_ref[:, at(which(j), TN)]).astype(BF16)

        def first(s, h):
            n = cuts[h + 1] - cuts[h]

            def body(j, carry):
                if h == 0:
                    @pl.when(s == 0)
                    def _():
                        for copy in weights(j):
                            copy.wait()

                p = project(h, j)
                for core in PAIR:
                    pstash[core, cuts[h]:cuts[h + 1], at(j * TN, TN)] = p[core * n:(core + 1) * n]
                return carry

            lax.fori_loop(0, 2 * nt, body, 0)

        def last(s, u, dst):
            base, spectrum = u * nt, u > 0
            h = n_cut - 1
            n = cuts[h + 1] - cuts[h]

            def flush(j):
                slot, copies = lax.rem(j, 2), []
                for half in range(per):
                    copies.append(pltpu.make_async_copy(q_st.at[slot, half], dst.at[j * per + half, s, :nbo], q_sem.at[slot, half]))
                    if spectrum:
                        copies.append(pltpu.make_async_copy(vh_st.at[slot, half], vhat.at[j * per + half, s, :nbo], vh_sem.at[slot, half]))
                return copies

            def body(j, carry):
                slot = lax.rem(j, 2)

                @pl.when(j >= 2)
                def _():
                    for copy in flush(j - 2):
                        copy.wait()

                taps = taps_ref[:, at(which(base + j), TN)]
                pbuf[0:8] = jnp.zeros((8, TN), F32)
                for core in PAIR:
                    old = pstash[core, :cuts[h], at((base + j) * TN, TN)].astype(F32)
                    pbuf[8 + core * n_pos:8 + core * n_pos + cuts[h]] = jnp.where(on_b, old, 0.0)
                p = project(h, base + j).astype(F32)
                for core in PAIR:
                    start = 8 + core * n_pos + cuts[h]
                    pbuf[start:start + n] = jnp.where(on_b, p[core * n:(core + 1) * n], 0.0)
                for b in range(nbo):
                    blk = short_conv(pbuf, taps, b * BLK, BLK)
                    for half in range(per):
                        q_st[slot, half, b] = blk[:, half * TC:(half + 1) * TC]
                    if spectrum:
                        spec = block_values(fwd3_ref, blk)
                        for half in range(per):
                            vh_st[slot, half, b] = spec[:, half * TC:(half + 1) * TC]
                for copy in flush(j):
                    copy.start()

                @pl.when(jnp.logical_and(s == n_seq - 1, jnp.logical_and(lax.rem(j, Q) == 1, j < nt - Q * u)))
                def _():
                    forward(u, j // Q)
                return carry

            lax.fori_loop(0, nt, body, 0)
            for j in (nt - 2, nt - 1):
                for copy in flush(j):
                    copy.wait()

        def one_seq(s, carry):
            for h in range(n_cut - 1):
                rows(s, h)
                first(s, h)
            rows(s, n_cut - 1)
            last(s, 0, qx)
            last(s, 1, qv)
            return carry

        lax.fori_loop(0, n_seq, one_seq, 0)

    pl.run_scoped(
        prev,
        pltpu.VMEM((2 * nt, width, TN), BF16), pltpu.SemaphoreType.DMA((2 * nt, 4)),
        pltpu.VMEM((2 * hp, width), BF16), pltpu.VMEM((2, hp, width), F32), pltpu.SemaphoreType.DMA((2,)),
        pltpu.VMEM((2, per, nbo, BLK, TC), BF16), pltpu.SemaphoreType.DMA((2, per)),
        pltpu.VMEM((2, per, nbo, 2 * BLK, TC), F32), pltpu.SemaphoreType.DMA((2, per)),
        pltpu.VMEM((n_own + 8, TN), F32), pltpu.VMEM((2, cuts[-2], 2 * half_w), BF16))

    @pl.when(on_a)
    def _():
        for u in range(n_tile):
            for f, own in enumerate((f1, f2)):
                fill(f, u, c, own, c * half_w + u * TC).start()
                fill(f, u, 1 - c, pf.at[f], u * TC).start()

    def conv(x1b, vb, x2b, vhb, farb, in_sem, vh_sem, kst, k_sem, sendbuf, *scratch):
        def fetch(t):
            slot, two = lax.rem(t, 3), lax.rem(t, 2)
            srcs = (qx.at[t, :, :2 * nbo], qv.at[t], qx.at[t, :, 2 * nbo:], far.at[t])
            copies = [pltpu.make_async_copy(r, b.at[slot], in_sem.at[slot, i])
                      for i, (r, b) in enumerate(zip(srcs, (x1b, vb, x2b, farb)))]
            return copies + [pltpu.make_async_copy(vhat.at[t, s], vhb.at[two, s], vh_sem.at[two, s]) for s in range(n_seq)]

        def flush(t):
            slot = lax.rem(t, 2)
            return pltpu.make_async_copy(kst.at[slot], keep.at[t], k_sem.at[slot])

        def swap_y(u):
            return remote(sendbuf.at[lax.rem(u, 2)], part.at[u], p_send.at[u], p_recv.at[u], (dp, other))

        tile = ConvTile(fwd6_ref, inv6_ref, *scratch)

        def inputs(t, back):
            slot, cols = lax.rem(t + 3 - back, 3), at(c * half_w + lax.rem(t + n_tile - back, n_tile) * TC, TC)
            return x1b.at[slot], vb.at[slot], x2b.at[slot], farb.at[slot], sk1_ref[:, cols], sk2_ref[:, cols]

        def emit(t):
            slot = lax.rem(t, 2)

            @pl.when(t >= 2)
            def _():
                flush(t - 2).wait()
                swap_y(t - 2).wait_send()

            tile.result(c, kst.at[slot], sendbuf.at[slot])
            flush(t).start()
            swap_y(t).start()

        for copy in fetch(0):
            copy.start()
        forward(1, Q - 1)

        def step(t, carry):
            @pl.when(t + 1 < n_tile)
            def _():
                for copy in fetch(t + 1):
                    copy.start()

            @pl.when(on_a)
            def _():
                for f in PAIR:
                    for side in PAIR:
                        fill(f, t, side, f1, 0).wait()

            @pl.when(on_b)
            def _():
                for q in range(Q):
                    for side in PAIR:
                        across(t, side, 1 - dp, q).wait_recv()

            for copy in fetch(t):
                copy.wait()

            def relay(q):
                @pl.when(t + 2 < n_tile)
                def _():
                    forward(t + 2, q)

            tile.step(land, t, vhb.at[lax.rem(t, 2)], inputs(t, 0), inputs(t, 1), relay)

            @pl.when(t >= 1)
            def _():
                emit(t - 1)
            return carry

        lax.fori_loop(0, n_tile, step, 0)
        tile.drain(inputs(n_tile, 1))
        emit(n_tile - 1)
        for u in (n_tile - 2, n_tile - 1):
            flush(u).wait()
            swap_y(u).wait_send()
        for u in range(n_tile):
            swap_y(u).wait_recv()

    nb = 2 * nbo
    pl.run_scoped(
        conv,
        pltpu.VMEM((3, n_seq, nb, BLK, TC), BF16), pltpu.VMEM((3, n_seq, nb, BLK, TC), BF16), pltpu.VMEM((3, n_seq, nbo, BLK, TC), BF16),
        pltpu.VMEM((2, n_seq, nb, 2 * BLK, TC), F32), pltpu.VMEM((3, 2, nbo, 2 * BLK, TC), F32),
        pltpu.SemaphoreType.DMA((3, 4)), pltpu.SemaphoreType.DMA((2, n_seq)),
        pltpu.VMEM((2, n_seq, n_pos, TC), BF16), pltpu.SemaphoreType.DMA((2,)), pltpu.VMEM((2, n_seq, n_pos, TC), F32),
        pltpu.VMEM((2, nbo, 3, BLK, TC), BF16),
        pltpu.VMEM((nbo + 1, 2 * BLK, TC), F32), pltpu.VMEM((nbo + 1, 2 * BLK, TC), F32), pltpu.VMEM((nbo, 2 * BLK, TC), F32),
        *[pltpu.VMEM((nb, 3, 2 * BLK, TC), BF16)] * n_seq,
        pltpu.VMEM((nb, 3, BLK, TC), BF16),
        *[pltpu.VMEM((nb, BLK, TC), F32)] * n_seq,
        pltpu.VMEM((nb, 2 * BLK, TC), F32),
        *[pltpu.VMEM((nbo, 3, 2 * BLK, TC), BF16)] * n_seq,
        pltpu.VMEM((n_seq, nbo, BLK, TC), BF16))

    for s in range(n_seq):
        swap_u(s).wait_send()
    for f in PAIR:
        swap_f(f).wait_send()

    @pl.when(sp == 1)
    def _():
        tail_copy().wait_send()

    @pl.when(sp == 3)
    def _():
        tail_across().wait_send()

    @pl.when(on_a)
    def _():
        for i in range(n_seq * n_cut):
            for k in PAIR:
                over(*divmod(i, n_cut), k).wait_send()
        for u in range(n_tile):
            for q in range(Q):
                for k in PAIR:
                    filt(f1, u, k, q).wait_send()

    @pl.when(on_b)
    def _():
        for i in range(n_seq * n_cut):
            for src in PAIR:
                onward(*divmod(i, n_cut), src).wait_send()
        for u in range(n_tile):
            for q in range(Q):
                for side in PAIR:
                    across(u, side, dp, q).wait_send()


def loop(trips):
    def run(body):
        def step(i, carry):
            body(i)
            return carry
        lax.fori_loop(0, trips, step, 0)
    return run


class ConvTile:
    def __init__(self, fwd6, inv6, hparts, g1, g2, raw2, sp0, sp1, zparts, zv0, zv1, zhat, sq0, sq1, ybuf):
        self.fwd6, self.inv6, self.hparts, self.g, self.raw2 = fwd6, inv6, hparts, (g1, g2), raw2
        self.first, self.second, self.zparts, self.zval, self.zhat, self.ybuf = (sp0, sp1), (sq0, sq1), zparts, (zv0, zv1), zhat, ybuf
        self.nb, self.nbo = sp0.shape[0], sq0.shape[0]

    def near(self, land, t, f):
        for side in PAIR:
            split_blocks(land.at[f, t, side], self.hparts.at[f], side * self.nbo // 2)

    def window(self, f, raw, far):
        g, nbo = self.g[f], self.nbo
        for j in range(nbo, 0, -1):
            cur = far.at[f, 0] if j == nbo else raw.at[j]
            for lo, sign in SIDES:
                re, im, new_re, new_im = shifted_add(cur, raw.at[j - 1], lo, sign)
                g[j, re], g[j, im] = new_re, new_im
        if raw is not g:
            g[0] = raw[0]

    def pointwise(self, xhat, f, far, dst, r, first):
        g, nbo = self.g[f], self.nbo
        re, im = pl.ds(pl.multiple_of(r * 16, 16), 16), pl.ds(pl.multiple_of(BLK + r * 16, 16), 16)
        for k in range(first, self.nb):
            acc_re = acc_im = None
            for j in range(k + 1):
                i = k - j
                gr, gi = (g[i, re], g[i, im]) if i <= nbo else (far[f, i - nbo, re], far[f, i - nbo, im])
                xr, xi = xhat[j, re], xhat[j, im]
                t_re, t_im = xr * gr - xi * gi, xr * gi + xi * gr
                acc_re = t_re if acc_re is None else acc_re + t_re
                acc_im = t_im if acc_im is None else acc_im + t_im
            for part, (a, b) in enumerate(zip(split3(acc_re), split3(acc_im))):
                dst[k - first, part, re], dst[k - first, part, im] = a, b

    def inverse(self, parts, k):
        return dot(self.inv6[...], stack6(parts[k, 0], parts[k, 1], parts[k, 2]))

    def gate_one(self, s, k, data):
        x1, v, _, _, skip, _ = data
        z = x1[s, k].astype(F32) * (self.inverse(self.first[s], k) + skip * v[s, k].astype(F32))
        self.zval[s][k] = z
        for part, a in enumerate(split3(z)):
            self.zparts[k, part] = a

    def spectrum(self, k):
        self.zhat[k] = block_spectrum(self.fwd6, self.zparts, k)

    def gate_two(self, s, k, data):
        y = data[2][s, k].astype(F32) * (self.inverse(self.second[s], k) + data[5] * self.zval[s][self.nbo + k])
        self.ybuf[s, k] = y.astype(BF16)

    def middle(self, s, data, i, point=None):
        for q in range(4):
            if point is not None:
                point(4 * i + q)
            for k in PAIR:
                if q < 2:
                    self.gate_one(s, 4 * i + 2 * q + k, data)
                else:
                    self.spectrum(4 * i + 2 * (q - 2) + k)

    def step(self, land, t, vhat, data, old, relay):
        nb, nbo = self.nb, self.nbo
        far = data[3]
        self.near(land, t, 0)
        for j in range(nbo):
            self.g[0][j] = block_spectrum(self.fwd6, self.hparts.at[0], j)
        self.near(land, t, 1)
        self.window(0, self.g[0], far)

        @loop(nb // 4)
        def _(i):
            self.middle(1, old, i, lambda r: self.pointwise(vhat.at[0], 0, far, self.first[0], r, 0))


        @loop(nbo // 2)
        def _(i):
            for q in range(4):
                self.pointwise(self.zhat, 1, old[3], self.second[1], 4 * i + q, nbo)
                if q < 2:
                    self.gate_two(0, 2 * i + q, old)
                else:
                    j = 2 * i + q - 2
                    self.raw2[j] = block_spectrum(self.fwd6, self.hparts.at[1], j)

        relay(0)
        self.window(1, self.raw2, far)

        @loop(nb // 4)
        def _(i):
            self.middle(0, data, i, lambda r: self.pointwise(vhat.at[1], 0, far, self.first[1], r, 0))

        @loop(nbo // 2)
        def _(i):
            for q in range(4):
                self.pointwise(self.zhat, 1, far, self.second[0], 4 * i + q, nbo)
                if q % 2 == 0:
                    self.gate_two(1, 2 * i + q // 2, old)

        relay(1)

    def drain(self, data):
        nb, nbo = self.nb, self.nbo

        @loop(nb // 4)
        def _(i):
            self.middle(1, data, i)

        @loop(nbo // 2)
        def _(i):
            for q in range(4):
                self.pointwise(self.zhat, 1, data[3], self.second[1], 4 * i + q, nbo)
                if q % 2 == 0:
                    self.gate_two(0, 2 * i + q // 2, data)

        for k in range(nbo):
            self.gate_two(1, k, data)

    def result(self, c, keep, send):
        hk = self.nbo // 2
        for s in range(self.ybuf.shape[0]):
            for b in range(hk):
                keep[s, b * BLK:(b + 1) * BLK] = self.ybuf[s, c * hk + b]
                send[s, b * BLK:(b + 1) * BLK] = self.ybuf[s, (1 - c) * hk + b].astype(F32)


def out_body(keep, part, w_out, u_in, out, wbuf, w_sem, lhs, keep_v, stage, in_sem, u_v, o_st, o_sem):
    c = lax.rem(lax.axis_index("sp"), 2)
    n_tile, n_seq, n_pos, _ = keep.shape
    half_w = n_tile * TC
    width = 2 * half_w
    n_col, rows = width // TN, width // 4

    def weights(j, slot):
        cols = pl.ds(pl.multiple_of(j * TN, TN), TN)
        return [pltpu.make_async_copy(w_out.at[i * rows:(i + 1) * rows, cols],
                                      wbuf.at[slot, i * rows:(i + 1) * rows], w_sem.at[slot, i]) for i in range(4)] + [
                    pltpu.make_async_copy(u_in.at[:, :, cols], u_v.at[slot], w_sem.at[slot, 4])]

    def flush(j):
        slot = lax.rem(j, 2)
        return pltpu.make_async_copy(o_st.at[slot], out.at[:, :, pl.ds(pl.multiple_of(j * TN, TN), TN)], o_sem.at[slot])

    loads = [pltpu.make_async_copy(part.at[u], stage.at[u], in_sem.at[u]) for u in range(n_tile)]
    loads += [pltpu.make_async_copy(keep.at[u], keep_v.at[u], in_sem.at[n_tile + u]) for u in range(n_tile)]
    for copy in loads:
        copy.start()
    for copy in weights(0, 0):
        copy.start()
    for u in range(n_tile):
        loads[u].wait()
        loads[n_tile + u].wait()
        for s in range(n_seq):
            lhs[s, :, pl.ds(pl.multiple_of((1 - c) * half_w + u * TC, TC), TC)] = stage[u, s].astype(BF16)
            lhs[s, :, pl.ds(pl.multiple_of(c * half_w + u * TC, TC), TC)] = keep_v[u, s]

    def step(j, carry):
        slot = lax.rem(j, 2)

        @pl.when(j + 1 < n_col)
        def _():
            for copy in weights(j + 1, 1 - slot):
                copy.start()

        for copy in weights(j, slot):
            copy.wait()

        @pl.when(j >= 2)
        def _():
            flush(j - 2).wait()

        for s in range(n_seq):
            o_st[slot, s] = (u_v[slot, s].astype(F32) + dot(lhs[s], wbuf[slot])).astype(BF16)
        flush(j).start()
        return carry

    lax.fori_loop(0, n_col, step, 0)
    for j in (n_col - 2, n_col - 1):
        flush(j).wait()


def solution(mesh):
    fwd3, fwd6, inv6 = transform_tables()

    def local_step(u_in, w_in, b_in, conv_taps, w_out, skip_one, skip_two, filt_one, filt_two):
        n_seq, n_pos, width = u_in.shape
        half_w = width // 2
        n_own = 2 * n_pos
        nb = 2 * n_own // BLK
        nbo = nb // 2
        n_tile = half_w // TC
        small, large = pl.BlockSpec(memory_space=pltpu.VMEM), pl.BlockSpec(memory_space=pl.ANY)
        dma = pltpu.SemaphoreType.DMA

        def shape(dims, dtype=F32):
            return jax.ShapeDtypeStruct(dims, dtype)

        keep, part, *_ = pl.pallas_call(
            main_body,
            in_specs=[small] * 7 + [large] * 4,
            out_specs=[large] * 12,
            out_shape=[
                shape((n_tile, n_seq, n_pos, TC), BF16), shape((n_tile, n_seq, n_pos, TC)),
                shape((n_tile, n_seq, nb + nbo, BLK, TC), BF16), shape((n_tile, n_seq, nb, BLK, TC), BF16),
                shape((n_tile, n_seq, nb, 2 * BLK, TC)), shape((n_tile, 2, nbo, 2 * BLK, TC)),
                shape((n_seq, n_pos, width)), shape((n_seq, 8, width)), shape((n_seq, n_pos, width)), shape((2, n_seq, n_pos, width)),
                shape((n_seq, 8, width)), shape((2, n_pos, half_w)),
            ],
            scratch_shapes=[
                pltpu.VMEM((2, n_tile, 2, n_pos, TC), F32),
                dma((1,)), dma((1,)), *[dma((n_seq, 3, 2))] * 4, *[dma((n_seq,))] * 2, *[dma((2,))] * 2,
                dma((2, n_tile, 2)), *[dma((n_tile, Q, 2))] * 4, *[dma((n_tile,))] * 2,
            ],
            compiler_params=pltpu.CompilerParams(vmem_limit_bytes=62 << 20, collective_id=0, has_side_effects=True),
            name="hyena_main",
        )(fwd3, fwd6, inv6, b_in.reshape(1, -1), conv_taps, skip_one.reshape(1, -1), skip_two.reshape(1, -1),
          u_in, w_in, filt_one, filt_two)

        return pl.pallas_call(
            out_body,
            in_specs=[large] * 4,
            out_specs=large,
            out_shape=shape((n_seq, n_pos, width), BF16),
            scratch_shapes=[
                pltpu.VMEM((2, width, TN), BF16), dma((2, 5)),
                pltpu.VMEM((n_seq, n_pos, width), BF16), pltpu.VMEM((n_tile, n_seq, n_pos, TC), BF16), pltpu.VMEM((n_tile, n_seq, n_pos, TC), F32),
                dma((2 * n_tile,)), pltpu.VMEM((2, n_seq, n_pos, TN), BF16), pltpu.VMEM((2, n_seq, n_pos, TN), BF16), dma((2,)),
            ],
            compiler_params=pltpu.CompilerParams(vmem_limit_bytes=60 << 20),
            name="out_proj",
        )(keep, part, w_out, u_in)

    seq_spec = P("dp", "sp", None)
    filt_spec = P("sp", None)
    return jax.shard_map(local_step, mesh=mesh, in_specs=(seq_spec, P(), P(), P(), P(), P(), P(), filt_spec, filt_spec), out_specs=seq_spec, check_vma=False)
```

```python
import functools

import jax
import jax.numpy as jnp
import numpy as np
from jax import lax
from jax.experimental import pallas as pl
from jax.experimental.pallas import tpu as pltpu
from jax.sharding import PartitionSpec as P

F32, BF16 = jnp.float32, jnp.bfloat16
BLK = 128
TN = 512
TC = 256
Q = 2
PAIR = (0, 1)
MESH = pl.DeviceIdType.MESH


def split_table(table):
    parts, rest = [], table.astype(np.float64)
    for _ in range(3):
        part = rest.astype(np.float32).astype(jnp.bfloat16)
        parts.append(part)
        rest = rest - part.astype(np.float64)
    return parts


def transform_tables():
    freq = np.concatenate([np.arange(0, BLK, 2), np.arange(1, BLK, 2)]) + 0.5
    angle = 2.0 * np.pi * freq[:, None] * np.arange(BLK)[None, :] / (2 * BLK)
    fwd = np.concatenate([np.cos(angle), -np.sin(angle)], 0)
    inv = np.concatenate([np.cos(angle).T, -np.sin(angle).T], 1) / BLK
    f1, f2, f3 = split_table(fwd)
    e1, e2, e3 = split_table(inv)
    fwd3 = np.concatenate([f1, f2, f3], 1)
    fwd6 = np.concatenate([f1, f1, f2, f2, f1, f3], 1)
    inv6 = np.concatenate([e1, e1, e2, e2, e1, e3], 1)
    return fwd3, fwd6, inv6


def parity(x):
    return lax.rem(x, 2)


def dot(a, b):
    return jnp.dot(a, b, preferred_element_type=F32)


def split3(x):
    hi = x.astype(BF16)
    rest = x - hi.astype(F32)
    mid = rest.astype(BF16)
    low = (rest - mid.astype(F32)).astype(BF16)
    return hi, mid, low


def stack6(hi, mid, low):
    return jnp.concatenate([hi, mid, hi, mid, low, hi], axis=0)


def split_blocks(src, parts, first):
    for j in range(src.shape[0] // BLK):
        for i, a in enumerate(split3(src[j * BLK:(j + 1) * BLK])):
            parts[first + j, i] = a


def block_spectrum(fwd6_ref, parts, j):
    return dot(fwd6_ref[...], stack6(parts[j, 0], parts[j, 1], parts[j, 2]))


def shifted_add(cur, old, lo, sign):
    re, im = slice(lo, lo + BLK // 2), slice(BLK + lo, BLK + lo + BLK // 2)
    return re, im, cur[re] - sign * old[im], cur[im] + sign * old[re]


SIDES = ((0, 1.0), (BLK // 2, -1.0))


def short_conv(pbuf, t, first, rows):
    return (t[0:1] * pbuf[8 + first:8 + first + rows] + t[1:2] * pbuf[7 + first:7 + first + rows] + t[2:3] * pbuf[6 + first:6 + first + rows]).astype(BF16)


def block_values(fwd3_ref, blk):
    return dot(fwd3_ref[...], jnp.concatenate([blk, blk, blk], axis=0))


def main_body(fwd3_ref, fwd6_ref, inv6_ref, bias_ref, taps_ref, sk1_ref, sk2_ref, u_bf, w_in, f1, f2,
              keep, part, qx, qv, vhat, far, u32, tsrc, u_sw, u_x, tail, pf,
              land, ts, tr, os, orr, ws, wr, ss, sr, fs, fr, l_sem, x_send, x_recv, y_send, y_recv, p_send, p_recv):
    sp, dp = lax.axis_index("sp"), lax.axis_index("dp")
    c = parity(sp)
    on_b = sp >= 2
    on_a = jnp.logical_not(on_b)
    other = sp + 1 - 2 * c
    n_seq, n_pos, width = u_bf.shape
    half_w = width // 2
    nt, n_tile, per = half_w // TN, half_w // TC, TN // TC
    n_own, hp = 2 * n_pos, n_pos // 2
    nbo = n_own // BLK
    cuts = (0, hp, hp + hp // 2, n_pos)
    n_cut = len(cuts) - 1

    def remote(src, dst, send, recv, peer):
        return pltpu.make_async_remote_copy(src, dst, send, recv, device_id=peer, device_id_type=MESH)

    def at(start, size):
        return pl.ds(pl.multiple_of(start, size), size)

    def share(s, h, k):
        rows = (cuts[h + 1] - cuts[h]) // 2
        return s, pl.ds(pl.multiple_of(cuts[h] + k * rows, rows), rows)

    def tail_copy():
        return remote(tsrc, tail, ts.at[0], tr.at[0], (dp, 3))

    def tail_across():
        return remote(tail, tail, ts.at[0], tr.at[0], (dp, other))

    def over(s, h, k):
        s, rows = share(s, h, k)
        return remote(u32.at[s, rows], u_x.at[c, s, rows], os.at[s, h, k], orr.at[s, h, c], (dp, 2 + k))

    def arrived(s, h, src):
        at_s, rows = share(s, h, 0)
        ref = u_x.at[src, at_s, rows]
        return remote(ref, ref, os.at[s, h, src], orr.at[s, h, src], (dp, sp))

    def onward(s, h, src):
        at_s, rows = share(s, h, c)
        ref = u_x.at[src, at_s, rows]
        return remote(ref, ref, ws.at[s, h, src], wr.at[s, h, src], (dp, other))

    def swap_u(s):
        return remote(u32.at[s], u_sw.at[s], ss.at[s], sr.at[s], (dp, other))

    def swap_f(f):
        return remote((f1, f2)[f].at[:, at((1 - c) * half_w, half_w)], pf.at[f], fs.at[f], fr.at[f], (dp, other))

    qr = n_pos // Q

    def filt(src, u, k, q):
        return remote(src.at[q * qr:(q + 1) * qr, at(k * half_w + u * TC, TC)], land.at[dp, u, c, q * qr:(q + 1) * qr],
                      x_send.at[u, q, k], x_recv.at[u, q, c], (dp, 2 + k))

    def landed(u, side, q):
        ref = land.at[dp, u, side, at(q * qr, qr)]
        return remote(ref, ref, x_send.at[u, q, side], x_recv.at[u, q, side], (dp, sp))

    def across(u, side, f, q):
        ref = land.at[f, u, side, at(q * qr, qr)]
        return remote(ref, ref, y_send.at[u, q, side], y_recv.at[u, q, side], (1 - dp, sp))

    def fill(f, u, side, src, start):
        return pltpu.make_async_copy(src.at[:, at(start, TC)], land.at[f, u, side], l_sem.at[f, u, side])

    def column(g, j):
        return (g + j // nt) * width + c * half_w + lax.rem(j, nt) * TN

    def load_rows(stage, st_sem, items):
        def copy(i):
            src, rows, _, _ = items[i]
            return pltpu.make_async_copy(src, stage.at[i % 2, :rows], st_sem.at[i % 2])

        copy(0).start()
        for i, (_, rows, dst, row) in enumerate(items):
            if i + 1 < len(items):
                copy(i + 1).start()
            copy(i).wait()
            dst[pl.ds(pl.multiple_of(row, 16), rows), :] = stage[i % 2, :rows].astype(BF16)

    barrier = pltpu.get_barrier_semaphore()
    for peer in ((dp, other), (dp, lax.rem(sp + 2, 4)), (dp, lax.rem(other + 2, 4)), (1 - dp, sp)):
        pl.semaphore_signal(barrier, inc=1, device_id=peer, device_id_type=MESH)
    pl.semaphore_wait(barrier, 4)

    def widen(raw, wide, tail_raw, tail_wide, in_sem, out_sem):
        step = hp // 2

        def part_of(ref, s, h):
            return ref.at[s, h * step:h * step + step]

        def load(s, h):
            return pltpu.make_async_copy(part_of(u_bf, s, h), raw.at[h % 2], in_sem.at[h % 2])

        last_rows = pltpu.make_async_copy(u_bf.at[:, n_pos - 8:], tail_raw, in_sem.at[2])
        last_out = pltpu.make_async_copy(tail_wide, tsrc, out_sem.at[2])
        order = [(s, h) for s in range(n_seq) for h in range(n_pos // step)]
        last_rows.start()
        load(*order[0]).start()
        last_rows.wait()
        tail_wide[...] = tail_raw[...].astype(F32)
        last_out.start()
        pending = {}
        for (s, h), following in zip(order, order[1:] + [None]):
            if following:
                load(*following).start()
            load(s, h).wait()
            slot = h % 2
            if slot in pending:
                pending.pop(slot).wait()
            wide[slot] = raw[slot].astype(F32)
            store = pltpu.make_async_copy(wide.at[slot], part_of(u32, s, h), out_sem.at[slot])
            store.start()
            if s + h:
                pending[slot] = store
                continue
            last_out.wait()

            @pl.when(sp == 1)
            def _():
                tail_copy().start()

            store.wait()

            @pl.when(on_a)
            def _():
                over(s, h, 0).start()

        for store in pending.values():
            store.wait()

    pl.run_scoped(
        widen, pltpu.VMEM((2, hp // 2, width), BF16), pltpu.VMEM((2, hp // 2, width), F32), pltpu.VMEM((n_seq, 8, width), BF16),
        pltpu.VMEM((n_seq, 8, width), F32), pltpu.SemaphoreType.DMA((3,)), pltpu.SemaphoreType.DMA((3,)))

    @pl.when(on_a)
    def _():
        for i in range(n_seq * n_cut):
            for k in PAIR:
                if i + k:
                    over(*divmod(i, n_cut), k).start()
        for which, src in ((0, f1), (1, f2)):
            @pl.when(dp == which)
            def _():
                for u in range(n_tile):
                    for q in range(Q):
                        for k in PAIR:
                            filt(src, u, k, q).start()

    for i in range(n_seq):
        swap_u(i).start()
    for f in PAIR:
        swap_f(f).start()

    def forward(u, q):
        @pl.when(on_b)
        def _():
            for side in PAIR:
                landed(u, side, q).wait_recv()
                across(u, side, dp, q).start()

    def front(wbuf, wsem, lhs, stage, st_sem, lhs_sem, tailbuf, q_st, q_sem, vh_st, vh_sem, pbuf):
        def weights(g, j, slot):
            rows = width // 4
            return [pltpu.make_async_copy(w_in.at[i * rows:(i + 1) * rows, at(column(g, j), TN)],
                                          wbuf.at[slot, i * rows:(i + 1) * rows], wsem.at[slot, i]) for i in range(4)]

        def stream(g, body, following, n=nt):
            def step(j, carry):
                slot = parity(j)

                @pl.when(j + 1 < n)
                def _():
                    for copy in weights(g, j + 1, 1 - slot):
                        copy.start()

                if following is not None:
                    @pl.when(j + 1 == n)
                    def _():
                        following(1 - slot)

                for copy in weights(g, j, slot):
                    copy.wait()
                body(j, slot, bias_ref[:, at(column(g, j), TN)], taps_ref[:, at(column(g, j), TN)])
                return carry

            lax.fori_loop(0, n, step, 0)

        def begin(g):
            def start(slot):
                for copy in weights(g, 0, slot):
                    copy.start()
            return start

        def project(rows_ref, slot, bias):
            return (dot(rows_ref, wbuf[slot]) + bias).astype(BF16).astype(F32)

        tail_rows = n_seq * 8
        begin(0)(0)
        own_rows = [pltpu.make_async_copy(u_bf.at[s], lhs.at[pl.ds(pl.multiple_of(tail_rows + s * n_own + c * n_pos, 16), n_pos)], lhs_sem.at[s])
                    for s in range(n_seq)]
        for copy in own_rows:
            copy.start()
        for s in range(n_seq):
            swap_u(s).wait_recv()
        load_rows(stage, st_sem, [(u_sw.at[s, h * hp:(h + 1) * hp], hp, lhs, tail_rows + s * n_own + (1 - c) * n_pos + h * hp)
                                  for s in range(n_seq) for h in PAIR])
        for copy in own_rows:
            copy.wait()

        @pl.when(on_b)
        def _():
            tail_copy().wait_recv()

            @pl.when(sp == 3)
            def _():
                tail_across().start()

            copy = pltpu.make_async_copy(tail, tailbuf, lhs_sem.at[0])
            copy.start()
            copy.wait()

        @pl.when(on_a)
        def _():
            tailbuf[...] = jnp.zeros_like(tailbuf)

        lhs[:tail_rows, :] = tailbuf[...].reshape(tail_rows, width).astype(BF16)
        chunk = n_pos

        def own_phase(g, n, dst, spectrum, following):
            def flush(j, slot):
                blocks = pl.ds(nbo * (1 + j // nt), nbo)
                copies = []
                for h in range(per):
                    u = lax.rem(j, nt) * per + h
                    copies.append(pltpu.make_async_copy(q_st.at[slot, h], dst.at[u, :, blocks], q_sem.at[slot, h]))
                    if spectrum:
                        copies.append(pltpu.make_async_copy(vh_st.at[slot, h], vhat.at[u, :, nbo:], vh_sem.at[slot, h]))
                return copies

            def body(j, slot, bias, taps):
                @pl.when(j >= 2)
                def _():
                    for copy in flush(j - 2, slot):
                        copy.wait()

                for i in range(n_seq * n_own // chunk):
                    s, r = divmod(i * chunk, n_own)
                    p = project(lhs[(tail_rows + i * chunk if i else 0):tail_rows + (i + 1) * chunk, :], slot, bias)
                    if i == 0:
                        for k in range(n_seq):
                            pbuf[k, 0:8] = jnp.where(on_b, p[8 * k:8 * k + 8], 0.0)
                        p = p[tail_rows:]
                    pbuf[s, 8 + r:8 + r + chunk] = p
                    q = short_conv(pbuf.at[s], taps, r, chunk)
                    for b in range(chunk // BLK):
                        blk = q[b * BLK:(b + 1) * BLK]
                        for h in range(per):
                            q_st[slot, h, s, r // BLK + b] = blk[:, h * TC:(h + 1) * TC]
                        if spectrum:
                            spec = block_values(fwd3_ref, blk)
                            for h in range(per):
                                vh_st[slot, h, s, r // BLK + b] = spec[:, h * TC:(h + 1) * TC]
                for copy in flush(j, slot):
                    copy.start()

            stream(g, body, following, n)
            for j in (n - 2, n - 1):
                for copy in flush(j, j % 2):
                    copy.wait()

        own_phase(0, 2 * nt, qx, False, begin(2))
        own_phase(2, nt, qv, True, None)

        def far_phase(fin, fin_sem, fout, fout_sem, parts):
            hk = n_pos // BLK

            def fetch(j, slot):
                mine = at(c * half_w + j * TC, TC)
                srcs = (f1.at[:, mine], f2.at[:, mine], pf.at[0, :, at(j * TC, TC)], pf.at[1, :, at(j * TC, TC)])
                return [pltpu.make_async_copy(src, fin.at[slot, i], fin_sem.at[slot, i]) for i, src in enumerate(srcs)]

            def flush(j, slot):
                return pltpu.make_async_copy(fout.at[slot], far.at[j], fout_sem.at[slot])

            for copy in fetch(0, 0):
                copy.start()

            def step(j, carry):
                slot = parity(j)

                @pl.when(j + 1 < n_tile)
                def _():
                    for copy in fetch(j + 1, 1 - slot):
                        copy.start()

                for copy in fetch(j, slot):
                    copy.wait()

                @pl.when(j >= 2)
                def _():
                    flush(j - 2, slot).wait()

                for f in PAIR:
                    split_blocks(fin.at[slot, f], parts.at[f], c * hk)
                    split_blocks(fin.at[slot, 2 + f], parts.at[f], (1 - c) * hk)
                g_ref = fout.at[slot]
                for f in PAIR:
                    for b in range(2 * hk):
                        g_ref[f, b] = block_spectrum(fwd6_ref, parts.at[f], b)
                    for b in range(2 * hk - 1, 0, -1):
                        for lo, sign in SIDES:
                            re, im, new_re, new_im = shifted_add(g_ref.at[f, b], g_ref.at[f, b - 1], lo, sign)
                            g_ref[f, b, re], g_ref[f, b, im] = new_re, new_im
                flush(j, slot).start()
                return carry

            lax.fori_loop(0, n_tile, step, 0)
            for j in (n_tile - 2, n_tile - 1):
                flush(j, j % 2).wait()

        for f in PAIR:
            swap_f(f).wait_recv()
        pl.run_scoped(
            far_phase, pltpu.VMEM((2, 4, n_pos, TC), F32), pltpu.SemaphoreType.DMA((2, 4)),
            pltpu.VMEM((2, 2, nbo, 2 * BLK, TC), F32), pltpu.SemaphoreType.DMA((2,)), pltpu.VMEM((2, nbo, 3, BLK, TC), BF16))

    pl.run_scoped(
        front,
        pltpu.VMEM((2, width, TN), BF16), pltpu.SemaphoreType.DMA((2, 4)),
        pltpu.VMEM((n_seq * n_own + 8 * n_seq, width), BF16),
        pltpu.VMEM((2, hp, width), F32), pltpu.SemaphoreType.DMA((2,)), pltpu.SemaphoreType.DMA((n_seq,)), pltpu.VMEM((n_seq, 8, width), F32),
        pltpu.VMEM((2, per, n_seq, nbo, BLK, TC), BF16), pltpu.SemaphoreType.DMA((2, per)),
        pltpu.VMEM((2, per, n_seq, nbo, 2 * BLK, TC), F32), pltpu.SemaphoreType.DMA((2, per)),
        pltpu.VMEM((n_seq, n_own + 8, TN), F32))

    def prev(wres, w_sem, lhs_p, stage, st_sem, q_st, q_sem, vh_st, vh_sem, pbuf, pstash):
        def weights(j):
            rows = width // 4
            return [pltpu.make_async_copy(w_in.at[i * rows:(i + 1) * rows, at(which(j), TN)],
                                          wres.at[j, i * rows:(i + 1) * rows], w_sem.at[j, i]) for i in range(4)]

        def which(j):
            return 2 * (j // nt) * width + c * half_w + lax.rem(j, nt) * TN

        def begin(j, carry):
            for copy in weights(j):
                copy.start()
            return carry

        @pl.when(on_b)
        def _():
            lax.fori_loop(0, 2 * nt, begin, 0)

        def rows(s, h):
            n = cuts[h + 1] - cuts[h]

            @pl.when(on_b)
            def _():
                for src in PAIR:
                    arrived(s, h, src).wait_recv()
                    onward(s, h, src).start()
                for src in PAIR:
                    onward(s, h, src).wait_recv()
                load_rows(stage, st_sem, [(u_x.at[src, s, cuts[h]:cuts[h + 1]], n, lhs_p, src * n) for src in PAIR])

            @pl.when(on_a)
            def _():
                lhs_p[...] = jnp.zeros_like(lhs_p)

        def project(h, j):
            n = 2 * (cuts[h + 1] - cuts[h])
            return (dot(lhs_p[:n, :], wres[j]) + bias_ref[:, at(which(j), TN)]).astype(BF16)

        def first(s, h):
            n = cuts[h + 1] - cuts[h]

            def body(j, carry):
                if h == 0:
                    @pl.when(jnp.logical_and(on_b, s == 0))
                    def _():
                        for copy in weights(j):
                            copy.wait()

                p = project(h, j)
                for core in PAIR:
                    pstash[core, cuts[h]:cuts[h + 1], at(j * TN, TN)] = p[core * n:(core + 1) * n]
                return carry

            lax.fori_loop(0, 2 * nt, body, 0)

        def last(s, u, dst):
            base, spectrum = u * nt, u > 0
            h = n_cut - 1
            n = cuts[h + 1] - cuts[h]

            def flush(j):
                slot, copies = parity(j), []
                for half in range(per):
                    copies.append(pltpu.make_async_copy(q_st.at[slot, half], dst.at[j * per + half, s, :nbo], q_sem.at[slot, half]))
                    if spectrum:
                        copies.append(pltpu.make_async_copy(vh_st.at[slot, half], vhat.at[j * per + half, s, :nbo], vh_sem.at[slot, half]))
                return copies

            def body(j, carry):
                slot = parity(j)

                @pl.when(j >= 2)
                def _():
                    for copy in flush(j - 2):
                        copy.wait()

                taps = taps_ref[:, at(which(base + j), TN)]
                pbuf[0:8] = jnp.zeros((8, TN), F32)
                for core in PAIR:
                    old = pstash[core, :cuts[h], at((base + j) * TN, TN)].astype(F32)
                    pbuf[8 + core * n_pos:8 + core * n_pos + cuts[h]] = jnp.where(on_b, old, 0.0)
                p = project(h, base + j).astype(F32)
                for core in PAIR:
                    start = 8 + core * n_pos + cuts[h]
                    pbuf[start:start + n] = jnp.where(on_b, p[core * n:(core + 1) * n], 0.0)
                for b in range(nbo):
                    blk = short_conv(pbuf, taps, b * BLK, BLK)
                    for half in range(per):
                        q_st[slot, half, b] = blk[:, half * TC:(half + 1) * TC]
                    if spectrum:
                        spec = block_values(fwd3_ref, blk)
                        for half in range(per):
                            vh_st[slot, half, b] = spec[:, half * TC:(half + 1) * TC]
                for copy in flush(j):
                    copy.start()

                @pl.when(jnp.logical_and(s == n_seq - 1, jnp.logical_and(lax.rem(j, Q) == 1, j < nt - Q * u)))
                def _():
                    forward(u, j // Q)
                return carry

            lax.fori_loop(0, nt, body, 0)
            for j in (nt - 2, nt - 1):
                for copy in flush(j):
                    copy.wait()

        def one_seq(s, carry):
            for h in range(n_cut - 1):
                rows(s, h)
                first(s, h)
            rows(s, n_cut - 1)
            last(s, 0, qx)
            last(s, 1, qv)
            return carry

        lax.fori_loop(0, n_seq, one_seq, 0)

    pl.run_scoped(
        prev,
        pltpu.VMEM((2 * nt, width, TN), BF16), pltpu.SemaphoreType.DMA((2 * nt, 4)),
        pltpu.VMEM((2 * hp, width), BF16), pltpu.VMEM((2, hp, width), F32), pltpu.SemaphoreType.DMA((2,)),
        pltpu.VMEM((2, per, nbo, BLK, TC), BF16), pltpu.SemaphoreType.DMA((2, per)),
        pltpu.VMEM((2, per, nbo, 2 * BLK, TC), F32), pltpu.SemaphoreType.DMA((2, per)),
        pltpu.VMEM((n_own + 8, TN), F32), pltpu.VMEM((2, cuts[-2], 2 * half_w), BF16))

    @pl.when(on_a)
    def _():
        for u in range(n_tile):
            for f, own in enumerate((f1, f2)):
                fill(f, u, c, own, c * half_w + u * TC).start()
                fill(f, u, 1 - c, pf.at[f], u * TC).start()

    def conv(x1b, vb, x2b, vhb, farb, in_sem, vh_sem, kst, k_sem, sendbuf, *scratch):
        def fetch(t):
            slot, two = lax.rem(t, 3), parity(t)
            srcs = (qx.at[t, :, :2 * nbo], qv.at[t], qx.at[t, :, 2 * nbo:], far.at[t])
            copies = [pltpu.make_async_copy(r, b.at[slot], in_sem.at[slot, i])
                      for i, (r, b) in enumerate(zip(srcs, (x1b, vb, x2b, farb)))]
            return copies + [pltpu.make_async_copy(vhat.at[t, s], vhb.at[two, s], vh_sem.at[two, s]) for s in range(n_seq)]

        def flush(t):
            slot = parity(t)
            return pltpu.make_async_copy(kst.at[slot], keep.at[t], k_sem.at[slot])

        def swap_y(u):
            return remote(sendbuf.at[parity(u)], part.at[u], p_send.at[u], p_recv.at[u], (dp, other))

        tile = ConvTile(fwd6_ref, inv6_ref, *scratch)

        def inputs(t, back):
            slot, cols = lax.rem(t + 3 - back, 3), at(c * half_w + lax.rem(t + n_tile - back, n_tile) * TC, TC)
            return x1b.at[slot], vb.at[slot], x2b.at[slot], farb.at[slot], sk1_ref[:, cols], sk2_ref[:, cols]

        def emit(t):
            slot = parity(t)

            @pl.when(t >= 2)
            def _():
                flush(t - 2).wait()
                swap_y(t - 2).wait_send()

            tile.result(c, kst.at[slot], sendbuf.at[slot])
            flush(t).start()
            swap_y(t).start()

        for copy in fetch(0):
            copy.start()
        forward(1, Q - 1)

        def step(t, carry):
            @pl.when(t + 1 < n_tile)
            def _():
                for copy in fetch(t + 1):
                    copy.start()

            @pl.when(on_a)
            def _():
                for f in PAIR:
                    for side in PAIR:
                        fill(f, t, side, f1, 0).wait()

            @pl.when(on_b)
            def _():
                for q in range(Q):
                    for side in PAIR:
                        across(t, side, 1 - dp, q).wait_recv()

            for copy in fetch(t):
                copy.wait()

            def relay(q):
                @pl.when(t + 2 < n_tile)
                def _():
                    forward(t + 2, q)

            tile.step(land, t, vhb.at[parity(t)], inputs(t, 0), inputs(t, 1), relay)

            @pl.when(t >= 1)
            def _():
                emit(t - 1)
            return carry

        lax.fori_loop(0, n_tile, step, 0)
        tile.drain(inputs(n_tile, 1))
        emit(n_tile - 1)
        for u in (n_tile - 2, n_tile - 1):
            flush(u).wait()
            swap_y(u).wait_send()
        for u in range(n_tile):
            swap_y(u).wait_recv()

    nb = 2 * nbo
    pl.run_scoped(
        conv,
        pltpu.VMEM((3, n_seq, nb, BLK, TC), BF16), pltpu.VMEM((3, n_seq, nb, BLK, TC), BF16), pltpu.VMEM((3, n_seq, nbo, BLK, TC), BF16),
        pltpu.VMEM((2, n_seq, nb, 2 * BLK, TC), F32), pltpu.VMEM((3, 2, nbo, 2 * BLK, TC), F32),
        pltpu.SemaphoreType.DMA((3, 4)), pltpu.SemaphoreType.DMA((2, n_seq)),
        pltpu.VMEM((2, n_seq, n_pos, TC), BF16), pltpu.SemaphoreType.DMA((2,)), pltpu.VMEM((2, n_seq, n_pos, TC), F32),
        pltpu.VMEM((2, nbo, 3, BLK, TC), BF16),
        pltpu.VMEM((nbo + 1, 2 * BLK, TC), F32), pltpu.VMEM((nbo + 1, 2 * BLK, TC), F32), pltpu.VMEM((nbo, 2 * BLK, TC), F32),
        *[pltpu.VMEM((nb, 3, 2 * BLK, TC), BF16)] * n_seq,
        pltpu.VMEM((nb, 3, BLK, TC), BF16),
        *[pltpu.VMEM((nb, BLK, TC), F32)] * n_seq,
        pltpu.VMEM((nb, 2 * BLK, TC), F32),
        *[pltpu.VMEM((nbo, 3, 2 * BLK, TC), BF16)] * n_seq,
        pltpu.VMEM((n_seq, nbo, BLK, TC), BF16))

    for s in range(n_seq):
        swap_u(s).wait_send()
    for f in PAIR:
        swap_f(f).wait_send()

    @pl.when(sp == 1)
    def _():
        tail_copy().wait_send()

    @pl.when(sp == 3)
    def _():
        tail_across().wait_send()

    @pl.when(on_a)
    def _():
        for i in range(n_seq * n_cut):
            for k in PAIR:
                over(*divmod(i, n_cut), k).wait_send()
        for u in range(n_tile):
            for q in range(Q):
                for k in PAIR:
                    filt(f1, u, k, q).wait_send()

    @pl.when(on_b)
    def _():
        for i in range(n_seq * n_cut):
            for src in PAIR:
                onward(*divmod(i, n_cut), src).wait_send()
        for u in range(n_tile):
            for q in range(Q):
                for side in PAIR:
                    across(u, side, dp, q).wait_send()


def loop(trips):
    def run(body):
        def step(i, carry):
            body(i)
            return carry
        lax.fori_loop(0, trips, step, 0)
    return run


class ConvTile:
    def __init__(self, fwd6, inv6, hparts, g1, g2, raw2, sp0, sp1, zparts, zv0, zv1, zhat, sq0, sq1, ybuf):
        self.fwd6, self.inv6, self.hparts, self.g, self.raw2 = fwd6, inv6, hparts, (g1, g2), raw2
        self.first, self.second, self.zparts, self.zval, self.zhat, self.ybuf = (sp0, sp1), (sq0, sq1), zparts, (zv0, zv1), zhat, ybuf
        self.nb, self.nbo = sp0.shape[0], sq0.shape[0]

    def near(self, land, t, f):
        for side in PAIR:
            split_blocks(land.at[f, t, side], self.hparts.at[f], side * self.nbo // 2)

    def window(self, f, raw, far):
        g, nbo = self.g[f], self.nbo
        for j in range(nbo, 0, -1):
            cur = far.at[f, 0] if j == nbo else raw.at[j]
            for lo, sign in SIDES:
                re, im, new_re, new_im = shifted_add(cur, raw.at[j - 1], lo, sign)
                g[j, re], g[j, im] = new_re, new_im
        if raw is not g:
            g[0] = raw[0]

    def pointwise(self, xhat, f, far, dst, r, first):
        g, nbo = self.g[f], self.nbo
        re, im = pl.ds(pl.multiple_of(r * 16, 16), 16), pl.ds(pl.multiple_of(BLK + r * 16, 16), 16)
        for k in range(first, self.nb):
            acc_re = acc_im = None
            for j in range(k + 1):
                i = k - j
                gr, gi = (g[i, re], g[i, im]) if i <= nbo else (far[f, i - nbo, re], far[f, i - nbo, im])
                xr, xi = xhat[j, re], xhat[j, im]
                t_re, t_im = xr * gr - xi * gi, xr * gi + xi * gr
                acc_re = t_re if acc_re is None else acc_re + t_re
                acc_im = t_im if acc_im is None else acc_im + t_im
            for part, (a, b) in enumerate(zip(split3(acc_re), split3(acc_im))):
                dst[k - first, part, re], dst[k - first, part, im] = a, b

    def inverse(self, parts, k):
        return dot(self.inv6[...], stack6(parts[k, 0], parts[k, 1], parts[k, 2]))

    def gate_one(self, s, k, data):
        x1, v, _, _, skip, _ = data
        z = x1[s, k].astype(F32) * (self.inverse(self.first[s], k) + skip * v[s, k].astype(F32))
        self.zval[s][k] = z
        for part, a in enumerate(split3(z)):
            self.zparts[k, part] = a

    def spectrum(self, k):
        self.zhat[k] = block_spectrum(self.fwd6, self.zparts, k)

    def gate_two(self, s, k, data):
        y = data[2][s, k].astype(F32) * (self.inverse(self.second[s], k) + data[5] * self.zval[s][self.nbo + k])
        self.ybuf[s, k] = y.astype(BF16)

    def middle(self, s, data, i, point=None):
        for q in range(4):
            if point is not None:
                point(4 * i + q)
            for k in PAIR:
                if q < 2:
                    self.gate_one(s, 4 * i + 2 * q + k, data)
                else:
                    self.spectrum(4 * i + 2 * (q - 2) + k)

    def step(self, land, t, vhat, data, old, relay):
        nb, nbo = self.nb, self.nbo
        far = data[3]
        self.near(land, t, 0)
        for j in range(nbo):
            self.g[0][j] = block_spectrum(self.fwd6, self.hparts.at[0], j)
        self.near(land, t, 1)
        self.window(0, self.g[0], far)

        @loop(nb // 4)
        def _(i):
            self.middle(1, old, i, lambda r: self.pointwise(vhat.at[0], 0, far, self.first[0], r, 0))


        @loop(nbo // 2)
        def _(i):
            for q in range(4):
                self.pointwise(self.zhat, 1, old[3], self.second[1], 4 * i + q, nbo)
                if q < 2:
                    self.gate_two(0, 2 * i + q, old)
                else:
                    j = 2 * i + q - 2
                    self.raw2[j] = block_spectrum(self.fwd6, self.hparts.at[1], j)

        relay(0)
        self.window(1, self.raw2, far)

        @loop(nb // 4)
        def _(i):
            self.middle(0, data, i, lambda r: self.pointwise(vhat.at[1], 0, far, self.first[1], r, 0))

        @loop(nbo // 2)
        def _(i):
            for q in range(4):
                self.pointwise(self.zhat, 1, far, self.second[0], 4 * i + q, nbo)
                if q % 2 == 0:
                    self.gate_two(1, 2 * i + q // 2, old)

        relay(1)

    def drain(self, data):
        nb, nbo = self.nb, self.nbo

        @loop(nb // 4)
        def _(i):
            self.middle(1, data, i)

        @loop(nbo // 2)
        def _(i):
            for q in range(4):
                self.pointwise(self.zhat, 1, data[3], self.second[1], 4 * i + q, nbo)
                if q % 2 == 0:
                    self.gate_two(0, 2 * i + q // 2, data)

        for k in range(nbo):
            self.gate_two(1, k, data)

    def result(self, c, keep, send):
        hk = self.nbo // 2
        for s in range(self.ybuf.shape[0]):
            for b in range(hk):
                keep[s, b * BLK:(b + 1) * BLK] = self.ybuf[s, c * hk + b]
                send[s, b * BLK:(b + 1) * BLK] = self.ybuf[s, (1 - c) * hk + b].astype(F32)


def out_body(keep, part, w_out, u_in, out, wbuf, w_sem, lhs, keep_v, stage, in_sem, u_v, acc, o_st, o_sem):
    c = lax.rem(lax.axis_index("sp"), 2)
    n_tile, n_seq, n_pos, _ = keep.shape
    half_w = n_tile * TC
    width = 2 * half_w
    n_col, rows = width // TN, width // 4

    def weights(j, slot):
        cols = pl.ds(pl.multiple_of(j * TN, TN), TN)
        return [pltpu.make_async_copy(w_out.at[i * rows:(i + 1) * rows, cols],
                                      wbuf.at[slot, i * rows:(i + 1) * rows], w_sem.at[slot, i]) for i in range(4)] + [
                    pltpu.make_async_copy(u_in.at[:, :, cols], u_v.at[slot], w_sem.at[slot, 4])]

    def flush(j):
        slot = parity(j)
        return pltpu.make_async_copy(o_st.at[slot], out.at[:, :, pl.ds(pl.multiple_of(j * TN, TN), TN)], o_sem.at[slot])

    def channels(k, size):
        return pl.ds(pl.multiple_of(k * size, size), size)

    loads = [[pltpu.make_async_copy(ref.at[u], dst.at[u], in_sem.at[i, u]) for u in range(n_tile)]
             for i, (ref, dst) in enumerate(((keep, keep_v), (part, stage)))]
    for copy in loads[0]:
        copy.start()
    for copy in weights(0, 0):
        copy.start()
    for copy in loads[1]:
        copy.start()
    for i, k in enumerate((c, 1 - c)):
        for u, copy in enumerate(loads[i]):
            copy.wait()
            for s in range(n_seq):
                lhs[s, :, channels(k * n_tile + u, TC)] = (keep_v, stage)[i][u, s].astype(BF16)
        if i == 0:
            for copy in weights(0, 0):
                copy.wait()
            for copy in weights(1, 1):
                copy.start()
            for s in range(n_seq):
                acc[s] = u_v[0, s].astype(F32) + dot(lhs[s, :, channels(k, half_w)], wbuf[0, channels(k, half_w)])
            continue
        for s in range(n_seq):
            o_st[0, s] = (acc[s] + dot(lhs[s, :, channels(k, half_w)], wbuf[0, channels(k, half_w)])).astype(BF16)
    flush(0).start()

    def step(j, carry):
        slot = parity(j)

        @pl.when(j + 1 < n_col)
        def _():
            for copy in weights(j + 1, 1 - slot):
                copy.start()

        for copy in weights(j, slot):
            copy.wait()

        @pl.when(j >= 2)
        def _():
            flush(j - 2).wait()

        for s in range(n_seq):
            o_st[slot, s] = (u_v[slot, s].astype(F32) + dot(lhs[s], wbuf[slot])).astype(BF16)
        flush(j).start()
        return carry

    lax.fori_loop(1, n_col, step, 0)
    for j in (n_col - 2, n_col - 1):
        flush(j).wait()


def solution(mesh):
    fwd3, fwd6, inv6 = transform_tables()

    def local_step(u_in, w_in, b_in, conv_taps, w_out, skip_one, skip_two, filt_one, filt_two):
        n_seq, n_pos, width = u_in.shape
        half_w = width // 2
        n_own = 2 * n_pos
        nb = 2 * n_own // BLK
        nbo = nb // 2
        n_tile = half_w // TC
        small, large = pl.BlockSpec(memory_space=pltpu.VMEM), pl.BlockSpec(memory_space=pl.ANY)
        dma = pltpu.SemaphoreType.DMA

        def shape(dims, dtype=F32):
            return jax.ShapeDtypeStruct(dims, dtype)

        keep, part, *_ = pl.pallas_call(
            main_body,
            in_specs=[small] * 7 + [large] * 4,
            out_specs=[large] * 12,
            out_shape=[
                shape((n_tile, n_seq, n_pos, TC), BF16), shape((n_tile, n_seq, n_pos, TC)),
                shape((n_tile, n_seq, nb + nbo, BLK, TC), BF16), shape((n_tile, n_seq, nb, BLK, TC), BF16),
                shape((n_tile, n_seq, nb, 2 * BLK, TC)), shape((n_tile, 2, nbo, 2 * BLK, TC)),
                shape((n_seq, n_pos, width)), shape((n_seq, 8, width)), shape((n_seq, n_pos, width)), shape((2, n_seq, n_pos, width)),
                shape((n_seq, 8, width)), shape((2, n_pos, half_w)),
            ],
            scratch_shapes=[
                pltpu.VMEM((2, n_tile, 2, n_pos, TC), F32),
                dma((1,)), dma((1,)), *[dma((n_seq, 3, 2))] * 4, *[dma((n_seq,))] * 2, *[dma((2,))] * 2,
                dma((2, n_tile, 2)), *[dma((n_tile, Q, 2))] * 4, *[dma((n_tile,))] * 2,
            ],
            compiler_params=pltpu.CompilerParams(vmem_limit_bytes=62 << 20, collective_id=0, has_side_effects=True),
            name="hyena_main",
        )(fwd3, fwd6, inv6, b_in.reshape(1, -1), conv_taps, skip_one.reshape(1, -1), skip_two.reshape(1, -1),
          u_in, w_in, filt_one, filt_two)

        return pl.pallas_call(
            out_body,
            in_specs=[large] * 4,
            out_specs=large,
            out_shape=shape((n_seq, n_pos, width), BF16),
            scratch_shapes=[
                pltpu.VMEM((2, width, TN), BF16), dma((2, 5)),
                pltpu.VMEM((n_seq, n_pos, width), BF16), pltpu.VMEM((n_tile, n_seq, n_pos, TC), BF16), pltpu.VMEM((n_tile, n_seq, n_pos, TC), F32),
                dma((2, n_tile)), pltpu.VMEM((2, n_seq, n_pos, TN), BF16), pltpu.VMEM((n_seq, n_pos, TN), F32), pltpu.VMEM((2, n_seq, n_pos, TN), BF16), dma((2,)),
            ],
            compiler_params=pltpu.CompilerParams(vmem_limit_bytes=60 << 20),
            name="out_proj",
        )(keep, part, w_out, u_in)

    seq_spec = P("dp", "sp", None)
    filt_spec = P("sp", None)
    return jax.shard_map(local_step, mesh=mesh, in_specs=(seq_spec, P(), P(), P(), P(), P(), P(), filt_spec, filt_spec), out_specs=seq_spec, check_vma=False)
```

```python
import functools

import jax
import jax.numpy as jnp
import numpy as np
from jax import lax
from jax.experimental import pallas as pl
from jax.experimental.pallas import tpu as pltpu
from jax.sharding import PartitionSpec as P

F32, BF16 = jnp.float32, jnp.bfloat16
BLK = 128
TN = 512
TC = 256
Q = 2
PAIR = (0, 1)
MESH = pl.DeviceIdType.MESH


def split_table(table):
    parts, rest = [], table.astype(np.float64)
    for _ in range(3):
        part = rest.astype(np.float32).astype(jnp.bfloat16)
        parts.append(part)
        rest = rest - part.astype(np.float64)
    return parts


def transform_tables():
    freq = np.concatenate([np.arange(0, BLK, 2), np.arange(1, BLK, 2)]) + 0.5
    angle = 2.0 * np.pi * freq[:, None] * np.arange(BLK)[None, :] / (2 * BLK)
    fwd = np.concatenate([np.cos(angle), -np.sin(angle)], 0)
    inv = np.concatenate([np.cos(angle).T, -np.sin(angle).T], 1) / BLK
    f1, f2, f3 = split_table(fwd)
    e1, e2, e3 = split_table(inv)
    fwd3 = np.concatenate([f1, f2, f3], 1)
    fwd6 = np.concatenate([f1, f1, f2, f2, f1, f3], 1)
    inv6 = np.concatenate([e1, e1, e2, e2, e1, e3], 1)
    return fwd3, fwd6, inv6


def parity(x):
    return lax.rem(x, 2)


def dot(a, b):
    return jnp.dot(a, b, preferred_element_type=F32)


def split3(x):
    hi = x.astype(BF16)
    rest = x - hi.astype(F32)
    mid = rest.astype(BF16)
    low = (rest - mid.astype(F32)).astype(BF16)
    return hi, mid, low


def stack6(hi, mid, low):
    return jnp.concatenate([hi, mid, hi, mid, low, hi], axis=0)


def split_blocks(src, parts, first):
    for j in range(src.shape[0] // BLK):
        for i, a in enumerate(split3(src[j * BLK:(j + 1) * BLK])):
            parts[first + j, i] = a


def block_spectrum(fwd6_ref, parts, j):
    return dot(fwd6_ref[...], stack6(parts[j, 0], parts[j, 1], parts[j, 2]))


def shifted_add(cur, old, lo, sign):
    re, im = slice(lo, lo + BLK // 2), slice(BLK + lo, BLK + lo + BLK // 2)
    return re, im, cur[re] - sign * old[im], cur[im] + sign * old[re]


SIDES = ((0, 1.0), (BLK // 2, -1.0))


def short_conv(pbuf, t, first, rows):
    return (t[0:1] * pbuf[8 + first:8 + first + rows] + t[1:2] * pbuf[7 + first:7 + first + rows] + t[2:3] * pbuf[6 + first:6 + first + rows]).astype(BF16)


def block_values(fwd3_ref, blk):
    return dot(fwd3_ref[...], jnp.concatenate([blk, blk, blk], axis=0))


def main_body(fwd3_ref, fwd6_ref, inv6_ref, bias_ref, taps_ref, sk1_ref, sk2_ref, u_bf, w_in, f1, f2,
              keep, part, qx, qv, vhat, far, u32, tsrc, u_sw, u_x, tail, pf,
              land, held, h_sem, ts, tr, os, orr, ws, wr, ss, sr, fs, fr, l_sem, x_send, x_recv, y_send, y_recv, p_send, p_recv):
    sp, dp = lax.axis_index("sp"), lax.axis_index("dp")
    c = parity(sp)
    on_b = sp >= 2
    on_a = jnp.logical_not(on_b)
    other = sp + 1 - 2 * c
    n_seq, n_pos, width = u_bf.shape
    half_w = width // 2
    nt, n_tile, per = half_w // TN, half_w // TC, TN // TC
    n_own, hp = 2 * n_pos, n_pos // 2
    nbo = n_own // BLK
    cuts = (0, hp, hp + hp // 2, n_pos)
    n_cut = len(cuts) - 1

    def remote(src, dst, send, recv, peer):
        return pltpu.make_async_remote_copy(src, dst, send, recv, device_id=peer, device_id_type=MESH)

    def at(start, size):
        return pl.ds(pl.multiple_of(start, size), size)

    def share(s, h, k):
        rows = (cuts[h + 1] - cuts[h]) // 2
        return s, pl.ds(pl.multiple_of(cuts[h] + k * rows, rows), rows)

    def tail_copy():
        return remote(tsrc, tail, ts.at[0], tr.at[0], (dp, 3))

    def tail_across():
        return remote(tail, tail, ts.at[0], tr.at[0], (dp, other))

    def over(s, h, k):
        s, rows = share(s, h, k)
        return remote(u32.at[s, rows], u_x.at[c, s, rows], os.at[s, h, k], orr.at[s, h, c], (dp, 2 + k))

    def arrived(s, h, src):
        at_s, rows = share(s, h, 0)
        ref = u_x.at[src, at_s, rows]
        return remote(ref, ref, os.at[s, h, src], orr.at[s, h, src], (dp, sp))

    def onward(s, h, src):
        at_s, rows = share(s, h, c)
        ref = u_x.at[src, at_s, rows]
        return remote(ref, ref, ws.at[s, h, src], wr.at[s, h, src], (dp, other))

    def swap_u(s):
        return remote(u32.at[s], u_sw.at[s], ss.at[s], sr.at[s], (dp, other))

    def swap_f(f):
        return remote((f1, f2)[f].at[:, at((1 - c) * half_w, half_w)], pf.at[f], fs.at[f], fr.at[f], (dp, other))

    qr = n_pos // Q

    def filt(u, k, q):
        rows = pl.ds(q * qr, qr)
        return remote(held.at[u, k, rows], land.at[dp, u, c, rows], x_send.at[u, q, k], x_recv.at[u, q, c], (dp, 2 + k))

    def hold(src, u, k):
        return pltpu.make_async_copy(src.at[:, at(k * half_w + u * TC, TC)], held.at[u, k], h_sem.at[u, k])

    def landed(u, side, q):
        ref = land.at[dp, u, side, at(q * qr, qr)]
        return remote(ref, ref, x_send.at[u, q, side], x_recv.at[u, q, side], (dp, sp))

    def across(u, side, f, q):
        ref = land.at[f, u, side, at(q * qr, qr)]
        return remote(ref, ref, y_send.at[u, q, side], y_recv.at[u, q, side], (1 - dp, sp))

    def fill(f, u, side, src, start):
        return pltpu.make_async_copy(src.at[:, at(start, TC)], land.at[f, u, side], l_sem.at[f, u, side])

    def column(g, j):
        return (g + j // nt) * width + c * half_w + lax.rem(j, nt) * TN

    def load_rows(stage, st_sem, items):
        size = stage.shape[1]
        cut = [(src.at[pl.ds(i, size)], dst, row + i) for src, rows, dst, row in items for i in range(0, rows, size)]

        def copy(i):
            return pltpu.make_async_copy(cut[i][0], stage.at[i % 2], st_sem.at[i % 2])

        copy(0).start()
        for i, (_, dst, row) in enumerate(cut):
            if i + 1 < len(cut):
                copy(i + 1).start()
            copy(i).wait()
            dst[pl.ds(pl.multiple_of(row, 16), size), :] = stage[i % 2].astype(BF16)

    barrier = pltpu.get_barrier_semaphore()
    for peer in ((dp, other), (dp, lax.rem(sp + 2, 4)), (dp, lax.rem(other + 2, 4)), (1 - dp, sp)):
        pl.semaphore_signal(barrier, inc=1, device_id=peer, device_id_type=MESH)
    pl.semaphore_wait(barrier, 4)

    def widen(raw, wide, tail_raw, tail_wide, in_sem, out_sem):
        def half(ref, s, h):
            return ref.at[s, h * hp:h * hp + hp]

        def load(s, h):
            return pltpu.make_async_copy(half(u_bf, s, h), raw.at[h], in_sem.at[h])

        last_rows = pltpu.make_async_copy(u_bf.at[:, n_pos - 8:], tail_raw, in_sem.at[2])
        last_out = pltpu.make_async_copy(tail_wide, tsrc, out_sem.at[2])
        order = [(s, h) for s in range(n_seq) for h in PAIR]
        last_rows.start()
        load(*order[0]).start()
        last_rows.wait()
        tail_wide[...] = tail_raw[...].astype(F32)
        last_out.start()
        pending = {}
        for (s, h), following in zip(order, order[1:] + [None]):
            if following:
                load(*following).start()
            load(s, h).wait()
            if h in pending:
                pending.pop(h).wait()
            wide[h] = raw[h].astype(F32)
            store = pltpu.make_async_copy(wide.at[h], half(u32, s, h), out_sem.at[h])
            store.start()
            if s + h:
                pending[h] = store
                continue
            last_out.wait()

            @pl.when(sp == 1)
            def _():
                tail_copy().start()

            store.wait()

            @pl.when(on_a)
            def _():
                for k in PAIR:
                    over(s, h, k).start()

        for store in pending.values():
            store.wait()

    pl.run_scoped(
        widen, pltpu.VMEM((2, hp, width), BF16), pltpu.VMEM((2, hp, width), F32), pltpu.VMEM((n_seq, 8, width), BF16),
        pltpu.VMEM((n_seq, 8, width), F32), pltpu.SemaphoreType.DMA((3,)), pltpu.SemaphoreType.DMA((3,)))

    @pl.when(on_a)
    def _():
        for i in range(1, n_seq * n_cut):
            for k in PAIR:
                over(*divmod(i, n_cut), k).start()
        for which, src in ((0, f1), (1, f2)):
            @pl.when(dp == which)
            def _():
                for u in range(n_tile):
                    for k in PAIR:
                        hold(src, u, k).start()

        for u in range(n_tile):
            for k in PAIR:
                hold(f1, u, k).wait()
        for u in range(n_tile):
            for q in range(Q):
                for k in PAIR:
                    filt(u, k, q).start()

    for i in range(n_seq):
        swap_u(i).start()
    for f in PAIR:
        swap_f(f).start()

    def forward(u, q):
        @pl.when(on_b)
        def _():
            for side in PAIR:
                landed(u, side, q).wait_recv()
                across(u, side, dp, q).start()

    def front(wbuf, wsem, lhs, stage, st_sem, lhs_sem, tailbuf, q_st, q_sem, vh_st, vh_sem, pbuf):
        def weights(g, j, slot):
            rows = width // 4
            return [pltpu.make_async_copy(w_in.at[i * rows:(i + 1) * rows, at(column(g, j), TN)],
                                          wbuf.at[slot, i * rows:(i + 1) * rows], wsem.at[slot, i]) for i in range(4)]

        def stream(g, body, following, n=nt):
            def step(j, carry):
                slot = parity(j)

                @pl.when(j + 1 < n)
                def _():
                    for copy in weights(g, j + 1, 1 - slot):
                        copy.start()

                if following is not None:
                    @pl.when(j + 1 == n)
                    def _():
                        following(1 - slot)

                for copy in weights(g, j, slot):
                    copy.wait()
                body(j, slot, bias_ref[:, at(column(g, j), TN)], taps_ref[:, at(column(g, j), TN)])
                return carry

            lax.fori_loop(0, n, step, 0)

        def begin(g):
            def start(slot):
                for copy in weights(g, 0, slot):
                    copy.start()
            return start

        def project(rows_ref, slot, bias):
            return (dot(rows_ref, wbuf[slot]) + bias).astype(BF16).astype(F32)

        tail_rows = n_seq * 8
        begin(0)(0)
        own_rows = [pltpu.make_async_copy(u_bf.at[s], lhs.at[pl.ds(pl.multiple_of(tail_rows + s * n_own + c * n_pos, 16), n_pos)], lhs_sem.at[s])
                    for s in range(n_seq)]
        for copy in own_rows:
            copy.start()
        for s in range(n_seq):
            swap_u(s).wait_recv()
        load_rows(stage, st_sem, [(u_sw.at[s, h * hp:(h + 1) * hp], hp, lhs, tail_rows + s * n_own + (1 - c) * n_pos + h * hp)
                                  for s in range(n_seq) for h in PAIR])
        for copy in own_rows:
            copy.wait()

        @pl.when(on_b)
        def _():
            tail_copy().wait_recv()

            @pl.when(sp == 3)
            def _():
                tail_across().start()

            copy = pltpu.make_async_copy(tail, tailbuf, lhs_sem.at[0])
            copy.start()
            copy.wait()

        @pl.when(on_a)
        def _():
            tailbuf[...] = jnp.zeros_like(tailbuf)

        lhs[:tail_rows, :] = tailbuf[...].reshape(tail_rows, width).astype(BF16)
        chunk = n_pos

        def own_phase(g, n, dst, spectrum, following):
            def flush(j, slot):
                blocks = pl.ds(nbo * (1 + j // nt), nbo)
                copies = []
                for h in range(per):
                    u = lax.rem(j, nt) * per + h
                    copies.append(pltpu.make_async_copy(q_st.at[slot, h], dst.at[u, :, blocks], q_sem.at[slot, h]))
                    if spectrum:
                        copies.append(pltpu.make_async_copy(vh_st.at[slot, h], vhat.at[u, :, nbo:], vh_sem.at[slot, h]))
                return copies

            def body(j, slot, bias, taps):
                @pl.when(j >= 2)
                def _():
                    for copy in flush(j - 2, slot):
                        copy.wait()

                for i in range(n_seq * n_own // chunk):
                    s, r = divmod(i * chunk, n_own)
                    p = project(lhs[(tail_rows + i * chunk if i else 0):tail_rows + (i + 1) * chunk, :], slot, bias)
                    if i == 0:
                        for k in range(n_seq):
                            pbuf[k, 0:8] = jnp.where(on_b, p[8 * k:8 * k + 8], 0.0)
                        p = p[tail_rows:]
                    pbuf[s, 8 + r:8 + r + chunk] = p
                    q = short_conv(pbuf.at[s], taps, r, chunk)
                    for b in range(chunk // BLK):
                        blk = q[b * BLK:(b + 1) * BLK]
                        for h in range(per):
                            q_st[slot, h, s, r // BLK + b] = blk[:, h * TC:(h + 1) * TC]
                        if spectrum:
                            spec = block_values(fwd3_ref, blk)
                            for h in range(per):
                                vh_st[slot, h, s, r // BLK + b] = spec[:, h * TC:(h + 1) * TC]
                for copy in flush(j, slot):
                    copy.start()

            stream(g, body, following, n)
            for j in (n - 2, n - 1):
                for copy in flush(j, j % 2):
                    copy.wait()

        own_phase(0, 2 * nt, qx, False, begin(2))
        own_phase(2, nt, qv, True, None)

        def far_phase(fin, fin_sem, fout, fout_sem, parts):
            hk = n_pos // BLK

            def fetch(j, slot):
                mine = at(c * half_w + j * TC, TC)
                srcs = (f1.at[:, mine], f2.at[:, mine], pf.at[0, :, at(j * TC, TC)], pf.at[1, :, at(j * TC, TC)])
                return [pltpu.make_async_copy(src, fin.at[slot, i], fin_sem.at[slot, i]) for i, src in enumerate(srcs)]

            def flush(j, slot):
                return pltpu.make_async_copy(fout.at[slot], far.at[j], fout_sem.at[slot])

            for copy in fetch(0, 0):
                copy.start()

            def step(j, carry):
                slot = parity(j)

                @pl.when(j + 1 < n_tile)
                def _():
                    for copy in fetch(j + 1, 1 - slot):
                        copy.start()

                for copy in fetch(j, slot):
                    copy.wait()

                @pl.when(j >= 2)
                def _():
                    flush(j - 2, slot).wait()

                for f in PAIR:
                    split_blocks(fin.at[slot, f], parts.at[f], c * hk)
                    split_blocks(fin.at[slot, 2 + f], parts.at[f], (1 - c) * hk)
                g_ref = fout.at[slot]
                for f in PAIR:
                    for b in range(2 * hk):
                        g_ref[f, b] = block_spectrum(fwd6_ref, parts.at[f], b)
                    for b in range(2 * hk - 1, 0, -1):
                        for lo, sign in SIDES:
                            re, im, new_re, new_im = shifted_add(g_ref.at[f, b], g_ref.at[f, b - 1], lo, sign)
                            g_ref[f, b, re], g_ref[f, b, im] = new_re, new_im
                flush(j, slot).start()
                return carry

            lax.fori_loop(0, n_tile, step, 0)
            for j in (n_tile - 2, n_tile - 1):
                flush(j, j % 2).wait()

        for f in PAIR:
            swap_f(f).wait_recv()
        pl.run_scoped(
            far_phase, pltpu.VMEM((2, 4, n_pos, TC), F32), pltpu.SemaphoreType.DMA((2, 4)),
            pltpu.VMEM((2, 2, nbo, 2 * BLK, TC), F32), pltpu.SemaphoreType.DMA((2,)), pltpu.VMEM((2, nbo, 3, BLK, TC), BF16))

    pl.run_scoped(
        front,
        pltpu.VMEM((2, width, TN), BF16), pltpu.SemaphoreType.DMA((2, 4)),
        pltpu.VMEM((n_seq * n_own + 8 * n_seq, width), BF16),
        pltpu.VMEM((2, hp // 2, width), F32), pltpu.SemaphoreType.DMA((2,)), pltpu.SemaphoreType.DMA((n_seq,)), pltpu.VMEM((n_seq, 8, width), F32),
        pltpu.VMEM((2, per, n_seq, nbo, BLK, TC), BF16), pltpu.SemaphoreType.DMA((2, per)),
        pltpu.VMEM((2, per, n_seq, nbo, 2 * BLK, TC), F32), pltpu.SemaphoreType.DMA((2, per)),
        pltpu.VMEM((n_seq, n_own + 8, TN), F32))

    def prev(wres, w_sem, lhs_p, stage, st_sem, q_st, q_sem, vh_st, vh_sem, pbuf, pstash):
        def weights(j):
            rows = width // 4
            return [pltpu.make_async_copy(w_in.at[i * rows:(i + 1) * rows, at(which(j), TN)],
                                          wres.at[j, i * rows:(i + 1) * rows], w_sem.at[j, i]) for i in range(4)]

        def which(j):
            return 2 * (j // nt) * width + c * half_w + lax.rem(j, nt) * TN

        def begin(j, carry):
            for copy in weights(j):
                copy.start()
            return carry

        lax.fori_loop(0, 2 * nt, begin, 0)

        def rows(s, h):
            n = cuts[h + 1] - cuts[h]

            @pl.when(on_b)
            def _():
                for src in PAIR:
                    arrived(s, h, src).wait_recv()
                    onward(s, h, src).start()
                for src in PAIR:
                    onward(s, h, src).wait_recv()
                load_rows(stage, st_sem, [(u_x.at[src, s, cuts[h]:cuts[h + 1]], n, lhs_p, src * n) for src in PAIR])

            @pl.when(on_a)
            def _():
                lhs_p[...] = jnp.zeros_like(lhs_p)

        def project(h, j):
            n = 2 * (cuts[h + 1] - cuts[h])
            return (dot(lhs_p[:n, :], wres[j]) + bias_ref[:, at(which(j), TN)]).astype(BF16)

        def first(s, h):
            n = cuts[h + 1] - cuts[h]

            def body(j, carry):
                if h == 0:
                    @pl.when(s == 0)
                    def _():
                        for copy in weights(j):
                            copy.wait()

                p = project(h, j)
                for core in PAIR:
                    pstash[core, cuts[h]:cuts[h + 1], at(j * TN, TN)] = p[core * n:(core + 1) * n]
                return carry

            lax.fori_loop(0, 2 * nt, body, 0)

        def last(s, u, dst):
            base, spectrum = u * nt, u > 0
            h = n_cut - 1
            n = cuts[h + 1] - cuts[h]

            def flush(j):
                copies = []
                for half in range(per):
                    copies.append(pltpu.make_async_copy(q_st.at[half], dst.at[j * per + half, s, :nbo], q_sem.at[half]))
                    if spectrum:
                        copies.append(pltpu.make_async_copy(vh_st.at[half], vhat.at[j * per + half, s, :nbo], vh_sem.at[half]))
                return copies

            def body(j, carry):
                taps = taps_ref[:, at(which(base + j), TN)]
                pbuf[0:8] = jnp.zeros((8, TN), F32)
                for core in PAIR:
                    old = pstash[core, :cuts[h], at((base + j) * TN, TN)].astype(F32)
                    pbuf[8 + core * n_pos:8 + core * n_pos + cuts[h]] = jnp.where(on_b, old, 0.0)
                p = project(h, base + j).astype(F32)
                for core in PAIR:
                    start = 8 + core * n_pos + cuts[h]
                    pbuf[start:start + n] = jnp.where(on_b, p[core * n:(core + 1) * n], 0.0)

                @pl.when(j > 0)
                def _():
                    for copy in flush(j - 1):
                        copy.wait()

                for b in range(nbo):
                    blk = short_conv(pbuf, taps, b * BLK, BLK)
                    for half in range(per):
                        q_st[half, b] = blk[:, half * TC:(half + 1) * TC]
                    if spectrum:
                        spec = block_values(fwd3_ref, blk)
                        for half in range(per):
                            vh_st[half, b] = spec[:, half * TC:(half + 1) * TC]
                for copy in flush(j):
                    copy.start()

                @pl.when(jnp.logical_and(s == n_seq - 1, jnp.logical_and(lax.rem(j, Q) == 1, j < nt - Q * u)))
                def _():
                    forward(u, j // Q)
                return carry

            lax.fori_loop(0, nt, body, 0)
            for copy in flush(nt - 1):
                copy.wait()

        def one_seq(s, carry):
            for h in range(n_cut - 1):
                rows(s, h)
                first(s, h)
            rows(s, n_cut - 1)
            last(s, 0, qx)
            last(s, 1, qv)
            return carry

        lax.fori_loop(0, n_seq, one_seq, 0)

    pl.run_scoped(
        prev,
        pltpu.VMEM((2 * nt, width, TN), BF16), pltpu.SemaphoreType.DMA((2 * nt, 4)),
        pltpu.VMEM((2 * hp, width), BF16), pltpu.VMEM((2, hp // 2, width), F32), pltpu.SemaphoreType.DMA((2,)),
        pltpu.VMEM((per, nbo, BLK, TC), BF16), pltpu.SemaphoreType.DMA((per,)),
        pltpu.VMEM((per, nbo, 2 * BLK, TC), F32), pltpu.SemaphoreType.DMA((per,)),
        pltpu.VMEM((n_own + 8, TN), F32), pltpu.VMEM((2, cuts[-2], 2 * half_w), BF16))

    @pl.when(on_a)
    def _():
        for u in range(n_tile):
            for f, own in enumerate((f1, f2)):
                fill(f, u, c, own, c * half_w + u * TC).start()
                fill(f, u, 1 - c, pf.at[f], u * TC).start()

    def conv(x1b, vb, x2b, vhb, farb, in_sem, vh_sem, kst, k_sem, sendbuf, *scratch):
        def fetch(t):
            slot, two = lax.rem(t, 3), parity(t)
            srcs = (qx.at[t, :, :2 * nbo], qv.at[t], qx.at[t, :, 2 * nbo:], far.at[t])
            copies = [pltpu.make_async_copy(r, b.at[slot], in_sem.at[slot, i])
                      for i, (r, b) in enumerate(zip(srcs, (x1b, vb, x2b, farb)))]
            return copies + [pltpu.make_async_copy(vhat.at[t, s], vhb.at[two, s], vh_sem.at[two, s]) for s in range(n_seq)]

        def flush(t):
            slot = parity(t)
            return pltpu.make_async_copy(kst.at[slot], keep.at[t], k_sem.at[slot])

        def swap_y(u):
            return remote(sendbuf.at[parity(u)], part.at[u], p_send.at[u], p_recv.at[u], (dp, other))

        tile = ConvTile(n_tile, fwd6_ref, inv6_ref, *scratch)

        def inputs(t, back):
            slot, cols = lax.rem(t + 3 - back, 3), at(c * half_w + lax.rem(t + n_tile - back, n_tile) * TC, TC)
            return x1b.at[slot], vb.at[slot], x2b.at[slot], farb.at[slot], sk1_ref[:, cols], sk2_ref[:, cols]

        def emit(t):
            slot = parity(t)

            @pl.when(t >= 2)
            def _():
                flush(t - 2).wait()
                swap_y(t - 2).wait_send()

            tile.result(c, kst.at[slot], sendbuf.at[slot])
            flush(t).start()
            swap_y(t).start()

        for copy in fetch(0):
            copy.start()
        forward(1, Q - 1)

        def step(t, carry):
            @pl.when(t + 1 < n_tile)
            def _():
                for copy in fetch(t + 1):
                    copy.start()

            @pl.when(on_a)
            def _():
                for f in PAIR:
                    for side in PAIR:
                        fill(f, t, side, f1, 0).wait()

            @pl.when(on_b)
            def _():
                for q in range(Q):
                    for side in PAIR:
                        across(t, side, 1 - dp, q).wait_recv()

            for copy in fetch(t):
                copy.wait()

            def relay(q, first, last):
                @pl.when(jnp.logical_and(t >= first, t < last))
                def _():
                    forward(t + 2 - first // (n_tile - 2), q)

            tile.step(land, t, vhb.at[parity(t)], inputs(t, 0), inputs(t, 1), relay)

            @pl.when(t >= 1)
            def _():
                emit(t - 1)
            return carry

        lax.fori_loop(0, n_tile, step, 0)
        tile.drain(inputs(n_tile, 1))
        emit(n_tile - 1)
        for u in (n_tile - 2, n_tile - 1):
            flush(u).wait()
            swap_y(u).wait_send()
        for u in range(n_tile):
            swap_y(u).wait_recv()

    nb = 2 * nbo
    pl.run_scoped(
        conv,
        pltpu.VMEM((3, n_seq, nb, BLK, TC), BF16), pltpu.VMEM((3, n_seq, nb, BLK, TC), BF16), pltpu.VMEM((3, n_seq, nbo, BLK, TC), BF16),
        pltpu.VMEM((2, n_seq, nb, 2 * BLK, TC), F32), pltpu.VMEM((3, 2, nbo, 2 * BLK, TC), F32),
        pltpu.SemaphoreType.DMA((3, 4)), pltpu.SemaphoreType.DMA((2, n_seq)),
        pltpu.VMEM((2, n_seq, n_pos, TC), BF16), pltpu.SemaphoreType.DMA((2,)), pltpu.VMEM((2, n_seq, n_pos, TC), F32),
        pltpu.VMEM((2, nbo, 3, BLK, TC), BF16),
        pltpu.VMEM((nbo + 1, 2 * BLK, TC), F32), pltpu.VMEM((nbo + 1, 2 * BLK, TC), F32), pltpu.VMEM((nbo, 2 * BLK, TC), F32),
        *[pltpu.VMEM((nb, 3, 2 * BLK, TC), BF16)] * n_seq,
        pltpu.VMEM((nb, 3, BLK, TC), BF16),
        *[pltpu.VMEM((nb, BLK, TC), F32)] * n_seq,
        pltpu.VMEM((nb, 2 * BLK, TC), F32),
        *[pltpu.VMEM((nbo, 3, 2 * BLK, TC), BF16)] * n_seq,
        pltpu.VMEM((n_seq, nbo, BLK, TC), BF16))

    for s in range(n_seq):
        swap_u(s).wait_send()
    for f in PAIR:
        swap_f(f).wait_send()

    @pl.when(sp == 1)
    def _():
        tail_copy().wait_send()

    @pl.when(sp == 3)
    def _():
        tail_across().wait_send()

    @pl.when(on_a)
    def _():
        for i in range(n_seq * n_cut):
            for k in PAIR:
                over(*divmod(i, n_cut), k).wait_send()
        for u in range(n_tile):
            for q in range(Q):
                for k in PAIR:
                    filt(u, k, q).wait_send()

    @pl.when(on_b)
    def _():
        for i in range(n_seq * n_cut):
            for src in PAIR:
                onward(*divmod(i, n_cut), src).wait_send()
        for u in range(n_tile):
            for q in range(Q):
                for side in PAIR:
                    across(u, side, dp, q).wait_send()


def loop(trips):
    def run(body):
        def step(i, carry):
            body(i)
            return carry
        lax.fori_loop(0, trips, step, 0)
    return run


class ConvTile:
    def __init__(self, steps, fwd6, inv6, hparts, g1, g2, raw2, sp0, sp1, zparts, zv0, zv1, zhat, sq0, sq1, ybuf):
        self.fwd6, self.inv6, self.hparts, self.g, self.raw2 = fwd6, inv6, hparts, (g1, g2), raw2
        self.first, self.second, self.zparts, self.zval, self.zhat, self.ybuf = (sp0, sp1), (sq0, sq1), zparts, (zv0, zv1), zhat, ybuf
        self.nb, self.nbo = sp0.shape[0], sq0.shape[0]
        self.steps = steps

    def near(self, land, t, f):
        for side in PAIR:
            split_blocks(land.at[f, t, side], self.hparts.at[f], side * self.nbo // 2)

    def window(self, f, raw, far):
        g, nbo = self.g[f], self.nbo
        for j in range(nbo, 0, -1):
            cur = far.at[f, 0] if j == nbo else raw.at[j]
            for lo, sign in SIDES:
                re, im, new_re, new_im = shifted_add(cur, raw.at[j - 1], lo, sign)
                g[j, re], g[j, im] = new_re, new_im
        if raw is not g:
            g[0] = raw[0]

    def pointwise(self, xhat, f, far, dst, r, first):
        g, nbo = self.g[f], self.nbo
        re, im = pl.ds(pl.multiple_of(r * 16, 16), 16), pl.ds(pl.multiple_of(BLK + r * 16, 16), 16)
        for k in range(first, self.nb):
            acc_re = acc_im = None
            for j in range(k + 1):
                i = k - j
                gr, gi = (g[i, re], g[i, im]) if i <= nbo else (far[f, i - nbo, re], far[f, i - nbo, im])
                xr, xi = xhat[j, re], xhat[j, im]
                t_re, t_im = xr * gr - xi * gi, xr * gi + xi * gr
                acc_re = t_re if acc_re is None else acc_re + t_re
                acc_im = t_im if acc_im is None else acc_im + t_im
            for part, (a, b) in enumerate(zip(split3(acc_re), split3(acc_im))):
                dst[k - first, part, re], dst[k - first, part, im] = a, b

    def inverse(self, parts, k):
        return dot(self.inv6[...], stack6(parts[k, 0], parts[k, 1], parts[k, 2]))

    def gate_one(self, s, k, data):
        x1, v, _, _, skip, _ = data
        z = x1[s, k].astype(F32) * (self.inverse(self.first[s], k) + skip * v[s, k].astype(F32))
        self.zval[s][k] = z
        for part, a in enumerate(split3(z)):
            self.zparts[k, part] = a

    def spectrum(self, k):
        self.zhat[k] = block_spectrum(self.fwd6, self.zparts, k)

    def gate_two(self, s, k, data):
        y = data[2][s, k].astype(F32) * (self.inverse(self.second[s], k) + data[5] * self.zval[s][self.nbo + k])
        self.ybuf[s, k] = y.astype(BF16)

    def middle(self, s, data, i, point=None):
        for q in range(4):
            if point is not None:
                point(4 * i + q)
            for k in PAIR:
                if q < 2:
                    self.gate_one(s, 4 * i + 2 * q + k, data)
                else:
                    self.spectrum(4 * i + 2 * (q - 2) + k)

    def step(self, land, t, vhat, data, old, relay):
        nb, nbo = self.nb, self.nbo
        far = data[3]
        self.near(land, t, 0)
        for j in range(nbo):
            self.g[0][j] = block_spectrum(self.fwd6, self.hparts.at[0], j)
        self.near(land, t, 1)
        self.window(0, self.g[0], far)

        @loop(nb // 4)
        def _(i):
            self.middle(1, old, i, lambda r: self.pointwise(vhat.at[0], 0, far, self.first[0], r, 0))

        relay(1, self.steps - 2, self.steps - 1)


        @loop(nbo // 2)
        def _(i):
            for q in range(4):
                self.pointwise(self.zhat, 1, old[3], self.second[1], 4 * i + q, nbo)
                if q < 2:
                    self.gate_two(0, 2 * i + q, old)
                else:
                    j = 2 * i + q - 2
                    self.raw2[j] = block_spectrum(self.fwd6, self.hparts.at[1], j)

        relay(0, 0, self.steps - 2)
        self.window(1, self.raw2, far)

        @loop(nb // 4)
        def _(i):
            self.middle(0, data, i, lambda r: self.pointwise(vhat.at[1], 0, far, self.first[1], r, 0))

        @loop(nbo // 2)
        def _(i):
            for q in range(4):
                self.pointwise(self.zhat, 1, far, self.second[0], 4 * i + q, nbo)
                if q % 2 == 0:
                    self.gate_two(1, 2 * i + q // 2, old)

        relay(1, 0, self.steps - 3)

    def drain(self, data):
        nb, nbo = self.nb, self.nbo

        @loop(nb // 4)
        def _(i):
            self.middle(1, data, i)

        @loop(nbo // 2)
        def _(i):
            for q in range(4):
                self.pointwise(self.zhat, 1, data[3], self.second[1], 4 * i + q, nbo)
                if q % 2 == 0:
                    self.gate_two(0, 2 * i + q // 2, data)

        for k in range(nbo):
            self.gate_two(1, k, data)

    def result(self, c, keep, send):
        hk = self.nbo // 2
        for s in range(self.ybuf.shape[0]):
            for b in range(hk):
                keep[s, b * BLK:(b + 1) * BLK] = self.ybuf[s, c * hk + b]
                send[s, b * BLK:(b + 1) * BLK] = self.ybuf[s, (1 - c) * hk + b].astype(F32)


def out_body(keep, part, w_out, u_in, out, wbuf, w_sem, lhs, keep_v, stage, in_sem, u_v, o_st, o_sem):
    c = lax.rem(lax.axis_index("sp"), 2)
    n_tile, n_seq, n_pos, _ = keep.shape
    half_w = n_tile * TC
    width = 2 * half_w
    n_col, rows = width // TN, width // 4

    def weights(j, slot):
        cols = pl.ds(pl.multiple_of(j * TN, TN), TN)
        return [pltpu.make_async_copy(w_out.at[i * rows:(i + 1) * rows, cols],
                                      wbuf.at[slot, i * rows:(i + 1) * rows], w_sem.at[slot, i]) for i in range(4)] + [
                    pltpu.make_async_copy(u_in.at[:, :, cols], u_v.at[slot], w_sem.at[slot, 4])]

    def flush(j):
        slot = parity(j)
        return pltpu.make_async_copy(o_st.at[slot], out.at[:, :, pl.ds(pl.multiple_of(j * TN, TN), TN)], o_sem.at[slot])

    loads = [pltpu.make_async_copy(part.at[u], stage.at[u], in_sem.at[u]) for u in range(n_tile)]
    loads += [pltpu.make_async_copy(keep.at[u], keep_v.at[u], in_sem.at[n_tile + u]) for u in range(n_tile)]
    for copy in loads:
        copy.start()
    for copy in weights(0, 0):
        copy.start()
    for u in range(n_tile):
        loads[u].wait()
        loads[n_tile + u].wait()
        for s in range(n_seq):
            lhs[s, :, pl.ds(pl.multiple_of((1 - c) * half_w + u * TC, TC), TC)] = stage[u, s].astype(BF16)
            lhs[s, :, pl.ds(pl.multiple_of(c * half_w + u * TC, TC), TC)] = keep_v[u, s]

    def step(j, carry):
        slot = parity(j)

        @pl.when(j + 1 < n_col)
        def _():
            for copy in weights(j + 1, 1 - slot):
                copy.start()

        for copy in weights(j, slot):
            copy.wait()

        @pl.when(j >= 2)
        def _():
            flush(j - 2).wait()

        for s in range(n_seq):
            o_st[slot, s] = (u_v[slot, s].astype(F32) + dot(lhs[s], wbuf[slot])).astype(BF16)
        flush(j).start()
        return carry

    lax.fori_loop(0, n_col, step, 0)
    for j in (n_col - 2, n_col - 1):
        flush(j).wait()


def solution(mesh):
    fwd3, fwd6, inv6 = transform_tables()

    def local_step(u_in, w_in, b_in, conv_taps, w_out, skip_one, skip_two, filt_one, filt_two):
        n_seq, n_pos, width = u_in.shape
        half_w = width // 2
        n_own = 2 * n_pos
        nb = 2 * n_own // BLK
        nbo = nb // 2
        n_tile = half_w // TC
        small, large = pl.BlockSpec(memory_space=pltpu.VMEM), pl.BlockSpec(memory_space=pl.ANY)
        dma = pltpu.SemaphoreType.DMA

        def shape(dims, dtype=F32):
            return jax.ShapeDtypeStruct(dims, dtype)

        keep, part, *_ = pl.pallas_call(
            main_body,
            in_specs=[small] * 7 + [large] * 4,
            out_specs=[large] * 12,
            out_shape=[
                shape((n_tile, n_seq, n_pos, TC), BF16), shape((n_tile, n_seq, n_pos, TC)),
                shape((n_tile, n_seq, nb + nbo, BLK, TC), BF16), shape((n_tile, n_seq, nb, BLK, TC), BF16),
                shape((n_tile, n_seq, nb, 2 * BLK, TC)), shape((n_tile, 2, nbo, 2 * BLK, TC)),
                shape((n_seq, n_pos, width)), shape((n_seq, 8, width)), shape((n_seq, n_pos, width)), shape((2, n_seq, n_pos, width)),
                shape((n_seq, 8, width)), shape((2, n_pos, half_w)),
            ],
            scratch_shapes=[
                pltpu.VMEM((2, n_tile, 2, n_pos, TC), F32), pltpu.VMEM((n_tile, 2, n_pos, TC), F32), dma((n_tile, 2)),
                dma((1,)), dma((1,)), *[dma((n_seq, 3, 2))] * 4, *[dma((n_seq,))] * 2, *[dma((2,))] * 2,
                dma((2, n_tile, 2)), *[dma((n_tile, Q, 2))] * 4, *[dma((n_tile,))] * 2,
            ],
            compiler_params=pltpu.CompilerParams(vmem_limit_bytes=67043328, collective_id=0, has_side_effects=True),
            name="hyena_main",
        )(fwd3, fwd6, inv6, b_in.reshape(1, -1), conv_taps, skip_one.reshape(1, -1), skip_two.reshape(1, -1),
          u_in, w_in, filt_one, filt_two)

        return pl.pallas_call(
            out_body,
            in_specs=[large] * 4,
            out_specs=large,
            out_shape=shape((n_seq, n_pos, width), BF16),
            scratch_shapes=[
                pltpu.VMEM((2, width, TN), BF16), dma((2, 5)),
                pltpu.VMEM((n_seq, n_pos, width), BF16), pltpu.VMEM((n_tile, n_seq, n_pos, TC), BF16), pltpu.VMEM((n_tile, n_seq, n_pos, TC), F32),
                dma((2 * n_tile,)), pltpu.VMEM((2, n_seq, n_pos, TN), BF16), pltpu.VMEM((2, n_seq, n_pos, TN), BF16), dma((2,)),
            ],
            compiler_params=pltpu.CompilerParams(vmem_limit_bytes=60 << 20),
            name="out_proj",
        )(keep, part, w_out, u_in)

    seq_spec = P("dp", "sp", None)
    filt_spec = P("sp", None)
    return jax.shard_map(local_step, mesh=mesh, in_specs=(seq_spec, P(), P(), P(), P(), P(), P(), filt_spec, filt_spec), out_specs=seq_spec, check_vma=False)
```

```python
import functools

import jax
import jax.numpy as jnp
import numpy as np
from jax import lax
from jax.experimental import pallas as pl
from jax.experimental.pallas import tpu as pltpu
from jax.sharding import PartitionSpec as P

F32, BF16 = jnp.float32, jnp.bfloat16
BLK = 128
TN = 512
TC = 256
Q = 2
PAIR = (0, 1)
GR = 32
MESH = pl.DeviceIdType.MESH


def split_table(table):
    parts, rest = [], table.astype(np.float64)
    for _ in range(3):
        part = rest.astype(np.float32).astype(jnp.bfloat16)
        parts.append(part)
        rest = rest - part.astype(np.float64)
    return parts


def transform_tables():
    freq = np.concatenate([np.arange(0, BLK, 2), np.arange(1, BLK, 2)]) + 0.5
    angle = 2.0 * np.pi * freq[:, None] * np.arange(BLK)[None, :] / (2 * BLK)
    fwd = np.concatenate([np.cos(angle), -np.sin(angle)], 0)
    inv = np.concatenate([np.cos(angle).T, -np.sin(angle).T], 1) / BLK
    f1, f2, f3 = split_table(fwd)
    e1, e2, e3 = split_table(inv)
    fwd3 = np.concatenate([f1, f2, f3], 1)
    fwd6 = np.concatenate([f1, f1, f2, f2, f1, f3], 1)
    inv6 = np.concatenate([e1, e1, e2, e2, e1, e3], 1)
    return fwd3, fwd6, inv6


def parity(x):
    return lax.rem(x, 2)


def dot(a, b):
    return jnp.dot(a, b, preferred_element_type=F32)


def split3(x):
    hi = x.astype(BF16)
    rest = x - hi.astype(F32)
    mid = rest.astype(BF16)
    low = (rest - mid.astype(F32)).astype(BF16)
    return hi, mid, low


def stack6(hi, mid, low):
    return jnp.concatenate([hi, mid, hi, mid, low, hi], axis=0)


def split_blocks(src, parts, first):
    for j in range(src.shape[0] // BLK):
        for i, a in enumerate(split3(src[j * BLK:(j + 1) * BLK])):
            parts[first + j, i] = a


def block_spectrum(fwd6_ref, parts, j):
    return dot(fwd6_ref[...], stack6(parts[j, 0], parts[j, 1], parts[j, 2]))


def shifted_add(cur, old, lo, sign):
    re, im = slice(lo, lo + BLK // 2), slice(BLK + lo, BLK + lo + BLK // 2)
    return re, im, cur[re] - sign * old[im], cur[im] + sign * old[re]


SIDES = ((0, 1.0), (BLK // 2, -1.0))


def short_conv(pbuf, t, first, rows):
    return (t[0:1] * pbuf[8 + first:8 + first + rows] + t[1:2] * pbuf[7 + first:7 + first + rows] + t[2:3] * pbuf[6 + first:6 + first + rows]).astype(BF16)


def block_values(fwd3_ref, blk):
    return dot(fwd3_ref[...], jnp.concatenate([blk, blk, blk], axis=0))


def main_body(fwd3_ref, fwd6_ref, inv6_ref, bias_ref, taps_ref, sk1_ref, sk2_ref, u_bf, w_in, f1, f2,
              keep, part, qx, qv, vhat, far, u32, tsrc, u_sw, u_x, tail, pf,
              land, ts, tr, os, orr, ws, wr, ss, sr, fs, fr, l_sem, x_send, x_recv, y_send, y_recv, p_send, p_recv):
    sp, dp = lax.axis_index("sp"), lax.axis_index("dp")
    c = parity(sp)
    on_b = sp >= 2
    on_a = jnp.logical_not(on_b)
    other = sp + 1 - 2 * c
    n_seq, n_pos, width = u_bf.shape
    half_w = width // 2
    nt, n_tile, per = half_w // TN, half_w // TC, TN // TC
    n_own, hp = 2 * n_pos, n_pos // 2
    nbo = n_own // BLK
    cuts = (0, hp, hp + hp // 2, n_pos)
    n_cut = len(cuts) - 1

    def remote(src, dst, send, recv, peer):
        return pltpu.make_async_remote_copy(src, dst, send, recv, device_id=peer, device_id_type=MESH)

    def at(start, size):
        return pl.ds(pl.multiple_of(start, size), size)

    def share(s, h, k):
        rows = (cuts[h + 1] - cuts[h]) // 2
        return s, pl.ds((cuts[h] + k * rows) // GR, rows // GR)

    def tail_copy():
        return remote(tsrc, tail, ts.at[0], tr.at[0], (dp, 3))

    def tail_across():
        return remote(tail, tail, ts.at[0], tr.at[0], (dp, other))

    def over(s, h, k):
        s, rows = share(s, h, k)
        return remote(u32.at[s, rows], u_x.at[c, s, rows], os.at[s, h, k], orr.at[s, h, c], (dp, 2 + k))

    def arrived(s, h, src):
        at_s, rows = share(s, h, 0)
        ref = u_x.at[src, at_s, rows]
        return remote(ref, ref, os.at[s, h, src], orr.at[s, h, src], (dp, sp))

    def onward(s, h, src):
        at_s, rows = share(s, h, c)
        ref = u_x.at[src, at_s, rows]
        return remote(ref, ref, ws.at[s, h, src], wr.at[s, h, src], (dp, other))

    def swap_u(s):
        return remote(u32.at[s], u_sw.at[s], ss.at[s], sr.at[s], (dp, other))

    def swap_f(f):
        return remote((f1, f2)[f].at[:, at((1 - c) * half_w, half_w)], pf.at[f], fs.at[f], fr.at[f], (dp, other))

    qr = n_pos // Q

    def filt(src, u, k, q):
        return remote(src.at[q * qr:(q + 1) * qr, at(k * half_w + u * TC, TC)], land.at[dp, u, c, q * qr:(q + 1) * qr],
                      x_send.at[u, q, k], x_recv.at[u, q, c], (dp, 2 + k))

    def landed(u, side, q):
        ref = land.at[dp, u, side, at(q * qr, qr)]
        return remote(ref, ref, x_send.at[u, q, side], x_recv.at[u, q, side], (dp, sp))

    def across(u, side, f, q):
        ref = land.at[f, u, side, at(q * qr, qr)]
        return remote(ref, ref, y_send.at[u, q, side], y_recv.at[u, q, side], (1 - dp, sp))

    def fill(f, u, side, src, start):
        return pltpu.make_async_copy(src.at[:, at(start, TC)], land.at[f, u, side], l_sem.at[f, u, side])

    def column(g, j):
        return (g + j // nt) * width + c * half_w + lax.rem(j, nt) * TN

    def load_rows(stage, st_sem, items):
        def copy(i):
            src, rows, _, _ = items[i]
            return pltpu.make_async_copy(src, stage.at[i % 2, :rows // GR], st_sem.at[i % 2])

        copy(0).start()
        for i, (_, rows, dst, row) in enumerate(items):
            if i + 1 < len(items):
                copy(i + 1).start()
            copy(i).wait()
            dst[pl.ds(pl.multiple_of(row, 16), rows), :] = stage[i % 2, :rows // GR].reshape(rows, width).astype(BF16)

    barrier = pltpu.get_barrier_semaphore()
    for peer in ((dp, other), (dp, lax.rem(sp + 2, 4)), (dp, lax.rem(other + 2, 4)), (1 - dp, sp)):
        pl.semaphore_signal(barrier, inc=1, device_id=peer, device_id_type=MESH)
    pl.semaphore_wait(barrier, 4)

    def widen(raw, wide, tail_raw, tail_wide, in_sem, out_sem):
        def half(ref, s, h):
            return ref.at[s, h * hp:h * hp + hp]

        def load(s, h):
            return pltpu.make_async_copy(half(u_bf, s, h), raw.at[h], in_sem.at[h])

        last_rows = pltpu.make_async_copy(u_bf.at[:, n_pos - 8:], tail_raw, in_sem.at[2])
        last_out = pltpu.make_async_copy(tail_wide, tsrc, out_sem.at[2])
        order = [(s, h) for s in range(n_seq) for h in PAIR]
        last_rows.start()
        load(*order[0]).start()
        last_rows.wait()
        tail_wide[...] = tail_raw[...].astype(F32)
        last_out.start()
        pending = {}
        for (s, h), following in zip(order, order[1:] + [None]):
            if following:
                load(*following).start()
            load(s, h).wait()
            if h in pending:
                pending.pop(h).wait()
            wide[h] = raw[h].astype(F32).reshape(wide.shape[1:])
            store = pltpu.make_async_copy(wide.at[h], u32.at[s, pl.ds(h * hp // GR, hp // GR)], out_sem.at[h])
            store.start()
            if s + h:
                pending[h] = store
                continue
            last_out.wait()

            @pl.when(sp == 1)
            def _():
                tail_copy().start()

            store.wait()

            @pl.when(on_a)
            def _():
                for k in PAIR:
                    over(s, h, k).start()

        for store in pending.values():
            store.wait()

    pl.run_scoped(
        widen, pltpu.VMEM((2, hp, width), BF16), pltpu.VMEM((2, hp // GR, GR, width), F32), pltpu.VMEM((n_seq, 8, width), BF16),
        pltpu.VMEM((n_seq, 8, width), F32), pltpu.SemaphoreType.DMA((3,)), pltpu.SemaphoreType.DMA((3,)))

    @pl.when(on_a)
    def _():
        for i in range(1, n_seq * n_cut):
            for k in PAIR:
                over(*divmod(i, n_cut), k).start()
        for which, src in ((0, f1), (1, f2)):
            @pl.when(dp == which)
            def _():
                for u in range(n_tile):
                    for q in range(Q):
                        for k in PAIR:
                            filt(src, u, k, q).start()

    for i in range(n_seq):
        swap_u(i).start()
    for f in PAIR:
        swap_f(f).start()

    def forward(u, q):
        @pl.when(on_b)
        def _():
            for side in PAIR:
                landed(u, side, q).wait_recv()
                across(u, side, dp, q).start()

    def front(wbuf, wsem, lhs, stage, st_sem, lhs_sem, tailbuf, q_st, q_sem, vh_st, vh_sem, pbuf):
        def weights(g, j, slot):
            rows = width // 4
            return [pltpu.make_async_copy(w_in.at[i * rows:(i + 1) * rows, at(column(g, j), TN)],
                                          wbuf.at[slot, i * rows:(i + 1) * rows], wsem.at[slot, i]) for i in range(4)]

        def stream(g, body, following, n=nt):
            def step(j, carry):
                slot = parity(j)

                @pl.when(j + 1 < n)
                def _():
                    for copy in weights(g, j + 1, 1 - slot):
                        copy.start()

                if following is not None:
                    @pl.when(j + 1 == n)
                    def _():
                        following(1 - slot)

                for copy in weights(g, j, slot):
                    copy.wait()
                body(j, slot, bias_ref[:, at(column(g, j), TN)], taps_ref[:, at(column(g, j), TN)])
                return carry

            lax.fori_loop(0, n, step, 0)

        def begin(g):
            def start(slot):
                for copy in weights(g, 0, slot):
                    copy.start()
            return start

        def project(rows_ref, slot, bias):
            return (dot(rows_ref, wbuf[slot]) + bias).astype(BF16).astype(F32)

        tail_rows = n_seq * 8
        begin(0)(0)
        own_rows = [pltpu.make_async_copy(u_bf.at[s], lhs.at[pl.ds(pl.multiple_of(tail_rows + s * n_own + c * n_pos, 16), n_pos)], lhs_sem.at[s])
                    for s in range(n_seq)]
        for copy in own_rows:
            copy.start()
        for s in range(n_seq):
            swap_u(s).wait_recv()
        load_rows(stage, st_sem, [(u_sw.at[s, pl.ds(h * hp // GR, hp // GR)], hp, lhs, tail_rows + s * n_own + (1 - c) * n_pos + h * hp)
                                  for s in range(n_seq) for h in PAIR])
        for copy in own_rows:
            copy.wait()

        @pl.when(on_b)
        def _():
            tail_copy().wait_recv()

            @pl.when(sp == 3)
            def _():
                tail_across().start()

            copy = pltpu.make_async_copy(tail, tailbuf, lhs_sem.at[0])
            copy.start()
            copy.wait()

        @pl.when(on_a)
        def _():
            tailbuf[...] = jnp.zeros_like(tailbuf)

        lhs[:tail_rows, :] = tailbuf[...].reshape(tail_rows, width).astype(BF16)
        chunk = n_pos

        def own_phase(g, n, dst, spectrum, following):
            def flush(j, slot):
                blocks = pl.ds(nbo * (1 + j // nt), nbo)
                copies = []
                for h in range(per):
                    u = lax.rem(j, nt) * per + h
                    copies.append(pltpu.make_async_copy(q_st.at[slot, h], dst.at[u, :, blocks], q_sem.at[slot, h]))
                    if spectrum:
                        copies.append(pltpu.make_async_copy(vh_st.at[slot, h], vhat.at[u, :, nbo:], vh_sem.at[slot, h]))
                return copies

            def body(j, slot, bias, taps):
                @pl.when(j >= 2)
                def _():
                    for copy in flush(j - 2, slot):
                        copy.wait()

                for i in range(n_seq * n_own // chunk):
                    s, r = divmod(i * chunk, n_own)
                    p = project(lhs[(tail_rows + i * chunk if i else 0):tail_rows + (i + 1) * chunk, :], slot, bias)
                    if i == 0:
                        for k in range(n_seq):
                            pbuf[k, 0:8] = jnp.where(on_b, p[8 * k:8 * k + 8], 0.0)
                        p = p[tail_rows:]
                    pbuf[s, 8 + r:8 + r + chunk] = p
                    q = short_conv(pbuf.at[s], taps, r, chunk)
                    for b in range(chunk // BLK):
                        blk = q[b * BLK:(b + 1) * BLK]
                        for h in range(per):
                            q_st[slot, h, s, r // BLK + b] = blk[:, h * TC:(h + 1) * TC]
                        if spectrum:
                            spec = block_values(fwd3_ref, blk)
                            for h in range(per):
                                vh_st[slot, h, s, r // BLK + b] = spec[:, h * TC:(h + 1) * TC]
                for copy in flush(j, slot):
                    copy.start()

            stream(g, body, following, n)
            for j in (n - 2, n - 1):
                for copy in flush(j, j % 2):
                    copy.wait()

        own_phase(0, 2 * nt, qx, False, begin(2))
        own_phase(2, nt, qv, True, None)

        def far_phase(fin, fin_sem, fout, fout_sem, parts):
            hk = n_pos // BLK

            def fetch(j, slot):
                mine = at(c * half_w + j * TC, TC)
                srcs = (f1.at[:, mine], f2.at[:, mine], pf.at[0, :, at(j * TC, TC)], pf.at[1, :, at(j * TC, TC)])
                return [pltpu.make_async_copy(src, fin.at[slot, i], fin_sem.at[slot, i]) for i, src in enumerate(srcs)]

            def flush(j, slot):
                return pltpu.make_async_copy(fout.at[slot], far.at[j], fout_sem.at[slot])

            for copy in fetch(0, 0):
                copy.start()

            def step(j, carry):
                slot = parity(j)

                @pl.when(j + 1 < n_tile)
                def _():
                    for copy in fetch(j + 1, 1 - slot):
                        copy.start()

                for copy in fetch(j, slot):
                    copy.wait()

                @pl.when(j >= 2)
                def _():
                    flush(j - 2, slot).wait()

                for f in PAIR:
                    split_blocks(fin.at[slot, f], parts.at[f], c * hk)
                    split_blocks(fin.at[slot, 2 + f], parts.at[f], (1 - c) * hk)
                g_ref = fout.at[slot]
                for f in PAIR:
                    for b in range(2 * hk):
                        g_ref[f, b] = block_spectrum(fwd6_ref, parts.at[f], b)
                    for b in range(2 * hk - 1, 0, -1):
                        for lo, sign in SIDES:
                            re, im, new_re, new_im = shifted_add(g_ref.at[f, b], g_ref.at[f, b - 1], lo, sign)
                            g_ref[f, b, re], g_ref[f, b, im] = new_re, new_im
                flush(j, slot).start()
                return carry

            lax.fori_loop(0, n_tile, step, 0)
            for j in (n_tile - 2, n_tile - 1):
                flush(j, j % 2).wait()

        for f in PAIR:
            swap_f(f).wait_recv()
        pl.run_scoped(
            far_phase, pltpu.VMEM((2, 4, n_pos, TC), F32), pltpu.SemaphoreType.DMA((2, 4)),
            pltpu.VMEM((2, 2, nbo, 2 * BLK, TC), F32), pltpu.SemaphoreType.DMA((2,)), pltpu.VMEM((2, nbo, 3, BLK, TC), BF16))

    pl.run_scoped(
        front,
        pltpu.VMEM((2, width, TN), BF16), pltpu.SemaphoreType.DMA((2, 4)),
        pltpu.VMEM((n_seq * n_own + 8 * n_seq, width), BF16),
        pltpu.VMEM((2, hp // GR, GR, width), F32), pltpu.SemaphoreType.DMA((2,)), pltpu.SemaphoreType.DMA((n_seq,)), pltpu.VMEM((n_seq, 8, width), F32),
        pltpu.VMEM((2, per, n_seq, nbo, BLK, TC), BF16), pltpu.SemaphoreType.DMA((2, per)),
        pltpu.VMEM((2, per, n_seq, nbo, 2 * BLK, TC), F32), pltpu.SemaphoreType.DMA((2, per)),
        pltpu.VMEM((n_seq, n_own + 8, TN), F32))

    def prev(wres, w_sem, lhs_p, stage, st_sem, q_st, q_sem, vh_st, vh_sem, pbuf, pstash):
        def weights(j):
            rows = width // 4
            return [pltpu.make_async_copy(w_in.at[i * rows:(i + 1) * rows, at(which(j), TN)],
                                          wres.at[j, i * rows:(i + 1) * rows], w_sem.at[j, i]) for i in range(4)]

        def which(j):
            return 2 * (j // nt) * width + c * half_w + lax.rem(j, nt) * TN

        def begin(j, carry):
            for copy in weights(j):
                copy.start()
            return carry

        lax.fori_loop(0, 2 * nt, begin, 0)

        def rows(s, h):
            n = cuts[h + 1] - cuts[h]

            @pl.when(on_b)
            def _():
                for src in PAIR:
                    arrived(s, h, src).wait_recv()
                    onward(s, h, src).start()
                for src in PAIR:
                    onward(s, h, src).wait_recv()
                load_rows(stage, st_sem, [(u_x.at[src, s, cuts[h] // GR:cuts[h + 1] // GR], n, lhs_p, src * n) for src in PAIR])

            @pl.when(on_a)
            def _():
                lhs_p[...] = jnp.zeros_like(lhs_p)

        def project(h, j):
            n = 2 * (cuts[h + 1] - cuts[h])
            return (dot(lhs_p[:n, :], wres[j]) + bias_ref[:, at(which(j), TN)]).astype(BF16)

        def first(s, h):
            n = cuts[h + 1] - cuts[h]

            def body(j, carry):
                if h == 0:
                    @pl.when(s == 0)
                    def _():
                        for copy in weights(j):
                            copy.wait()

                p = project(h, j)
                for core in PAIR:
                    pstash[core, cuts[h]:cuts[h + 1], at(j * TN, TN)] = p[core * n:(core + 1) * n]
                return carry

            lax.fori_loop(0, 2 * nt, body, 0)

        def last(s, u, dst):
            base, spectrum = u * nt, u > 0
            h = n_cut - 1
            n = cuts[h + 1] - cuts[h]

            def flush(j):
                slot, copies = parity(j), []
                for half in range(per):
                    copies.append(pltpu.make_async_copy(q_st.at[slot, half], dst.at[j * per + half, s, :nbo], q_sem.at[slot, half]))
                    if spectrum:
                        copies.append(pltpu.make_async_copy(vh_st.at[slot, half], vhat.at[j * per + half, s, :nbo], vh_sem.at[slot, half]))
                return copies

            def body(j, carry):
                slot = parity(j)

                @pl.when(j >= 2)
                def _():
                    for copy in flush(j - 2):
                        copy.wait()

                taps = taps_ref[:, at(which(base + j), TN)]
                pbuf[0:8] = jnp.zeros((8, TN), F32)
                for core in PAIR:
                    old = pstash[core, :cuts[h], at((base + j) * TN, TN)].astype(F32)
                    pbuf[8 + core * n_pos:8 + core * n_pos + cuts[h]] = jnp.where(on_b, old, 0.0)
                p = project(h, base + j).astype(F32)
                for core in PAIR:
                    start = 8 + core * n_pos + cuts[h]
                    pbuf[start:start + n] = jnp.where(on_b, p[core * n:(core + 1) * n], 0.0)
                for b in range(nbo):
                    blk = short_conv(pbuf, taps, b * BLK, BLK)
                    for half in range(per):
                        q_st[slot, half, b] = blk[:, half * TC:(half + 1) * TC]
                    if spectrum:
                        spec = block_values(fwd3_ref, blk)
                        for half in range(per):
                            vh_st[slot, half, b] = spec[:, half * TC:(half + 1) * TC]
                for copy in flush(j):
                    copy.start()

                @pl.when(jnp.logical_and(s == n_seq - 1, jnp.logical_and(lax.rem(j, Q) == 1, j < nt - Q * u)))
                def _():
                    forward(u, j // Q)
                return carry

            lax.fori_loop(0, nt, body, 0)
            for j in (nt - 2, nt - 1):
                for copy in flush(j):
                    copy.wait()

        def one_seq(s, carry):
            for h in range(n_cut - 1):
                rows(s, h)
                first(s, h)
            rows(s, n_cut - 1)
            last(s, 0, qx)
            last(s, 1, qv)
            return carry

        lax.fori_loop(0, n_seq, one_seq, 0)

    pl.run_scoped(
        prev,
        pltpu.VMEM((2 * nt, width, TN), BF16), pltpu.SemaphoreType.DMA((2 * nt, 4)),
        pltpu.VMEM((2 * hp, width), BF16), pltpu.VMEM((2, hp // GR, GR, width), F32), pltpu.SemaphoreType.DMA((2,)),
        pltpu.VMEM((2, per, nbo, BLK, TC), BF16), pltpu.SemaphoreType.DMA((2, per)),
        pltpu.VMEM((2, per, nbo, 2 * BLK, TC), F32), pltpu.SemaphoreType.DMA((2, per)),
        pltpu.VMEM((n_own + 8, TN), F32), pltpu.VMEM((2, cuts[-2], 2 * half_w), BF16))

    @pl.when(on_a)
    def _():
        for u in range(n_tile):
            for f, own in enumerate((f1, f2)):
                fill(f, u, c, own, c * half_w + u * TC).start()
                fill(f, u, 1 - c, pf.at[f], u * TC).start()

    def conv(x1b, vb, x2b, vhb, farb, in_sem, vh_sem, kst, k_sem, sendbuf, *scratch):
        def fetch(t):
            slot, two = lax.rem(t, 3), parity(t)
            srcs = (qx.at[t, :, :2 * nbo], qv.at[t], qx.at[t, :, 2 * nbo:], far.at[t])
            copies = [pltpu.make_async_copy(r, b.at[slot], in_sem.at[slot, i])
                      for i, (r, b) in enumerate(zip(srcs, (x1b, vb, x2b, farb)))]
            return copies + [pltpu.make_async_copy(vhat.at[t, s], vhb.at[two, s], vh_sem.at[two, s]) for s in range(n_seq)]

        def flush(t):
            slot = parity(t)
            return pltpu.make_async_copy(kst.at[slot], keep.at[t], k_sem.at[slot])

        def swap_y(u):
            return remote(sendbuf.at[parity(u)], part.at[u], p_send.at[u], p_recv.at[u], (dp, other))

        tile = ConvTile(fwd6_ref, inv6_ref, *scratch)

        def inputs(t, back):
            slot, cols = lax.rem(t + 3 - back, 3), at(c * half_w + lax.rem(t + n_tile - back, n_tile) * TC, TC)
            return x1b.at[slot], vb.at[slot], x2b.at[slot], farb.at[slot], sk1_ref[:, cols], sk2_ref[:, cols]

        def emit(t):
            slot = parity(t)

            @pl.when(t >= 2)
            def _():
                flush(t - 2).wait()
                swap_y(t - 2).wait_send()

            tile.result(c, kst.at[slot], sendbuf.at[slot])
            flush(t).start()
            swap_y(t).start()

        for copy in fetch(0):
            copy.start()
        forward(1, Q - 1)

        def step(t, carry):
            @pl.when(t + 1 < n_tile)
            def _():
                for copy in fetch(t + 1):
                    copy.start()

            @pl.when(on_a)
            def _():
                for f in PAIR:
                    for side in PAIR:
                        fill(f, t, side, f1, 0).wait()

            @pl.when(on_b)
            def _():
                for q in range(Q):
                    for side in PAIR:
                        across(t, side, 1 - dp, q).wait_recv()

            for copy in fetch(t):
                copy.wait()

            def relay(q):
                @pl.when(t + 2 < n_tile)
                def _():
                    forward(t + 2, q)

            tile.step(land, t, vhb.at[parity(t)], inputs(t, 0), inputs(t, 1), relay)

            @pl.when(t >= 1)
            def _():
                emit(t - 1)
            return carry

        lax.fori_loop(0, n_tile, step, 0)
        tile.drain(inputs(n_tile, 1))
        emit(n_tile - 1)
        for u in (n_tile - 2, n_tile - 1):
            flush(u).wait()
            swap_y(u).wait_send()
        for u in range(n_tile):
            swap_y(u).wait_recv()

    nb = 2 * nbo
    pl.run_scoped(
        conv,
        pltpu.VMEM((3, n_seq, nb, BLK, TC), BF16), pltpu.VMEM((3, n_seq, nb, BLK, TC), BF16), pltpu.VMEM((3, n_seq, nbo, BLK, TC), BF16),
        pltpu.VMEM((2, n_seq, nb, 2 * BLK, TC), F32), pltpu.VMEM((3, 2, nbo, 2 * BLK, TC), F32),
        pltpu.SemaphoreType.DMA((3, 4)), pltpu.SemaphoreType.DMA((2, n_seq)),
        pltpu.VMEM((2, n_seq, n_pos, TC), BF16), pltpu.SemaphoreType.DMA((2,)), pltpu.VMEM((2, n_seq, n_pos, TC), F32),
        pltpu.VMEM((2, nbo, 3, BLK, TC), BF16),
        pltpu.VMEM((nbo + 1, 2 * BLK, TC), F32), pltpu.VMEM((nbo + 1, 2 * BLK, TC), F32), pltpu.VMEM((nbo, 2 * BLK, TC), F32),
        *[pltpu.VMEM((nb, 3, 2 * BLK, TC), BF16)] * n_seq,
        pltpu.VMEM((nb, 3, BLK, TC), BF16),
        *[pltpu.VMEM((nb, BLK, TC), F32)] * n_seq,
        pltpu.VMEM((nb, 2 * BLK, TC), F32),
        *[pltpu.VMEM((nbo, 3, 2 * BLK, TC), BF16)] * n_seq,
        pltpu.VMEM((n_seq, nbo, BLK, TC), BF16))

    for s in range(n_seq):
        swap_u(s).wait_send()
    for f in PAIR:
        swap_f(f).wait_send()

    @pl.when(sp == 1)
    def _():
        tail_copy().wait_send()

    @pl.when(sp == 3)
    def _():
        tail_across().wait_send()

    @pl.when(on_a)
    def _():
        for i in range(n_seq * n_cut):
            for k in PAIR:
                over(*divmod(i, n_cut), k).wait_send()
        for u in range(n_tile):
            for q in range(Q):
                for k in PAIR:
                    filt(f1, u, k, q).wait_send()

    @pl.when(on_b)
    def _():
        for i in range(n_seq * n_cut):
            for src in PAIR:
                onward(*divmod(i, n_cut), src).wait_send()
        for u in range(n_tile):
            for q in range(Q):
                for side in PAIR:
                    across(u, side, dp, q).wait_send()


def loop(trips):
    def run(body):
        def step(i, carry):
            body(i)
            return carry
        lax.fori_loop(0, trips, step, 0)
    return run


class ConvTile:
    def __init__(self, fwd6, inv6, hparts, g1, g2, raw2, sp0, sp1, zparts, zv0, zv1, zhat, sq0, sq1, ybuf):
        self.fwd6, self.inv6, self.hparts, self.g, self.raw2 = fwd6, inv6, hparts, (g1, g2), raw2
        self.first, self.second, self.zparts, self.zval, self.zhat, self.ybuf = (sp0, sp1), (sq0, sq1), zparts, (zv0, zv1), zhat, ybuf
        self.nb, self.nbo = sp0.shape[0], sq0.shape[0]

    def near(self, land, t, f):
        for side in PAIR:
            split_blocks(land.at[f, t, side], self.hparts.at[f], side * self.nbo // 2)

    def window(self, f, raw, far):
        g, nbo = self.g[f], self.nbo
        for j in range(nbo, 0, -1):
            cur = far.at[f, 0] if j == nbo else raw.at[j]
            for lo, sign in SIDES:
                re, im, new_re, new_im = shifted_add(cur, raw.at[j - 1], lo, sign)
                g[j, re], g[j, im] = new_re, new_im
        if raw is not g:
            g[0] = raw[0]

    def pointwise(self, xhat, f, far, dst, r, first):
        g, nbo = self.g[f], self.nbo
        re, im = pl.ds(pl.multiple_of(r * 16, 16), 16), pl.ds(pl.multiple_of(BLK + r * 16, 16), 16)
        for k in range(first, self.nb):
            acc_re = acc_im = None
            for j in range(k + 1):
                i = k - j
                gr, gi = (g[i, re], g[i, im]) if i <= nbo else (far[f, i - nbo, re], far[f, i - nbo, im])
                xr, xi = xhat[j, re], xhat[j, im]
                t_re, t_im = xr * gr - xi * gi, xr * gi + xi * gr
                acc_re = t_re if acc_re is None else acc_re + t_re
                acc_im = t_im if acc_im is None else acc_im + t_im
            for part, (a, b) in enumerate(zip(split3(acc_re), split3(acc_im))):
                dst[k - first, part, re], dst[k - first, part, im] = a, b

    def inverse(self, parts, k):
        return dot(self.inv6[...], stack6(parts[k, 0], parts[k, 1], parts[k, 2]))

    def gate_one(self, s, k, data):
        x1, v, _, _, skip, _ = data
        z = x1[s, k].astype(F32) * (self.inverse(self.first[s], k) + skip * v[s, k].astype(F32))
        self.zval[s][k] = z
        for part, a in enumerate(split3(z)):
            self.zparts[k, part] = a

    def spectrum(self, k):
        self.zhat[k] = block_spectrum(self.fwd6, self.zparts, k)

    def gate_two(self, s, k, data):
        y = data[2][s, k].astype(F32) * (self.inverse(self.second[s], k) + data[5] * self.zval[s][self.nbo + k])
        self.ybuf[s, k] = y.astype(BF16)

    def middle(self, s, data, i, point=None):
        for q in range(4):
            if point is not None:
                point(4 * i + q)
            for k in PAIR:
                if q < 2:
                    self.gate_one(s, 4 * i + 2 * q + k, data)
                else:
                    self.spectrum(4 * i + 2 * (q - 2) + k)

    def step(self, land, t, vhat, data, old, relay):
        nb, nbo = self.nb, self.nbo
        far = data[3]
        self.near(land, t, 0)
        for j in range(nbo):
            self.g[0][j] = block_spectrum(self.fwd6, self.hparts.at[0], j)
        self.near(land, t, 1)
        self.window(0, self.g[0], far)

        @loop(nb // 4)
        def _(i):
            self.middle(1, old, i, lambda r: self.pointwise(vhat.at[0], 0, far, self.first[0], r, 0))


        @loop(nbo // 2)
        def _(i):
            for q in range(4):
                self.pointwise(self.zhat, 1, old[3], self.second[1], 4 * i + q, nbo)
                if q < 2:
                    self.gate_two(0, 2 * i + q, old)
                else:
                    j = 2 * i + q - 2
                    self.raw2[j] = block_spectrum(self.fwd6, self.hparts.at[1], j)

        relay(0)
        self.window(1, self.raw2, far)

        @loop(nb // 4)
        def _(i):
            self.middle(0, data, i, lambda r: self.pointwise(vhat.at[1], 0, far, self.first[1], r, 0))

        @loop(nbo // 2)
        def _(i):
            for q in range(4):
                self.pointwise(self.zhat, 1, far, self.second[0], 4 * i + q, nbo)
                if q % 2 == 0:
                    self.gate_two(1, 2 * i + q // 2, old)

        relay(1)

    def drain(self, data):
        nb, nbo = self.nb, self.nbo

        @loop(nb // 4)
        def _(i):
            self.middle(1, data, i)

        @loop(nbo // 2)
        def _(i):
            for q in range(4):
                self.pointwise(self.zhat, 1, data[3], self.second[1], 4 * i + q, nbo)
                if q % 2 == 0:
                    self.gate_two(0, 2 * i + q // 2, data)

        for k in range(nbo):
            self.gate_two(1, k, data)

    def result(self, c, keep, send):
        hk = self.nbo // 2
        for s in range(self.ybuf.shape[0]):
            for b in range(hk):
                keep[s, b * BLK:(b + 1) * BLK] = self.ybuf[s, c * hk + b]
                send[s, b * BLK:(b + 1) * BLK] = self.ybuf[s, (1 - c) * hk + b].astype(F32)


def out_body(keep, part, w_out, u_in, out, wbuf, w_sem, lhs, keep_v, stage, in_sem, u_v, o_st, o_sem):
    c = lax.rem(lax.axis_index("sp"), 2)
    n_tile, n_seq, n_pos, _ = keep.shape
    half_w = n_tile * TC
    width = 2 * half_w
    n_col, rows = width // TN, width // 4

    def weights(j, slot):
        cols = pl.ds(pl.multiple_of(j * TN, TN), TN)
        return [pltpu.make_async_copy(w_out.at[i * rows:(i + 1) * rows, cols],
                                      wbuf.at[slot, i * rows:(i + 1) * rows], w_sem.at[slot, i]) for i in range(4)] + [
                    pltpu.make_async_copy(u_in.at[:, :, cols], u_v.at[slot], w_sem.at[slot, 4])]

    def flush(j):
        slot = parity(j)
        return pltpu.make_async_copy(o_st.at[slot], out.at[:, :, pl.ds(pl.multiple_of(j * TN, TN), TN)], o_sem.at[slot])

    loads = [pltpu.make_async_copy(part.at[u], stage.at[u], in_sem.at[u]) for u in range(n_tile)]
    loads += [pltpu.make_async_copy(keep.at[u], keep_v.at[u], in_sem.at[n_tile + u]) for u in range(n_tile)]
    for copy in loads:
        copy.start()
    for copy in weights(0, 0):
        copy.start()
    for u in range(n_tile):
        loads[u].wait()
        loads[n_tile + u].wait()
        for s in range(n_seq):
            lhs[s, :, pl.ds(pl.multiple_of((1 - c) * half_w + u * TC, TC), TC)] = stage[u, s].astype(BF16)
            lhs[s, :, pl.ds(pl.multiple_of(c * half_w + u * TC, TC), TC)] = keep_v[u, s]

    def step(j, carry):
        slot = parity(j)

        @pl.when(j + 1 < n_col)
        def _():
            for copy in weights(j + 1, 1 - slot):
                copy.start()

        for copy in weights(j, slot):
            copy.wait()

        @pl.when(j >= 2)
        def _():
            flush(j - 2).wait()

        for s in range(n_seq):
            o_st[slot, s] = (u_v[slot, s].astype(F32) + dot(lhs[s], wbuf[slot])).astype(BF16)
        flush(j).start()
        return carry

    lax.fori_loop(0, n_col, step, 0)
    for j in (n_col - 2, n_col - 1):
        flush(j).wait()


def solution(mesh):
    fwd3, fwd6, inv6 = transform_tables()

    def local_step(u_in, w_in, b_in, conv_taps, w_out, skip_one, skip_two, filt_one, filt_two):
        n_seq, n_pos, width = u_in.shape
        half_w = width // 2
        n_own = 2 * n_pos
        nb = 2 * n_own // BLK
        nbo = nb // 2
        n_tile = half_w // TC
        rows = n_pos // GR, GR, width
        small, large = pl.BlockSpec(memory_space=pltpu.VMEM), pl.BlockSpec(memory_space=pl.ANY)
        dma = pltpu.SemaphoreType.DMA

        def shape(dims, dtype=F32):
            return jax.ShapeDtypeStruct(dims, dtype)

        keep, part, *_ = pl.pallas_call(
            main_body,
            in_specs=[small] * 7 + [large] * 4,
            out_specs=[large] * 12,
            out_shape=[
                shape((n_tile, n_seq, n_pos, TC), BF16), shape((n_tile, n_seq, n_pos, TC)),
                shape((n_tile, n_seq, nb + nbo, BLK, TC), BF16), shape((n_tile, n_seq, nb, BLK, TC), BF16),
                shape((n_tile, n_seq, nb, 2 * BLK, TC)), shape((n_tile, 2, nbo, 2 * BLK, TC)),
                shape((n_seq, *rows)), shape((n_seq, 8, width)), shape((n_seq, *rows)), shape((2, n_seq, *rows)),
                shape((n_seq, 8, width)), shape((2, n_pos, half_w)),
            ],
            scratch_shapes=[
                pltpu.VMEM((2, n_tile, 2, n_pos, TC), F32),
                dma((1,)), dma((1,)), *[dma((n_seq, 3, 2))] * 4, *[dma((n_seq,))] * 2, *[dma((2,))] * 2,
                dma((2, n_tile, 2)), *[dma((n_tile, Q, 2))] * 4, *[dma((n_tile,))] * 2,
            ],
            compiler_params=pltpu.CompilerParams(vmem_limit_bytes=62 << 20, collective_id=0, has_side_effects=True),
            name="hyena_main",
        )(fwd3, fwd6, inv6, b_in.reshape(1, -1), conv_taps, skip_one.reshape(1, -1), skip_two.reshape(1, -1),
          u_in, w_in, filt_one, filt_two)

        return pl.pallas_call(
            out_body,
            in_specs=[large] * 4,
            out_specs=large,
            out_shape=shape((n_seq, n_pos, width), BF16),
            scratch_shapes=[
                pltpu.VMEM((2, width, TN), BF16), dma((2, 5)),
                pltpu.VMEM((n_seq, n_pos, width), BF16), pltpu.VMEM((n_tile, n_seq, n_pos, TC), BF16), pltpu.VMEM((n_tile, n_seq, n_pos, TC), F32),
                dma((2 * n_tile,)), pltpu.VMEM((2, n_seq, n_pos, TN), BF16), pltpu.VMEM((2, n_seq, n_pos, TN), BF16), dma((2,)),
            ],
            compiler_params=pltpu.CompilerParams(vmem_limit_bytes=60 << 20),
            name="out_proj",
        )(keep, part, w_out, u_in)

    seq_spec = P("dp", "sp", None)
    filt_spec = P("sp", None)
    return jax.shard_map(local_step, mesh=mesh, in_specs=(seq_spec, P(), P(), P(), P(), P(), P(), filt_spec, filt_spec), out_specs=seq_spec, check_vma=False)
```

```python
import functools

import jax
import jax.numpy as jnp
import numpy as np
from jax import lax
from jax.experimental import pallas as pl
from jax.experimental.pallas import tpu as pltpu
from jax.sharding import PartitionSpec as P

F32, BF16 = jnp.float32, jnp.bfloat16
BLK = 128
TN = 512
TC = 256
Q = 2
PAIR = (0, 1)
GR = 32
MESH = pl.DeviceIdType.MESH


def split_table(table):
    parts, rest = [], table.astype(np.float64)
    for _ in range(3):
        part = rest.astype(np.float32).astype(jnp.bfloat16)
        parts.append(part)
        rest = rest - part.astype(np.float64)
    return parts


def transform_tables():
    freq = np.concatenate([np.arange(0, BLK, 2), np.arange(1, BLK, 2)]) + 0.5
    angle = 2.0 * np.pi * freq[:, None] * np.arange(BLK)[None, :] / (2 * BLK)
    fwd = np.concatenate([np.cos(angle), -np.sin(angle)], 0)
    inv = np.concatenate([np.cos(angle).T, -np.sin(angle).T], 1) / BLK
    f1, f2, f3 = split_table(fwd)
    e1, e2, e3 = split_table(inv)
    fwd3 = np.concatenate([f1, f2, f3], 1)
    fwd6 = np.concatenate([f1, f1, f2, f2, f1, f3], 1)
    inv6 = np.concatenate([e1, e1, e2, e2, e1, e3], 1)
    return fwd3, fwd6, inv6


def parity(x):
    return lax.rem(x, 2)


def dot(a, b):
    return jnp.dot(a, b, preferred_element_type=F32)


def split3(x):
    hi = x.astype(BF16)
    rest = x - hi.astype(F32)
    mid = rest.astype(BF16)
    low = (rest - mid.astype(F32)).astype(BF16)
    return hi, mid, low


def stack6(hi, mid, low):
    return jnp.concatenate([hi, mid, hi, mid, low, hi], axis=0)


def split_blocks(src, parts, first):
    for j in range(src.shape[0] // BLK):
        for i, a in enumerate(split3(src[j * BLK:(j + 1) * BLK])):
            parts[first + j, i] = a


def block_spectrum(fwd6_ref, parts, j):
    return dot(fwd6_ref[...], stack6(parts[j, 0], parts[j, 1], parts[j, 2]))


def shifted_add(cur, old, lo, sign):
    re, im = slice(lo, lo + BLK // 2), slice(BLK + lo, BLK + lo + BLK // 2)
    return re, im, cur[re] - sign * old[im], cur[im] + sign * old[re]


SIDES = ((0, 1.0), (BLK // 2, -1.0))


def short_conv(pbuf, t, first, rows):
    return (t[0:1] * pbuf[8 + first:8 + first + rows] + t[1:2] * pbuf[7 + first:7 + first + rows] + t[2:3] * pbuf[6 + first:6 + first + rows]).astype(BF16)


def block_values(fwd3_ref, blk):
    return dot(fwd3_ref[...], jnp.concatenate([blk, blk, blk], axis=0))


def main_body(fwd3_ref, fwd6_ref, inv6_ref, bias_ref, taps_ref, sk1_ref, sk2_ref, u_bf, w_in, f1, f2,
              keep, part, qx, qv, vhat, far, u32, tsrc, u_sw, u_x, tail, pf,
              land, ts, tr, os, orr, ws, wr, ss, sr, fs, fr, l_sem, x_send, x_recv, y_send, y_recv, p_send, p_recv):
    sp, dp = lax.axis_index("sp"), lax.axis_index("dp")
    c = parity(sp)
    on_b = sp >= 2
    on_a = jnp.logical_not(on_b)
    other = sp + 1 - 2 * c
    n_seq, n_pos, width = u_bf.shape
    half_w = width // 2
    nt, n_tile, per = half_w // TN, half_w // TC, TN // TC
    n_own, hp = 2 * n_pos, n_pos // 2
    nbo = n_own // BLK
    cuts = (0, hp, hp + hp // 2, n_pos)
    n_cut = len(cuts) - 1

    def remote(src, dst, send, recv, peer):
        return pltpu.make_async_remote_copy(src, dst, send, recv, device_id=peer, device_id_type=MESH)

    def at(start, size):
        return pl.ds(pl.multiple_of(start, size), size)

    def share(s, h, k):
        rows = (cuts[h + 1] - cuts[h]) // 2
        return s, pl.ds((cuts[h] + k * rows) // GR, rows // GR)

    def tail_copy():
        return remote(tsrc, tail, ts.at[0], tr.at[0], (dp, 3))

    def tail_across():
        return remote(tail, tail, ts.at[0], tr.at[0], (dp, other))

    def over(s, h, k):
        s, rows = share(s, h, k)
        return remote(u32.at[s, rows], u_x.at[c, s, rows], os.at[s, h, k], orr.at[s, h, c], (dp, 2 + k))

    def arrived(s, h, src):
        at_s, rows = share(s, h, 0)
        ref = u_x.at[src, at_s, rows]
        return remote(ref, ref, os.at[s, h, src], orr.at[s, h, src], (dp, sp))

    def onward(s, h, src):
        at_s, rows = share(s, h, c)
        ref = u_x.at[src, at_s, rows]
        return remote(ref, ref, ws.at[s, h, src], wr.at[s, h, src], (dp, other))

    def swap_u(s):
        return remote(u32.at[s], u_sw.at[s], ss.at[s], sr.at[s], (dp, other))

    def swap_f(f):
        return remote((f1, f2)[f].at[:, at((1 - c) * half_w, half_w)], pf.at[f], fs.at[f], fr.at[f], (dp, other))

    qr = n_pos // Q

    def filt(src, u, k, q):
        return remote(src.at[q * qr:(q + 1) * qr, at(k * half_w + u * TC, TC)], land.at[dp, u, c, q * qr:(q + 1) * qr],
                      x_send.at[u, q, k], x_recv.at[u, q, c], (dp, 2 + k))

    def direct(src, k):
        u, q = n_tile - 1, Q - 1
        return remote(src.at[q * qr:(q + 1) * qr, at(k * half_w + u * TC, TC)], land.at[1 - dp, u, c, q * qr:(q + 1) * qr],
                      y_send.at[u, q, k], y_recv.at[u, q, c], (dp, 2 + k))

    def landed(u, side, q):
        ref = land.at[dp, u, side, at(q * qr, qr)]
        return remote(ref, ref, x_send.at[u, q, side], x_recv.at[u, q, side], (dp, sp))

    def across(u, side, f, q):
        ref = land.at[f, u, side, at(q * qr, qr)]
        return remote(ref, ref, y_send.at[u, q, side], y_recv.at[u, q, side], (1 - dp, sp))

    def fill(f, u, side, src, start):
        return pltpu.make_async_copy(src.at[:, at(start, TC)], land.at[f, u, side], l_sem.at[f, u, side])

    def column(g, j):
        return (g + j // nt) * width + c * half_w + lax.rem(j, nt) * TN

    def load_rows(stage, st_sem, items):
        def copy(i):
            src, rows, _, _ = items[i]
            return pltpu.make_async_copy(src, stage.at[i % 2, :rows // GR], st_sem.at[i % 2])

        copy(0).start()
        for i, (_, rows, dst, row) in enumerate(items):
            if i + 1 < len(items):
                copy(i + 1).start()
            copy(i).wait()
            dst[pl.ds(pl.multiple_of(row, 16), rows), :] = stage[i % 2, :rows // GR].reshape(rows, width).astype(BF16)

    barrier = pltpu.get_barrier_semaphore()
    for peer in ((dp, other), (dp, lax.rem(sp + 2, 4)), (dp, lax.rem(other + 2, 4)), (1 - dp, sp)):
        pl.semaphore_signal(barrier, inc=1, device_id=peer, device_id_type=MESH)
    pl.semaphore_wait(barrier, 4)

    def widen(raw, wide, tail_raw, tail_wide, in_sem, out_sem):
        def half(ref, s, h):
            return ref.at[s, h * hp:h * hp + hp]

        def load(s, h):
            return pltpu.make_async_copy(half(u_bf, s, h), raw.at[h], in_sem.at[h])

        last_rows = pltpu.make_async_copy(u_bf.at[:, n_pos - 8:], tail_raw, in_sem.at[2])
        last_out = pltpu.make_async_copy(tail_wide, tsrc, out_sem.at[2])
        order = [(s, h) for s in range(n_seq) for h in PAIR]
        last_rows.start()
        load(*order[0]).start()
        last_rows.wait()
        tail_wide[...] = tail_raw[...].astype(F32)
        last_out.start()
        pending = {}
        for (s, h), following in zip(order, order[1:] + [None]):
            if following:
                load(*following).start()
            load(s, h).wait()
            if h in pending:
                pending.pop(h).wait()
            wide[h] = raw[h].astype(F32).reshape(wide.shape[1:])
            store = pltpu.make_async_copy(wide.at[h], u32.at[s, pl.ds(h * hp // GR, hp // GR)], out_sem.at[h])
            store.start()
            if s + h:
                pending[h] = store
                continue
            last_out.wait()

            @pl.when(sp == 1)
            def _():
                tail_copy().start()

            store.wait()

            @pl.when(on_a)
            def _():
                for k in PAIR:
                    over(s, h, k).start()

        for store in pending.values():
            store.wait()

    pl.run_scoped(
        widen, pltpu.VMEM((2, hp, width), BF16), pltpu.VMEM((2, hp // GR, GR, width), F32), pltpu.VMEM((n_seq, 8, width), BF16),
        pltpu.VMEM((n_seq, 8, width), F32), pltpu.SemaphoreType.DMA((3,)), pltpu.SemaphoreType.DMA((3,)))

    @pl.when(on_a)
    def _():
        for i in range(1, n_seq * n_cut):
            for k in PAIR:
                over(*divmod(i, n_cut), k).start()
        for which, src, rest in ((0, f1, f2), (1, f2, f1)):
            @pl.when(dp == which)
            def _():
                for u in range(n_tile):
                    for q in range(Q):
                        for k in PAIR:
                            filt(src, u, k, q).start()
                for k in PAIR:
                    direct(rest, k).start()

    for i in range(n_seq):
        swap_u(i).start()
    for f in PAIR:
        swap_f(f).start()

    def forward(u, q):
        @pl.when(on_b)
        def _():
            for side in PAIR:
                landed(u, side, q).wait_recv()
                across(u, side, dp, q).start()

    def front(wbuf, wsem, lhs, stage, st_sem, lhs_sem, tailbuf, q_st, q_sem, vh_st, vh_sem, pbuf):
        def weights(g, j, slot):
            rows = width // 4
            return [pltpu.make_async_copy(w_in.at[i * rows:(i + 1) * rows, at(column(g, j), TN)],
                                          wbuf.at[slot, i * rows:(i + 1) * rows], wsem.at[slot, i]) for i in range(4)]

        def stream(g, body, following, n=nt):
            def step(j, carry):
                slot = parity(j)

                @pl.when(j + 1 < n)
                def _():
                    for copy in weights(g, j + 1, 1 - slot):
                        copy.start()

                if following is not None:
                    @pl.when(j + 1 == n)
                    def _():
                        following(1 - slot)

                for copy in weights(g, j, slot):
                    copy.wait()
                body(j, slot, bias_ref[:, at(column(g, j), TN)], taps_ref[:, at(column(g, j), TN)])
                return carry

            lax.fori_loop(0, n, step, 0)

        def begin(g):
            def start(slot):
                for copy in weights(g, 0, slot):
                    copy.start()
            return start

        def project(rows_ref, slot, bias):
            return (dot(rows_ref, wbuf[slot]) + bias).astype(BF16).astype(F32)

        tail_rows = n_seq * 8
        begin(0)(0)
        own_rows = [pltpu.make_async_copy(u_bf.at[s], lhs.at[pl.ds(pl.multiple_of(tail_rows + s * n_own + c * n_pos, 16), n_pos)], lhs_sem.at[s])
                    for s in range(n_seq)]
        for copy in own_rows:
            copy.start()
        for s in range(n_seq):
            swap_u(s).wait_recv()
        load_rows(stage, st_sem, [(u_sw.at[s, pl.ds(h * hp // GR, hp // GR)], hp, lhs, tail_rows + s * n_own + (1 - c) * n_pos + h * hp)
                                  for s in range(n_seq) for h in PAIR])
        for copy in own_rows:
            copy.wait()

        @pl.when(on_b)
        def _():
            tail_copy().wait_recv()

            @pl.when(sp == 3)
            def _():
                tail_across().start()

            copy = pltpu.make_async_copy(tail, tailbuf, lhs_sem.at[0])
            copy.start()
            copy.wait()

        @pl.when(on_a)
        def _():
            tailbuf[...] = jnp.zeros_like(tailbuf)

        lhs[:tail_rows, :] = tailbuf[...].reshape(tail_rows, width).astype(BF16)
        chunk = n_pos

        def own_phase(g, n, dst, spectrum, following):
            def flush(j, slot):
                blocks = pl.ds(nbo * (1 + j // nt), nbo)
                copies = []
                for h in range(per):
                    u = lax.rem(j, nt) * per + h
                    copies.append(pltpu.make_async_copy(q_st.at[slot, h], dst.at[u, :, blocks], q_sem.at[slot, h]))
                    if spectrum:
                        copies.append(pltpu.make_async_copy(vh_st.at[slot, h], vhat.at[u, :, nbo:], vh_sem.at[slot, h]))
                return copies

            def body(j, slot, bias, taps):
                @pl.when(j >= 2)
                def _():
                    for copy in flush(j - 2, slot):
                        copy.wait()

                for i in range(n_seq * n_own // chunk):
                    s, r = divmod(i * chunk, n_own)
                    p = project(lhs[(tail_rows + i * chunk if i else 0):tail_rows + (i + 1) * chunk, :], slot, bias)
                    if i == 0:
                        for k in range(n_seq):
                            pbuf[k, 0:8] = jnp.where(on_b, p[8 * k:8 * k + 8], 0.0)
                        p = p[tail_rows:]
                    pbuf[s, 8 + r:8 + r + chunk] = p
                    q = short_conv(pbuf.at[s], taps, r, chunk)
                    for b in range(chunk // BLK):
                        blk = q[b * BLK:(b + 1) * BLK]
                        for h in range(per):
                            q_st[slot, h, s, r // BLK + b] = blk[:, h * TC:(h + 1) * TC]
                        if spectrum:
                            spec = block_values(fwd3_ref, blk)
                            for h in range(per):
                                vh_st[slot, h, s, r // BLK + b] = spec[:, h * TC:(h + 1) * TC]
                for copy in flush(j, slot):
                    copy.start()

            stream(g, body, following, n)
            for j in (n - 2, n - 1):
                for copy in flush(j, j % 2):
                    copy.wait()

        own_phase(0, 2 * nt, qx, False, begin(2))
        own_phase(2, nt, qv, True, None)

        def far_phase(fin, fin_sem, fout, fout_sem, parts):
            hk = n_pos // BLK

            def fetch(j, slot):
                mine = at(c * half_w + j * TC, TC)
                srcs = (f1.at[:, mine], f2.at[:, mine], pf.at[0, :, at(j * TC, TC)], pf.at[1, :, at(j * TC, TC)])
                return [pltpu.make_async_copy(src, fin.at[slot, i], fin_sem.at[slot, i]) for i, src in enumerate(srcs)]

            def flush(j, slot):
                return pltpu.make_async_copy(fout.at[slot], far.at[j], fout_sem.at[slot])

            for copy in fetch(0, 0):
                copy.start()

            def step(j, carry):
                slot = parity(j)

                @pl.when(j + 1 < n_tile)
                def _():
                    for copy in fetch(j + 1, 1 - slot):
                        copy.start()

                for copy in fetch(j, slot):
                    copy.wait()

                @pl.when(j >= 2)
                def _():
                    flush(j - 2, slot).wait()

                for f in PAIR:
                    split_blocks(fin.at[slot, f], parts.at[f], c * hk)
                    split_blocks(fin.at[slot, 2 + f], parts.at[f], (1 - c) * hk)
                g_ref = fout.at[slot]
                for f in PAIR:
                    for b in range(2 * hk):
                        g_ref[f, b] = block_spectrum(fwd6_ref, parts.at[f], b)
                    for b in range(2 * hk - 1, 0, -1):
                        for lo, sign in SIDES:
                            re, im, new_re, new_im = shifted_add(g_ref.at[f, b], g_ref.at[f, b - 1], lo, sign)
                            g_ref[f, b, re], g_ref[f, b, im] = new_re, new_im
                flush(j, slot).start()
                return carry

            lax.fori_loop(0, n_tile, step, 0)
            for j in (n_tile - 2, n_tile - 1):
                flush(j, j % 2).wait()

        for f in PAIR:
            swap_f(f).wait_recv()
        pl.run_scoped(
            far_phase, pltpu.VMEM((2, 4, n_pos, TC), F32), pltpu.SemaphoreType.DMA((2, 4)),
            pltpu.VMEM((2, 2, nbo, 2 * BLK, TC), F32), pltpu.SemaphoreType.DMA((2,)), pltpu.VMEM((2, nbo, 3, BLK, TC), BF16))

    pl.run_scoped(
        front,
        pltpu.VMEM((2, width, TN), BF16), pltpu.SemaphoreType.DMA((2, 4)),
        pltpu.VMEM((n_seq * n_own + 8 * n_seq, width), BF16),
        pltpu.VMEM((2, hp // GR, GR, width), F32), pltpu.SemaphoreType.DMA((2,)), pltpu.SemaphoreType.DMA((n_seq,)), pltpu.VMEM((n_seq, 8, width), F32),
        pltpu.VMEM((2, per, n_seq, nbo, BLK, TC), BF16), pltpu.SemaphoreType.DMA((2, per)),
        pltpu.VMEM((2, per, n_seq, nbo, 2 * BLK, TC), F32), pltpu.SemaphoreType.DMA((2, per)),
        pltpu.VMEM((n_seq, n_own + 8, TN), F32))

    def prev(wres, w_sem, lhs_p, stage, st_sem, q_st, q_sem, vh_st, vh_sem, pbuf, pstash):
        def weights(j):
            rows = width // 4
            return [pltpu.make_async_copy(w_in.at[i * rows:(i + 1) * rows, at(which(j), TN)],
                                          wres.at[j, i * rows:(i + 1) * rows], w_sem.at[j, i]) for i in range(4)]

        def which(j):
            return 2 * (j // nt) * width + c * half_w + lax.rem(j, nt) * TN

        def begin(j, carry):
            for copy in weights(j):
                copy.start()
            return carry

        lax.fori_loop(0, 2 * nt, begin, 0)

        def rows(s, h):
            n = cuts[h + 1] - cuts[h]

            @pl.when(on_b)
            def _():
                for src in PAIR:
                    arrived(s, h, src).wait_recv()
                    onward(s, h, src).start()
                for src in PAIR:
                    onward(s, h, src).wait_recv()
                load_rows(stage, st_sem, [(u_x.at[src, s, cuts[h] // GR:cuts[h + 1] // GR], n, lhs_p, src * n) for src in PAIR])

            @pl.when(on_a)
            def _():
                lhs_p[...] = jnp.zeros_like(lhs_p)

        def project(h, j):
            n = 2 * (cuts[h + 1] - cuts[h])
            return (dot(lhs_p[:n, :], wres[j]) + bias_ref[:, at(which(j), TN)]).astype(BF16)

        def first(s, h):
            n = cuts[h + 1] - cuts[h]

            def body(j, carry):
                if h == 0:
                    @pl.when(s == 0)
                    def _():
                        for copy in weights(j):
                            copy.wait()

                p = project(h, j)
                for core in PAIR:
                    pstash[core, cuts[h]:cuts[h + 1], at(j * TN, TN)] = p[core * n:(core + 1) * n]
                return carry

            lax.fori_loop(0, 2 * nt, body, 0)

        def last(s, u, dst):
            base, spectrum = u * nt, u > 0
            h = n_cut - 1
            n = cuts[h + 1] - cuts[h]

            def flush(j):
                slot, copies = parity(j), []
                for half in range(per):
                    copies.append(pltpu.make_async_copy(q_st.at[slot, half], dst.at[j * per + half, s, :nbo], q_sem.at[slot, half]))
                    if spectrum:
                        copies.append(pltpu.make_async_copy(vh_st.at[slot, half], vhat.at[j * per + half, s, :nbo], vh_sem.at[slot, half]))
                return copies

            def body(j, carry):
                slot = parity(j)

                @pl.when(j >= 2)
                def _():
                    for copy in flush(j - 2):
                        copy.wait()

                taps = taps_ref[:, at(which(base + j), TN)]
                pbuf[0:8] = jnp.zeros((8, TN), F32)
                for core in PAIR:
                    old = pstash[core, :cuts[h], at((base + j) * TN, TN)].astype(F32)
                    pbuf[8 + core * n_pos:8 + core * n_pos + cuts[h]] = jnp.where(on_b, old, 0.0)
                p = project(h, base + j).astype(F32)
                for core in PAIR:
                    start = 8 + core * n_pos + cuts[h]
                    pbuf[start:start + n] = jnp.where(on_b, p[core * n:(core + 1) * n], 0.0)
                for b in range(nbo):
                    blk = short_conv(pbuf, taps, b * BLK, BLK)
                    for half in range(per):
                        q_st[slot, half, b] = blk[:, half * TC:(half + 1) * TC]
                    if spectrum:
                        spec = block_values(fwd3_ref, blk)
                        for half in range(per):
                            vh_st[slot, half, b] = spec[:, half * TC:(half + 1) * TC]
                for copy in flush(j):
                    copy.start()

                @pl.when(jnp.logical_and(s == n_seq - 1, jnp.logical_and(lax.rem(j, Q) == 1, j < nt - Q * u)))
                def _():
                    forward(u, j // Q)
                return carry

            lax.fori_loop(0, nt, body, 0)
            for j in (nt - 2, nt - 1):
                for copy in flush(j):
                    copy.wait()

        def one_seq(s, carry):
            for h in range(n_cut - 1):
                rows(s, h)
                first(s, h)
            rows(s, n_cut - 1)
            last(s, 0, qx)
            last(s, 1, qv)
            return carry

        lax.fori_loop(0, n_seq, one_seq, 0)

    pl.run_scoped(
        prev,
        pltpu.VMEM((2 * nt, width, TN), BF16), pltpu.SemaphoreType.DMA((2 * nt, 4)),
        pltpu.VMEM((2 * hp, width), BF16), pltpu.VMEM((2, hp // GR, GR, width), F32), pltpu.SemaphoreType.DMA((2,)),
        pltpu.VMEM((2, per, nbo, BLK, TC), BF16), pltpu.SemaphoreType.DMA((2, per)),
        pltpu.VMEM((2, per, nbo, 2 * BLK, TC), F32), pltpu.SemaphoreType.DMA((2, per)),
        pltpu.VMEM((n_own + 8, TN), F32), pltpu.VMEM((2, cuts[-2], 2 * half_w), BF16))

    @pl.when(on_a)
    def _():
        for u in range(n_tile):
            for f, own in enumerate((f1, f2)):
                fill(f, u, c, own, c * half_w + u * TC).start()
                fill(f, u, 1 - c, pf.at[f], u * TC).start()

    def conv(x1b, vb, x2b, vhb, farb, in_sem, vh_sem, kst, k_sem, sendbuf, *scratch):
        def fetch(t):
            slot, two = lax.rem(t, 3), parity(t)
            srcs = (qx.at[t, :, :2 * nbo], qv.at[t], qx.at[t, :, 2 * nbo:], far.at[t])
            copies = [pltpu.make_async_copy(r, b.at[slot], in_sem.at[slot, i])
                      for i, (r, b) in enumerate(zip(srcs, (x1b, vb, x2b, farb)))]
            return copies + [pltpu.make_async_copy(vhat.at[t, s], vhb.at[two, s], vh_sem.at[two, s]) for s in range(n_seq)]

        def flush(t):
            slot = parity(t)
            return pltpu.make_async_copy(kst.at[slot], keep.at[t], k_sem.at[slot])

        def swap_y(u):
            return remote(sendbuf.at[parity(u)], part.at[u], p_send.at[u], p_recv.at[u], (dp, other))

        tile = ConvTile(fwd6_ref, inv6_ref, *scratch)

        def inputs(t, back):
            slot, cols = lax.rem(t + 3 - back, 3), at(c * half_w + lax.rem(t + n_tile - back, n_tile) * TC, TC)
            return x1b.at[slot], vb.at[slot], x2b.at[slot], farb.at[slot], sk1_ref[:, cols], sk2_ref[:, cols]

        def emit(t):
            slot = parity(t)

            @pl.when(t >= 2)
            def _():
                flush(t - 2).wait()
                swap_y(t - 2).wait_send()

            tile.result(c, kst.at[slot], sendbuf.at[slot])
            flush(t).start()
            swap_y(t).start()

        for copy in fetch(0):
            copy.start()
        forward(1, Q - 1)

        def step(t, carry):
            @pl.when(t + 1 < n_tile)
            def _():
                for copy in fetch(t + 1):
                    copy.start()

            @pl.when(on_a)
            def _():
                for f in PAIR:
                    for side in PAIR:
                        fill(f, t, side, f1, 0).wait()

            @pl.when(on_b)
            def _():
                for q in range(Q):
                    for side in PAIR:
                        across(t, side, 1 - dp, q).wait_recv()

            @pl.when(jnp.logical_and(on_b, t == n_tile - 1))
            def _():
                for side in PAIR:
                    landed(t, side, Q - 1).wait_recv()

            for copy in fetch(t):
                copy.wait()

            def relay(q):
                @pl.when(t + 2 + q // (Q - 1) < n_tile)
                def _():
                    forward(t + 2, q)

            tile.step(land, t, vhb.at[parity(t)], inputs(t, 0), inputs(t, 1), relay)

            @pl.when(t >= 1)
            def _():
                emit(t - 1)
            return carry

        lax.fori_loop(0, n_tile, step, 0)
        tile.drain(inputs(n_tile, 1))
        emit(n_tile - 1)
        for u in (n_tile - 2, n_tile - 1):
            flush(u).wait()
            swap_y(u).wait_send()
        for u in range(n_tile):
            swap_y(u).wait_recv()

    nb = 2 * nbo
    pl.run_scoped(
        conv,
        pltpu.VMEM((3, n_seq, nb, BLK, TC), BF16), pltpu.VMEM((3, n_seq, nb, BLK, TC), BF16), pltpu.VMEM((3, n_seq, nbo, BLK, TC), BF16),
        pltpu.VMEM((2, n_seq, nb, 2 * BLK, TC), F32), pltpu.VMEM((3, 2, nbo, 2 * BLK, TC), F32),
        pltpu.SemaphoreType.DMA((3, 4)), pltpu.SemaphoreType.DMA((2, n_seq)),
        pltpu.VMEM((2, n_seq, n_pos, TC), BF16), pltpu.SemaphoreType.DMA((2,)), pltpu.VMEM((2, n_seq, n_pos, TC), F32),
        pltpu.VMEM((2, nbo, 3, BLK, TC), BF16),
        pltpu.VMEM((nbo + 1, 2 * BLK, TC), F32), pltpu.VMEM((nbo + 1, 2 * BLK, TC), F32), pltpu.VMEM((nbo, 2 * BLK, TC), F32),
        *[pltpu.VMEM((nb, 3, 2 * BLK, TC), BF16)] * n_seq,
        pltpu.VMEM((nb, 3, BLK, TC), BF16),
        *[pltpu.VMEM((nb, BLK, TC), F32)] * n_seq,
        pltpu.VMEM((nb, 2 * BLK, TC), F32),
        *[pltpu.VMEM((nbo, 3, 2 * BLK, TC), BF16)] * n_seq,
        pltpu.VMEM((n_seq, nbo, BLK, TC), BF16))

    for s in range(n_seq):
        swap_u(s).wait_send()
    for f in PAIR:
        swap_f(f).wait_send()

    @pl.when(sp == 1)
    def _():
        tail_copy().wait_send()

    @pl.when(sp == 3)
    def _():
        tail_across().wait_send()

    @pl.when(on_a)
    def _():
        for i in range(n_seq * n_cut):
            for k in PAIR:
                over(*divmod(i, n_cut), k).wait_send()
        for u in range(n_tile):
            for q in range(Q):
                for k in PAIR:
                    filt(f1, u, k, q).wait_send()
        for k in PAIR:
            direct(f1, k).wait_send()

    @pl.when(on_b)
    def _():
        for i in range(n_seq * n_cut):
            for src in PAIR:
                onward(*divmod(i, n_cut), src).wait_send()
        for u in range(n_tile):
            for q in range(Q - u // (n_tile - 1)):
                for side in PAIR:
                    across(u, side, dp, q).wait_send()


def loop(trips):
    def run(body):
        def step(i, carry):
            body(i)
            return carry
        lax.fori_loop(0, trips, step, 0)
    return run


class ConvTile:
    def __init__(self, fwd6, inv6, hparts, g1, g2, raw2, sp0, sp1, zparts, zv0, zv1, zhat, sq0, sq1, ybuf):
        self.fwd6, self.inv6, self.hparts, self.g, self.raw2 = fwd6, inv6, hparts, (g1, g2), raw2
        self.first, self.second, self.zparts, self.zval, self.zhat, self.ybuf = (sp0, sp1), (sq0, sq1), zparts, (zv0, zv1), zhat, ybuf
        self.nb, self.nbo = sp0.shape[0], sq0.shape[0]

    def near(self, land, t, f):
        for side in PAIR:
            split_blocks(land.at[f, t, side], self.hparts.at[f], side * self.nbo // 2)

    def window(self, f, raw, far):
        g, nbo = self.g[f], self.nbo
        for j in range(nbo, 0, -1):
            cur = far.at[f, 0] if j == nbo else raw.at[j]
            for lo, sign in SIDES:
                re, im, new_re, new_im = shifted_add(cur, raw.at[j - 1], lo, sign)
                g[j, re], g[j, im] = new_re, new_im
        if raw is not g:
            g[0] = raw[0]

    def pointwise(self, xhat, f, far, dst, r, first):
        g, nbo = self.g[f], self.nbo
        re, im = pl.ds(pl.multiple_of(r * 16, 16), 16), pl.ds(pl.multiple_of(BLK + r * 16, 16), 16)
        for k in range(first, self.nb):
            acc_re = acc_im = None
            for j in range(k + 1):
                i = k - j
                gr, gi = (g[i, re], g[i, im]) if i <= nbo else (far[f, i - nbo, re], far[f, i - nbo, im])
                xr, xi = xhat[j, re], xhat[j, im]
                t_re, t_im = xr * gr - xi * gi, xr * gi + xi * gr
                acc_re = t_re if acc_re is None else acc_re + t_re
                acc_im = t_im if acc_im is None else acc_im + t_im
            for part, (a, b) in enumerate(zip(split3(acc_re), split3(acc_im))):
                dst[k - first, part, re], dst[k - first, part, im] = a, b

    def inverse(self, parts, k):
        return dot(self.inv6[...], stack6(parts[k, 0], parts[k, 1], parts[k, 2]))

    def gate_one(self, s, k, data):
        x1, v, _, _, skip, _ = data
        z = x1[s, k].astype(F32) * (self.inverse(self.first[s], k) + skip * v[s, k].astype(F32))
        self.zval[s][k] = z
        for part, a in enumerate(split3(z)):
            self.zparts[k, part] = a

    def spectrum(self, k):
        self.zhat[k] = block_spectrum(self.fwd6, self.zparts, k)

    def gate_two(self, s, k, data):
        y = data[2][s, k].astype(F32) * (self.inverse(self.second[s], k) + data[5] * self.zval[s][self.nbo + k])
        self.ybuf[s, k] = y.astype(BF16)

    def middle(self, s, data, i, point=None):
        for q in range(4):
            if point is not None:
                point(4 * i + q)
            for k in PAIR:
                if q < 2:
                    self.gate_one(s, 4 * i + 2 * q + k, data)
                else:
                    self.spectrum(4 * i + 2 * (q - 2) + k)

    def step(self, land, t, vhat, data, old, relay):
        nb, nbo = self.nb, self.nbo
        far = data[3]
        self.near(land, t, 0)
        for j in range(nbo):
            self.g[0][j] = block_spectrum(self.fwd6, self.hparts.at[0], j)
        self.near(land, t, 1)
        self.window(0, self.g[0], far)

        @loop(nb // 4)
        def _(i):
            self.middle(1, old, i, lambda r: self.pointwise(vhat.at[0], 0, far, self.first[0], r, 0))


        @loop(nbo // 2)
        def _(i):
            for q in range(4):
                self.pointwise(self.zhat, 1, old[3], self.second[1], 4 * i + q, nbo)
                if q < 2:
                    self.gate_two(0, 2 * i + q, old)
                else:
                    j = 2 * i + q - 2
                    self.raw2[j] = block_spectrum(self.fwd6, self.hparts.at[1], j)

        relay(0)
        self.window(1, self.raw2, far)

        @loop(nb // 4)
        def _(i):
            self.middle(0, data, i, lambda r: self.pointwise(vhat.at[1], 0, far, self.first[1], r, 0))

        @loop(nbo // 2)
        def _(i):
            for q in range(4):
                self.pointwise(self.zhat, 1, far, self.second[0], 4 * i + q, nbo)
                if q % 2 == 0:
                    self.gate_two(1, 2 * i + q // 2, old)

        relay(1)

    def drain(self, data):
        nb, nbo = self.nb, self.nbo

        @loop(nb // 4)
        def _(i):
            self.middle(1, data, i)

        @loop(nbo // 2)
        def _(i):
            for q in range(4):
                self.pointwise(self.zhat, 1, data[3], self.second[1], 4 * i + q, nbo)
                if q % 2 == 0:
                    self.gate_two(0, 2 * i + q // 2, data)

        for k in range(nbo):
            self.gate_two(1, k, data)

    def result(self, c, keep, send):
        hk = self.nbo // 2
        for s in range(self.ybuf.shape[0]):
            for b in range(hk):
                keep[s, b * BLK:(b + 1) * BLK] = self.ybuf[s, c * hk + b]
                send[s, b * BLK:(b + 1) * BLK] = self.ybuf[s, (1 - c) * hk + b].astype(F32)


def out_body(keep, part, w_out, u_in, out, wbuf, w_sem, lhs, keep_v, stage, in_sem, u_v, o_st, o_sem):
    c = lax.rem(lax.axis_index("sp"), 2)
    n_tile, n_seq, n_pos, _ = keep.shape
    half_w = n_tile * TC
    width = 2 * half_w
    n_col, rows = width // TN, width // 4

    def weights(j, slot):
        cols = pl.ds(pl.multiple_of(j * TN, TN), TN)
        return [pltpu.make_async_copy(w_out.at[i * rows:(i + 1) * rows, cols],
                                      wbuf.at[slot, i * rows:(i + 1) * rows], w_sem.at[slot, i]) for i in range(4)] + [
                    pltpu.make_async_copy(u_in.at[:, :, cols], u_v.at[slot], w_sem.at[slot, 4])]

    def flush(j):
        slot = parity(j)
        return pltpu.make_async_copy(o_st.at[slot], out.at[:, :, pl.ds(pl.multiple_of(j * TN, TN), TN)], o_sem.at[slot])

    loads = [pltpu.make_async_copy(part.at[u], stage.at[u], in_sem.at[u]) for u in range(n_tile)]
    loads += [pltpu.make_async_copy(keep.at[u], keep_v.at[u], in_sem.at[n_tile + u]) for u in range(n_tile)]
    for copy in loads:
        copy.start()
    for copy in weights(0, 0):
        copy.start()
    for u in range(n_tile):
        loads[u].wait()
        loads[n_tile + u].wait()
        for s in range(n_seq):
            lhs[s, :, pl.ds(pl.multiple_of((1 - c) * half_w + u * TC, TC), TC)] = stage[u, s].astype(BF16)
            lhs[s, :, pl.ds(pl.multiple_of(c * half_w + u * TC, TC), TC)] = keep_v[u, s]

    def step(j, carry):
        slot = parity(j)

        @pl.when(j + 1 < n_col)
        def _():
            for copy in weights(j + 1, 1 - slot):
                copy.start()

        for copy in weights(j, slot):
            copy.wait()

        @pl.when(j >= 2)
        def _():
            flush(j - 2).wait()

        for s in range(n_seq):
            o_st[slot, s] = (u_v[slot, s].astype(F32) + dot(lhs[s], wbuf[slot])).astype(BF16)
        flush(j).start()
        return carry

    lax.fori_loop(0, n_col, step, 0)
    for j in (n_col - 2, n_col - 1):
        flush(j).wait()


def solution(mesh):
    fwd3, fwd6, inv6 = transform_tables()

    def local_step(u_in, w_in, b_in, conv_taps, w_out, skip_one, skip_two, filt_one, filt_two):
        n_seq, n_pos, width = u_in.shape
        half_w = width // 2
        n_own = 2 * n_pos
        nb = 2 * n_own // BLK
        nbo = nb // 2
        n_tile = half_w // TC
        rows = n_pos // GR, GR, width
        small, large = pl.BlockSpec(memory_space=pltpu.VMEM), pl.BlockSpec(memory_space=pl.ANY)
        dma = pltpu.SemaphoreType.DMA

        def shape(dims, dtype=F32):
            return jax.ShapeDtypeStruct(dims, dtype)

        keep, part, *_ = pl.pallas_call(
            main_body,
            in_specs=[small] * 7 + [large] * 4,
            out_specs=[large] * 12,
            out_shape=[
                shape((n_tile, n_seq, n_pos, TC), BF16), shape((n_tile, n_seq, n_pos, TC)),
                shape((n_tile, n_seq, nb + nbo, BLK, TC), BF16), shape((n_tile, n_seq, nb, BLK, TC), BF16),
                shape((n_tile, n_seq, nb, 2 * BLK, TC)), shape((n_tile, 2, nbo, 2 * BLK, TC)),
                shape((n_seq, *rows)), shape((n_seq, 8, width)), shape((n_seq, *rows)), shape((2, n_seq, *rows)),
                shape((n_seq, 8, width)), shape((2, n_pos, half_w)),
            ],
            scratch_shapes=[
                pltpu.VMEM((2, n_tile, 2, n_pos, TC), F32),
                dma((1,)), dma((1,)), *[dma((n_seq, 3, 2))] * 4, *[dma((n_seq,))] * 2, *[dma((2,))] * 2,
                dma((2, n_tile, 2)), *[dma((n_tile, Q, 2))] * 4, *[dma((n_tile,))] * 2,
            ],
            compiler_params=pltpu.CompilerParams(vmem_limit_bytes=62 << 20, collective_id=0, has_side_effects=True),
            name="hyena_main",
        )(fwd3, fwd6, inv6, b_in.reshape(1, -1), conv_taps, skip_one.reshape(1, -1), skip_two.reshape(1, -1),
          u_in, w_in, filt_one, filt_two)

        return pl.pallas_call(
            out_body,
            in_specs=[large] * 4,
            out_specs=large,
            out_shape=shape((n_seq, n_pos, width), BF16),
            scratch_shapes=[
                pltpu.VMEM((2, width, TN), BF16), dma((2, 5)),
                pltpu.VMEM((n_seq, n_pos, width), BF16), pltpu.VMEM((n_tile, n_seq, n_pos, TC), BF16), pltpu.VMEM((n_tile, n_seq, n_pos, TC), F32),
                dma((2 * n_tile,)), pltpu.VMEM((2, n_seq, n_pos, TN), BF16), pltpu.VMEM((2, n_seq, n_pos, TN), BF16), dma((2,)),
            ],
            compiler_params=pltpu.CompilerParams(vmem_limit_bytes=60 << 20),
            name="out_proj",
        )(keep, part, w_out, u_in)

    seq_spec = P("dp", "sp", None)
    filt_spec = P("sp", None)
    return jax.shard_map(local_step, mesh=mesh, in_specs=(seq_spec, P(), P(), P(), P(), P(), P(), filt_spec, filt_spec), out_specs=seq_spec, check_vma=False)
```

```python
import functools

import jax
import jax.numpy as jnp
import numpy as np
from jax import lax
from jax.experimental import pallas as pl
from jax.experimental.pallas import tpu as pltpu
from jax.sharding import PartitionSpec as P

F32, BF16 = jnp.float32, jnp.bfloat16
BLK = 128
TN = 512
TC = 256
Q = 2
PAIR = (0, 1)
GR = 32
MESH = pl.DeviceIdType.MESH


def split_table(table):
    parts, rest = [], table.astype(np.float64)
    for _ in range(3):
        part = rest.astype(np.float32).astype(jnp.bfloat16)
        parts.append(part)
        rest = rest - part.astype(np.float64)
    return parts


def transform_tables():
    freq = np.concatenate([np.arange(0, BLK, 2), np.arange(1, BLK, 2)]) + 0.5
    angle = 2.0 * np.pi * freq[:, None] * np.arange(BLK)[None, :] / (2 * BLK)
    fwd = np.concatenate([np.cos(angle), -np.sin(angle)], 0)
    inv = np.concatenate([np.cos(angle).T, -np.sin(angle).T], 1) / BLK
    f1, f2, f3 = split_table(fwd)
    e1, e2, e3 = split_table(inv)
    fwd3 = np.concatenate([f1, f2, f3], 1)
    fwd6 = np.concatenate([f1, f1, f2, f2, f1, f3], 1)
    inv6 = np.concatenate([e1, e1, e2, e2, e1, e3], 1)
    return fwd3, fwd6, inv6


def parity(x):
    return lax.rem(x, 2)


def dot(a, b):
    return jnp.dot(a, b, preferred_element_type=F32)


def split3(x):
    hi = x.astype(BF16)
    rest = x - hi.astype(F32)
    mid = rest.astype(BF16)
    low = (rest - mid.astype(F32)).astype(BF16)
    return hi, mid, low


def stack6(hi, mid, low):
    return jnp.concatenate([hi, mid, hi, mid, low, hi], axis=0)


def split_blocks(src, parts, first):
    for j in range(src.shape[0] // BLK):
        for i, a in enumerate(split3(src[j * BLK:(j + 1) * BLK])):
            parts[first + j, i] = a


def block_spectrum(fwd6_ref, parts, j):
    return dot(fwd6_ref[...], stack6(parts[j, 0], parts[j, 1], parts[j, 2]))


def shifted_add(cur, old, lo, sign):
    re, im = slice(lo, lo + BLK // 2), slice(BLK + lo, BLK + lo + BLK // 2)
    return re, im, cur[re] - sign * old[im], cur[im] + sign * old[re]


SIDES = ((0, 1.0), (BLK // 2, -1.0))


def short_conv(pbuf, t, first, rows):
    return (t[0:1] * pbuf[8 + first:8 + first + rows] + t[1:2] * pbuf[7 + first:7 + first + rows] + t[2:3] * pbuf[6 + first:6 + first + rows]).astype(BF16)


def block_values(fwd3_ref, blk):
    return dot(fwd3_ref[...], jnp.concatenate([blk, blk, blk], axis=0))


def main_body(fwd3_ref, fwd6_ref, inv6_ref, bias_ref, taps_ref, sk1_ref, sk2_ref, u_bf, w_in, f1, f2,
              keep, part, qx, qv, vhat, far, u32, tsrc, u_sw, u_x, tail, pf,
              land, ts, tr, os, orr, ws, wr, ss, sr, fs, fr, l_sem, x_send, x_recv, y_send, y_recv, p_send, p_recv):
    sp, dp = lax.axis_index("sp"), lax.axis_index("dp")
    c = parity(sp)
    on_b = sp >= 2
    on_a = jnp.logical_not(on_b)
    other = sp + 1 - 2 * c
    n_seq, n_pos, width = u_bf.shape
    half_w = width // 2
    nt, n_tile, per = half_w // TN, half_w // TC, TN // TC
    n_own, hp = 2 * n_pos, n_pos // 2
    nbo = n_own // BLK
    cuts = (0, hp, hp + hp // 2, n_pos)
    n_cut = len(cuts) - 1

    def remote(src, dst, send, recv, peer):
        return pltpu.make_async_remote_copy(src, dst, send, recv, device_id=peer, device_id_type=MESH)

    def at(start, size):
        return pl.ds(pl.multiple_of(start, size), size)

    def share(s, h, k):
        rows = (cuts[h + 1] - cuts[h]) // 2
        return s, pl.ds((cuts[h] + k * rows) // GR, rows // GR)

    def tail_copy():
        return remote(tsrc, tail, ts.at[0], tr.at[0], (dp, 3))

    def tail_across():
        return remote(tail, tail, ts.at[0], tr.at[0], (dp, other))

    def over(s, h, k):
        s, rows = share(s, h, k)
        return remote(u32.at[s, rows], u_x.at[c, s, rows], os.at[s, h, k], orr.at[s, h, c], (dp, 2 + k))

    def arrived(s, h, src):
        at_s, rows = share(s, h, 0)
        ref = u_x.at[src, at_s, rows]
        return remote(ref, ref, os.at[s, h, src], orr.at[s, h, src], (dp, sp))

    def onward(s, h, src):
        at_s, rows = share(s, h, c)
        ref = u_x.at[src, at_s, rows]
        return remote(ref, ref, ws.at[s, h, src], wr.at[s, h, src], (dp, other))

    def swap_u(s):
        return remote(u32.at[s], u_sw.at[s], ss.at[s], sr.at[s], (dp, other))

    def swap_f(f):
        return remote((f1, f2)[f].at[:, at((1 - c) * half_w, half_w)], pf.at[f], fs.at[f], fr.at[f], (dp, other))

    qr = n_pos // Q

    def filt(src, u, k, q):
        return remote(src.at[q * qr:(q + 1) * qr, at(k * half_w + u * TC, TC)], land.at[dp, u, c, q * qr:(q + 1) * qr],
                      x_send.at[u, q, k], x_recv.at[u, q, c], (dp, 2 + k))

    def direct(src, k):
        u, q = n_tile - 1, Q - 1
        return remote(src.at[q * qr:(q + 1) * qr, at(k * half_w + u * TC, TC)], land.at[1 - dp, u, c, q * qr:(q + 1) * qr],
                      y_send.at[u, q, k], y_recv.at[u, q, c], (dp, 2 + k))

    def landed(u, side, q):
        ref = land.at[dp, u, side, at(q * qr, qr)]
        return remote(ref, ref, x_send.at[u, q, side], x_recv.at[u, q, side], (dp, sp))

    def across(u, side, f, q):
        ref = land.at[f, u, side, at(q * qr, qr)]
        return remote(ref, ref, y_send.at[u, q, side], y_recv.at[u, q, side], (1 - dp, sp))

    def fill(f, u, side, src, start):
        return pltpu.make_async_copy(src.at[:, at(start, TC)], land.at[f, u, side], l_sem.at[f, u, side])

    def column(g, j):
        return (g + j // nt) * width + c * half_w + lax.rem(j, nt) * TN

    def load_rows(stage, st_sem, items):
        def copy(i):
            src, rows, _, _ = items[i]
            return pltpu.make_async_copy(src, stage.at[i % 2, :rows // GR], st_sem.at[i % 2])

        copy(0).start()
        for i, (_, rows, dst, row) in enumerate(items):
            if i + 1 < len(items):
                copy(i + 1).start()
            copy(i).wait()
            dst[pl.ds(pl.multiple_of(row, 16), rows), :] = stage[i % 2, :rows // GR].reshape(rows, width).astype(BF16)

    barrier = pltpu.get_barrier_semaphore()
    for peer in ((dp, other), (dp, lax.rem(sp + 2, 4)), (dp, lax.rem(other + 2, 4)), (1 - dp, sp)):
        pl.semaphore_signal(barrier, inc=1, device_id=peer, device_id_type=MESH)
    pl.semaphore_wait(barrier, 4)

    def widen(raw, wide, tail_raw, tail_wide, in_sem, out_sem):
        def half(ref, s, h):
            return ref.at[s, h * hp:h * hp + hp]

        def load(s, h):
            return pltpu.make_async_copy(half(u_bf, s, h), raw.at[h], in_sem.at[h])

        last_rows = pltpu.make_async_copy(u_bf.at[:, n_pos - 8:], tail_raw, in_sem.at[2])
        last_out = pltpu.make_async_copy(tail_wide, tsrc, out_sem.at[2])
        order = [(s, h) for s in range(n_seq) for h in PAIR]
        last_rows.start()
        load(*order[0]).start()
        last_rows.wait()
        tail_wide[...] = tail_raw[...].astype(F32)
        last_out.start()
        pending = {}
        for (s, h), following in zip(order, order[1:] + [None]):
            if following:
                load(*following).start()
            load(s, h).wait()
            if h in pending:
                pending.pop(h).wait()
            wide[h] = raw[h].astype(F32).reshape(wide.shape[1:])
            store = pltpu.make_async_copy(wide.at[h], u32.at[s, pl.ds(h * hp // GR, hp // GR)], out_sem.at[h])
            store.start()
            if s + h:
                pending[h] = store
                continue
            last_out.wait()

            @pl.when(sp == 1)
            def _():
                tail_copy().start()

            store.wait()

            @pl.when(on_a)
            def _():
                for k in PAIR:
                    over(s, h, k).start()

        for store in pending.values():
            store.wait()

    pl.run_scoped(
        widen, pltpu.VMEM((2, hp, width), BF16), pltpu.VMEM((2, hp // GR, GR, width), F32), pltpu.VMEM((n_seq, 8, width), BF16),
        pltpu.VMEM((n_seq, 8, width), F32), pltpu.SemaphoreType.DMA((3,)), pltpu.SemaphoreType.DMA((3,)))

    @pl.when(on_a)
    def _():
        for i in range(1, n_seq * n_cut):
            for k in PAIR:
                over(*divmod(i, n_cut), k).start()
        for which, src, rest in ((0, f1, f2), (1, f2, f1)):
            @pl.when(dp == which)
            def _():
                for u in range(n_tile):
                    for q in range(Q):
                        for k in PAIR:
                            filt(src, u, k, q).start()
                for k in PAIR:
                    direct(rest, k).start()

    for i in range(n_seq):
        swap_u(i).start()
    for f in PAIR:
        swap_f(f).start()

    def forward(u, q):
        @pl.when(on_b)
        def _():
            for side in PAIR:
                landed(u, side, q).wait_recv()
                across(u, side, dp, q).start()

    def front(wbuf, wsem, lhs, stage, st_sem, lhs_sem, tailbuf, q_st, q_sem, vh_st, vh_sem, pbuf):
        def weights(g, j, slot):
            rows = width // 4
            return [pltpu.make_async_copy(w_in.at[i * rows:(i + 1) * rows, at(column(g, j), TN)],
                                          wbuf.at[slot, i * rows:(i + 1) * rows], wsem.at[slot, i]) for i in range(4)]

        def stream(g, body, following, n=nt):
            def step(j, carry):
                slot = parity(j)

                @pl.when(j + 1 < n)
                def _():
                    for copy in weights(g, j + 1, 1 - slot):
                        copy.start()

                if following is not None:
                    @pl.when(j + 1 == n)
                    def _():
                        following(1 - slot)

                for copy in weights(g, j, slot):
                    copy.wait()
                body(j, slot, bias_ref[:, at(column(g, j), TN)], taps_ref[:, at(column(g, j), TN)])
                return carry

            lax.fori_loop(0, n, step, 0)

        def begin(g):
            def start(slot):
                for copy in weights(g, 0, slot):
                    copy.start()
            return start

        def project(rows_ref, slot, bias):
            return (dot(rows_ref, wbuf[slot]) + bias).astype(BF16).astype(F32)

        tail_rows = n_seq * 8
        begin(0)(0)
        own_rows = [pltpu.make_async_copy(u_bf.at[s], lhs.at[pl.ds(pl.multiple_of(tail_rows + s * n_own + c * n_pos, 16), n_pos)], lhs_sem.at[s])
                    for s in range(n_seq)]
        for copy in own_rows:
            copy.start()
        for s in range(n_seq):
            swap_u(s).wait_recv()
        load_rows(stage, st_sem, [(u_sw.at[s, pl.ds(h * hp // GR, hp // GR)], hp, lhs, tail_rows + s * n_own + (1 - c) * n_pos + h * hp)
                                  for s in range(n_seq) for h in PAIR])
        for copy in own_rows:
            copy.wait()

        @pl.when(on_b)
        def _():
            tail_copy().wait_recv()

            @pl.when(sp == 3)
            def _():
                tail_across().start()

            copy = pltpu.make_async_copy(tail, tailbuf, lhs_sem.at[0])
            copy.start()
            copy.wait()

        @pl.when(on_a)
        def _():
            tailbuf[...] = jnp.zeros_like(tailbuf)

        lhs[:tail_rows, :] = tailbuf[...].reshape(tail_rows, width).astype(BF16)
        chunk = n_pos

        def own_phase(g, n, dst, spectrum, following):
            def flush(j, slot):
                blocks = pl.ds(nbo * (1 + j // nt), nbo)
                copies = []
                for h in range(per):
                    u = lax.rem(j, nt) * per + h
                    copies.append(pltpu.make_async_copy(q_st.at[slot, h], dst.at[u, :, blocks], q_sem.at[slot, h]))
                    if spectrum:
                        copies.append(pltpu.make_async_copy(vh_st.at[slot, h], vhat.at[u, :, nbo:], vh_sem.at[slot, h]))
                return copies

            def body(j, slot, bias, taps):
                @pl.when(j >= 2)
                def _():
                    for copy in flush(j - 2, slot):
                        copy.wait()

                for i in range(n_seq * n_own // chunk):
                    s, r = divmod(i * chunk, n_own)
                    p = project(lhs[(tail_rows + i * chunk if i else 0):tail_rows + (i + 1) * chunk, :], slot, bias)
                    if i == 0:
                        for k in range(n_seq):
                            pbuf[k, 0:8] = jnp.where(on_b, p[8 * k:8 * k + 8], 0.0)
                        p = p[tail_rows:]
                    pbuf[s, 8 + r:8 + r + chunk] = p
                    q = short_conv(pbuf.at[s], taps, r, chunk)
                    for b in range(chunk // BLK):
                        blk = q[b * BLK:(b + 1) * BLK]
                        for h in range(per):
                            q_st[slot, h, s, r // BLK + b] = blk[:, h * TC:(h + 1) * TC]
                        if spectrum:
                            spec = block_values(fwd3_ref, blk)
                            for h in range(per):
                                vh_st[slot, h, s, r // BLK + b] = spec[:, h * TC:(h + 1) * TC]
                for copy in flush(j, slot):
                    copy.start()

            stream(g, body, following, n)
            for j in (n - 2, n - 1):
                for copy in flush(j, j % 2):
                    copy.wait()

        own_phase(0, 2 * nt, qx, False, begin(2))
        own_phase(2, nt, qv, True, None)

        def far_phase(fin, fin_sem, fout, fout_sem, parts):
            hk = n_pos // BLK

            def fetch(j, slot):
                mine = at(c * half_w + j * TC, TC)
                srcs = (f1.at[:, mine], f2.at[:, mine], pf.at[0, :, at(j * TC, TC)], pf.at[1, :, at(j * TC, TC)])
                return [pltpu.make_async_copy(src, fin.at[slot, i], fin_sem.at[slot, i]) for i, src in enumerate(srcs)]

            def flush(j, slot):
                return pltpu.make_async_copy(fout.at[slot], far.at[j], fout_sem.at[slot])

            for copy in fetch(0, 0):
                copy.start()

            def step(j, carry):
                slot = parity(j)

                @pl.when(j + 1 < n_tile)
                def _():
                    for copy in fetch(j + 1, 1 - slot):
                        copy.start()

                for copy in fetch(j, slot):
                    copy.wait()

                @pl.when(j >= 2)
                def _():
                    flush(j - 2, slot).wait()

                for f in PAIR:
                    split_blocks(fin.at[slot, f], parts.at[f], c * hk)
                    split_blocks(fin.at[slot, 2 + f], parts.at[f], (1 - c) * hk)
                g_ref = fout.at[slot]
                for f in PAIR:
                    for b in range(2 * hk):
                        g_ref[f, b] = block_spectrum(fwd6_ref, parts.at[f], b)
                    for b in range(2 * hk - 1, 0, -1):
                        for lo, sign in SIDES:
                            re, im, new_re, new_im = shifted_add(g_ref.at[f, b], g_ref.at[f, b - 1], lo, sign)
                            g_ref[f, b, re], g_ref[f, b, im] = new_re, new_im
                flush(j, slot).start()
                return carry

            lax.fori_loop(0, n_tile, step, 0)
            for j in (n_tile - 2, n_tile - 1):
                flush(j, j % 2).wait()

        for f in PAIR:
            swap_f(f).wait_recv()
        pl.run_scoped(
            far_phase, pltpu.VMEM((2, 4, n_pos, TC), F32), pltpu.SemaphoreType.DMA((2, 4)),
            pltpu.VMEM((2, 2, nbo, 2 * BLK, TC), F32), pltpu.SemaphoreType.DMA((2,)), pltpu.VMEM((2, nbo, 3, BLK, TC), BF16))

    pl.run_scoped(
        front,
        pltpu.VMEM((2, width, TN), BF16), pltpu.SemaphoreType.DMA((2, 4)),
        pltpu.VMEM((n_seq * n_own + 8 * n_seq, width), BF16),
        pltpu.VMEM((2, hp // GR, GR, width), F32), pltpu.SemaphoreType.DMA((2,)), pltpu.SemaphoreType.DMA((n_seq,)), pltpu.VMEM((n_seq, 8, width), F32),
        pltpu.VMEM((2, per, n_seq, nbo, BLK, TC), BF16), pltpu.SemaphoreType.DMA((2, per)),
        pltpu.VMEM((2, per, n_seq, nbo, 2 * BLK, TC), F32), pltpu.SemaphoreType.DMA((2, per)),
        pltpu.VMEM((n_seq, n_own + 8, TN), F32))

    def prev(wres, w_sem, lhs_p, stage, st_sem, q_st, q_sem, vh_st, vh_sem, pbuf, pstash):
        def weights(j):
            rows = width // 4
            return [pltpu.make_async_copy(w_in.at[i * rows:(i + 1) * rows, at(which(j), TN)],
                                          wres.at[j, i * rows:(i + 1) * rows], w_sem.at[j, i]) for i in range(4)]

        def which(j):
            return 2 * (j // nt) * width + c * half_w + lax.rem(j, nt) * TN

        def begin(j, carry):
            for copy in weights(j):
                copy.start()
            return carry

        lax.fori_loop(0, 2 * nt, begin, 0)

        def rows(s, h):
            n = cuts[h + 1] - cuts[h]

            @pl.when(on_b)
            def _():
                for src in PAIR:
                    arrived(s, h, src).wait_recv()
                    onward(s, h, src).start()
                for src in PAIR:
                    onward(s, h, src).wait_recv()
                load_rows(stage, st_sem, [(u_x.at[src, s, cuts[h] // GR:cuts[h + 1] // GR], n, lhs_p, src * n) for src in PAIR])

            @pl.when(on_a)
            def _():
                lhs_p[...] = jnp.zeros_like(lhs_p)

        def project(h, j):
            n = 2 * (cuts[h + 1] - cuts[h])
            return (dot(lhs_p[:n, :], wres[j]) + bias_ref[:, at(which(j), TN)]).astype(BF16)

        def first(s, h):
            n = cuts[h + 1] - cuts[h]

            def body(j, carry):
                if h == 0:
                    @pl.when(s == 0)
                    def _():
                        for copy in weights(j):
                            copy.wait()

                p = project(h, j)
                for core in PAIR:
                    pstash[core, cuts[h]:cuts[h + 1], at(j * TN, TN)] = p[core * n:(core + 1) * n]
                return carry

            lax.fori_loop(0, 2 * nt, body, 0)

        def last(s, u, dst):
            base, spectrum = u * nt, u > 0
            h = n_cut - 1
            n = cuts[h + 1] - cuts[h]

            def flush(j):
                slot, copies = parity(j), []
                for half in range(per):
                    copies.append(pltpu.make_async_copy(q_st.at[slot, half], dst.at[j * per + half, s, :nbo], q_sem.at[slot, half]))
                    if spectrum:
                        copies.append(pltpu.make_async_copy(vh_st.at[slot, half], vhat.at[j * per + half, s, :nbo], vh_sem.at[slot, half]))
                return copies

            def body(j, carry):
                slot = parity(j)

                @pl.when(j >= 2)
                def _():
                    for copy in flush(j - 2):
                        copy.wait()

                taps = taps_ref[:, at(which(base + j), TN)]
                pbuf[0:8] = jnp.zeros((8, TN), F32)
                for core in PAIR:
                    old = pstash[core, :cuts[h], at((base + j) * TN, TN)].astype(F32)
                    pbuf[8 + core * n_pos:8 + core * n_pos + cuts[h]] = jnp.where(on_b, old, 0.0)
                p = project(h, base + j).astype(F32)
                for core in PAIR:
                    start = 8 + core * n_pos + cuts[h]
                    pbuf[start:start + n] = jnp.where(on_b, p[core * n:(core + 1) * n], 0.0)
                for b in range(nbo):
                    blk = short_conv(pbuf, taps, b * BLK, BLK)
                    for half in range(per):
                        q_st[slot, half, b] = blk[:, half * TC:(half + 1) * TC]
                    if spectrum:
                        spec = block_values(fwd3_ref, blk)
                        for half in range(per):
                            vh_st[slot, half, b] = spec[:, half * TC:(half + 1) * TC]
                for copy in flush(j):
                    copy.start()

                @pl.when(jnp.logical_and(s == n_seq - 1, jnp.logical_and(lax.rem(j, Q) == 1, j < nt - Q * u)))
                def _():
                    forward(u, j // Q)
                return carry

            lax.fori_loop(0, nt, body, 0)
            for j in (nt - 2, nt - 1):
                for copy in flush(j):
                    copy.wait()

        def one_seq(s, carry):
            for h in range(n_cut - 1):
                rows(s, h)
                first(s, h)
            rows(s, n_cut - 1)
            last(s, 0, qx)
            last(s, 1, qv)
            return carry

        lax.fori_loop(0, n_seq, one_seq, 0)

    pl.run_scoped(
        prev,
        pltpu.VMEM((2 * nt, width, TN), BF16), pltpu.SemaphoreType.DMA((2 * nt, 4)),
        pltpu.VMEM((2 * hp, width), BF16), pltpu.VMEM((2, hp // GR, GR, width), F32), pltpu.SemaphoreType.DMA((2,)),
        pltpu.VMEM((2, per, nbo, BLK, TC), BF16), pltpu.SemaphoreType.DMA((2, per)),
        pltpu.VMEM((2, per, nbo, 2 * BLK, TC), F32), pltpu.SemaphoreType.DMA((2, per)),
        pltpu.VMEM((n_own + 8, TN), F32), pltpu.VMEM((2, cuts[-2], 2 * half_w), BF16))

    @pl.when(on_a)
    def _():
        for u in range(n_tile):
            for f, own in enumerate((f1, f2)):
                fill(f, u, c, own, c * half_w + u * TC).start()
                fill(f, u, 1 - c, pf.at[f], u * TC).start()

    def conv(x1b, vb, x2b, vhb, farb, in_sem, vh_sem, kst, k_sem, sendbuf, *scratch):
        def fetch(t):
            slot, two = lax.rem(t, 3), parity(t)
            srcs = (qx.at[t, :, :2 * nbo], qv.at[t], qx.at[t, :, 2 * nbo:], far.at[t])
            copies = [pltpu.make_async_copy(r, b.at[slot], in_sem.at[slot, i])
                      for i, (r, b) in enumerate(zip(srcs, (x1b, vb, x2b, farb)))]
            return copies + [pltpu.make_async_copy(vhat.at[t, s], vhb.at[two, s], vh_sem.at[two, s]) for s in range(n_seq)]

        def flush(t):
            slot = parity(t)
            return pltpu.make_async_copy(kst.at[slot], keep.at[t], k_sem.at[slot])

        def swap_y(u):
            return remote(sendbuf.at[parity(u)], part.at[u], p_send.at[u], p_recv.at[u], (dp, other))

        tile = ConvTile(fwd6_ref, inv6_ref, *scratch)

        def inputs(t, back):
            slot, cols = lax.rem(t + 3 - back, 3), at(c * half_w + lax.rem(t + n_tile - back, n_tile) * TC, TC)
            return x1b.at[slot], vb.at[slot], x2b.at[slot], farb.at[slot], sk1_ref[:, cols], sk2_ref[:, cols]

        def emit(t):
            slot = parity(t)

            @pl.when(t >= 2)
            def _():
                flush(t - 2).wait()
                swap_y(t - 2).wait_send()

            tile.result(c, kst.at[slot], sendbuf.at[slot])
            flush(t).start()
            swap_y(t).start()

        for copy in fetch(0):
            copy.start()
        forward(1, Q - 1)

        def step(t, carry):
            @pl.when(t + 1 < n_tile)
            def _():
                for copy in fetch(t + 1):
                    copy.start()

            @pl.when(on_a)
            def _():
                for f in PAIR:
                    for side in PAIR:
                        fill(f, t, side, f1, 0).wait()

            @pl.when(on_b)
            def _():
                for q in range(Q):
                    for side in PAIR:
                        across(t, side, 1 - dp, q).wait_recv()

            @pl.when(jnp.logical_and(on_b, t == n_tile - 1))
            def _():
                for side in PAIR:
                    landed(t, side, Q - 1).wait_recv()

            for copy in fetch(t):
                copy.wait()

            def relay(q):
                ahead = 2 - q

                @pl.when(jnp.logical_and(t >= q, t + ahead + q < n_tile))
                def _():
                    forward(t + ahead, q)

            tile.step(land, t, vhb.at[parity(t)], inputs(t, 0), inputs(t, 1), relay)

            @pl.when(t >= 1)
            def _():
                emit(t - 1)
            return carry

        lax.fori_loop(0, n_tile, step, 0)
        tile.drain(inputs(n_tile, 1))
        emit(n_tile - 1)
        for u in (n_tile - 2, n_tile - 1):
            flush(u).wait()
            swap_y(u).wait_send()
        for u in range(n_tile):
            swap_y(u).wait_recv()

    nb = 2 * nbo
    pl.run_scoped(
        conv,
        pltpu.VMEM((3, n_seq, nb, BLK, TC), BF16), pltpu.VMEM((3, n_seq, nb, BLK, TC), BF16), pltpu.VMEM((3, n_seq, nbo, BLK, TC), BF16),
        pltpu.VMEM((2, n_seq, nb, 2 * BLK, TC), F32), pltpu.VMEM((3, 2, nbo, 2 * BLK, TC), F32),
        pltpu.SemaphoreType.DMA((3, 4)), pltpu.SemaphoreType.DMA((2, n_seq)),
        pltpu.VMEM((2, n_seq, n_pos, TC), BF16), pltpu.SemaphoreType.DMA((2,)), pltpu.VMEM((2, n_seq, n_pos, TC), F32),
        pltpu.VMEM((2, nbo, 3, BLK, TC), BF16),
        pltpu.VMEM((nbo + 1, 2 * BLK, TC), F32), pltpu.VMEM((nbo + 1, 2 * BLK, TC), F32), pltpu.VMEM((nbo, 2 * BLK, TC), F32),
        *[pltpu.VMEM((nb, 3, 2 * BLK, TC), BF16)] * n_seq,
        pltpu.VMEM((nb, 3, BLK, TC), BF16),
        *[pltpu.VMEM((nb, BLK, TC), F32)] * n_seq,
        pltpu.VMEM((nb, 2 * BLK, TC), F32),
        *[pltpu.VMEM((nbo, 3, 2 * BLK, TC), BF16)] * n_seq,
        pltpu.VMEM((n_seq, nbo, BLK, TC), BF16))

    for s in range(n_seq):
        swap_u(s).wait_send()
    for f in PAIR:
        swap_f(f).wait_send()

    @pl.when(sp == 1)
    def _():
        tail_copy().wait_send()

    @pl.when(sp == 3)
    def _():
        tail_across().wait_send()

    @pl.when(on_a)
    def _():
        for i in range(n_seq * n_cut):
            for k in PAIR:
                over(*divmod(i, n_cut), k).wait_send()
        for u in range(n_tile):
            for q in range(Q):
                for k in PAIR:
                    filt(f1, u, k, q).wait_send()
        for k in PAIR:
            direct(f1, k).wait_send()

    @pl.when(on_b)
    def _():
        for i in range(n_seq * n_cut):
            for src in PAIR:
                onward(*divmod(i, n_cut), src).wait_send()
        for u in range(n_tile):
            for q in range(Q - u // (n_tile - 1)):
                for side in PAIR:
                    across(u, side, dp, q).wait_send()


def loop(trips):
    def run(body):
        def step(i, carry):
            body(i)
            return carry
        lax.fori_loop(0, trips, step, 0)
    return run


class ConvTile:
    def __init__(self, fwd6, inv6, hparts, g1, g2, raw2, sp0, sp1, zparts, zv0, zv1, zhat, sq0, sq1, ybuf):
        self.fwd6, self.inv6, self.hparts, self.g, self.raw2 = fwd6, inv6, hparts, (g1, g2), raw2
        self.first, self.second, self.zparts, self.zval, self.zhat, self.ybuf = (sp0, sp1), (sq0, sq1), zparts, (zv0, zv1), zhat, ybuf
        self.nb, self.nbo = sp0.shape[0], sq0.shape[0]

    def near(self, land, t, f):
        for side in PAIR:
            split_blocks(land.at[f, t, side], self.hparts.at[f], side * self.nbo // 2)

    def window(self, f, raw, far):
        g, nbo = self.g[f], self.nbo
        for j in range(nbo, 0, -1):
            cur = far.at[f, 0] if j == nbo else raw.at[j]
            for lo, sign in SIDES:
                re, im, new_re, new_im = shifted_add(cur, raw.at[j - 1], lo, sign)
                g[j, re], g[j, im] = new_re, new_im
        if raw is not g:
            g[0] = raw[0]

    def pointwise(self, xhat, f, far, dst, r, first):
        g, nbo = self.g[f], self.nbo
        re, im = pl.ds(pl.multiple_of(r * 16, 16), 16), pl.ds(pl.multiple_of(BLK + r * 16, 16), 16)
        for k in range(first, self.nb):
            acc_re = acc_im = None
            for j in range(k + 1):
                i = k - j
                gr, gi = (g[i, re], g[i, im]) if i <= nbo else (far[f, i - nbo, re], far[f, i - nbo, im])
                xr, xi = xhat[j, re], xhat[j, im]
                t_re, t_im = xr * gr - xi * gi, xr * gi + xi * gr
                acc_re = t_re if acc_re is None else acc_re + t_re
                acc_im = t_im if acc_im is None else acc_im + t_im
            for part, (a, b) in enumerate(zip(split3(acc_re), split3(acc_im))):
                dst[k - first, part, re], dst[k - first, part, im] = a, b

    def inverse(self, parts, k):
        return dot(self.inv6[...], stack6(parts[k, 0], parts[k, 1], parts[k, 2]))

    def gate_one(self, s, k, data):
        x1, v, _, _, skip, _ = data
        z = x1[s, k].astype(F32) * (self.inverse(self.first[s], k) + skip * v[s, k].astype(F32))
        self.zval[s][k] = z
        for part, a in enumerate(split3(z)):
            self.zparts[k, part] = a

    def spectrum(self, k):
        self.zhat[k] = block_spectrum(self.fwd6, self.zparts, k)

    def gate_two(self, s, k, data):
        y = data[2][s, k].astype(F32) * (self.inverse(self.second[s], k) + data[5] * self.zval[s][self.nbo + k])
        self.ybuf[s, k] = y.astype(BF16)

    def middle(self, s, data, i, point=None):
        for q in range(4):
            if point is not None:
                point(4 * i + q)
            for k in PAIR:
                if q < 2:
                    self.gate_one(s, 4 * i + 2 * q + k, data)
                else:
                    self.spectrum(4 * i + 2 * (q - 2) + k)

    def step(self, land, t, vhat, data, old, relay):
        nb, nbo = self.nb, self.nbo
        far = data[3]
        self.near(land, t, 0)
        for j in range(nbo):
            self.g[0][j] = block_spectrum(self.fwd6, self.hparts.at[0], j)
        self.near(land, t, 1)
        self.window(0, self.g[0], far)
        relay(1)

        @loop(nb // 4)
        def _(i):
            self.middle(1, old, i, lambda r: self.pointwise(vhat.at[0], 0, far, self.first[0], r, 0))


        @loop(nbo // 2)
        def _(i):
            for q in range(4):
                self.pointwise(self.zhat, 1, old[3], self.second[1], 4 * i + q, nbo)
                if q < 2:
                    self.gate_two(0, 2 * i + q, old)
                else:
                    j = 2 * i + q - 2
                    self.raw2[j] = block_spectrum(self.fwd6, self.hparts.at[1], j)

        relay(0)
        self.window(1, self.raw2, far)

        @loop(nb // 4)
        def _(i):
            self.middle(0, data, i, lambda r: self.pointwise(vhat.at[1], 0, far, self.first[1], r, 0))

        @loop(nbo // 2)
        def _(i):
            for q in range(4):
                self.pointwise(self.zhat, 1, far, self.second[0], 4 * i + q, nbo)
                if q % 2 == 0:
                    self.gate_two(1, 2 * i + q // 2, old)

    def drain(self, data):
        nb, nbo = self.nb, self.nbo

        @loop(nb // 4)
        def _(i):
            self.middle(1, data, i)

        @loop(nbo // 2)
        def _(i):
            for q in range(4):
                self.pointwise(self.zhat, 1, data[3], self.second[1], 4 * i + q, nbo)
                if q % 2 == 0:
                    self.gate_two(0, 2 * i + q // 2, data)

        for k in range(nbo):
            self.gate_two(1, k, data)

    def result(self, c, keep, send):
        hk = self.nbo // 2
        for s in range(self.ybuf.shape[0]):
            for b in range(hk):
                keep[s, b * BLK:(b + 1) * BLK] = self.ybuf[s, c * hk + b]
                send[s, b * BLK:(b + 1) * BLK] = self.ybuf[s, (1 - c) * hk + b].astype(F32)


def out_body(keep, part, w_out, u_in, out, wbuf, w_sem, lhs, keep_v, stage, in_sem, u_v, o_st, o_sem):
    c = lax.rem(lax.axis_index("sp"), 2)
    n_tile, n_seq, n_pos, _ = keep.shape
    half_w = n_tile * TC
    width = 2 * half_w
    n_col, rows = width // TN, width // 4

    def weights(j, slot):
        cols = pl.ds(pl.multiple_of(j * TN, TN), TN)
        return [pltpu.make_async_copy(w_out.at[i * rows:(i + 1) * rows, cols],
                                      wbuf.at[slot, i * rows:(i + 1) * rows], w_sem.at[slot, i]) for i in range(4)] + [
                    pltpu.make_async_copy(u_in.at[:, :, cols], u_v.at[slot], w_sem.at[slot, 4])]

    def flush(j):
        slot = parity(j)
        return pltpu.make_async_copy(o_st.at[slot], out.at[:, :, pl.ds(pl.multiple_of(j * TN, TN), TN)], o_sem.at[slot])

    loads = [pltpu.make_async_copy(part.at[u], stage.at[u], in_sem.at[u]) for u in range(n_tile)]
    loads += [pltpu.make_async_copy(keep.at[u], keep_v.at[u], in_sem.at[n_tile + u]) for u in range(n_tile)]
    for copy in loads:
        copy.start()
    for copy in weights(0, 0):
        copy.start()
    for u in range(n_tile):
        loads[u].wait()
        loads[n_tile + u].wait()
        for s in range(n_seq):
            lhs[s, :, pl.ds(pl.multiple_of((1 - c) * half_w + u * TC, TC), TC)] = stage[u, s].astype(BF16)
            lhs[s, :, pl.ds(pl.multiple_of(c * half_w + u * TC, TC), TC)] = keep_v[u, s]

    def step(j, carry):
        slot = parity(j)

        @pl.when(j + 1 < n_col)
        def _():
            for copy in weights(j + 1, 1 - slot):
                copy.start()

        for copy in weights(j, slot):
            copy.wait()

        @pl.when(j >= 2)
        def _():
            flush(j - 2).wait()

        for s in range(n_seq):
            o_st[slot, s] = (u_v[slot, s].astype(F32) + dot(lhs[s], wbuf[slot])).astype(BF16)
        flush(j).start()
        return carry

    lax.fori_loop(0, n_col, step, 0)
    for j in (n_col - 2, n_col - 1):
        flush(j).wait()


def solution(mesh):
    fwd3, fwd6, inv6 = transform_tables()

    def local_step(u_in, w_in, b_in, conv_taps, w_out, skip_one, skip_two, filt_one, filt_two):
        n_seq, n_pos, width = u_in.shape
        half_w = width // 2
        n_own = 2 * n_pos
        nb = 2 * n_own // BLK
        nbo = nb // 2
        n_tile = half_w // TC
        rows = n_pos // GR, GR, width
        small, large = pl.BlockSpec(memory_space=pltpu.VMEM), pl.BlockSpec(memory_space=pl.ANY)
        dma = pltpu.SemaphoreType.DMA

        def shape(dims, dtype=F32):
            return jax.ShapeDtypeStruct(dims, dtype)

        keep, part, *_ = pl.pallas_call(
            main_body,
            in_specs=[small] * 7 + [large] * 4,
            out_specs=[large] * 12,
            out_shape=[
                shape((n_tile, n_seq, n_pos, TC), BF16), shape((n_tile, n_seq, n_pos, TC)),
                shape((n_tile, n_seq, nb + nbo, BLK, TC), BF16), shape((n_tile, n_seq, nb, BLK, TC), BF16),
                shape((n_tile, n_seq, nb, 2 * BLK, TC)), shape((n_tile, 2, nbo, 2 * BLK, TC)),
                shape((n_seq, *rows)), shape((n_seq, 8, width)), shape((n_seq, *rows)), shape((2, n_seq, *rows)),
                shape((n_seq, 8, width)), shape((2, n_pos, half_w)),
            ],
            scratch_shapes=[
                pltpu.VMEM((2, n_tile, 2, n_pos, TC), F32),
                dma((1,)), dma((1,)), *[dma((n_seq, 3, 2))] * 4, *[dma((n_seq,))] * 2, *[dma((2,))] * 2,
                dma((2, n_tile, 2)), *[dma((n_tile, Q, 2))] * 4, *[dma((n_tile,))] * 2,
            ],
            compiler_params=pltpu.CompilerParams(vmem_limit_bytes=62 << 20, collective_id=0, has_side_effects=True),
            name="hyena_main",
        )(fwd3, fwd6, inv6, b_in.reshape(1, -1), conv_taps, skip_one.reshape(1, -1), skip_two.reshape(1, -1),
          u_in, w_in, filt_one, filt_two)

        return pl.pallas_call(
            out_body,
            in_specs=[large] * 4,
            out_specs=large,
            out_shape=shape((n_seq, n_pos, width), BF16),
            scratch_shapes=[
                pltpu.VMEM((2, width, TN), BF16), dma((2, 5)),
                pltpu.VMEM((n_seq, n_pos, width), BF16), pltpu.VMEM((n_tile, n_seq, n_pos, TC), BF16), pltpu.VMEM((n_tile, n_seq, n_pos, TC), F32),
                dma((2 * n_tile,)), pltpu.VMEM((2, n_seq, n_pos, TN), BF16), pltpu.VMEM((2, n_seq, n_pos, TN), BF16), dma((2,)),
            ],
            compiler_params=pltpu.CompilerParams(vmem_limit_bytes=60 << 20),
            name="out_proj",
        )(keep, part, w_out, u_in)

    seq_spec = P("dp", "sp", None)
    filt_spec = P("sp", None)
    return jax.shard_map(local_step, mesh=mesh, in_specs=(seq_spec, P(), P(), P(), P(), P(), P(), filt_spec, filt_spec), out_specs=seq_spec, check_vma=False)
```

```python
import functools

import jax
import jax.numpy as jnp
import numpy as np
from jax import lax
from jax.experimental import pallas as pl
from jax.experimental.pallas import tpu as pltpu
from jax.sharding import PartitionSpec as P

F32, BF16 = jnp.float32, jnp.bfloat16
BLK = 128
TN = 512
TC = 256
Q = 2
PAIR = (0, 1)
GR = 32
MESH = pl.DeviceIdType.MESH


def split_table(table):
    parts, rest = [], table.astype(np.float64)
    for _ in range(3):
        part = rest.astype(np.float32).astype(jnp.bfloat16)
        parts.append(part)
        rest = rest - part.astype(np.float64)
    return parts


def transform_tables():
    freq = np.concatenate([np.arange(0, BLK, 2), np.arange(1, BLK, 2)]) + 0.5
    angle = 2.0 * np.pi * freq[:, None] * np.arange(BLK)[None, :] / (2 * BLK)
    fwd = np.concatenate([np.cos(angle), -np.sin(angle)], 0)
    inv = np.concatenate([np.cos(angle).T, -np.sin(angle).T], 1) / BLK
    f1, f2, f3 = split_table(fwd)
    e1, e2, e3 = split_table(inv)
    fwd3 = np.concatenate([f1, f2, f3], 1)
    fwd6 = np.concatenate([f1, f1, f2, f2, f1, f3], 1)
    inv6 = np.concatenate([e1, e1, e2, e2, e1, e3], 1)
    return fwd3, fwd6, inv6


def parity(x):
    return lax.rem(x, 2)


def dot(a, b):
    return jnp.dot(a, b, preferred_element_type=F32)


def split3(x):
    hi = x.astype(BF16)
    rest = x - hi.astype(F32)
    mid = rest.astype(BF16)
    low = (rest - mid.astype(F32)).astype(BF16)
    return hi, mid, low


def stack6(hi, mid, low):
    return jnp.concatenate([hi, mid, hi, mid, low, hi], axis=0)


def split_blocks(src, parts, first):
    for j in range(src.shape[0] // BLK):
        for i, a in enumerate(split3(src[j * BLK:(j + 1) * BLK])):
            parts[first + j, i] = a


def block_spectrum(fwd6_ref, parts, j):
    return dot(fwd6_ref[...], stack6(parts[j, 0], parts[j, 1], parts[j, 2]))


def shifted_add(cur, old, lo, sign):
    re, im = slice(lo, lo + BLK // 2), slice(BLK + lo, BLK + lo + BLK // 2)
    return re, im, cur[re] - sign * old[im], cur[im] + sign * old[re]


SIDES = ((0, 1.0), (BLK // 2, -1.0))


def short_conv(pbuf, t, first, rows):
    return (t[0:1] * pbuf[8 + first:8 + first + rows] + t[1:2] * pbuf[7 + first:7 + first + rows] + t[2:3] * pbuf[6 + first:6 + first + rows]).astype(BF16)


def block_values(fwd3_ref, blk):
    return dot(fwd3_ref[...], jnp.concatenate([blk, blk, blk], axis=0))


def main_body(fwd3_ref, fwd6_ref, inv6_ref, bias_ref, taps_ref, sk1_ref, sk2_ref, u_bf, w_in, f1, f2,
              keep, part, qx, qv, vhat, far, u32, tsrc, u_sw, u_x, tail, pf,
              land, ts, tr, os, orr, ws, wr, ss, sr, fs, fr, l_sem, x_send, x_recv, y_send, y_recv, p_send, p_recv):
    sp, dp = lax.axis_index("sp"), lax.axis_index("dp")
    c = parity(sp)
    on_b = sp >= 2
    on_a = jnp.logical_not(on_b)
    other = sp + 1 - 2 * c
    n_seq, n_pos, width = u_bf.shape
    half_w = width // 2
    nt, n_tile, per = half_w // TN, half_w // TC, TN // TC
    n_own, hp = 2 * n_pos, n_pos // 2
    nbo = n_own // BLK
    cuts = (0, hp, hp + hp // 2, n_pos)
    n_cut = len(cuts) - 1

    def remote(src, dst, send, recv, peer):
        return pltpu.make_async_remote_copy(src, dst, send, recv, device_id=peer, device_id_type=MESH)

    def at(start, size):
        return pl.ds(pl.multiple_of(start, size), size)

    def share(s, h, k):
        rows = (cuts[h + 1] - cuts[h]) // 2
        return s, pl.ds((cuts[h] + k * rows) // GR, rows // GR)

    def tail_copy():
        return remote(tsrc, tail, ts.at[0], tr.at[0], (dp, 3))

    def tail_across():
        return remote(tail, tail, ts.at[0], tr.at[0], (dp, other))

    def over(s, h, k):
        s, rows = share(s, h, k)
        return remote(u32.at[s, rows], u_x.at[c, s, rows], os.at[s, h, k], orr.at[s, h, c], (dp, 2 + k))

    def arrived(s, h, src):
        at_s, rows = share(s, h, 0)
        ref = u_x.at[src, at_s, rows]
        return remote(ref, ref, os.at[s, h, src], orr.at[s, h, src], (dp, sp))

    def onward(s, h, src):
        at_s, rows = share(s, h, c)
        ref = u_x.at[src, at_s, rows]
        return remote(ref, ref, ws.at[s, h, src], wr.at[s, h, src], (dp, other))

    def swap_u(s):
        return remote(u32.at[s], u_sw.at[s], ss.at[s], sr.at[s], (dp, other))

    def swap_f(f):
        return remote((f1, f2)[f].at[:, at((1 - c) * half_w, half_w)], pf.at[f], fs.at[f], fr.at[f], (dp, other))

    qr = n_pos // Q

    def filt(src, u, k, q):
        return remote(src.at[q * qr:(q + 1) * qr, at(k * half_w + u * TC, TC)], land.at[dp, u, c, q * qr:(q + 1) * qr],
                      x_send.at[u, q, k], x_recv.at[u, q, c], (dp, 2 + k))

    def direct(src, k):
        u, q = n_tile - 1, Q - 1
        return remote(src.at[q * qr:(q + 1) * qr, at(k * half_w + u * TC, TC)], land.at[1 - dp, u, c, q * qr:(q + 1) * qr],
                      y_send.at[u, q, k], y_recv.at[u, q, c], (dp, 2 + k))

    def landed(u, side, q):
        ref = land.at[dp, u, side, at(q * qr, qr)]
        return remote(ref, ref, x_send.at[u, q, side], x_recv.at[u, q, side], (dp, sp))

    def across(u, side, f, q):
        ref = land.at[f, u, side, at(q * qr, qr)]
        return remote(ref, ref, y_send.at[u, q, side], y_recv.at[u, q, side], (1 - dp, sp))

    def fill(f, u, side, src, start):
        return pltpu.make_async_copy(src.at[:, at(start, TC)], land.at[f, u, side], l_sem.at[f, u, side])

    def column(g, j):
        return (g + j // nt) * width + c * half_w + lax.rem(j, nt) * TN

    def load_rows(stage, st_sem, items):
        def copy(i):
            src, rows, _, _ = items[i]
            return pltpu.make_async_copy(src, stage.at[i % 2, :rows // GR], st_sem.at[i % 2])

        copy(0).start()
        for i, (_, rows, dst, row) in enumerate(items):
            if i + 1 < len(items):
                copy(i + 1).start()
            copy(i).wait()
            dst[pl.ds(pl.multiple_of(row, 16), rows), :] = stage[i % 2, :rows // GR].reshape(rows, width).astype(BF16)

    barrier = pltpu.get_barrier_semaphore()
    for peer in ((dp, other), (dp, lax.rem(sp + 2, 4)), (dp, lax.rem(other + 2, 4)), (1 - dp, sp)):
        pl.semaphore_signal(barrier, inc=1, device_id=peer, device_id_type=MESH)
    pl.semaphore_wait(barrier, 4)

    def widen(raw, wide, tail_raw, tail_wide, in_sem, out_sem):
        def half(ref, s, h):
            return ref.at[s, h * hp:h * hp + hp]

        def load(s, h):
            return pltpu.make_async_copy(half(u_bf, s, h), raw.at[h], in_sem.at[h])

        last_rows = pltpu.make_async_copy(u_bf.at[:, n_pos - 8:], tail_raw, in_sem.at[2])
        last_out = pltpu.make_async_copy(tail_wide, tsrc, out_sem.at[2])
        order = [(s, h) for s in range(n_seq) for h in PAIR]
        last_rows.start()
        load(*order[0]).start()
        last_rows.wait()
        tail_wide[...] = tail_raw[...].astype(F32)
        last_out.start()
        pending = {}
        for (s, h), following in zip(order, order[1:] + [None]):
            if following:
                load(*following).start()
            load(s, h).wait()
            if h in pending:
                pending.pop(h).wait()
            wide[h] = raw[h].astype(F32).reshape(wide.shape[1:])
            store = pltpu.make_async_copy(wide.at[h], u32.at[s, pl.ds(h * hp // GR, hp // GR)], out_sem.at[h])
            store.start()
            if s + h:
                pending[h] = store
                continue
            last_out.wait()

            @pl.when(sp == 1)
            def _():
                tail_copy().start()

            store.wait()

            @pl.when(on_a)
            def _():
                for k in PAIR:
                    over(s, h, k).start()

        for store in pending.values():
            store.wait()

    pl.run_scoped(
        widen, pltpu.VMEM((2, hp, width), BF16), pltpu.VMEM((2, hp // GR, GR, width), F32), pltpu.VMEM((n_seq, 8, width), BF16),
        pltpu.VMEM((n_seq, 8, width), F32), pltpu.SemaphoreType.DMA((3,)), pltpu.SemaphoreType.DMA((3,)))

    @pl.when(on_a)
    def _():
        for i in range(1, n_seq * n_cut):
            for k in PAIR:
                over(*divmod(i, n_cut), k).start()
        for which, src, rest in ((0, f1, f2), (1, f2, f1)):
            @pl.when(dp == which)
            def _():
                for u in range(n_tile):
                    for q in range(Q):
                        for k in PAIR:
                            filt(src, u, k, q).start()
                for k in PAIR:
                    direct(rest, k).start()

    for i in range(n_seq):
        swap_u(i).start()
    for f in PAIR:
        swap_f(f).start()

    def forward(u, q):
        @pl.when(on_b)
        def _():
            for side in PAIR:
                landed(u, side, q).wait_recv()
                across(u, side, dp, q).start()

    def front(wbuf, wsem, lhs, stage, st_sem, lhs_sem, tailbuf, q_st, q_sem, vh_st, vh_sem, pbuf):
        def weights(g, j, slot):
            rows = width // 4
            return [pltpu.make_async_copy(w_in.at[i * rows:(i + 1) * rows, at(column(g, j), TN)],
                                          wbuf.at[slot, i * rows:(i + 1) * rows], wsem.at[slot, i]) for i in range(4)]

        def stream(g, body, following, n=nt):
            def step(j, carry):
                slot = parity(j)

                @pl.when(j + 1 < n)
                def _():
                    for copy in weights(g, j + 1, 1 - slot):
                        copy.start()

                if following is not None:
                    @pl.when(j + 1 == n)
                    def _():
                        following(1 - slot)

                for copy in weights(g, j, slot):
                    copy.wait()
                body(j, slot, bias_ref[:, at(column(g, j), TN)], taps_ref[:, at(column(g, j), TN)])
                return carry

            lax.fori_loop(0, n, step, 0)

        def begin(g):
            def start(slot):
                for copy in weights(g, 0, slot):
                    copy.start()
            return start

        def project(rows_ref, slot, bias):
            return (dot(rows_ref, wbuf[slot]) + bias).astype(BF16).astype(F32)

        tail_rows = n_seq * 8
        begin(0)(0)
        own_rows = [pltpu.make_async_copy(u_bf.at[s], lhs.at[pl.ds(pl.multiple_of(tail_rows + s * n_own + c * n_pos, 16), n_pos)], lhs_sem.at[s])
                    for s in range(n_seq)]
        for copy in own_rows:
            copy.start()
        for s in range(n_seq):
            swap_u(s).wait_recv()
        load_rows(stage, st_sem, [(u_sw.at[s, pl.ds(h * hp // GR, hp // GR)], hp, lhs, tail_rows + s * n_own + (1 - c) * n_pos + h * hp)
                                  for s in range(n_seq) for h in PAIR])
        for copy in own_rows:
            copy.wait()

        @pl.when(on_b)
        def _():
            tail_copy().wait_recv()

            @pl.when(sp == 3)
            def _():
                tail_across().start()

            copy = pltpu.make_async_copy(tail, tailbuf, lhs_sem.at[0])
            copy.start()
            copy.wait()

        @pl.when(on_a)
        def _():
            tailbuf[...] = jnp.zeros_like(tailbuf)

        lhs[:tail_rows, :] = tailbuf[...].reshape(tail_rows, width).astype(BF16)
        chunk = n_pos

        def own_phase(g, n, dst, spectrum, following):
            def flush(j, slot):
                blocks = pl.ds(nbo * (1 + j // nt), nbo)
                copies = []
                for h in range(per):
                    u = lax.rem(j, nt) * per + h
                    copies.append(pltpu.make_async_copy(q_st.at[slot, h], dst.at[u, :, blocks], q_sem.at[slot, h]))
                    if spectrum:
                        copies.append(pltpu.make_async_copy(vh_st.at[slot, h], vhat.at[u, :, nbo:], vh_sem.at[slot, h]))
                return copies

            def body(j, slot, bias, taps):
                @pl.when(j >= 2)
                def _():
                    for copy in flush(j - 2, slot):
                        copy.wait()

                for i in range(n_seq * n_own // chunk):
                    s, r = divmod(i * chunk, n_own)
                    p = project(lhs[(tail_rows + i * chunk if i else 0):tail_rows + (i + 1) * chunk, :], slot, bias)
                    if i == 0:
                        for k in range(n_seq):
                            pbuf[k, 0:8] = jnp.where(on_b, p[8 * k:8 * k + 8], 0.0)
                        p = p[tail_rows:]
                    pbuf[s, 8 + r:8 + r + chunk] = p
                    q = short_conv(pbuf.at[s], taps, r, chunk)
                    for b in range(chunk // BLK):
                        blk = q[b * BLK:(b + 1) * BLK]
                        for h in range(per):
                            q_st[slot, h, s, r // BLK + b] = blk[:, h * TC:(h + 1) * TC]
                        if spectrum:
                            spec = block_values(fwd3_ref, blk)
                            for h in range(per):
                                vh_st[slot, h, s, r // BLK + b] = spec[:, h * TC:(h + 1) * TC]
                for copy in flush(j, slot):
                    copy.start()

            stream(g, body, following, n)
            for j in (n - 2, n - 1):
                for copy in flush(j, j % 2):
                    copy.wait()

        own_phase(0, 2 * nt, qx, False, begin(2))
        own_phase(2, nt, qv, True, None)

        def far_phase(fin, fin_sem, fout, fout_sem, parts):
            hk = n_pos // BLK

            def fetch(j, slot):
                mine = at(c * half_w + j * TC, TC)
                srcs = (f1.at[:, mine], f2.at[:, mine], pf.at[0, :, at(j * TC, TC)], pf.at[1, :, at(j * TC, TC)])
                return [pltpu.make_async_copy(src, fin.at[slot, i], fin_sem.at[slot, i]) for i, src in enumerate(srcs)]

            def flush(j, slot):
                return pltpu.make_async_copy(fout.at[slot], far.at[j], fout_sem.at[slot])

            for copy in fetch(0, 0):
                copy.start()

            def step(j, carry):
                slot = parity(j)

                @pl.when(j + 1 < n_tile)
                def _():
                    for copy in fetch(j + 1, 1 - slot):
                        copy.start()

                for copy in fetch(j, slot):
                    copy.wait()

                @pl.when(j >= 2)
                def _():
                    flush(j - 2, slot).wait()

                for f in PAIR:
                    split_blocks(fin.at[slot, f], parts.at[f], c * hk)
                    split_blocks(fin.at[slot, 2 + f], parts.at[f], (1 - c) * hk)
                g_ref = fout.at[slot]
                for f in PAIR:
                    for b in range(2 * hk):
                        g_ref[f, b] = block_spectrum(fwd6_ref, parts.at[f], b)
                    for b in range(2 * hk - 1, 0, -1):
                        for lo, sign in SIDES:
                            re, im, new_re, new_im = shifted_add(g_ref.at[f, b], g_ref.at[f, b - 1], lo, sign)
                            g_ref[f, b, re], g_ref[f, b, im] = new_re, new_im
                flush(j, slot).start()
                return carry

            lax.fori_loop(0, n_tile, step, 0)
            for j in (n_tile - 2, n_tile - 1):
                flush(j, j % 2).wait()

        for f in PAIR:
            swap_f(f).wait_recv()
        pl.run_scoped(
            far_phase, pltpu.VMEM((2, 4, n_pos, TC), F32), pltpu.SemaphoreType.DMA((2, 4)),
            pltpu.VMEM((2, 2, nbo, 2 * BLK, TC), F32), pltpu.SemaphoreType.DMA((2,)), pltpu.VMEM((2, nbo, 3, BLK, TC), BF16))

    pl.run_scoped(
        front,
        pltpu.VMEM((2, width, TN), BF16), pltpu.SemaphoreType.DMA((2, 4)),
        pltpu.VMEM((n_seq * n_own + 8 * n_seq, width), BF16),
        pltpu.VMEM((2, hp // GR, GR, width), F32), pltpu.SemaphoreType.DMA((2,)), pltpu.SemaphoreType.DMA((n_seq,)), pltpu.VMEM((n_seq, 8, width), F32),
        pltpu.VMEM((2, per, n_seq, nbo, BLK, TC), BF16), pltpu.SemaphoreType.DMA((2, per)),
        pltpu.VMEM((2, per, n_seq, nbo, 2 * BLK, TC), F32), pltpu.SemaphoreType.DMA((2, per)),
        pltpu.VMEM((n_seq, n_own + 8, TN), F32))

    def prev(wres, w_sem, lhs_p, stage, st_sem, q_st, q_sem, vh_st, vh_sem, pbuf, pstash):
        def weights(j):
            rows = width // 4
            return [pltpu.make_async_copy(w_in.at[i * rows:(i + 1) * rows, at(which(j), TN)],
                                          wres.at[j, i * rows:(i + 1) * rows], w_sem.at[j, i]) for i in range(4)]

        def which(j):
            return 2 * (j // nt) * width + c * half_w + lax.rem(j, nt) * TN

        def begin(j, carry):
            for copy in weights(j):
                copy.start()
            return carry

        lax.fori_loop(0, 2 * nt, begin, 0)

        def rows(s, h):
            n = cuts[h + 1] - cuts[h]

            @pl.when(on_b)
            def _():
                for src in PAIR:
                    arrived(s, h, src).wait_recv()
                    onward(s, h, src).start()
                for src in PAIR:
                    onward(s, h, src).wait_recv()
                load_rows(stage, st_sem, [(u_x.at[src, s, cuts[h] // GR:cuts[h + 1] // GR], n, lhs_p, src * n) for src in PAIR])

            @pl.when(on_a)
            def _():
                lhs_p[...] = jnp.zeros_like(lhs_p)

        def project(h, j):
            n = 2 * (cuts[h + 1] - cuts[h])
            return (dot(lhs_p[:n, :], wres[j]) + bias_ref[:, at(which(j), TN)]).astype(BF16)

        def first(s, h):
            n = cuts[h + 1] - cuts[h]

            def body(j, carry):
                if h == 0:
                    @pl.when(s == 0)
                    def _():
                        for copy in weights(j):
                            copy.wait()

                p = project(h, j)
                for core in PAIR:
                    pstash[core, cuts[h]:cuts[h + 1], at(j * TN, TN)] = p[core * n:(core + 1) * n]
                return carry

            lax.fori_loop(0, 2 * nt, body, 0)

        def last(s, u, dst):
            base, spectrum = u * nt, u > 0
            h = n_cut - 1
            n = cuts[h + 1] - cuts[h]

            def flush(j):
                slot, copies = parity(j), []
                for half in range(per):
                    copies.append(pltpu.make_async_copy(q_st.at[slot, half], dst.at[j * per + half, s, :nbo], q_sem.at[slot, half]))
                    if spectrum:
                        copies.append(pltpu.make_async_copy(vh_st.at[slot, half], vhat.at[j * per + half, s, :nbo], vh_sem.at[slot, half]))
                return copies

            def body(j, carry):
                slot = parity(j)

                @pl.when(j >= 2)
                def _():
                    for copy in flush(j - 2):
                        copy.wait()

                taps = taps_ref[:, at(which(base + j), TN)]
                pbuf[0:8] = jnp.zeros((8, TN), F32)
                for core in PAIR:
                    old = pstash[core, :cuts[h], at((base + j) * TN, TN)].astype(F32)
                    pbuf[8 + core * n_pos:8 + core * n_pos + cuts[h]] = jnp.where(on_b, old, 0.0)
                p = project(h, base + j).astype(F32)
                for core in PAIR:
                    start = 8 + core * n_pos + cuts[h]
                    pbuf[start:start + n] = jnp.where(on_b, p[core * n:(core + 1) * n], 0.0)
                for b in range(nbo):
                    blk = short_conv(pbuf, taps, b * BLK, BLK)
                    for half in range(per):
                        q_st[slot, half, b] = blk[:, half * TC:(half + 1) * TC]
                    if spectrum:
                        spec = block_values(fwd3_ref, blk)
                        for half in range(per):
                            vh_st[slot, half, b] = spec[:, half * TC:(half + 1) * TC]
                for copy in flush(j):
                    copy.start()

                @pl.when(jnp.logical_and(s == n_seq - 1, jnp.logical_and(lax.rem(j, Q) == 1, j < nt - Q * u)))
                def _():
                    forward(u, j // Q)
                return carry

            lax.fori_loop(0, nt, body, 0)
            for j in (nt - 2, nt - 1):
                for copy in flush(j):
                    copy.wait()

        def one_seq(s, carry):
            for h in range(n_cut - 1):
                rows(s, h)
                first(s, h)
            rows(s, n_cut - 1)
            last(s, 0, qx)
            last(s, 1, qv)
            return carry

        lax.fori_loop(0, n_seq, one_seq, 0)

    pl.run_scoped(
        prev,
        pltpu.VMEM((2 * nt, width, TN), BF16), pltpu.SemaphoreType.DMA((2 * nt, 4)),
        pltpu.VMEM((2 * hp, width), BF16), pltpu.VMEM((2, hp // GR, GR, width), F32), pltpu.SemaphoreType.DMA((2,)),
        pltpu.VMEM((2, per, nbo, BLK, TC), BF16), pltpu.SemaphoreType.DMA((2, per)),
        pltpu.VMEM((2, per, nbo, 2 * BLK, TC), F32), pltpu.SemaphoreType.DMA((2, per)),
        pltpu.VMEM((n_own + 8, TN), F32), pltpu.VMEM((2, cuts[-2], 2 * half_w), BF16))

    @pl.when(on_a)
    def _():
        for u in range(n_tile):
            for f, own in enumerate((f1, f2)):
                fill(f, u, c, own, c * half_w + u * TC).start()
                fill(f, u, 1 - c, pf.at[f], u * TC).start()

    def conv(x1b, vb, x2b, vhb, farb, in_sem, vh_sem, kst, k_sem, sendbuf, *scratch):
        def fetch(t):
            slot, two = lax.rem(t, 3), parity(t)
            srcs = (qx.at[t, :, :2 * nbo], qv.at[t], qx.at[t, :, 2 * nbo:], far.at[t])
            copies = [pltpu.make_async_copy(r, b.at[slot], in_sem.at[slot, i])
                      for i, (r, b) in enumerate(zip(srcs, (x1b, vb, x2b, farb)))]
            return copies + [pltpu.make_async_copy(vhat.at[t, s], vhb.at[two, s], vh_sem.at[two, s]) for s in range(n_seq)]

        def flush(t):
            slot = parity(t)
            return pltpu.make_async_copy(kst.at[slot], keep.at[t], k_sem.at[slot])

        def swap_y(u):
            return remote(sendbuf.at[parity(u)], part.at[u], p_send.at[u], p_recv.at[u], (dp, other))

        tile = ConvTile(fwd6_ref, inv6_ref, *scratch)

        def inputs(t, back):
            slot, cols = lax.rem(t + 3 - back, 3), at(c * half_w + lax.rem(t + n_tile - back, n_tile) * TC, TC)
            return x1b.at[slot], vb.at[slot], x2b.at[slot], farb.at[slot], sk1_ref[:, cols], sk2_ref[:, cols]

        def emit(t):
            slot = parity(t)

            @pl.when(t >= 2)
            def _():
                flush(t - 2).wait()
                swap_y(t - 2).wait_send()

            tile.result(c, kst.at[slot], sendbuf.at[slot])
            flush(t).start()
            swap_y(t).start()

        for copy in fetch(0):
            copy.start()
        forward(1, Q - 1)

        def step(t, carry):
            @pl.when(t + 1 < n_tile)
            def _():
                for copy in fetch(t + 1):
                    copy.start()

            @pl.when(on_a)
            def _():
                for f in PAIR:
                    for side in PAIR:
                        fill(f, t, side, f1, 0).wait()

            @pl.when(on_b)
            def _():
                for q in range(Q):
                    for side in PAIR:
                        across(t, side, 1 - dp, q).wait_recv()

            @pl.when(jnp.logical_and(on_b, t == n_tile - 1))
            def _():
                for side in PAIR:
                    landed(t, side, Q - 1).wait_recv()

            for copy in fetch(t):
                copy.wait()

            def relay(q):
                ahead = 2 - q

                @pl.when(jnp.logical_and(t >= q, t + ahead + q < n_tile))
                def _():
                    forward(t + ahead, q)

            tile.step(land, t, vhb.at[parity(t)], inputs(t, 0), inputs(t, 1), relay)

            @pl.when(t >= 1)
            def _():
                emit(t - 1)
            return carry

        lax.fori_loop(0, n_tile, step, 0)
        tile.drain(inputs(n_tile, 1))
        emit(n_tile - 1)
        for u in (n_tile - 2, n_tile - 1):
            flush(u).wait()
            swap_y(u).wait_send()
        for u in range(n_tile):
            swap_y(u).wait_recv()

    nb = 2 * nbo
    pl.run_scoped(
        conv,
        pltpu.VMEM((3, n_seq, nb, BLK, TC), BF16), pltpu.VMEM((3, n_seq, nb, BLK, TC), BF16), pltpu.VMEM((3, n_seq, nbo, BLK, TC), BF16),
        pltpu.VMEM((2, n_seq, nb, 2 * BLK, TC), F32), pltpu.VMEM((3, 2, nbo, 2 * BLK, TC), F32),
        pltpu.SemaphoreType.DMA((3, 4)), pltpu.SemaphoreType.DMA((2, n_seq)),
        pltpu.VMEM((2, n_seq, n_pos, TC), BF16), pltpu.SemaphoreType.DMA((2,)), pltpu.VMEM((2, n_seq, n_pos, TC), F32),
        pltpu.VMEM((2, nbo, 3, BLK, TC), BF16),
        pltpu.VMEM((nbo + 1, 2 * BLK, TC), F32), pltpu.VMEM((nbo + 1, 2 * BLK, TC), F32), pltpu.VMEM((nbo, 2 * BLK, TC), F32),
        *[pltpu.VMEM((nb, 3, 2 * BLK, TC), BF16)] * n_seq,
        pltpu.VMEM((nb, 3, BLK, TC), BF16),
        *[pltpu.VMEM((nb, BLK, TC), F32)] * n_seq,
        pltpu.VMEM((nb, 2 * BLK, TC), F32),
        *[pltpu.VMEM((nbo, 3, 2 * BLK, TC), BF16)] * n_seq,
        pltpu.VMEM((n_seq, nbo, BLK, TC), BF16))

    for s in range(n_seq):
        swap_u(s).wait_send()
    for f in PAIR:
        swap_f(f).wait_send()

    @pl.when(sp == 1)
    def _():
        tail_copy().wait_send()

    @pl.when(sp == 3)
    def _():
        tail_across().wait_send()

    @pl.when(on_a)
    def _():
        for i in range(n_seq * n_cut):
            for k in PAIR:
                over(*divmod(i, n_cut), k).wait_send()
        for u in range(n_tile):
            for q in range(Q):
                for k in PAIR:
                    filt(f1, u, k, q).wait_send()
        for k in PAIR:
            direct(f1, k).wait_send()

    @pl.when(on_b)
    def _():
        for i in range(n_seq * n_cut):
            for src in PAIR:
                onward(*divmod(i, n_cut), src).wait_send()
        for u in range(n_tile):
            for q in range(Q - u // (n_tile - 1)):
                for side in PAIR:
                    across(u, side, dp, q).wait_send()


def loop(trips):
    def run(body):
        def step(i, carry):
            body(i)
            return carry
        lax.fori_loop(0, trips, step, 0)
    return run


class ConvTile:
    def __init__(self, fwd6, inv6, hparts, g1, g2, raw2, sp0, sp1, zparts, zv0, zv1, zhat, sq0, sq1, ybuf):
        self.fwd6, self.inv6, self.hparts, self.g, self.raw2 = fwd6, inv6, hparts, (g1, g2), raw2
        self.first, self.second, self.zparts, self.zval, self.zhat, self.ybuf = (sp0, sp1), (sq0, sq1), zparts, (zv0, zv1), zhat, ybuf
        self.nb, self.nbo = sp0.shape[0], sq0.shape[0]

    def near(self, land, t, f):
        for side in PAIR:
            split_blocks(land.at[f, t, side], self.hparts.at[f], side * self.nbo // 2)

    def window(self, f, raw, far):
        g, nbo = self.g[f], self.nbo
        for j in range(nbo, 0, -1):
            cur = far.at[f, 0] if j == nbo else raw.at[j]
            for lo, sign in SIDES:
                re, im, new_re, new_im = shifted_add(cur, raw.at[j - 1], lo, sign)
                g[j, re], g[j, im] = new_re, new_im
        if raw is not g:
            g[0] = raw[0]

    def pointwise(self, xhat, f, far, dst, r, first):
        g, nbo = self.g[f], self.nbo
        re, im = pl.ds(pl.multiple_of(r * 16, 16), 16), pl.ds(pl.multiple_of(BLK + r * 16, 16), 16)
        for k in range(first, self.nb):
            acc_re = acc_im = None
            for j in range(k + 1):
                i = k - j
                gr, gi = (g[i, re], g[i, im]) if i <= nbo else (far[f, i - nbo, re], far[f, i - nbo, im])
                xr, xi = xhat[j, re], xhat[j, im]
                t_re, t_im = xr * gr - xi * gi, xr * gi + xi * gr
                acc_re = t_re if acc_re is None else acc_re + t_re
                acc_im = t_im if acc_im is None else acc_im + t_im
            for part, (a, b) in enumerate(zip(split3(acc_re), split3(acc_im))):
                dst[k - first, part, re], dst[k - first, part, im] = a, b

    def inverse(self, parts, k):
        return dot(self.inv6[...], stack6(parts[k, 0], parts[k, 1], parts[k, 2]))

    def gate_one(self, s, k, data):
        x1, v, _, _, skip, _ = data
        z = x1[s, k].astype(F32) * (self.inverse(self.first[s], k) + skip * v[s, k].astype(F32))
        self.zval[s][k] = z
        for part, a in enumerate(split3(z)):
            self.zparts[k, part] = a

    def spectrum(self, k):
        self.zhat[k] = block_spectrum(self.fwd6, self.zparts, k)

    def gate_two(self, s, k, data):
        y = data[2][s, k].astype(F32) * (self.inverse(self.second[s], k) + data[5] * self.zval[s][self.nbo + k])
        self.ybuf[s, k] = y.astype(BF16)

    def middle(self, s, data, i, point=None):
        for q in range(4):
            if point is not None:
                point(4 * i + q)
            for k in PAIR:
                if q < 2:
                    self.gate_one(s, 4 * i + 2 * q + k, data)
                else:
                    self.spectrum(4 * i + 2 * (q - 2) + k)

    def step(self, land, t, vhat, data, old, relay):
        nb, nbo = self.nb, self.nbo
        far = data[3]
        self.near(land, t, 0)
        for j in range(nbo):
            self.g[0][j] = block_spectrum(self.fwd6, self.hparts.at[0], j)
        self.near(land, t, 1)
        self.window(0, self.g[0], far)
        relay(1)

        @loop(nb // 4)
        def _(i):
            self.middle(1, old, i, lambda r: self.pointwise(vhat.at[0], 0, far, self.first[0], r, 0))


        @loop(nbo // 2)
        def _(i):
            for q in range(4):
                self.pointwise(self.zhat, 1, old[3], self.second[1], 4 * i + q, nbo)
                if q < 2:
                    self.gate_two(0, 2 * i + q, old)
                else:
                    j = 2 * i + q - 2
                    self.raw2[j] = block_spectrum(self.fwd6, self.hparts.at[1], j)

        relay(0)
        self.window(1, self.raw2, far)

        @loop(nb // 4)
        def _(i):
            self.middle(0, data, i, lambda r: self.pointwise(vhat.at[1], 0, far, self.first[1], r, 0))

        @loop(nbo // 2)
        def _(i):
            for q in range(4):
                self.pointwise(self.zhat, 1, far, self.second[0], 4 * i + q, nbo)
                if q % 2 == 0:
                    self.gate_two(1, 2 * i + q // 2, old)

    def drain(self, data):
        nb, nbo = self.nb, self.nbo

        @loop(nb // 4)
        def _(i):
            self.middle(1, data, i)

        @loop(nbo // 2)
        def _(i):
            for q in range(4):
                self.pointwise(self.zhat, 1, data[3], self.second[1], 4 * i + q, nbo)
                if q % 2 == 0:
                    self.gate_two(0, 2 * i + q // 2, data)

        for k in range(nbo):
            self.gate_two(1, k, data)

    def result(self, c, keep, send):
        hk = self.nbo // 2
        for s in range(self.ybuf.shape[0]):
            for b in range(hk):
                keep[s, b * BLK:(b + 1) * BLK] = self.ybuf[s, c * hk + b]
                send[s, b * BLK:(b + 1) * BLK] = self.ybuf[s, (1 - c) * hk + b].astype(F32)


def out_body(keep, part, w_out, u_in, out, wbuf, w_sem, lhs, keep_v, stage, in_sem, u_v, o_st, o_sem):
    c = lax.rem(lax.axis_index("sp"), 2)
    n_tile, n_seq, n_pos, _ = keep.shape
    half_w = n_tile * TC
    width = 2 * half_w
    n_col, rows = width // TN, width // 4

    def weights(j, slot):
        cols = pl.ds(pl.multiple_of(j * TN, TN), TN)
        return [pltpu.make_async_copy(w_out.at[i * rows:(i + 1) * rows, cols],
                                      wbuf.at[slot, i * rows:(i + 1) * rows], w_sem.at[slot, i]) for i in range(4)] + [
                    pltpu.make_async_copy(u_in.at[:, :, cols], u_v.at[slot], w_sem.at[slot, 4])]

    def flush(j):
        slot = parity(j)
        return pltpu.make_async_copy(o_st.at[slot], out.at[:, :, pl.ds(pl.multiple_of(j * TN, TN), TN)], o_sem.at[slot])

    loads = [pltpu.make_async_copy(part.at[u], stage.at[u], in_sem.at[u]) for u in range(n_tile)]
    loads += [pltpu.make_async_copy(keep.at[u], keep_v.at[u], in_sem.at[n_tile + u]) for u in range(n_tile)]
    for copy in loads:
        copy.start()
    for j in PAIR:
        for copy in weights(j, j):
            copy.start()
    for u in range(n_tile):
        loads[u].wait()
        loads[n_tile + u].wait()
        for s in range(n_seq):
            lhs[s, :, pl.ds(pl.multiple_of((1 - c) * half_w + u * TC, TC), TC)] = stage[u, s].astype(BF16)
            lhs[s, :, pl.ds(pl.multiple_of(c * half_w + u * TC, TC), TC)] = keep_v[u, s]

    def step(j, carry):
        slot, held = parity(j), lax.rem(j, 3)

        @pl.when(j + 2 < n_col)
        def _():
            for copy in weights(j + 2, lax.rem(j + 2, 3)):
                copy.start()

        for copy in weights(j, held):
            copy.wait()

        @pl.when(j >= 2)
        def _():
            flush(j - 2).wait()

        for s in range(n_seq):
            o_st[slot, s] = (u_v[held, s].astype(F32) + dot(lhs[s], wbuf[held])).astype(BF16)
        flush(j).start()
        return carry

    lax.fori_loop(0, n_col, step, 0)
    for j in (n_col - 2, n_col - 1):
        flush(j).wait()


def solution(mesh):
    fwd3, fwd6, inv6 = transform_tables()

    def local_step(u_in, w_in, b_in, conv_taps, w_out, skip_one, skip_two, filt_one, filt_two):
        n_seq, n_pos, width = u_in.shape
        half_w = width // 2
        n_own = 2 * n_pos
        nb = 2 * n_own // BLK
        nbo = nb // 2
        n_tile = half_w // TC
        rows = n_pos // GR, GR, width
        small, large = pl.BlockSpec(memory_space=pltpu.VMEM), pl.BlockSpec(memory_space=pl.ANY)
        dma = pltpu.SemaphoreType.DMA

        def shape(dims, dtype=F32):
            return jax.ShapeDtypeStruct(dims, dtype)

        keep, part, *_ = pl.pallas_call(
            main_body,
            in_specs=[small] * 7 + [large] * 4,
            out_specs=[large] * 12,
            out_shape=[
                shape((n_tile, n_seq, n_pos, TC), BF16), shape((n_tile, n_seq, n_pos, TC)),
                shape((n_tile, n_seq, nb + nbo, BLK, TC), BF16), shape((n_tile, n_seq, nb, BLK, TC), BF16),
                shape((n_tile, n_seq, nb, 2 * BLK, TC)), shape((n_tile, 2, nbo, 2 * BLK, TC)),
                shape((n_seq, *rows)), shape((n_seq, 8, width)), shape((n_seq, *rows)), shape((2, n_seq, *rows)),
                shape((n_seq, 8, width)), shape((2, n_pos, half_w)),
            ],
            scratch_shapes=[
                pltpu.VMEM((2, n_tile, 2, n_pos, TC), F32),
                dma((1,)), dma((1,)), *[dma((n_seq, 3, 2))] * 4, *[dma((n_seq,))] * 2, *[dma((2,))] * 2,
                dma((2, n_tile, 2)), *[dma((n_tile, Q, 2))] * 4, *[dma((n_tile,))] * 2,
            ],
            compiler_params=pltpu.CompilerParams(vmem_limit_bytes=62 << 20, collective_id=0, has_side_effects=True),
            name="hyena_main",
        )(fwd3, fwd6, inv6, b_in.reshape(1, -1), conv_taps, skip_one.reshape(1, -1), skip_two.reshape(1, -1),
          u_in, w_in, filt_one, filt_two)

        return pl.pallas_call(
            out_body,
            in_specs=[large] * 4,
            out_specs=large,
            out_shape=shape((n_seq, n_pos, width), BF16),
            scratch_shapes=[
                pltpu.VMEM((3, width, TN), BF16), dma((3, 5)),
                pltpu.VMEM((n_seq, n_pos, width), BF16), pltpu.VMEM((n_tile, n_seq, n_pos, TC), BF16), pltpu.VMEM((n_tile, n_seq, n_pos, TC), F32),
                dma((2 * n_tile,)), pltpu.VMEM((3, n_seq, n_pos, TN), BF16), pltpu.VMEM((2, n_seq, n_pos, TN), BF16), dma((2,)),
            ],
            compiler_params=pltpu.CompilerParams(vmem_limit_bytes=60 << 20),
            name="out_proj",
        )(keep, part, w_out, u_in)

    seq_spec = P("dp", "sp", None)
    filt_spec = P("sp", None)
    return jax.shard_map(local_step, mesh=mesh, in_specs=(seq_spec, P(), P(), P(), P(), P(), P(), filt_spec, filt_spec), out_specs=seq_spec, check_vma=False)
```

```python
import functools

import jax
import jax.numpy as jnp
import numpy as np
from jax import lax
from jax.experimental import pallas as pl
from jax.experimental.pallas import tpu as pltpu
from jax.sharding import PartitionSpec as P

F32, BF16 = jnp.float32, jnp.bfloat16
BLK = 128
TN = 512
TC = 256
Q = 2
PAIR = (0, 1)
GR = 32
MESH = pl.DeviceIdType.MESH


def split_table(table):
    parts, rest = [], table.astype(np.float64)
    for _ in range(3):
        part = rest.astype(np.float32).astype(jnp.bfloat16)
        parts.append(part)
        rest = rest - part.astype(np.float64)
    return parts


def transform_tables():
    freq = np.concatenate([np.arange(0, BLK, 2), np.arange(1, BLK, 2)]) + 0.5
    angle = 2.0 * np.pi * freq[:, None] * np.arange(BLK)[None, :] / (2 * BLK)
    fwd = np.concatenate([np.cos(angle), -np.sin(angle)], 0)
    inv = np.concatenate([np.cos(angle).T, -np.sin(angle).T], 1) / BLK
    f1, f2, f3 = split_table(fwd)
    e1, e2, e3 = split_table(inv)
    fwd3 = np.concatenate([f1, f2, f3], 1)
    fwd6 = np.concatenate([f1, f1, f2, f2, f1, f3], 1)
    inv6 = np.concatenate([e1, e1, e2, e2, e1, e3], 1)
    return fwd3, fwd6, inv6


def parity(x):
    return lax.rem(x, 2)


def dot(a, b):
    return jnp.dot(a, b, preferred_element_type=F32)


def split3(x):
    hi = x.astype(BF16)
    rest = x - hi.astype(F32)
    mid = rest.astype(BF16)
    low = (rest - mid.astype(F32)).astype(BF16)
    return hi, mid, low


def stack6(hi, mid, low):
    return jnp.concatenate([hi, mid, hi, mid, low, hi], axis=0)


def split_blocks(src, parts, first):
    for j in range(src.shape[0] // BLK):
        for i, a in enumerate(split3(src[j * BLK:(j + 1) * BLK])):
            parts[first + j, i] = a


def block_spectrum(fwd6_ref, parts, j):
    return dot(fwd6_ref[...], stack6(parts[j, 0], parts[j, 1], parts[j, 2]))


def shifted_add(cur, old, lo, sign):
    re, im = slice(lo, lo + BLK // 2), slice(BLK + lo, BLK + lo + BLK // 2)
    return re, im, cur[re] - sign * old[im], cur[im] + sign * old[re]


SIDES = ((0, 1.0), (BLK // 2, -1.0))


def short_conv(pbuf, t, first, rows):
    return (t[0:1] * pbuf[8 + first:8 + first + rows] + t[1:2] * pbuf[7 + first:7 + first + rows] + t[2:3] * pbuf[6 + first:6 + first + rows]).astype(BF16)


def block_values(fwd3_ref, blk):
    return dot(fwd3_ref[...], jnp.concatenate([blk, blk, blk], axis=0))


def main_body(fwd3_ref, fwd6_ref, inv6_ref, bias_ref, taps_ref, sk1_ref, sk2_ref, u_bf, w_in, f1, f2,
              keep, part, qx, qv, vhat, far, u32, tsrc, u_sw, u_x, tail, pf,
              land, ts, tr, os, orr, ws, wr, ss, sr, fs, fr, l_sem, x_send, x_recv, y_send, y_recv, p_send, p_recv):
    sp, dp = lax.axis_index("sp"), lax.axis_index("dp")
    c = parity(sp)
    on_b = sp >= 2
    on_a = jnp.logical_not(on_b)
    other = sp + 1 - 2 * c
    n_seq, n_pos, width = u_bf.shape
    half_w = width // 2
    nt, n_tile, per = half_w // TN, half_w // TC, TN // TC
    n_own, hp = 2 * n_pos, n_pos // 2
    nbo = n_own // BLK
    cuts = (0, hp, hp + hp // 2, n_pos)
    n_cut = len(cuts) - 1

    def remote(src, dst, send, recv, peer):
        return pltpu.make_async_remote_copy(src, dst, send, recv, device_id=peer, device_id_type=MESH)

    def at(start, size):
        return pl.ds(pl.multiple_of(start, size), size)

    def share(s, h, k):
        rows = (cuts[h + 1] - cuts[h]) // 2
        return s, pl.ds((cuts[h] + k * rows) // GR, rows // GR)

    def tail_copy():
        return remote(tsrc, tail, ts.at[0], tr.at[0], (dp, 3))

    def tail_across():
        return remote(tail, tail, ts.at[0], tr.at[0], (dp, other))

    def over(s, h, k):
        s, rows = share(s, h, k)
        return remote(u32.at[s, rows], u_x.at[c, s, rows], os.at[s, h, k], orr.at[s, h, c], (dp, 2 + k))

    def arrived(s, h, src):
        at_s, rows = share(s, h, 0)
        ref = u_x.at[src, at_s, rows]
        return remote(ref, ref, os.at[s, h, src], orr.at[s, h, src], (dp, sp))

    def onward(s, h, src):
        at_s, rows = share(s, h, c)
        ref = u_x.at[src, at_s, rows]
        return remote(ref, ref, ws.at[s, h, src], wr.at[s, h, src], (dp, other))

    def swap_u(s):
        return remote(u32.at[s], u_sw.at[s], ss.at[s], sr.at[s], (dp, other))

    def swap_f(f):
        return remote((f1, f2)[f].at[:, at((1 - c) * half_w, half_w)], pf.at[f], fs.at[f], fr.at[f], (dp, other))

    qr = n_pos // Q

    def filt(src, u, k, q):
        return remote(src.at[q * qr:(q + 1) * qr, at(k * half_w + u * TC, TC)], land.at[dp, u, c, q * qr:(q + 1) * qr],
                      x_send.at[u, q, k], x_recv.at[u, q, c], (dp, 2 + k))

    def direct(src, k):
        u, q = n_tile - 1, Q - 1
        return remote(src.at[q * qr:(q + 1) * qr, at(k * half_w + u * TC, TC)], land.at[1 - dp, u, c, q * qr:(q + 1) * qr],
                      y_send.at[u, q, k], y_recv.at[u, q, c], (dp, 2 + k))

    def landed(u, side, q):
        ref = land.at[dp, u, side, at(q * qr, qr)]
        return remote(ref, ref, x_send.at[u, q, side], x_recv.at[u, q, side], (dp, sp))

    def across(u, side, f, q):
        ref = land.at[f, u, side, at(q * qr, qr)]
        return remote(ref, ref, y_send.at[u, q, side], y_recv.at[u, q, side], (1 - dp, sp))

    def fill(f, u, side, src, start):
        return pltpu.make_async_copy(src.at[:, at(start, TC)], land.at[f, u, side], l_sem.at[f, u, side])

    def column(g, j):
        return (g + j // nt) * width + c * half_w + lax.rem(j, nt) * TN

    def load_rows(stage, st_sem, items):
        def copy(i):
            src, rows, _, _ = items[i]
            return pltpu.make_async_copy(src, stage.at[i % 2, :rows // GR], st_sem.at[i % 2])

        copy(0).start()
        for i, (_, rows, dst, row) in enumerate(items):
            if i + 1 < len(items):
                copy(i + 1).start()
            copy(i).wait()
            dst[pl.ds(pl.multiple_of(row, 16), rows), :] = stage[i % 2, :rows // GR].reshape(rows, width).astype(BF16)

    barrier = pltpu.get_barrier_semaphore()
    for peer in ((dp, other), (dp, lax.rem(sp + 2, 4)), (dp, lax.rem(other + 2, 4)), (1 - dp, sp)):
        pl.semaphore_signal(barrier, inc=1, device_id=peer, device_id_type=MESH)
    pl.semaphore_wait(barrier, 4)

    def widen(raw, wide, tail_raw, tail_wide, in_sem, out_sem):
        def half(ref, s, h):
            return ref.at[s, h * hp:h * hp + hp]

        def load(s, h):
            return pltpu.make_async_copy(half(u_bf, s, h), raw.at[h], in_sem.at[h])

        last_rows = pltpu.make_async_copy(u_bf.at[:, n_pos - 8:], tail_raw, in_sem.at[2])
        last_out = pltpu.make_async_copy(tail_wide, tsrc, out_sem.at[2])
        order = [(s, h) for s in range(n_seq) for h in PAIR]
        last_rows.start()
        load(*order[0]).start()
        last_rows.wait()
        tail_wide[...] = tail_raw[...].astype(F32)
        last_out.start()
        pending = {}
        for (s, h), following in zip(order, order[1:] + [None]):
            if following:
                load(*following).start()
            load(s, h).wait()
            if h in pending:
                pending.pop(h).wait()
            wide[h] = raw[h].astype(F32).reshape(wide.shape[1:])
            store = pltpu.make_async_copy(wide.at[h], u32.at[s, pl.ds(h * hp // GR, hp // GR)], out_sem.at[h])
            store.start()
            if s + h:
                pending[h] = store
                continue
            last_out.wait()

            @pl.when(sp == 1)
            def _():
                tail_copy().start()

            store.wait()

            @pl.when(on_a)
            def _():
                for k in PAIR:
                    over(s, h, k).start()

        for store in pending.values():
            store.wait()

    pl.run_scoped(
        widen, pltpu.VMEM((2, hp, width), BF16), pltpu.VMEM((2, hp // GR, GR, width), F32), pltpu.VMEM((n_seq, 8, width), BF16),
        pltpu.VMEM((n_seq, 8, width), F32), pltpu.SemaphoreType.DMA((3,)), pltpu.SemaphoreType.DMA((3,)))

    @pl.when(on_a)
    def _():
        for i in range(1, n_seq * n_cut):
            for k in PAIR:
                over(*divmod(i, n_cut), k).start()
        for which, src, rest in ((0, f1, f2), (1, f2, f1)):
            @pl.when(dp == which)
            def _():
                for u in range(n_tile):
                    for q in range(Q):
                        for k in PAIR:
                            filt(src, u, k, q).start()
                for k in PAIR:
                    direct(rest, k).start()

    for i in range(n_seq):
        swap_u(i).start()
    for f in PAIR:
        swap_f(f).start()

    def forward(u, q):
        @pl.when(on_b)
        def _():
            for side in PAIR:
                landed(u, side, q).wait_recv()
                across(u, side, dp, q).start()

    def front(wbuf, wsem, lhs, stage, st_sem, lhs_sem, tailbuf, q_st, q_sem, vh_st, vh_sem, pbuf):
        def weights(g, j, slot):
            rows = width // 4
            return [pltpu.make_async_copy(w_in.at[i * rows:(i + 1) * rows, at(column(g, j), TN)],
                                          wbuf.at[slot, i * rows:(i + 1) * rows], wsem.at[slot, i]) for i in range(4)]

        def stream(g, body, following, n=nt):
            def step(j, carry):
                slot = parity(j)

                @pl.when(j + 1 < n)
                def _():
                    for copy in weights(g, j + 1, 1 - slot):
                        copy.start()

                if following is not None:
                    @pl.when(j + 1 == n)
                    def _():
                        following(1 - slot)

                for copy in weights(g, j, slot):
                    copy.wait()
                body(j, slot, bias_ref[:, at(column(g, j), TN)], taps_ref[:, at(column(g, j), TN)])
                return carry

            lax.fori_loop(0, n, step, 0)

        def begin(g):
            def start(slot):
                for copy in weights(g, 0, slot):
                    copy.start()
            return start

        def project(rows_ref, slot, bias):
            return (dot(rows_ref, wbuf[slot]) + bias).astype(BF16).astype(F32)

        tail_rows = n_seq * 8
        begin(0)(0)
        own_rows = [pltpu.make_async_copy(u_bf.at[s], lhs.at[pl.ds(pl.multiple_of(tail_rows + s * n_own + c * n_pos, 16), n_pos)], lhs_sem.at[s])
                    for s in range(n_seq)]
        for copy in own_rows:
            copy.start()
        for s in range(n_seq):
            swap_u(s).wait_recv()
        load_rows(stage, st_sem, [(u_sw.at[s, pl.ds(h * hp // GR, hp // GR)], hp, lhs, tail_rows + s * n_own + (1 - c) * n_pos + h * hp)
                                  for s in range(n_seq) for h in PAIR])
        for copy in own_rows:
            copy.wait()

        @pl.when(on_b)
        def _():
            tail_copy().wait_recv()

            @pl.when(sp == 3)
            def _():
                tail_across().start()

            copy = pltpu.make_async_copy(tail, tailbuf, lhs_sem.at[0])
            copy.start()
            copy.wait()

        @pl.when(on_a)
        def _():
            tailbuf[...] = jnp.zeros_like(tailbuf)

        lhs[:tail_rows, :] = tailbuf[...].reshape(tail_rows, width).astype(BF16)
        chunk = n_pos

        def own_phase(g, n, dst, spectrum, following):
            def flush(j, slot):
                blocks = pl.ds(nbo * (1 + j // nt), nbo)
                copies = []
                for h in range(per):
                    u = lax.rem(j, nt) * per + h
                    copies.append(pltpu.make_async_copy(q_st.at[slot, h], dst.at[u, :, blocks], q_sem.at[slot, h]))
                    if spectrum:
                        copies.append(pltpu.make_async_copy(vh_st.at[slot, h], vhat.at[u, :, nbo:], vh_sem.at[slot, h]))
                return copies

            def body(j, slot, bias, taps):
                @pl.when(j >= 2)
                def _():
                    for copy in flush(j - 2, slot):
                        copy.wait()

                for i in range(n_seq * n_own // chunk):
                    s, r = divmod(i * chunk, n_own)
                    p = project(lhs[(tail_rows + i * chunk if i else 0):tail_rows + (i + 1) * chunk, :], slot, bias)
                    if i == 0:
                        for k in range(n_seq):
                            pbuf[k, 0:8] = jnp.where(on_b, p[8 * k:8 * k + 8], 0.0)
                        p = p[tail_rows:]
                    pbuf[s, 8 + r:8 + r + chunk] = p
                    q = short_conv(pbuf.at[s], taps, r, chunk)
                    for b in range(chunk // BLK):
                        blk = q[b * BLK:(b + 1) * BLK]
                        for h in range(per):
                            q_st[slot, h, s, r // BLK + b] = blk[:, h * TC:(h + 1) * TC]
                        if spectrum:
                            spec = block_values(fwd3_ref, blk)
                            for h in range(per):
                                vh_st[slot, h, s, r // BLK + b] = spec[:, h * TC:(h + 1) * TC]
                for copy in flush(j, slot):
                    copy.start()

            stream(g, body, following, n)
            for j in (n - 2, n - 1):
                for copy in flush(j, j % 2):
                    copy.wait()

        own_phase(0, 2 * nt, qx, False, begin(2))
        own_phase(2, nt, qv, True, None)

        def far_phase(fin, fin_sem, fout, fout_sem, parts):
            hk = n_pos // BLK

            def fetch(j, slot):
                mine = at(c * half_w + j * TC, TC)
                srcs = (f1.at[:, mine], f2.at[:, mine], pf.at[0, :, at(j * TC, TC)], pf.at[1, :, at(j * TC, TC)])
                return [pltpu.make_async_copy(src, fin.at[slot, i], fin_sem.at[slot, i]) for i, src in enumerate(srcs)]

            def flush(j, slot):
                return pltpu.make_async_copy(fout.at[slot], far.at[j], fout_sem.at[slot])

            for copy in fetch(0, 0):
                copy.start()

            def step(j, carry):
                slot = parity(j)

                @pl.when(j + 1 < n_tile)
                def _():
                    for copy in fetch(j + 1, 1 - slot):
                        copy.start()

                for copy in fetch(j, slot):
                    copy.wait()

                @pl.when(j >= 2)
                def _():
                    flush(j - 2, slot).wait()

                for f in PAIR:
                    split_blocks(fin.at[slot, f], parts.at[f], c * hk)
                    split_blocks(fin.at[slot, 2 + f], parts.at[f], (1 - c) * hk)
                g_ref = fout.at[slot]
                for f in PAIR:
                    for b in range(2 * hk):
                        g_ref[f, b] = block_spectrum(fwd6_ref, parts.at[f], b)
                    for b in range(2 * hk - 1, 0, -1):
                        for lo, sign in SIDES:
                            re, im, new_re, new_im = shifted_add(g_ref.at[f, b], g_ref.at[f, b - 1], lo, sign)
                            g_ref[f, b, re], g_ref[f, b, im] = new_re, new_im
                flush(j, slot).start()
                return carry

            lax.fori_loop(0, n_tile, step, 0)
            for j in (n_tile - 2, n_tile - 1):
                flush(j, j % 2).wait()

        for f in PAIR:
            swap_f(f).wait_recv()
        pl.run_scoped(
            far_phase, pltpu.VMEM((2, 4, n_pos, TC), F32), pltpu.SemaphoreType.DMA((2, 4)),
            pltpu.VMEM((2, 2, nbo, 2 * BLK, TC), F32), pltpu.SemaphoreType.DMA((2,)), pltpu.VMEM((2, nbo, 3, BLK, TC), BF16))

    pl.run_scoped(
        front,
        pltpu.VMEM((2, width, TN), BF16), pltpu.SemaphoreType.DMA((2, 4)),
        pltpu.VMEM((n_seq * n_own + 8 * n_seq, width), BF16),
        pltpu.VMEM((2, hp // GR, GR, width), F32), pltpu.SemaphoreType.DMA((2,)), pltpu.SemaphoreType.DMA((n_seq,)), pltpu.VMEM((n_seq, 8, width), F32),
        pltpu.VMEM((2, per, n_seq, nbo, BLK, TC), BF16), pltpu.SemaphoreType.DMA((2, per)),
        pltpu.VMEM((2, per, n_seq, nbo, 2 * BLK, TC), F32), pltpu.SemaphoreType.DMA((2, per)),
        pltpu.VMEM((n_seq, n_own + 8, TN), F32))

    def prev(wres, w_sem, lhs_p, stage, st_sem, q_st, q_sem, vh_st, vh_sem, pbuf, pstash):
        def weights(j):
            rows = width // 4
            return [pltpu.make_async_copy(w_in.at[i * rows:(i + 1) * rows, at(which(j), TN)],
                                          wres.at[j, i * rows:(i + 1) * rows], w_sem.at[j, i]) for i in range(4)]

        def which(j):
            return 2 * (j // nt) * width + c * half_w + lax.rem(j, nt) * TN

        def begin(j, carry):
            for copy in weights(j):
                copy.start()
            return carry

        lax.fori_loop(0, 2 * nt, begin, 0)

        def rows(s, h):
            n = cuts[h + 1] - cuts[h]

            @pl.when(on_b)
            def _():
                for src in PAIR:
                    arrived(s, h, src).wait_recv()
                    onward(s, h, src).start()
                for src in PAIR:
                    onward(s, h, src).wait_recv()
                load_rows(stage, st_sem, [(u_x.at[src, s, cuts[h] // GR:cuts[h + 1] // GR], n, lhs_p, src * n) for src in PAIR])

            @pl.when(on_a)
            def _():
                lhs_p[...] = jnp.zeros_like(lhs_p)

        def project(h, j):
            n = 2 * (cuts[h + 1] - cuts[h])
            return (dot(lhs_p[:n, :], wres[j]) + bias_ref[:, at(which(j), TN)]).astype(BF16)

        def first(s, h):
            n = cuts[h + 1] - cuts[h]

            def body(j, carry):
                if h == 0:
                    @pl.when(s == 0)
                    def _():
                        for copy in weights(j):
                            copy.wait()

                p = project(h, j)
                for core in PAIR:
                    pstash[core, cuts[h]:cuts[h + 1], at(j * TN, TN)] = p[core * n:(core + 1) * n]
                return carry

            lax.fori_loop(0, 2 * nt, body, 0)

        def last(s, u, dst):
            base, spectrum = u * nt, u > 0
            h = n_cut - 1
            n = cuts[h + 1] - cuts[h]

            def flush(j):
                slot, copies = parity(j), []
                for half in range(per):
                    copies.append(pltpu.make_async_copy(q_st.at[slot, half], dst.at[j * per + half, s, :nbo], q_sem.at[slot, half]))
                    if spectrum:
                        copies.append(pltpu.make_async_copy(vh_st.at[slot, half], vhat.at[j * per + half, s, :nbo], vh_sem.at[slot, half]))
                return copies

            def body(j, carry):
                slot = parity(j)

                @pl.when(j >= 2)
                def _():
                    for copy in flush(j - 2):
                        copy.wait()

                taps = taps_ref[:, at(which(base + j), TN)]
                pbuf[0:8] = jnp.zeros((8, TN), F32)
                for core in PAIR:
                    old = pstash[core, :cuts[h], at((base + j) * TN, TN)].astype(F32)
                    pbuf[8 + core * n_pos:8 + core * n_pos + cuts[h]] = jnp.where(on_b, old, 0.0)
                p = project(h, base + j).astype(F32)
                for core in PAIR:
                    start = 8 + core * n_pos + cuts[h]
                    pbuf[start:start + n] = jnp.where(on_b, p[core * n:(core + 1) * n], 0.0)
                for b in range(nbo):
                    blk = short_conv(pbuf, taps, b * BLK, BLK)
                    for half in range(per):
                        q_st[slot, half, b] = blk[:, half * TC:(half + 1) * TC]
                    if spectrum:
                        spec = block_values(fwd3_ref, blk)
                        for half in range(per):
                            vh_st[slot, half, b] = spec[:, half * TC:(half + 1) * TC]
                for copy in flush(j):
                    copy.start()

                @pl.when(jnp.logical_and(s == n_seq - 1, jnp.logical_and(lax.rem(j, Q) == 1, j < nt - Q * u)))
                def _():
                    forward(u, j // Q)
                return carry

            lax.fori_loop(0, nt, body, 0)
            for j in (nt - 2, nt - 1):
                for copy in flush(j):
                    copy.wait()

        def one_seq(s, carry):
            for h in range(n_cut - 1):
                rows(s, h)
                first(s, h)
            rows(s, n_cut - 1)
            last(s, 0, qx)
            last(s, 1, qv)
            return carry

        lax.fori_loop(0, n_seq, one_seq, 0)

    pl.run_scoped(
        prev,
        pltpu.VMEM((2 * nt, width, TN), BF16), pltpu.SemaphoreType.DMA((2 * nt, 4)),
        pltpu.VMEM((2 * hp, width), BF16), pltpu.VMEM((2, hp // GR, GR, width), F32), pltpu.SemaphoreType.DMA((2,)),
        pltpu.VMEM((2, per, nbo, BLK, TC), BF16), pltpu.SemaphoreType.DMA((2, per)),
        pltpu.VMEM((2, per, nbo, 2 * BLK, TC), F32), pltpu.SemaphoreType.DMA((2, per)),
        pltpu.VMEM((n_own + 8, TN), F32), pltpu.VMEM((2, cuts[-2], 2 * half_w), BF16))

    @pl.when(on_a)
    def _():
        for u in range(n_tile):
            for f, own in enumerate((f1, f2)):
                fill(f, u, c, own, c * half_w + u * TC).start()
                fill(f, u, 1 - c, pf.at[f], u * TC).start()

    def conv(x1b, vb, x2b, vhb, farb, in_sem, vh_sem, kst, k_sem, sendbuf, *scratch):
        def fetch(t):
            slot, two = lax.rem(t, 3), parity(t)
            srcs = (qx.at[t, :, :2 * nbo], qv.at[t], qx.at[t, :, 2 * nbo:], far.at[t])
            copies = [pltpu.make_async_copy(r, b.at[slot], in_sem.at[slot, i])
                      for i, (r, b) in enumerate(zip(srcs, (x1b, vb, x2b, farb)))]
            return copies + [pltpu.make_async_copy(vhat.at[t, s], vhb.at[two, s], vh_sem.at[two, s]) for s in range(n_seq)]

        def flush(t):
            slot = parity(t)
            return pltpu.make_async_copy(kst.at[slot], keep.at[t], k_sem.at[slot])

        def swap_y(u):
            return remote(sendbuf.at[parity(u)], part.at[u], p_send.at[u], p_recv.at[u], (dp, other))

        tile = ConvTile(fwd6_ref, inv6_ref, *scratch)

        def inputs(t, back):
            slot, cols = lax.rem(t + 3 - back, 3), at(c * half_w + lax.rem(t + n_tile - back, n_tile) * TC, TC)
            return x1b.at[slot], vb.at[slot], x2b.at[slot], farb.at[slot], sk1_ref[:, cols], sk2_ref[:, cols]

        def emit(t):
            slot = parity(t)

            @pl.when(t >= 2)
            def _():
                flush(t - 2).wait()
                swap_y(t - 2).wait_send()

            tile.result(c, kst.at[slot], sendbuf.at[slot])
            flush(t).start()
            swap_y(t).start()

        for copy in fetch(0):
            copy.start()
        forward(1, Q - 1)

        def step(t, carry):
            @pl.when(t + 1 < n_tile)
            def _():
                for copy in fetch(t + 1):
                    copy.start()

            @pl.when(on_a)
            def _():
                for f in PAIR:
                    for side in PAIR:
                        fill(f, t, side, f1, 0).wait()

            @pl.when(on_b)
            def _():
                for q in range(Q):
                    for side in PAIR:
                        across(t, side, 1 - dp, q).wait_recv()

            @pl.when(jnp.logical_and(on_b, t == n_tile - 1))
            def _():
                for side in PAIR:
                    landed(t, side, Q - 1).wait_recv()

            for copy in fetch(t):
                copy.wait()

            def relay(q):
                ahead = 2 - q

                @pl.when(jnp.logical_and(t >= q, t + ahead + q < n_tile))
                def _():
                    forward(t + ahead, q)

            tile.step(land, t, vhb.at[parity(t)], inputs(t, 0), inputs(t, 1), relay)

            @pl.when(t >= 1)
            def _():
                emit(t - 1)
            return carry

        lax.fori_loop(0, n_tile, step, 0)
        tile.drain(inputs(n_tile, 1))
        emit(n_tile - 1)
        for u in (n_tile - 2, n_tile - 1):
            flush(u).wait()
            swap_y(u).wait_send()
        for u in range(n_tile):
            swap_y(u).wait_recv()

    nb = 2 * nbo
    pl.run_scoped(
        conv,
        pltpu.VMEM((3, n_seq, nb, BLK, TC), BF16), pltpu.VMEM((3, n_seq, nb, BLK, TC), BF16), pltpu.VMEM((3, n_seq, nbo, BLK, TC), BF16),
        pltpu.VMEM((2, n_seq, nb, 2 * BLK, TC), F32), pltpu.VMEM((3, 2, nbo, 2 * BLK, TC), F32),
        pltpu.SemaphoreType.DMA((3, 4)), pltpu.SemaphoreType.DMA((2, n_seq)),
        pltpu.VMEM((2, n_seq, n_pos, TC), BF16), pltpu.SemaphoreType.DMA((2,)), pltpu.VMEM((2, n_seq, n_pos, TC), F32),
        pltpu.VMEM((2, nbo, 3, BLK, TC), BF16),
        pltpu.VMEM((nbo + 1, 2 * BLK, TC), F32), pltpu.VMEM((nbo + 1, 2 * BLK, TC), F32), pltpu.VMEM((nbo, 2 * BLK, TC), F32),
        *[pltpu.VMEM((nb, 3, 2 * BLK, TC), BF16)] * n_seq,
        pltpu.VMEM((nb, 3, BLK, TC), BF16),
        *[pltpu.VMEM((nb, BLK, TC), F32)] * n_seq,
        pltpu.VMEM((nb, 2 * BLK, TC), F32),
        *[pltpu.VMEM((nbo, 3, 2 * BLK, TC), BF16)] * n_seq,
        pltpu.VMEM((n_seq, nbo, BLK, TC), BF16))

    for s in range(n_seq):
        swap_u(s).wait_send()
    for f in PAIR:
        swap_f(f).wait_send()

    @pl.when(sp == 1)
    def _():
        tail_copy().wait_send()

    @pl.when(sp == 3)
    def _():
        tail_across().wait_send()

    @pl.when(on_a)
    def _():
        for i in range(n_seq * n_cut):
            for k in PAIR:
                over(*divmod(i, n_cut), k).wait_send()
        for u in range(n_tile):
            for q in range(Q):
                for k in PAIR:
                    filt(f1, u, k, q).wait_send()
        for k in PAIR:
            direct(f1, k).wait_send()

    @pl.when(on_b)
    def _():
        for i in range(n_seq * n_cut):
            for src in PAIR:
                onward(*divmod(i, n_cut), src).wait_send()
        for u in range(n_tile):
            for q in range(Q - u // (n_tile - 1)):
                for side in PAIR:
                    across(u, side, dp, q).wait_send()


def loop(trips):
    def run(body):
        def step(i, carry):
            body(i)
            return carry
        lax.fori_loop(0, trips, step, 0)
    return run


class ConvTile:
    def __init__(self, fwd6, inv6, hparts, g1, g2, raw2, sp0, sp1, zparts, zv0, zv1, zhat, sq0, sq1, ybuf):
        self.fwd6, self.inv6, self.hparts, self.g, self.raw2 = fwd6, inv6, hparts, (g1, g2), raw2
        self.first, self.second, self.zparts, self.zval, self.zhat, self.ybuf = (sp0, sp1), (sq0, sq1), zparts, (zv0, zv1), zhat, ybuf
        self.nb, self.nbo = sp0.shape[0], sq0.shape[0]

    def near(self, land, t, f):
        for side in PAIR:
            split_blocks(land.at[f, t, side], self.hparts.at[f], side * self.nbo // 2)

    def window(self, f, raw, far):
        g, nbo = self.g[f], self.nbo
        for j in range(nbo, 0, -1):
            cur = far.at[f, 0] if j == nbo else raw.at[j]
            for lo, sign in SIDES:
                re, im, new_re, new_im = shifted_add(cur, raw.at[j - 1], lo, sign)
                g[j, re], g[j, im] = new_re, new_im
        if raw is not g:
            g[0] = raw[0]

    def pointwise(self, xhat, f, far, dst, r, first):
        g, nbo = self.g[f], self.nbo
        re, im = pl.ds(pl.multiple_of(r * 16, 16), 16), pl.ds(pl.multiple_of(BLK + r * 16, 16), 16)
        for k in range(first, self.nb):
            acc_re = acc_im = None
            for j in range(k + 1):
                i = k - j
                gr, gi = (g[i, re], g[i, im]) if i <= nbo else (far[f, i - nbo, re], far[f, i - nbo, im])
                xr, xi = xhat[j, re], xhat[j, im]
                t_re, t_im = xr * gr - xi * gi, xr * gi + xi * gr
                acc_re = t_re if acc_re is None else acc_re + t_re
                acc_im = t_im if acc_im is None else acc_im + t_im
            for part, (a, b) in enumerate(zip(split3(acc_re), split3(acc_im))):
                dst[k - first, part, re], dst[k - first, part, im] = a, b

    def inverse(self, parts, k):
        return dot(self.inv6[...], stack6(parts[k, 0], parts[k, 1], parts[k, 2]))

    def gate_one(self, s, k, data):
        x1, v, _, _, skip, _ = data
        z = x1[s, k].astype(F32) * (self.inverse(self.first[s], k) + skip * v[s, k].astype(F32))
        self.zval[s][k] = z
        for part, a in enumerate(split3(z)):
            self.zparts[k, part] = a

    def spectrum(self, k):
        self.zhat[k] = block_spectrum(self.fwd6, self.zparts, k)

    def gate_two(self, s, k, data):
        y = data[2][s, k].astype(F32) * (self.inverse(self.second[s], k) + data[5] * self.zval[s][self.nbo + k])
        self.ybuf[s, k] = y.astype(BF16)

    def middle(self, s, data, i, point=None):
        for q in range(4):
            if point is not None:
                point(4 * i + q)
            for k in PAIR:
                if q < 2:
                    self.gate_one(s, 4 * i + 2 * q + k, data)
                else:
                    self.spectrum(4 * i + 2 * (q - 2) + k)

    def step(self, land, t, vhat, data, old, relay):
        nb, nbo = self.nb, self.nbo
        far = data[3]
        self.near(land, t, 0)
        for j in range(nbo):
            self.g[0][j] = block_spectrum(self.fwd6, self.hparts.at[0], j)
        self.near(land, t, 1)
        self.window(0, self.g[0], far)
        relay(1)

        @loop(nb // 4)
        def _(i):
            self.middle(1, old, i, lambda r: self.pointwise(vhat.at[0], 0, far, self.first[0], r, 0))


        @loop(nbo // 2)
        def _(i):
            for q in range(4):
                self.pointwise(self.zhat, 1, old[3], self.second[1], 4 * i + q, nbo)
                if q < 2:
                    self.gate_two(0, 2 * i + q, old)
                else:
                    j = 2 * i + q - 2
                    self.raw2[j] = block_spectrum(self.fwd6, self.hparts.at[1], j)

        relay(0)
        self.window(1, self.raw2, far)

        @loop(nb // 4)
        def _(i):
            self.middle(0, data, i, lambda r: self.pointwise(vhat.at[1], 0, far, self.first[1], r, 0))

        @loop(nbo // 2)
        def _(i):
            for q in range(4):
                self.pointwise(self.zhat, 1, far, self.second[0], 4 * i + q, nbo)
                if q % 2 == 0:
                    self.gate_two(1, 2 * i + q // 2, old)

    def drain(self, data):
        nb, nbo = self.nb, self.nbo

        @loop(nb // 4)
        def _(i):
            self.middle(1, data, i)

        @loop(nbo // 2)
        def _(i):
            for q in range(4):
                self.pointwise(self.zhat, 1, data[3], self.second[1], 4 * i + q, nbo)
                if q % 2 == 0:
                    self.gate_two(0, 2 * i + q // 2, data)

        for k in range(nbo):
            self.gate_two(1, k, data)

    def result(self, c, keep, send):
        hk = self.nbo // 2
        for s in range(self.ybuf.shape[0]):
            for b in range(hk):
                keep[s, b * BLK:(b + 1) * BLK] = self.ybuf[s, c * hk + b]
                send[s, b * BLK:(b + 1) * BLK] = self.ybuf[s, (1 - c) * hk + b].astype(F32)


def out_body(keep, part, w_out, u_in, out, wbuf, w_sem, lhs, keep_v, stage, in_sem, u_v, o_st, o_sem):
    c = lax.rem(lax.axis_index("sp"), 2)
    n_tile, n_seq, n_pos, _ = keep.shape
    half_w = n_tile * TC
    width = 2 * half_w
    n_col, rows = width // TC, width // 4

    def weights(j, slot):
        cols = pl.ds(pl.multiple_of(j * TC, TC), TC)
        return [pltpu.make_async_copy(w_out.at[i * rows:(i + 1) * rows, cols],
                                      wbuf.at[slot, i * rows:(i + 1) * rows], w_sem.at[slot, i]) for i in range(4)] + [
                    pltpu.make_async_copy(u_in.at[:, :, cols], u_v.at[slot], w_sem.at[slot, 4])]

    def flush(j):
        slot = parity(j)
        return pltpu.make_async_copy(o_st.at[slot], out.at[:, :, pl.ds(pl.multiple_of(j * TC, TC), TC)], o_sem.at[slot])

    loads = [pltpu.make_async_copy(part.at[u], stage.at[u], in_sem.at[u]) for u in range(n_tile)]
    loads += [pltpu.make_async_copy(keep.at[u], keep_v.at[u], in_sem.at[n_tile + u]) for u in range(n_tile)]
    for copy in loads:
        copy.start()
    for copy in weights(0, 0):
        copy.start()
    for u in range(n_tile):
        loads[u].wait()
        loads[n_tile + u].wait()
        for s in range(n_seq):
            lhs[s, :, pl.ds(pl.multiple_of((1 - c) * half_w + u * TC, TC), TC)] = stage[u, s].astype(BF16)
            lhs[s, :, pl.ds(pl.multiple_of(c * half_w + u * TC, TC), TC)] = keep_v[u, s]

    def step(j, carry):
        slot = parity(j)

        @pl.when(j + 1 < n_col)
        def _():
            for copy in weights(j + 1, 1 - slot):
                copy.start()

        for copy in weights(j, slot):
            copy.wait()

        @pl.when(j >= 2)
        def _():
            flush(j - 2).wait()

        for s in range(n_seq):
            o_st[slot, s] = (u_v[slot, s].astype(F32) + dot(lhs[s], wbuf[slot])).astype(BF16)
        flush(j).start()
        return carry

    lax.fori_loop(0, n_col, step, 0)
    for j in (n_col - 2, n_col - 1):
        flush(j).wait()


def solution(mesh):
    fwd3, fwd6, inv6 = transform_tables()

    def local_step(u_in, w_in, b_in, conv_taps, w_out, skip_one, skip_two, filt_one, filt_two):
        n_seq, n_pos, width = u_in.shape
        half_w = width // 2
        n_own = 2 * n_pos
        nb = 2 * n_own // BLK
        nbo = nb // 2
        n_tile = half_w // TC
        rows = n_pos // GR, GR, width
        small, large = pl.BlockSpec(memory_space=pltpu.VMEM), pl.BlockSpec(memory_space=pl.ANY)
        dma = pltpu.SemaphoreType.DMA

        def shape(dims, dtype=F32):
            return jax.ShapeDtypeStruct(dims, dtype)

        keep, part, *_ = pl.pallas_call(
            main_body,
            in_specs=[small] * 7 + [large] * 4,
            out_specs=[large] * 12,
            out_shape=[
                shape((n_tile, n_seq, n_pos, TC), BF16), shape((n_tile, n_seq, n_pos, TC)),
                shape((n_tile, n_seq, nb + nbo, BLK, TC), BF16), shape((n_tile, n_seq, nb, BLK, TC), BF16),
                shape((n_tile, n_seq, nb, 2 * BLK, TC)), shape((n_tile, 2, nbo, 2 * BLK, TC)),
                shape((n_seq, *rows)), shape((n_seq, 8, width)), shape((n_seq, *rows)), shape((2, n_seq, *rows)),
                shape((n_seq, 8, width)), shape((2, n_pos, half_w)),
            ],
            scratch_shapes=[
                pltpu.VMEM((2, n_tile, 2, n_pos, TC), F32),
                dma((1,)), dma((1,)), *[dma((n_seq, 3, 2))] * 4, *[dma((n_seq,))] * 2, *[dma((2,))] * 2,
                dma((2, n_tile, 2)), *[dma((n_tile, Q, 2))] * 4, *[dma((n_tile,))] * 2,
            ],
            compiler_params=pltpu.CompilerParams(vmem_limit_bytes=62 << 20, collective_id=0, has_side_effects=True),
            name="hyena_main",
        )(fwd3, fwd6, inv6, b_in.reshape(1, -1), conv_taps, skip_one.reshape(1, -1), skip_two.reshape(1, -1),
          u_in, w_in, filt_one, filt_two)

        return pl.pallas_call(
            out_body,
            in_specs=[large] * 4,
            out_specs=large,
            out_shape=shape((n_seq, n_pos, width), BF16),
            scratch_shapes=[
                pltpu.VMEM((2, width, TC), BF16), dma((2, 5)),
                pltpu.VMEM((n_seq, n_pos, width), BF16), pltpu.VMEM((n_tile, n_seq, n_pos, TC), BF16), pltpu.VMEM((n_tile, n_seq, n_pos, TC), F32),
                dma((2 * n_tile,)), pltpu.VMEM((2, n_seq, n_pos, TC), BF16), pltpu.VMEM((2, n_seq, n_pos, TC), BF16), dma((2,)),
            ],
            compiler_params=pltpu.CompilerParams(vmem_limit_bytes=60 << 20),
            name="out_proj",
        )(keep, part, w_out, u_in)

    seq_spec = P("dp", "sp", None)
    filt_spec = P("sp", None)
    return jax.shard_map(local_step, mesh=mesh, in_specs=(seq_spec, P(), P(), P(), P(), P(), P(), filt_spec, filt_spec), out_specs=seq_spec, check_vma=False)
```
